32 devices in a mesh: sys: 2 (over x), aux: 4 (over z), orb: 4 (over y, core).
Axes of the slice: x: 2, y: 2, z: 4, core: 2. Of those that a mesh axis runs over, the one named last changes fastest.
Arguments:
- aux_ints: float32 [928, 232, 232], P(('sys', 'aux'), 'orb'), parts along dimension 0
- metric: float32 [928, 464], P(('sys', 'aux')), parts along dimension 0
- orbitals: float32 [16, 232, 20], P('sys'), parts along dimension 0
Outputs:
- output: float32 [16, 232, 232], P('sys', 'orb', 'aux'), parts along dimension 0
There are 2 independent parts. The reference program is written for one: setup_inputs(seed, part) draws one part's arguments, and reference() takes and returns one part's arrays. A program takes and returns all parts, laid end to end along the dimension named above; each array names one.
All inputs are finite; a program needn't handle non-finite values.
Results may differ from the reference program's by a relative error of at most 0.001.
Values are sent between devices in bfloat16 or wider.
A program may use at most 1 GiB of HBM per device.

```python
import jax
import jax.numpy as jnp
from jax import lax

N_AUX = 464
N_BASIS = 232
N_OCC = 20
DENS = 8

PRECISE = lax.Precision.HIGHEST


def setup_inputs(seed: int = 0, part: int = 0) -> dict:
    base_key = jax.random.fold_in(jax.random.key(seed), part)
    sub_keys = jax.random.split(base_key, 6)
    rank_b = 4
    rank_m = 4
    coh_scale = (2.0 * N_AUX * N_OCC) ** -0.5 * rank_b ** -0.25
    noise_scale = 2.0 * coh_scale
    coeffs = jax.random.normal(sub_keys[0], (N_AUX, rank_b), jnp.float32)
    patterns = jax.random.normal(sub_keys[1], (rank_b, N_BASIS), jnp.float32)
    row_keys = jax.random.split(sub_keys[2], N_AUX)

    def one_row(row_args):
        row_key, coeff_row = row_args
        noise_mat = jax.random.normal(row_key, (N_BASIS, N_BASIS), jnp.float32)
        sym_noise = (noise_mat + noise_mat.T) * (0.5 ** 0.5)
        low_rank = jnp.einsum('k,km,kl->ml', coeff_row, patterns, patterns)
        return noise_scale * sym_noise + coh_scale * low_rank

    aux_ints = lax.map(one_row, (row_keys, coeffs))
    spread = jax.random.normal(sub_keys[3], (N_AUX, N_AUX), jnp.float32)
    sym_spread = (spread + spread.T) * (0.125 / N_AUX) ** 0.5
    directions = jax.random.normal(sub_keys[4], (rank_m, N_AUX), jnp.float32) * N_AUX ** -0.5
    boost_scale = (N_AUX / rank_m) ** 0.5
    metric = jnp.eye(N_AUX, dtype=jnp.float32) + sym_spread + boost_scale * jnp.dot(directions.T, directions)
    orbitals = jax.random.normal(sub_keys[5], (DENS, N_BASIS, N_OCC), jnp.float32) * N_BASIS ** -0.5
    return {'aux_ints': aux_ints, 'metric': metric, 'orbitals': orbitals}


def reference(aux_ints, metric, orbitals):
    def one_density(coeff_mat):
        half_tr = jnp.einsum('qml,li->qmi', aux_ints, coeff_mat, precision=PRECISE)
        fitted = jnp.einsum('pq,qmi->pmi', metric, half_tr, precision=PRECISE)
        exchange = jnp.einsum('pmi,pni->mn', fitted, fitted, precision=PRECISE)
        gamma_raw = jnp.einsum('qmi,mi->q', half_tr, coeff_mat, precision=PRECISE)
        gamma_fit = jnp.dot(metric, gamma_raw, precision=PRECISE)
        weights = jnp.dot(gamma_fit, metric, precision=PRECISE)
        coulomb = jnp.einsum('q,qmn->mn', weights, aux_ints, precision=PRECISE)
        return 2.0 * coulomb - exchange

    return lax.map(one_density, orbitals)
```

```python
import jax
import jax.numpy as jnp
from jax import lax
from jax.sharding import PartitionSpec as P

PRECISE = lax.Precision.HIGHEST
F32 = jnp.float32


def solution(mesh):
    na, no = mesh.shape['aux'], mesh.shape['orb']
    ng = na * no

    def local_fock(ints_blk, metric_blk, orbitals):
        nq, m_loc, nb = ints_blk.shape
        nd, _, ni = orbitals.shape
        ncol = nd * ni // ng
        a, o = lax.axis_index('aux'), lax.axis_index('orb')
        me = a * no + o
        row_start = o * m_loc
        half_tr = jnp.einsum('dli,qml->dimq', orbitals, ints_blk, precision=PRECISE, preferred_element_type=F32)
        orb_rows = lax.dynamic_slice_in_dim(orbitals, row_start, m_loc, axis=1)
        blocks = half_tr.reshape(ng, ncol, m_loc, nq)
        got = lax.all_to_all(blocks.astype(jnp.bfloat16), ('aux', 'orb'), split_axis=0, concat_axis=0, tiled=True).astype(F32)
        own = lax.dynamic_slice_in_dim(blocks, me, 1, axis=0)
        got = lax.dynamic_update_slice_in_dim(got, own, me, axis=0)
        metric = lax.all_gather(metric_blk, 'aux', axis=0, tiled=True)
        gamma_part = jnp.einsum('dimq,dmi->dq', half_tr, orb_rows, precision=PRECISE, preferred_element_type=F32)
        gamma_raw = lax.psum(gamma_part, 'orb')
        gamma_all = lax.all_gather(gamma_raw, 'aux', axis=1, tiled=True)
        gamma_fit = jnp.einsum('dq,pq->dp', gamma_all, metric, precision=PRECISE, preferred_element_type=F32)
        weights = jnp.einsum('dp,qp->dq', gamma_fit, metric_blk, precision=PRECISE, preferred_element_type=F32)
        coulomb = jnp.einsum('dq,qmn->dmn', weights, ints_blk, precision=PRECISE, preferred_element_type=F32)
        cols = got.reshape(na, no, ncol, m_loc, nq).transpose(2, 1, 3, 0, 4).reshape(ncol, nb, na * nq)
        fitted = jnp.einsum('cmq,pq->cmp', cols, metric, precision=PRECISE, preferred_element_type=F32)
        kpart = jnp.einsum('cmp,cnp->mn', fitted, fitted, precision=PRECISE, preferred_element_type=F32)
        kp = kpart.reshape(no, m_loc, na, nb // na).transpose(2, 0, 1, 3).reshape(ng, m_loc, nb // na)
        kg = lax.all_to_all(kp, ('aux', 'orb'), split_axis=0, concat_axis=0, tiled=True)
        exchange = kg.reshape(nd, ng // nd, m_loc, nb // na).sum(1)
        return 2.0 * lax.psum_scatter(coulomb, 'aux', scatter_dimension=2, tiled=True) - exchange

    return jax.shard_map(local_fock, mesh=mesh, in_specs=(P(('sys', 'aux'), 'orb', None), P(('sys', 'aux'), None), P('sys', None, None)), out_specs=P('sys', 'orb', 'aux'), check_vma=False)
```

```python
import jax
import jax.numpy as jnp
from jax import lax
from jax.experimental import pallas as pl
from jax.experimental.pallas import tpu as pltpu
from jax.sharding import PartitionSpec as P

F32 = jnp.float32
BF = jnp.bfloat16
MESH = pl.DeviceIdType.MESH
NN = (((1,), (0,)), ((), ()))
NT = (((1,), (1,)), ((), ()))
LANES = 128
MROW = 64
NT8 = 8
SP = 168


def split3(x):
    hi = x.astype(BF)
    rest = x - hi.astype(F32)
    mid = rest.astype(BF)
    return hi, mid, (rest - mid.astype(F32)).astype(BF)


def dot(x, y, dims):
    return lax.dot_general(x, y, dims, preferred_element_type=F32)


def lhs6(x, axis):
    h, m, l = x
    return jnp.concatenate([h, h, m, m, h, l], axis=axis)


def rhs6(x, axis):
    h, m, l = x
    return jnp.concatenate([h, m, h, m, l, h], axis=axis)


def kernel(nm, nl, nq, nd, ni, bt, mt, ct, out, bv, mv, cv, ctp, tr, sbuf, rbuf, own, mloc, mq, msp, gsend, grecv, jsend, jrecv, zbuf, kacc, kin, kful, kmsg, krecv, gbuf,
           bsem, lsem, tsend, trecv, mzsend, mzrecv, mosend, morecv, gssem, grsem, jssem, jrsem, kxs, kxr, kss, krs):
    sy, a, o = lax.axis_index('sys'), lax.axis_index('aux'), lax.axis_index('orb')
    me = a * 4 + o
    dens, half = me // 2, me % 2
    nh = ni // 2
    npair = nh // 2

    def dev(aa, oo):
        return (sy, aa, oo)

    pltpu.make_async_copy(ct, cv, lsem.at[0]).start()
    for t in range(NT8):
        n = min(8, nm - 8 * t)
        pltpu.make_async_copy(bt.at[pl.ds(8 * t, n)], bv.at[pl.ds(8 * t, n)], bsem.at[t]).start()
        if t == 0:
            pltpu.make_async_copy(mt, mv, lsem.at[1]).start()
    barrier = pltpu.get_barrier_semaphore()

    def tell(k, c):
        g = lax.rem(me + k, 16)
        pl.semaphore_signal(barrier, inc=1, device_id=dev(g // 4, g % 4), device_id_type=MESH)
        return c
    lax.fori_loop(1, 16, tell, 0)

    pltpu.make_async_copy(ct, cv, lsem.at[0]).wait()
    ctp[...] = jnp.concatenate([cv[...], jnp.zeros((nd * ni, 256 - nl), F32)], axis=1)
    lhs = lhs6(split3(ctp[...]), 1)
    pltpu.make_async_copy(mt, mv, lsem.at[1]).wait()
    for b in range(4):
        blk = jnp.concatenate([mv[nq * b:nq * (b + 1), :], jnp.zeros((nq, LANES - nq), F32)], axis=1)
        mloc[b] = jnp.concatenate([blk, jnp.zeros((LANES - nq, LANES), F32)], axis=0)
    pl.semaphore_wait(barrier, 15)

    def mz(j, c):
        aa = lax.rem(a + j, 4)
        pltpu.make_async_remote_copy(src_ref=mloc.at[o], dst_ref=mq.at[a, o], send_sem=mzsend, recv_sem=mzrecv,
                                     device_id=dev(aa, o), device_id_type=MESH).start()
        return c
    lax.fori_loop(1, 4, mz, 0)

    gam = jnp.zeros((nd, LANES), F32)
    tr2 = tr

    def tile(t, pairs, gam):
        n = 2 * pairs
        pltpu.make_async_copy(bt.at[pl.ds(0, n)], bv.at[pl.ds(0, n)], bsem.at[t]).wait()
        cols = pltpu.roll(ctp[...], lax.rem(512 - (nm * o + 8 * t), 256), 1)
        for r in range(0, n, 2):
            x = jnp.concatenate([jnp.concatenate([bv[8 * t + r + e], jnp.zeros((nl, LANES - nq), F32)], axis=1) for e in range(2)], axis=1)
            x = jnp.concatenate([x, jnp.zeros((256 - nl, 2 * LANES), F32)], axis=0)
            y = dot(lhs, rhs6(split3(x), 0), NN)
            for e in range(2):
                ye = y[:, e * LANES:(e + 1) * LANES]
                tr2[pl.ds((r + e) * SP, nd * ni), :] = ye
                w = ye * cols[:, r + e:r + e + 1]
                gam = gam + w.reshape(ni, nd, LANES).sum(0)
        for g in range(16):
            d, h = g // 2, g % 2
            for p in range(npair):
                two = [tr2[pl.ds((h * nh + 2 * p + e) * nd + d, 8, stride=SP), :] for e in range(2)]
                sbuf[g, p, t] = jnp.concatenate(two, axis=0).astype(BF)
        for p in range(npair):
            two = [tr2[pl.ds((half * nh + 2 * p + e) * nd + dens, 8, stride=SP), :] for e in range(2)]
            _, mid, low = split3(jnp.concatenate(two, axis=0))
            own[0, p, t] = mid
            own[1, p, t] = low
        return gam

    def send_t1(p, t0, nt):
        def one(k, c):
            j, u = k // 4, k % 4
            aa = lax.rem(a + 2 + j, 4)
            oo = lax.rem(o + 1 + u, 4)
            g = aa * 4 + oo
            src = sbuf.at[g, p, pl.ds(t0, nt)]
            dst = rbuf.at[a, p, o, pl.ds(t0, nt)]

            @pl.when(k != 11)
            def _():
                pltpu.make_async_remote_copy(src_ref=src, dst_ref=dst, send_sem=tsend, recv_sem=trecv.at[p],
                                             device_id=dev(aa, oo), device_id_type=MESH).start()

            @pl.when(k == 11)
            def _():
                pltpu.make_async_copy(src, dst, trecv.at[p]).start()
            return c
        lax.fori_loop(0, 16, one, 0)

    def two_tiles(u, gam):
        gam = tile(2 * u, 4, gam)
        gam = tile(2 * u + 1, 4, gam)
        send_t1(0, 2 * u, 2)
        return gam
    gam = lax.fori_loop(0, 3, two_tiles, gam)
    gam = tile(6, 4, gam)
    gam = tile(7, 1, gam)
    send_t1(0, 6, 2)

    gsend[...] = gam

    def gs(k, c):
        g = lax.rem(me + k, 16)
        pltpu.make_async_remote_copy(src_ref=gsend, dst_ref=grecv.at[a, o], send_sem=gssem, recv_sem=grsem,
                                     device_id=dev(g // 4, g % 4), device_id_type=MESH).start()
        return c
    lax.fori_loop(1, 16, gs, 0)
    pltpu.make_async_copy(gsend, grecv.at[a, o], grsem).start()

    pltpu.make_async_copy(mq.at[pl.ds(0, 3), 0], mq.at[pl.ds(0, 3), 0], mzrecv).wait()

    def mo(k, c):
        aa, oo = lax.rem(a + 1 + k // 3, 4), lax.rem(o + 1 + k % 3, 4)
        pltpu.make_async_remote_copy(src_ref=mq.at[aa, o], dst_ref=mq.at[aa, o], send_sem=mosend, recv_sem=morecv,
                                     device_id=dev(a, oo), device_id_type=MESH).start()
        return c
    lax.fori_loop(0, 9, mo, 0)
    for p in range(1, npair):
        send_t1(p, 0, NT8)
    mq[a] = mloc[...]
    pltpu.make_async_copy(mq.at[pl.ds(0, 3), pl.ds(0, 3)], mq.at[pl.ds(0, 3), pl.ds(0, 3)], morecv).wait()
    for b in range(4):
        parts = split3(jnp.concatenate([mq[aa, b] for aa in range(4)], axis=1))
        for s in range(3):
            msp[s, pl.ds(b * LANES, LANES)] = parts[s]

    pltpu.make_async_copy(grecv, grecv, grsem).wait()
    graw = jnp.concatenate([grecv[aa, 0] + grecv[aa, 1] + grecv[aa, 2] + grecv[aa, 3] for aa in range(4)], axis=1)
    m3 = [msp[s] for s in range(3)]
    gfit = dot(lhs6(split3(graw), 1), rhs6(m3, 0), NN)
    mown = split3(jnp.concatenate([mloc[b] for b in range(4)], axis=0))
    wts = dot(lhs6(split3(gfit), 1), rhs6(mown, 0), NN)
    wl = lhs6(split3(wts), 1)
    low64 = lax.broadcasted_iota(jnp.int32, (nd, LANES), 1) < 64

    def jpair(u, c):
        ys = []
        for e in range(2):
            x = jnp.concatenate([bv[2 * u + e], jnp.zeros((nl, LANES - nq), F32)], axis=1)
            x = jnp.concatenate([x, jnp.zeros((256 - nl, LANES), F32)], axis=0)
            ys.append(dot(wl, rhs6(split3(x), 1), NT))
        for aa in range(4):
            lo = pltpu.roll(ys[0], (256 - nm * aa) % 256, 1)[:, :LANES]
            hi = pltpu.roll(ys[1], (256 + 64 - nm * aa) % 256, 1)[:, :LANES]
            jsend[aa, u] = jnp.where(low64, lo, hi)
        return c

    def fit(p):
        pltpu.make_async_copy(rbuf.at[:, p], rbuf.at[:, p], trecv.at[p]).wait()
        for q in range(4):
            x = jnp.concatenate([rbuf[s, p, q].reshape(LANES, LANES) for s in range(4)], axis=1)
            z = dot(jnp.concatenate([x, x, x], axis=1), msp[...].reshape(3 * 512, 512), NN)
            zbuf[pl.ds(8 * q, 8)] = z.reshape(8, 2, 8, 512)
        mid, low = own[0, p].reshape(LANES, LANES), own[1, p].reshape(LANES, LANES)
        rows = pl.ds(pl.multiple_of(a * LANES, LANES), LANES)
        mh, mm = msp[0, rows], msp[1, rows]
        z = dot(jnp.concatenate([mid, mid, low], axis=1), jnp.concatenate([mh, mm, mh], axis=0), NN)
        mine = pl.ds(8 * o, 8)
        zbuf[mine] = zbuf[mine] + z.reshape(8, 2, 8, 512)
        for e in range(2):
            s3 = split3(zbuf[:, e].reshape(4 * MROW, 512))
            k = dot(lhs6(s3, 1), rhs6(s3, 1), NT)
            if p == 0 and e == 0:
                kacc[0] = k[:, :LANES]
                kacc[1] = k[:, LANES:]
            else:
                kacc[0] = kacc[0] + k[:, :LANES]
                kacc[1] = kacc[1] + k[:, LANES:]

    fit(0)
    lax.fori_loop(0, nm // 2, jpair, 0)

    def js(j, c):
        aa = lax.rem(a + j, 4)
        pltpu.make_async_remote_copy(src_ref=jsend.at[aa], dst_ref=jrecv.at[a], send_sem=jssem, recv_sem=jrsem,
                                     device_id=dev(aa, o), device_id_type=MESH).start()
        return c
    lax.fori_loop(1, 4, js, 0)
    pltpu.make_async_copy(jsend.at[a], jrecv.at[a], jrsem).start()
    for p in range(1, npair):
        fit(p)

    mate = o + 1 - 2 * half
    swap = pltpu.make_async_remote_copy(src_ref=kacc.at[1 - half], dst_ref=kin, send_sem=kxs, recv_sem=kxr,
                                        device_id=dev(a, mate), device_id_type=MESH)
    swap.start()
    swap.wait_recv()
    kful[...] = kacc[half] + kin[...]
    low32 = lax.broadcasted_iota(jnp.int32, (32, LANES), 1) < 64
    for oo in range(4):
        ev = kful[pl.ds(MROW * oo, 32, stride=2), :]
        od = kful[pl.ds(MROW * oo + 1, 32, stride=2), :]
        kmsg[0, oo] = jnp.where(low32, ev, pltpu.roll(od, 64, 1))
        kmsg[1, oo] = jnp.where(low32, pltpu.roll(ev, 64, 1), od)

    def ks(k, c):
        al, oo = k // 4, k % 4
        aa = 2 * half + al
        same = jnp.logical_and(aa == a, oo == o)

        @pl.when(jnp.logical_not(same))
        def _():
            pltpu.make_async_remote_copy(src_ref=kmsg.at[al, oo], dst_ref=krecv.at[pl.ds(dens * 32, 32)], send_sem=kss, recv_sem=krs,
                                         device_id=dev(aa, oo), device_id_type=MESH).start()

        @pl.when(same)
        def _():
            cp = pltpu.make_async_copy(kmsg.at[al, oo], krecv.at[pl.ds(dens * 32, 32)], krs)
            cp.start()
        return c
    lax.fori_loop(0, 8, ks, 0)

    pltpu.make_async_copy(jrecv, jrecv, jrsem).wait()
    pltpu.make_async_copy(krecv, krecv, krs).wait()
    for u in range(nm // 2):
        j = jrecv[0, u] + jrecv[1, u] + jrecv[2, u] + jrecv[3, u]
        g = 2.0 * j - krecv[pl.ds(u, nd, stride=32), :]
        out[2 * u] = g[:, :nm]
        out[2 * u + 1] = pltpu.roll(g, 64, 1)[:, :nm]

    pltpu.make_async_copy(sbuf.at[pl.ds(0, 15)], sbuf.at[pl.ds(0, 15)], tsend).wait()
    pltpu.make_async_copy(mq.at[pl.ds(0, 3), 0], mq.at[pl.ds(0, 3), 0], mzsend).wait()
    pltpu.make_async_copy(mq.at[pl.ds(0, 3), pl.ds(0, 3)], mq.at[pl.ds(0, 3), pl.ds(0, 3)], mosend).wait()
    pltpu.make_async_copy(gbuf, gbuf, gssem).wait()
    pltpu.make_async_copy(jsend.at[pl.ds(0, 3)], jsend.at[pl.ds(0, 3)], jssem).wait()
    swap.wait_send()
    inset = (a // 2) == half

    @pl.when(inset)
    def _():
        pltpu.make_async_copy(krecv.at[pl.ds(0, 224)], krecv.at[pl.ds(0, 224)], kss).wait()

    @pl.when(jnp.logical_not(inset))
    def _():
        pltpu.make_async_copy(krecv, krecv, kss).wait()


def solution(mesh):
    def local_fock(ints_blk, metric_blk, orbitals):
        nq, nm, nl = ints_blk.shape
        nd, _, ni = orbitals.shape
        bt = jnp.transpose(ints_blk, (1, 2, 0))
        mt = metric_blk.T
        ct = jnp.transpose(orbitals, (2, 0, 1)).reshape(ni * nd, nl)
        npair = ni // 4
        V = pltpu.VMEM
        dma = pltpu.SemaphoreType.DMA
        g = pl.pallas_call(
            lambda *refs: kernel(nm, nl, nq, nd, ni, *refs),
            out_shape=jax.ShapeDtypeStruct((nm, nd, nm), F32),
            in_specs=[pl.BlockSpec(memory_space=pl.ANY)] * 3,
            out_specs=pl.BlockSpec(memory_space=pltpu.VMEM),
            scratch_shapes=[
                V((nm, nl, nq), F32), V((4 * nq, nq), F32), V((ni * nd, nl), F32), V((ni * nd, 256), F32),
                V((8 * SP, LANES), F32), V((16, npair, NT8, 16, LANES), BF), V((4, npair, 4, NT8, 16, LANES), BF),
                V((2, npair, NT8, 16, LANES), BF), V((4, LANES, LANES), F32), V((4, 4, LANES, LANES), F32), V((3, 512, 512), BF),
                V((nd, LANES), F32), V((4, 4, nd, LANES), F32), V((4, nm // 2, nd, LANES), F32), V((4, nm // 2, nd, LANES), F32),
                V((32, 2, 8, 512), F32), V((2, 256, LANES), F32), V((256, LANES), F32), V((256, LANES), F32), V((2, 4, 32, LANES), F32),
                V((8 * 32, LANES), F32), V((15, nd, LANES), F32),
                dma((NT8,)), dma((2,)), dma, dma((npair,)), dma, dma, dma, dma, dma, dma, dma, dma, dma, dma, dma, dma],
            compiler_params=pltpu.CompilerParams(collective_id=0, has_side_effects=True, vmem_limit_bytes=60 * 2**20),
        )(bt, mt, ct)
        return jnp.transpose(g, (1, 0, 2))

    return jax.shard_map(local_fock, mesh=mesh, in_specs=(P(('sys', 'aux'), 'orb', None), P(('sys', 'aux'), None), P('sys', None, None)), out_specs=P('sys', 'orb', 'aux'), check_vma=False)
```

```python
import jax
import jax.numpy as jnp
from jax import lax
from jax.experimental import pallas as pl
from jax.experimental.pallas import tpu as pltpu
from jax.sharding import PartitionSpec as P

F32 = jnp.float32
BF = jnp.bfloat16
MESH = pl.DeviceIdType.MESH
NN = (((1,), (0,)), ((), ()))
NT = (((1,), (1,)), ((), ()))
LANES = 128
MROW = 64
NT8 = 8
SP = 168


def split3(x):
    hi = x.astype(BF)
    rest = x - hi.astype(F32)
    mid = rest.astype(BF)
    return hi, mid, (rest - mid.astype(F32)).astype(BF)


def dot(x, y, dims):
    return lax.dot_general(x, y, dims, preferred_element_type=F32)


def lhs6(x, axis):
    h, m, l = x
    return jnp.concatenate([h, h, m, m, h, l], axis=axis)


def rhs6(x, axis):
    h, m, l = x
    return jnp.concatenate([h, m, h, m, l, h], axis=axis)


def kernel(nm, nl, nq, nd, ni, bt, mt, ct, out, bv, mv, cv, ctp, tr, sbuf, rbuf, own, mloc, mq, msp, gsend, grecv, jsend, jrecv, zbuf, kacc, kin, kful, kmsg, krecv, gbuf,
           bsem, lsem, tsend, trecv, mzsend, mzrecv, mosend, morecv, gssem, grsem, jssem, jrsem, kxs, kxr, kss, krs):
    sy, a, o = lax.axis_index('sys'), lax.axis_index('aux'), lax.axis_index('orb')
    me = a * 4 + o
    dens, half = me // 2, me % 2
    nh = ni // 2
    npair = nh // 2

    def dev(aa, oo):
        return (sy, aa, oo)

    pltpu.make_async_copy(ct, cv, lsem.at[0]).start()
    for t in range(NT8):
        n = min(8, nm - 8 * t)
        pltpu.make_async_copy(bt.at[pl.ds(8 * t, n)], bv.at[pl.ds(8 * t, n)], bsem.at[t]).start()
        if t == 0:
            pltpu.make_async_copy(mt, mv, lsem.at[1]).start()
    barrier = pltpu.get_barrier_semaphore()

    def tell(k, c):
        g = lax.rem(me + k, 16)
        pl.semaphore_signal(barrier, inc=1, device_id=dev(g // 4, g % 4), device_id_type=MESH)
        return c
    lax.fori_loop(1, 16, tell, 0)

    pltpu.make_async_copy(ct, cv, lsem.at[0]).wait()
    ctp[...] = jnp.concatenate([cv[...], jnp.zeros((nd * ni, 256 - nl), F32)], axis=1)
    lhs = lhs6(split3(ctp[...]), 1)
    pltpu.make_async_copy(mt, mv, lsem.at[1]).wait()
    for b in range(4):
        blk = jnp.concatenate([mv[nq * b:nq * (b + 1), :], jnp.zeros((nq, LANES - nq), F32)], axis=1)
        mloc[b] = jnp.concatenate([blk, jnp.zeros((LANES - nq, LANES), F32)], axis=0)
    pl.semaphore_wait(barrier, 15)

    def mz(j, c):
        aa = lax.rem(a + j, 4)
        pltpu.make_async_remote_copy(src_ref=mloc.at[o], dst_ref=mq.at[a, o], send_sem=mzsend, recv_sem=mzrecv,
                                     device_id=dev(aa, o), device_id_type=MESH).start()
        return c
    lax.fori_loop(1, 4, mz, 0)

    gam = jnp.zeros((nd, LANES), F32)
    tr2 = tr

    def tile(t, pairs, gam):
        n = 2 * pairs
        pltpu.make_async_copy(bt.at[pl.ds(0, n)], bv.at[pl.ds(0, n)], bsem.at[t]).wait()
        cols = pltpu.roll(ctp[...], lax.rem(512 - (nm * o + 8 * t), 256), 1)
        for r in range(0, n, 2):
            x = jnp.concatenate([jnp.concatenate([bv[8 * t + r + e], jnp.zeros((nl, LANES - nq), F32)], axis=1) for e in range(2)], axis=1)
            x = jnp.concatenate([x, jnp.zeros((256 - nl, 2 * LANES), F32)], axis=0)
            y = dot(lhs, rhs6(split3(x), 0), NN)
            for e in range(2):
                ye = y[:, e * LANES:(e + 1) * LANES]
                tr2[pl.ds((r + e) * SP, nd * ni), :] = ye
                w = ye * cols[:, r + e:r + e + 1]
                gam = gam + w.reshape(ni, nd, LANES).sum(0)
        for g in range(16):
            d, h = g // 2, g % 2
            for p in range(npair):
                two = [tr2[pl.ds((h * nh + 2 * p + e) * nd + d, 8, stride=SP), :] for e in range(2)]
                sbuf[g, p, t] = jnp.concatenate(two, axis=0).astype(BF)
        for p in range(npair):
            two = [tr2[pl.ds((half * nh + 2 * p + e) * nd + dens, 8, stride=SP), :] for e in range(2)]
            _, mid, low = split3(jnp.concatenate(two, axis=0))
            own[0, p, t] = mid
            own[1, p, t] = low
        return gam

    def send_t1(p, t0, nt):
        def one(k, c):
            j, u = k % 4, k // 4
            aa = lax.rem(a + 2 + j, 4)
            oo = lax.rem(o + 1 + u, 4)
            g = aa * 4 + oo
            src = sbuf.at[g, p, pl.ds(t0, nt)]
            dst = rbuf.at[a, p, o, pl.ds(t0, nt)]

            @pl.when(k != 14)
            def _():
                pltpu.make_async_remote_copy(src_ref=src, dst_ref=dst, send_sem=tsend, recv_sem=trecv.at[p],
                                             device_id=dev(aa, oo), device_id_type=MESH).start()

            @pl.when(k == 14)
            def _():
                pltpu.make_async_copy(src, dst, trecv.at[p]).start()
            return c
        lax.fori_loop(0, 16, one, 0)

    def two_tiles(u, gam):
        gam = tile(2 * u, 4, gam)
        gam = tile(2 * u + 1, 4, gam)
        send_t1(0, 2 * u, 2)
        return gam
    gam = lax.fori_loop(0, 3, two_tiles, gam)
    gam = tile(6, 4, gam)
    gam = tile(7, 1, gam)
    send_t1(0, 6, 2)

    gsend[...] = gam

    def gs(k, c):
        g = lax.rem(me + k, 16)
        pltpu.make_async_remote_copy(src_ref=gsend, dst_ref=grecv.at[a, o], send_sem=gssem, recv_sem=grsem,
                                     device_id=dev(g // 4, g % 4), device_id_type=MESH).start()
        return c
    lax.fori_loop(1, 16, gs, 0)
    pltpu.make_async_copy(gsend, grecv.at[a, o], grsem).start()

    pltpu.make_async_copy(mq.at[pl.ds(0, 3), 0], mq.at[pl.ds(0, 3), 0], mzrecv).wait()

    def mo(k, c):
        aa, oo = lax.rem(a + 1 + k // 3, 4), lax.rem(o + 1 + k % 3, 4)
        pltpu.make_async_remote_copy(src_ref=mq.at[aa, o], dst_ref=mq.at[aa, o], send_sem=mosend, recv_sem=morecv,
                                     device_id=dev(a, oo), device_id_type=MESH).start()
        return c
    lax.fori_loop(0, 9, mo, 0)
    send_t1(1, 0, NT8)
    mq[a] = mloc[...]
    pltpu.make_async_copy(mq.at[pl.ds(0, 3), pl.ds(0, 3)], mq.at[pl.ds(0, 3), pl.ds(0, 3)], morecv).wait()
    for b in range(4):
        parts = split3(jnp.concatenate([mq[aa, b] for aa in range(4)], axis=1))
        for s in range(3):
            msp[s, pl.ds(b * LANES, LANES)] = parts[s]

    pltpu.make_async_copy(grecv, grecv, grsem).wait()
    graw = jnp.concatenate([grecv[aa, 0] + grecv[aa, 1] + grecv[aa, 2] + grecv[aa, 3] for aa in range(4)], axis=1)
    m3 = [msp[s] for s in range(3)]
    gfit = dot(lhs6(split3(graw), 1), rhs6(m3, 0), NN)
    mown = split3(jnp.concatenate([mloc[b] for b in range(4)], axis=0))
    wts = dot(lhs6(split3(gfit), 1), rhs6(mown, 0), NN)
    wl = lhs6(split3(wts), 1)
    low64 = lax.broadcasted_iota(jnp.int32, (nd, LANES), 1) < 64

    def jpair(u, c):
        ys = []
        for e in range(2):
            x = jnp.concatenate([bv[2 * u + e], jnp.zeros((nl, LANES - nq), F32)], axis=1)
            x = jnp.concatenate([x, jnp.zeros((256 - nl, LANES), F32)], axis=0)
            ys.append(dot(wl, rhs6(split3(x), 1), NT))
        for aa in range(4):
            lo = pltpu.roll(ys[0], (256 - nm * aa) % 256, 1)[:, :LANES]
            hi = pltpu.roll(ys[1], (256 + 64 - nm * aa) % 256, 1)[:, :LANES]
            jsend[aa, u] = jnp.where(low64, lo, hi)
        return c

    def fit(p):
        pltpu.make_async_copy(rbuf.at[:, p], rbuf.at[:, p], trecv.at[p]).wait()
        if p + 2 < npair:
            send_t1(p + 2, 0, NT8)
        for q in range(4):
            x = jnp.concatenate([rbuf[s, p, q].reshape(LANES, LANES) for s in range(4)], axis=1)
            z = dot(jnp.concatenate([x, x, x], axis=1), msp[...].reshape(3 * 512, 512), NN)
            zbuf[pl.ds(8 * q, 8)] = z.reshape(8, 2, 8, 512)
        mid, low = own[0, p].reshape(LANES, LANES), own[1, p].reshape(LANES, LANES)
        rows = pl.ds(pl.multiple_of(a * LANES, LANES), LANES)
        mh, mm = msp[0, rows], msp[1, rows]
        z = dot(jnp.concatenate([mid, mid, low], axis=1), jnp.concatenate([mh, mm, mh], axis=0), NN)
        mine = pl.ds(8 * o, 8)
        zbuf[mine] = zbuf[mine] + z.reshape(8, 2, 8, 512)
        for e in range(2):
            s3 = split3(zbuf[:, e].reshape(4 * MROW, 512))
            k = dot(lhs6(s3, 1), rhs6(s3, 1), NT)
            if p == 0 and e == 0:
                kacc[0] = k[:, :LANES]
                kacc[1] = k[:, LANES:]
            else:
                kacc[0] = kacc[0] + k[:, :LANES]
                kacc[1] = kacc[1] + k[:, LANES:]

    fit(0)
    lax.fori_loop(0, nm // 2, jpair, 0)

    def js(j, c):
        aa = lax.rem(a + j, 4)
        pltpu.make_async_remote_copy(src_ref=jsend.at[aa], dst_ref=jrecv.at[a], send_sem=jssem, recv_sem=jrsem,
                                     device_id=dev(aa, o), device_id_type=MESH).start()
        return c
    lax.fori_loop(1, 4, js, 0)
    pltpu.make_async_copy(jsend.at[a], jrecv.at[a], jrsem).start()
    for p in range(1, npair):
        fit(p)

    mate = o + 1 - 2 * half
    swap = pltpu.make_async_remote_copy(src_ref=kacc.at[1 - half], dst_ref=kin, send_sem=kxs, recv_sem=kxr,
                                        device_id=dev(a, mate), device_id_type=MESH)
    swap.start()
    swap.wait_recv()
    kful[...] = kacc[half] + kin[...]
    low32 = lax.broadcasted_iota(jnp.int32, (32, LANES), 1) < 64
    for oo in range(4):
        ev = kful[pl.ds(MROW * oo, 32, stride=2), :]
        od = kful[pl.ds(MROW * oo + 1, 32, stride=2), :]
        kmsg[0, oo] = jnp.where(low32, ev, pltpu.roll(od, 64, 1))
        kmsg[1, oo] = jnp.where(low32, pltpu.roll(ev, 64, 1), od)

    def ks(k, c):
        al, oo = k // 4, k % 4
        aa = 2 * half + al
        same = jnp.logical_and(aa == a, oo == o)

        @pl.when(jnp.logical_not(same))
        def _():
            pltpu.make_async_remote_copy(src_ref=kmsg.at[al, oo], dst_ref=krecv.at[pl.ds(dens * 32, 32)], send_sem=kss, recv_sem=krs,
                                         device_id=dev(aa, oo), device_id_type=MESH).start()

        @pl.when(same)
        def _():
            cp = pltpu.make_async_copy(kmsg.at[al, oo], krecv.at[pl.ds(dens * 32, 32)], krs)
            cp.start()
        return c
    lax.fori_loop(0, 8, ks, 0)

    pltpu.make_async_copy(jrecv, jrecv, jrsem).wait()
    pltpu.make_async_copy(krecv, krecv, krs).wait()
    for u in range(nm // 2):
        j = jrecv[0, u] + jrecv[1, u] + jrecv[2, u] + jrecv[3, u]
        g = 2.0 * j - krecv[pl.ds(u, nd, stride=32), :]
        out[2 * u] = g[:, :nm]
        out[2 * u + 1] = pltpu.roll(g, 64, 1)[:, :nm]

    pltpu.make_async_copy(sbuf.at[pl.ds(0, 15)], sbuf.at[pl.ds(0, 15)], tsend).wait()
    pltpu.make_async_copy(mq.at[pl.ds(0, 3), 0], mq.at[pl.ds(0, 3), 0], mzsend).wait()
    pltpu.make_async_copy(mq.at[pl.ds(0, 3), pl.ds(0, 3)], mq.at[pl.ds(0, 3), pl.ds(0, 3)], mosend).wait()
    pltpu.make_async_copy(gbuf, gbuf, gssem).wait()
    pltpu.make_async_copy(jsend.at[pl.ds(0, 3)], jsend.at[pl.ds(0, 3)], jssem).wait()
    swap.wait_send()
    inset = (a // 2) == half

    @pl.when(inset)
    def _():
        pltpu.make_async_copy(krecv.at[pl.ds(0, 224)], krecv.at[pl.ds(0, 224)], kss).wait()

    @pl.when(jnp.logical_not(inset))
    def _():
        pltpu.make_async_copy(krecv, krecv, kss).wait()


def solution(mesh):
    def local_fock(ints_blk, metric_blk, orbitals):
        nq, nm, nl = ints_blk.shape
        nd, _, ni = orbitals.shape
        bt = jnp.transpose(ints_blk, (1, 2, 0))
        mt = metric_blk.T
        ct = jnp.transpose(orbitals, (2, 0, 1)).reshape(ni * nd, nl)
        npair = ni // 4
        V = pltpu.VMEM
        dma = pltpu.SemaphoreType.DMA
        g = pl.pallas_call(
            lambda *refs: kernel(nm, nl, nq, nd, ni, *refs),
            out_shape=jax.ShapeDtypeStruct((nm, nd, nm), F32),
            in_specs=[pl.BlockSpec(memory_space=pl.ANY)] * 3,
            out_specs=pl.BlockSpec(memory_space=pltpu.VMEM),
            scratch_shapes=[
                V((nm, nl, nq), F32), V((4 * nq, nq), F32), V((ni * nd, nl), F32), V((ni * nd, 256), F32),
                V((8 * SP, LANES), F32), V((16, npair, NT8, 16, LANES), BF), V((4, npair, 4, NT8, 16, LANES), BF),
                V((2, npair, NT8, 16, LANES), BF), V((4, LANES, LANES), F32), V((4, 4, LANES, LANES), F32), V((3, 512, 512), BF),
                V((nd, LANES), F32), V((4, 4, nd, LANES), F32), V((4, nm // 2, nd, LANES), F32), V((4, nm // 2, nd, LANES), F32),
                V((32, 2, 8, 512), F32), V((2, 256, LANES), F32), V((256, LANES), F32), V((256, LANES), F32), V((2, 4, 32, LANES), F32),
                V((8 * 32, LANES), F32), V((15, nd, LANES), F32),
                dma((NT8,)), dma((2,)), dma, dma((npair,)), dma, dma, dma, dma, dma, dma, dma, dma, dma, dma, dma, dma],
            compiler_params=pltpu.CompilerParams(collective_id=0, has_side_effects=True, vmem_limit_bytes=60 * 2**20),
        )(bt, mt, ct)
        return jnp.transpose(g, (1, 0, 2))

    return jax.shard_map(local_fock, mesh=mesh, in_specs=(P(('sys', 'aux'), 'orb', None), P(('sys', 'aux'), None), P('sys', None, None)), out_specs=P('sys', 'orb', 'aux'), check_vma=False)
```

```python
import jax
import jax.numpy as jnp
from jax import lax
from jax.experimental import pallas as pl
from jax.experimental.pallas import tpu as pltpu
from jax.sharding import PartitionSpec as P

F32 = jnp.float32
BF = jnp.bfloat16
MESH = pl.DeviceIdType.MESH
NN = (((1,), (0,)), ((), ()))
NT = (((1,), (1,)), ((), ()))
LANES = 128
MROW = 64
NT8 = 8
SP = 168


def split3(x):
    hi = x.astype(BF)
    rest = x - hi.astype(F32)
    mid = rest.astype(BF)
    return hi, mid, (rest - mid.astype(F32)).astype(BF)


def dot(x, y, dims):
    return lax.dot_general(x, y, dims, preferred_element_type=F32)


def lhs6(x, axis):
    h, m, l = x
    return jnp.concatenate([h, h, m, m, h, l], axis=axis)


def rhs6(x, axis):
    h, m, l = x
    return jnp.concatenate([h, m, h, m, l, h], axis=axis)


def kernel(nm, nl, nq, nd, ni, bt, mt, ct, out, bv, mv, cv, ctp, tr, sbuf, rbuf, own, mloc, mq, msp, gsend, grecv, jsend, jrecv, zbuf, kacc, kin, kful, kmsg, krecv, gbuf,
           bsem, lsem, tsend, trecv, mzsend, mzrecv, mosend, morecv, gssem, grsem, jssem, jrsem, kxs, kxr, kss, krs):
    sy, a, o = lax.axis_index('sys'), lax.axis_index('aux'), lax.axis_index('orb')
    me = a * 4 + o
    dens, half = me // 2, me % 2
    nh = ni // 2
    npair = nh // 2

    def dev(aa, oo):
        return (sy, aa, oo)

    pltpu.make_async_copy(ct, cv, lsem.at[0]).start()
    for t in range(NT8):
        n = min(8, nm - 8 * t)
        pltpu.make_async_copy(bt.at[pl.ds(8 * t, n)], bv.at[pl.ds(8 * t, n)], bsem.at[t]).start()
        if t == 0:
            pltpu.make_async_copy(mt, mv, lsem.at[1]).start()
    barrier = pltpu.get_barrier_semaphore()

    def tell(k, c):
        g = lax.rem(me + k, 16)
        pl.semaphore_signal(barrier, inc=1, device_id=dev(g // 4, g % 4), device_id_type=MESH)
        return c
    lax.fori_loop(1, 16, tell, 0)

    pltpu.make_async_copy(ct, cv, lsem.at[0]).wait()
    ctp[...] = jnp.concatenate([cv[...], jnp.zeros((nd * ni, 256 - nl), F32)], axis=1)
    lhs = lhs6(split3(ctp[...]), 1)
    pltpu.make_async_copy(mt, mv, lsem.at[1]).wait()
    for b in range(4):
        blk = jnp.concatenate([mv[nq * b:nq * (b + 1), :], jnp.zeros((nq, LANES - nq), F32)], axis=1)
        mloc[b] = jnp.concatenate([blk, jnp.zeros((LANES - nq, LANES), F32)], axis=0)
    pl.semaphore_wait(barrier, 15)

    def mz(j, c):
        aa = lax.rem(a + j, 4)
        pltpu.make_async_remote_copy(src_ref=mloc.at[o], dst_ref=mq.at[a, o], send_sem=mzsend, recv_sem=mzrecv,
                                     device_id=dev(aa, o), device_id_type=MESH).start()
        return c
    lax.fori_loop(1, 4, mz, 0)

    gam = jnp.zeros((nd, LANES), F32)
    tr2 = tr

    def tile(t, pairs, gam):
        n = 2 * pairs
        pltpu.make_async_copy(bt.at[pl.ds(0, n)], bv.at[pl.ds(0, n)], bsem.at[t]).wait()
        cols = pltpu.roll(ctp[...], lax.rem(512 - (nm * o + 8 * t), 256), 1)
        for r in range(0, n, 2):
            x = jnp.concatenate([jnp.concatenate([bv[8 * t + r + e], jnp.zeros((nl, LANES - nq), F32)], axis=1) for e in range(2)], axis=1)
            x = jnp.concatenate([x, jnp.zeros((256 - nl, 2 * LANES), F32)], axis=0)
            y = dot(lhs, rhs6(split3(x), 0), NN)
            for e in range(2):
                ye = y[:, e * LANES:(e + 1) * LANES]
                tr2[pl.ds((r + e) * SP, nd * ni), :] = ye
                w = ye * cols[:, r + e:r + e + 1]
                gam = gam + w.reshape(ni, nd, LANES).sum(0)
        for g in range(16):
            d, h = g // 2, g % 2
            for p in range(npair):
                two = [tr2[pl.ds((h * nh + 2 * p + e) * nd + d, 8, stride=SP), :] for e in range(2)]
                sbuf[g, p, t] = jnp.concatenate(two, axis=0).astype(BF)
        for p in range(npair):
            two = [tr2[pl.ds((half * nh + 2 * p + e) * nd + dens, 8, stride=SP), :] for e in range(2)]
            _, mid, low = split3(jnp.concatenate(two, axis=0))
            own[0, p, t] = mid
            own[1, p, t] = low
        return gam

    def send_t1(p, t0, nt):
        def one(k, c):
            j, u = k % 4, k // 4
            aa = lax.rem(a + 2 + j, 4)
            oo = lax.rem(o + 1 + u, 4)
            g = aa * 4 + oo
            src = sbuf.at[g, p, pl.ds(t0, nt)]
            dst = rbuf.at[a, p, o, pl.ds(t0, nt)]

            @pl.when(k != 14)
            def _():
                pltpu.make_async_remote_copy(src_ref=src, dst_ref=dst, send_sem=tsend, recv_sem=trecv.at[p],
                                             device_id=dev(aa, oo), device_id_type=MESH).start()

            @pl.when(k == 14)
            def _():
                pltpu.make_async_copy(src, dst, trecv.at[p]).start()
            return c
        lax.fori_loop(0, 16, one, 0)

    def two_tiles(u, gam):
        gam = tile(2 * u, 4, gam)
        gam = tile(2 * u + 1, 4, gam)
        send_t1(0, 2 * u, 2)
        return gam
    gam = lax.fori_loop(0, 3, two_tiles, gam)
    gam = tile(6, 4, gam)
    gam = tile(7, 1, gam)
    send_t1(0, 6, 2)

    gsend[...] = gam

    def gs(k, c):
        g = lax.rem(me + k, 16)
        pltpu.make_async_remote_copy(src_ref=gsend, dst_ref=grecv.at[a, o], send_sem=gssem, recv_sem=grsem,
                                     device_id=dev(g // 4, g % 4), device_id_type=MESH).start()
        return c
    lax.fori_loop(1, 16, gs, 0)
    pltpu.make_async_copy(gsend, grecv.at[a, o], grsem).start()

    pltpu.make_async_copy(mq.at[pl.ds(0, 3), 0], mq.at[pl.ds(0, 3), 0], mzrecv).wait()

    def mo(k, c):
        aa, oo = lax.rem(a + 1 + k // 3, 4), lax.rem(o + 1 + k % 3, 4)
        pltpu.make_async_remote_copy(src_ref=mq.at[aa, o], dst_ref=mq.at[aa, o], send_sem=mosend, recv_sem=morecv,
                                     device_id=dev(a, oo), device_id_type=MESH).start()
        return c
    lax.fori_loop(0, 9, mo, 0)
    for p in range(1, npair):
        send_t1(p, 0, NT8)
    mq[a] = mloc[...]
    pltpu.make_async_copy(mq.at[pl.ds(0, 3), pl.ds(0, 3)], mq.at[pl.ds(0, 3), pl.ds(0, 3)], morecv).wait()
    for b in range(4):
        parts = split3(jnp.concatenate([mq[aa, b] for aa in range(4)], axis=1))
        for s in range(3):
            msp[s, pl.ds(b * LANES, LANES)] = parts[s]

    pltpu.make_async_copy(grecv, grecv, grsem).wait()
    graw = jnp.concatenate([grecv[aa, 0] + grecv[aa, 1] + grecv[aa, 2] + grecv[aa, 3] for aa in range(4)], axis=1)
    m3 = [msp[s] for s in range(3)]
    gfit = dot(lhs6(split3(graw), 1), rhs6(m3, 0), NN)
    mown = split3(jnp.concatenate([mloc[b] for b in range(4)], axis=0))
    wts = dot(lhs6(split3(gfit), 1), rhs6(mown, 0), NN)
    wl = lhs6(split3(wts), 1)
    low64 = lax.broadcasted_iota(jnp.int32, (nd, LANES), 1) < 64

    def jpair(u, c):
        ys = []
        for e in range(2):
            x = jnp.concatenate([bv[2 * u + e], jnp.zeros((nl, LANES - nq), F32)], axis=1)
            x = jnp.concatenate([x, jnp.zeros((256 - nl, LANES), F32)], axis=0)
            ys.append(dot(wl, rhs6(split3(x), 1), NT))
        for aa in range(4):
            lo = pltpu.roll(ys[0], (256 - nm * aa) % 256, 1)[:, :LANES]
            hi = pltpu.roll(ys[1], (256 + 64 - nm * aa) % 256, 1)[:, :LANES]
            jsend[aa, u] = jnp.where(low64, lo, hi)
        return c

    def fit(p):
        pltpu.make_async_copy(rbuf.at[:, p], rbuf.at[:, p], trecv.at[p]).wait()
        for q in range(4):
            x = jnp.concatenate([rbuf[s, p, q].reshape(LANES, LANES) for s in range(4)], axis=1)
            z = dot(jnp.concatenate([x, x, x], axis=1), msp[...].reshape(3 * 512, 512), NN)
            zbuf[pl.ds(8 * q, 8)] = z.reshape(8, 2, 8, 512)
        mid, low = own[0, p].reshape(LANES, LANES), own[1, p].reshape(LANES, LANES)
        rows = pl.ds(pl.multiple_of(a * LANES, LANES), LANES)
        mh, mm = msp[0, rows], msp[1, rows]
        z = dot(jnp.concatenate([mid, mid, low], axis=1), jnp.concatenate([mh, mm, mh], axis=0), NN)
        mine = pl.ds(8 * o, 8)
        zbuf[mine] = zbuf[mine] + z.reshape(8, 2, 8, 512)
        for e in range(2):
            s3 = split3(zbuf[:, e].reshape(4 * MROW, 512))
            k = dot(lhs6(s3, 1), rhs6(s3, 1), NT)
            if p == 0 and e == 0:
                kacc[0] = k[:, :LANES]
                kacc[1] = k[:, LANES:]
            else:
                kacc[0] = kacc[0] + k[:, :LANES]
                kacc[1] = kacc[1] + k[:, LANES:]

    fit(0)
    lax.fori_loop(0, nm // 2, jpair, 0)

    def js(j, c):
        aa = lax.rem(a + j, 4)
        pltpu.make_async_remote_copy(src_ref=jsend.at[aa], dst_ref=jrecv.at[a], send_sem=jssem, recv_sem=jrsem,
                                     device_id=dev(aa, o), device_id_type=MESH).start()
        return c
    lax.fori_loop(1, 4, js, 0)
    pltpu.make_async_copy(jsend.at[a], jrecv.at[a], jrsem).start()
    for p in range(1, npair):
        fit(p)

    mate = o + 1 - 2 * half
    swap = pltpu.make_async_remote_copy(src_ref=kacc.at[1 - half], dst_ref=kin, send_sem=kxs, recv_sem=kxr,
                                        device_id=dev(a, mate), device_id_type=MESH)
    swap.start()
    swap.wait_recv()
    kful[...] = kacc[half] + kin[...]
    low32 = lax.broadcasted_iota(jnp.int32, (32, LANES), 1) < 64
    for oo in range(4):
        ev = kful[pl.ds(MROW * oo, 32, stride=2), :]
        od = kful[pl.ds(MROW * oo + 1, 32, stride=2), :]
        kmsg[0, oo] = jnp.where(low32, ev, pltpu.roll(od, 64, 1))
        kmsg[1, oo] = jnp.where(low32, pltpu.roll(ev, 64, 1), od)

    def ks(k, c):
        al, oo = k // 4, k % 4
        aa = 2 * half + al
        same = jnp.logical_and(aa == a, oo == o)

        @pl.when(jnp.logical_not(same))
        def _():
            pltpu.make_async_remote_copy(src_ref=kmsg.at[al, oo], dst_ref=krecv.at[pl.ds(dens * 32, 32)], send_sem=kss, recv_sem=krs,
                                         device_id=dev(aa, oo), device_id_type=MESH).start()

        @pl.when(same)
        def _():
            cp = pltpu.make_async_copy(kmsg.at[al, oo], krecv.at[pl.ds(dens * 32, 32)], krs)
            cp.start()
        return c
    lax.fori_loop(0, 8, ks, 0)

    pltpu.make_async_copy(jrecv, jrecv, jrsem).wait()
    pltpu.make_async_copy(krecv, krecv, krs).wait()
    for u in range(nm // 2):
        j = jrecv[0, u] + jrecv[1, u] + jrecv[2, u] + jrecv[3, u]
        g = 2.0 * j - krecv[pl.ds(u, nd, stride=32), :]
        out[2 * u] = g[:, :nm]
        out[2 * u + 1] = pltpu.roll(g, 64, 1)[:, :nm]

    pltpu.make_async_copy(sbuf.at[pl.ds(0, 15)], sbuf.at[pl.ds(0, 15)], tsend).wait()
    pltpu.make_async_copy(mq.at[pl.ds(0, 3), 0], mq.at[pl.ds(0, 3), 0], mzsend).wait()
    pltpu.make_async_copy(mq.at[pl.ds(0, 3), pl.ds(0, 3)], mq.at[pl.ds(0, 3), pl.ds(0, 3)], mosend).wait()
    pltpu.make_async_copy(gbuf, gbuf, gssem).wait()
    pltpu.make_async_copy(jsend.at[pl.ds(0, 3)], jsend.at[pl.ds(0, 3)], jssem).wait()
    swap.wait_send()
    inset = (a // 2) == half

    @pl.when(inset)
    def _():
        pltpu.make_async_copy(krecv.at[pl.ds(0, 224)], krecv.at[pl.ds(0, 224)], kss).wait()

    @pl.when(jnp.logical_not(inset))
    def _():
        pltpu.make_async_copy(krecv, krecv, kss).wait()


def solution(mesh):
    def local_fock(ints_blk, metric_blk, orbitals):
        nq, nm, nl = ints_blk.shape
        nd, _, ni = orbitals.shape
        bt = jnp.transpose(ints_blk, (1, 2, 0))
        mt = metric_blk.T
        ct = jnp.transpose(orbitals, (2, 0, 1)).reshape(ni * nd, nl)
        npair = ni // 4
        V = pltpu.VMEM
        dma = pltpu.SemaphoreType.DMA
        g = pl.pallas_call(
            lambda *refs: kernel(nm, nl, nq, nd, ni, *refs),
            out_shape=jax.ShapeDtypeStruct((nm, nd, nm), F32),
            in_specs=[pl.BlockSpec(memory_space=pl.ANY)] * 3,
            out_specs=pl.BlockSpec(memory_space=pltpu.VMEM),
            scratch_shapes=[
                V((nm, nl, nq), F32), V((4 * nq, nq), F32), V((ni * nd, nl), F32), V((ni * nd, 256), F32),
                V((8 * SP, LANES), F32), V((16, npair, NT8, 16, LANES), BF), V((4, npair, 4, NT8, 16, LANES), BF),
                V((2, npair, NT8, 16, LANES), BF), V((4, LANES, LANES), F32), V((4, 4, LANES, LANES), F32), V((3, 512, 512), BF),
                V((nd, LANES), F32), V((4, 4, nd, LANES), F32), V((4, nm // 2, nd, LANES), F32), V((4, nm // 2, nd, LANES), F32),
                V((32, 2, 8, 512), F32), V((2, 256, LANES), F32), V((256, LANES), F32), V((256, LANES), F32), V((2, 4, 32, LANES), F32),
                V((8 * 32, LANES), F32), V((15, nd, LANES), F32),
                dma((NT8,)), dma((2,)), dma, dma((npair,)), dma, dma, dma, dma, dma, dma, dma, dma, dma, dma, dma, dma],
            compiler_params=pltpu.CompilerParams(collective_id=0, has_side_effects=True, vmem_limit_bytes=60 * 2**20),
        )(bt, mt, ct)
        return jnp.transpose(g, (1, 0, 2))

    return jax.shard_map(local_fock, mesh=mesh, in_specs=(P(('sys', 'aux'), 'orb', None), P(('sys', 'aux'), None), P('sys', None, None)), out_specs=P('sys', 'orb', 'aux'), check_vma=False)
```

```python
import jax
import jax.numpy as jnp
from jax import lax
from jax.experimental import pallas as pl
from jax.experimental.pallas import tpu as pltpu
from jax.sharding import PartitionSpec as P

F32 = jnp.float32
BF = jnp.bfloat16
MESH = pl.DeviceIdType.MESH
NN = (((1,), (0,)), ((), ()))
NT = (((1,), (1,)), ((), ()))
LANES = 128
MROW = 64
NT8 = 7
PIECE = 12
SP = 168


def split3(x):
    hi = x.astype(BF)
    rest = x - hi.astype(F32)
    mid = rest.astype(BF)
    return hi, mid, (rest - mid.astype(F32)).astype(BF)


def dot(x, y, dims):
    return lax.dot_general(x, y, dims, preferred_element_type=F32)


def lhs6(x, axis):
    h, m, l = x
    return jnp.concatenate([h, h, m, m, h, l], axis=axis)


def rhs6(x, axis):
    h, m, l = x
    return jnp.concatenate([h, m, h, m, l, h], axis=axis)


def kernel(nm, nl, nq, nd, ni, bt, mt, ct, out, bv, mv, cv, ctp, tr, sbuf, rbuf, own, mloc, mq, msp, gsend, grecv, jsend, jrecv, zbuf, kacc, kin, kful, kmsg, krecv, gbuf,
           bsem, lsem, tsend, trecv, mzsend, mzrecv, mosend, morecv, gssem, grsem, jssem, jrsem, kxs, kxr, kss, krs):
    sy, a, o = lax.axis_index('sys'), lax.axis_index('aux'), lax.axis_index('orb')
    me = a * 4 + o
    dens, half = me // 2, me % 2
    nh = ni // 2
    npair = nh // 2

    def dev(aa, oo):
        return (sy, aa, oo)

    pltpu.make_async_copy(ct, cv, lsem.at[0]).start()
    pltpu.make_async_copy(bt.at[pl.ds(8 * NT8, 2)], bv.at[pl.ds(8 * NT8, 2)], lsem.at[2]).start()
    for t in range(NT8):
        pltpu.make_async_copy(bt.at[pl.ds(8 * t, 8)], bv.at[pl.ds(8 * t, 8)], bsem.at[t]).start()
        if t == 0:
            pltpu.make_async_copy(mt, mv, lsem.at[1]).start()
    barrier = pltpu.get_barrier_semaphore()

    def tell(k, c):
        g = lax.rem(me + k, 16)
        pl.semaphore_signal(barrier, inc=1, device_id=dev(g // 4, g % 4), device_id_type=MESH)
        return c
    lax.fori_loop(1, 16, tell, 0)

    pltpu.make_async_copy(ct, cv, lsem.at[0]).wait()
    ctp[...] = jnp.concatenate([cv[...], jnp.zeros((nd * ni, 256 - nl), F32)], axis=1)
    lhs = lhs6(split3(ctp[...]), 1)
    pltpu.make_async_copy(mt, mv, lsem.at[1]).wait()
    for b in range(4):
        blk = jnp.concatenate([mv[nq * b:nq * (b + 1), :], jnp.zeros((nq, LANES - nq), F32)], axis=1)
        mloc[b] = jnp.concatenate([blk, jnp.zeros((LANES - nq, LANES), F32)], axis=0)
    pl.semaphore_wait(barrier, 15)

    def mz(j, c):
        aa = lax.rem(a + j, 4)
        pltpu.make_async_remote_copy(src_ref=mloc.at[o], dst_ref=mq.at[a, o], send_sem=mzsend, recv_sem=mzrecv,
                                     device_id=dev(aa, o), device_id_type=MESH).start()
        return c
    lax.fori_loop(1, 4, mz, 0)

    gam = jnp.zeros((nd, LANES), F32)
    tr2 = tr

    lane = lax.broadcasted_iota(jnp.int32, (1, LANES), 1)
    data = lane < nq

    def tile(t, gam, tail, first):
        pltpu.make_async_copy(bt.at[pl.ds(0, 8)], bv.at[pl.ds(0, 8)], bsem.at[t]).wait()
        cols = pltpu.roll(ctp[...], lax.rem(512 - (nm * o + 8 * t), 256), 1)
        count = 0
        if tail is not None:
            count = min(8, 10 - first)
            spare = jnp.concatenate([bv[8 * NT8 + tail], jnp.zeros((nl, LANES - nq), F32)], axis=1)
            tcol = pltpu.roll(ctp[...], lax.rem(512 - (nm * o + 8 * NT8 + tail), 256), 1)[:, 0:1]
        for r in range(0, 8, 2):
            xs = []
            for e in range(2):
                x = jnp.concatenate([bv[8 * t + r + e], jnp.zeros((nl, LANES - nq), F32)], axis=1)
                if r + e < count:
                    x = jnp.where(data, x, pltpu.roll(spare, (nq - PIECE * (first + r + e)) % LANES, 1))
                xs.append(x)
            x = jnp.concatenate(xs, axis=1)
            x = jnp.concatenate([x, jnp.zeros((256 - nl, 2 * LANES), F32)], axis=0)
            y = dot(lhs, rhs6(split3(x), 0), NN)
            for e in range(2):
                ye = y[:, e * LANES:(e + 1) * LANES]
                tr2[pl.ds((r + e) * SP, nd * ni), :] = ye
                col = cols[:, r + e:r + e + 1]
                if r + e < count:
                    w = (ye * jnp.where(data, col, tcol)).reshape(ni, nd, LANES).sum(0)
                    moved = pltpu.roll(jnp.where(data, 0.0, w), (PIECE * (first + r + e) - nq) % LANES, 1)
                    gam = gam + jnp.where(data, w, 0.0) + moved
                else:
                    gam = gam + (ye * col).reshape(ni, nd, LANES).sum(0)
        for g in range(16):
            d, h = g // 2, g % 2
            for p in range(npair):
                two = [tr2[pl.ds((h * nh + 2 * p + e) * nd + d, 8, stride=SP), :] for e in range(2)]
                sbuf[g, p, t] = jnp.concatenate(two, axis=0).astype(BF)
        for p in range(npair):
            two = [tr2[pl.ds((half * nh + 2 * p + e) * nd + dens, 8, stride=SP), :] for e in range(2)]
            _, mid, low = split3(jnp.concatenate(two, axis=0))
            own[0, p, t] = mid
            own[1, p, t] = low
        return gam

    def send_t1(p, t0, nt):
        def one(k, c):
            j, u = k % 4, k // 4
            aa = lax.rem(a + 2 + j, 4)
            oo = lax.rem(o + 1 + u, 4)
            g = aa * 4 + oo
            src = sbuf.at[g, p, pl.ds(t0, nt)]
            dst = rbuf.at[a, p, o, pl.ds(t0, nt)]

            @pl.when(k != 14)
            def _():
                pltpu.make_async_remote_copy(src_ref=src, dst_ref=dst, send_sem=tsend, recv_sem=trecv.at[p],
                                             device_id=dev(aa, oo), device_id_type=MESH).start()

            @pl.when(k == 14)
            def _():
                pltpu.make_async_copy(src, dst, trecv.at[p]).start()
            return c
        lax.fori_loop(0, 16, one, 0)

    pltpu.make_async_copy(bt.at[pl.ds(0, 2)], bv.at[pl.ds(0, 2)], lsem.at[2]).wait()

    def two_tiles(u, gam):
        gam = tile(2 * u, gam, u, 0)
        gam = tile(2 * u + 1, gam, u, 8)
        send_t1(0, 2 * u, 2)
        return gam
    gam = lax.fori_loop(0, 2, two_tiles, gam)

    def one_tile(t, gam):
        gam = tile(t, gam, None, 0)
        send_t1(0, t, 1)
        return gam
    gam = lax.fori_loop(4, NT8, one_tile, gam)

    gsend[...] = gam

    def gs(k, c):
        g = lax.rem(me + k, 16)
        pltpu.make_async_remote_copy(src_ref=gsend, dst_ref=grecv.at[a, o], send_sem=gssem, recv_sem=grsem,
                                     device_id=dev(g // 4, g % 4), device_id_type=MESH).start()
        return c
    lax.fori_loop(1, 16, gs, 0)
    pltpu.make_async_copy(gsend, grecv.at[a, o], grsem).start()

    pltpu.make_async_copy(mq.at[pl.ds(0, 3), 0], mq.at[pl.ds(0, 3), 0], mzrecv).wait()

    def mo(k, c):
        aa, oo = lax.rem(a + 1 + k // 3, 4), lax.rem(o + 1 + k % 3, 4)
        pltpu.make_async_remote_copy(src_ref=mq.at[aa, o], dst_ref=mq.at[aa, o], send_sem=mosend, recv_sem=morecv,
                                     device_id=dev(a, oo), device_id_type=MESH).start()
        return c
    lax.fori_loop(0, 9, mo, 0)
    for p in range(1, npair):
        send_t1(p, 0, NT8)
    mq[a] = mloc[...]
    pltpu.make_async_copy(mq.at[pl.ds(0, 3), pl.ds(0, 3)], mq.at[pl.ds(0, 3), pl.ds(0, 3)], morecv).wait()
    for b in range(4):
        parts = split3(jnp.concatenate([mq[aa, b] for aa in range(4)], axis=1))
        for s in range(3):
            msp[s, pl.ds(b * LANES, LANES)] = parts[s]

    pltpu.make_async_copy(grecv, grecv, grsem).wait()
    graw = jnp.concatenate([grecv[aa, 0] + grecv[aa, 1] + grecv[aa, 2] + grecv[aa, 3] for aa in range(4)], axis=1)
    m3 = [msp[s] for s in range(3)]
    gfit = dot(lhs6(split3(graw), 1), rhs6(m3, 0), NN)
    mown = split3(jnp.concatenate([mloc[b] for b in range(4)], axis=0))
    wts = dot(lhs6(split3(gfit), 1), rhs6(mown, 0), NN)
    wl = lhs6(split3(wts), 1)
    low64 = lax.broadcasted_iota(jnp.int32, (nd, LANES), 1) < 64

    def jpair(u, c):
        ys = []
        for e in range(2):
            x = jnp.concatenate([bv[2 * u + e], jnp.zeros((nl, LANES - nq), F32)], axis=1)
            x = jnp.concatenate([x, jnp.zeros((256 - nl, LANES), F32)], axis=0)
            ys.append(dot(wl, rhs6(split3(x), 1), NT))
        for aa in range(4):
            lo = pltpu.roll(ys[0], (256 - nm * aa) % 256, 1)[:, :LANES]
            hi = pltpu.roll(ys[1], (256 + 64 - nm * aa) % 256, 1)[:, :LANES]
            jsend[aa, u] = jnp.where(low64, lo, hi)
        return c

    row8 = lax.broadcasted_iota(jnp.int32, (8, LANES), 0)
    lane8 = lax.broadcasted_iota(jnp.int32, (8, LANES), 1)
    at0 = lane8 - PIECE * row8
    at1 = lane8 - PIECE * (row8 + 8)
    here0 = jnp.logical_and(at0 >= 0, at0 < PIECE)
    here1 = jnp.logical_and(jnp.logical_and(at1 >= 0, at1 < PIECE), lane8 < nq)
    zbuf[:, NT8] = jnp.zeros((4, 2, 8, 512), F32)

    def tails(x):
        f = [x[t].astype(F32) for t in range(4)]
        out = []
        for e in range(2):
            for u in range(2):
                v0 = pltpu.roll(f[2 * u][8 * e:8 * e + 8], LANES - nq, 1, stride=PIECE, stride_axis=0)
                f1 = f[2 * u + 1][8 * e:8 * e + 8]
                v1 = jnp.where(row8 == 0, pltpu.roll(f1, (8 * PIECE - nq) % LANES, 1), pltpu.roll(f1, (9 * PIECE - nq) % LANES, 1))
                v = jnp.where(here0, v0, jnp.where(here1, v1, 0.0))
                out.append(v.sum(0, keepdims=True))
        return out

    def fit(p):
        pltpu.make_async_copy(rbuf.at[:, p], rbuf.at[:, p], trecv.at[p]).wait()
        xs = []
        for s in range(4):
            rest = [w for q in range(4) for w in tails(rbuf[s, p, q, pl.ds(0, 4)])]
            xs.append(jnp.concatenate([rbuf[s, p].reshape(4 * NT8 * 16, LANES), jnp.concatenate(rest, axis=0).astype(BF)], axis=0))
        x = jnp.concatenate(xs, axis=1)
        z = dot(jnp.concatenate([x, x, x], axis=1), msp[...].reshape(3 * 512, 512), NN)
        main = 4 * NT8 * 16
        zbuf[:, pl.ds(0, NT8)] = z[:main].reshape(4, NT8, 2, 8, 512)
        for q in range(4):
            for e in range(2):
                zbuf[q, NT8, e, pl.ds(0, 2)] = z[main + 4 * q + 2 * e:main + 4 * q + 2 * e + 2]
        ml = []
        for s in range(2):
            rest = tails(own[s, p, pl.ds(0, 4)]) + [jnp.zeros((12, LANES), F32)]
            ml.append(jnp.concatenate([own[s, p].reshape(NT8 * 16, LANES), jnp.concatenate(rest, axis=0).astype(BF)], axis=0))
        mid, low = ml
        rows = pl.ds(pl.multiple_of(a * LANES, LANES), LANES)
        mh, mm = msp[0, rows], msp[1, rows]
        z = dot(jnp.concatenate([mid, mid, low], axis=1), jnp.concatenate([mh, mm, mh], axis=0), NN)
        zbuf[o, pl.ds(0, NT8)] = zbuf[o, pl.ds(0, NT8)] + z[:NT8 * 16].reshape(NT8, 2, 8, 512)
        for e in range(2):
            zbuf[o, NT8, e, pl.ds(0, 2)] = zbuf[o, NT8, e, pl.ds(0, 2)] + z[NT8 * 16 + 2 * e:NT8 * 16 + 2 * e + 2]
        for e in range(2):
            s3 = split3(zbuf[:, :, e].reshape(4 * MROW, 512))
            k = dot(lhs6(s3, 1), rhs6(s3, 1), NT)
            if p == 0 and e == 0:
                kacc[0] = k[:, :LANES]
                kacc[1] = k[:, LANES:]
            else:
                kacc[0] = kacc[0] + k[:, :LANES]
                kacc[1] = kacc[1] + k[:, LANES:]

    fit(0)
    lax.fori_loop(0, nm // 2, jpair, 0)

    def js(j, c):
        aa = lax.rem(a + j, 4)
        pltpu.make_async_remote_copy(src_ref=jsend.at[aa], dst_ref=jrecv.at[a], send_sem=jssem, recv_sem=jrsem,
                                     device_id=dev(aa, o), device_id_type=MESH).start()
        return c
    lax.fori_loop(1, 4, js, 0)
    pltpu.make_async_copy(jsend.at[a], jrecv.at[a], jrsem).start()
    for p in range(1, npair):
        fit(p)

    mate = o + 1 - 2 * half
    swap = pltpu.make_async_remote_copy(src_ref=kacc.at[1 - half], dst_ref=kin, send_sem=kxs, recv_sem=kxr,
                                        device_id=dev(a, mate), device_id_type=MESH)
    swap.start()
    swap.wait_recv()
    kful[...] = kacc[half] + kin[...]
    low32 = lax.broadcasted_iota(jnp.int32, (32, LANES), 1) < 64
    for oo in range(4):
        ev = kful[pl.ds(MROW * oo, 32, stride=2), :]
        od = kful[pl.ds(MROW * oo + 1, 32, stride=2), :]
        kmsg[0, oo] = jnp.where(low32, ev, pltpu.roll(od, 64, 1))
        kmsg[1, oo] = jnp.where(low32, pltpu.roll(ev, 64, 1), od)

    def ks(k, c):
        al, oo = k // 4, k % 4
        aa = 2 * half + al
        same = jnp.logical_and(aa == a, oo == o)

        @pl.when(jnp.logical_not(same))
        def _():
            pltpu.make_async_remote_copy(src_ref=kmsg.at[al, oo], dst_ref=krecv.at[pl.ds(dens * 32, 32)], send_sem=kss, recv_sem=krs,
                                         device_id=dev(aa, oo), device_id_type=MESH).start()

        @pl.when(same)
        def _():
            cp = pltpu.make_async_copy(kmsg.at[al, oo], krecv.at[pl.ds(dens * 32, 32)], krs)
            cp.start()
        return c
    lax.fori_loop(0, 8, ks, 0)

    pltpu.make_async_copy(jrecv, jrecv, jrsem).wait()
    pltpu.make_async_copy(krecv, krecv, krs).wait()
    for u in range(nm // 2):
        j = jrecv[0, u] + jrecv[1, u] + jrecv[2, u] + jrecv[3, u]
        g = 2.0 * j - krecv[pl.ds(u, nd, stride=32), :]
        out[2 * u] = g[:, :nm]
        out[2 * u + 1] = pltpu.roll(g, 64, 1)[:, :nm]

    pltpu.make_async_copy(sbuf.at[pl.ds(0, 15)], sbuf.at[pl.ds(0, 15)], tsend).wait()
    pltpu.make_async_copy(mq.at[pl.ds(0, 3), 0], mq.at[pl.ds(0, 3), 0], mzsend).wait()
    pltpu.make_async_copy(mq.at[pl.ds(0, 3), pl.ds(0, 3)], mq.at[pl.ds(0, 3), pl.ds(0, 3)], mosend).wait()
    pltpu.make_async_copy(gbuf, gbuf, gssem).wait()
    pltpu.make_async_copy(jsend.at[pl.ds(0, 3)], jsend.at[pl.ds(0, 3)], jssem).wait()
    swap.wait_send()
    inset = (a // 2) == half

    @pl.when(inset)
    def _():
        pltpu.make_async_copy(krecv.at[pl.ds(0, 224)], krecv.at[pl.ds(0, 224)], kss).wait()

    @pl.when(jnp.logical_not(inset))
    def _():
        pltpu.make_async_copy(krecv, krecv, kss).wait()


def solution(mesh):
    def local_fock(ints_blk, metric_blk, orbitals):
        nq, nm, nl = ints_blk.shape
        nd, _, ni = orbitals.shape
        bt = jnp.transpose(ints_blk, (1, 2, 0))
        mt = metric_blk.T
        ct = jnp.transpose(orbitals, (2, 0, 1)).reshape(ni * nd, nl)
        npair = ni // 4
        V = pltpu.VMEM
        dma = pltpu.SemaphoreType.DMA
        g = pl.pallas_call(
            lambda *refs: kernel(nm, nl, nq, nd, ni, *refs),
            out_shape=jax.ShapeDtypeStruct((nm, nd, nm), F32),
            in_specs=[pl.BlockSpec(memory_space=pl.ANY)] * 3,
            out_specs=pl.BlockSpec(memory_space=pltpu.VMEM),
            scratch_shapes=[
                V((nm, nl, nq), F32), V((4 * nq, nq), F32), V((ni * nd, nl), F32), V((ni * nd, 256), F32),
                V((8 * SP, LANES), F32), V((16, npair, NT8, 16, LANES), BF), V((4, npair, 4, NT8, 16, LANES), BF),
                V((2, npair, NT8, 16, LANES), BF), V((4, LANES, LANES), F32), V((4, 4, LANES, LANES), F32), V((3, 512, 512), BF),
                V((nd, LANES), F32), V((4, 4, nd, LANES), F32), V((4, nm // 2, nd, LANES), F32), V((4, nm // 2, nd, LANES), F32),
                V((4, 8, 2, 8, 512), F32), V((2, 256, LANES), F32), V((256, LANES), F32), V((256, LANES), F32), V((2, 4, 32, LANES), F32),
                V((8 * 32, LANES), F32), V((15, nd, LANES), F32),
                dma((NT8,)), dma((3,)), dma, dma((npair,)), dma, dma, dma, dma, dma, dma, dma, dma, dma, dma, dma, dma],
            compiler_params=pltpu.CompilerParams(collective_id=0, has_side_effects=True, vmem_limit_bytes=60 * 2**20),
        )(bt, mt, ct)
        return jnp.transpose(g, (1, 0, 2))

    return jax.shard_map(local_fock, mesh=mesh, in_specs=(P(('sys', 'aux'), 'orb', None), P(('sys', 'aux'), None), P('sys', None, None)), out_specs=P('sys', 'orb', 'aux'), check_vma=False)
```

```python
import jax
import jax.numpy as jnp
from jax import lax
from jax.experimental import pallas as pl
from jax.experimental.pallas import tpu as pltpu
from jax.sharding import PartitionSpec as P

F32 = jnp.float32
BF = jnp.bfloat16
MESH = pl.DeviceIdType.MESH
NN = (((1,), (0,)), ((), ()))
NT = (((1,), (1,)), ((), ()))
LANES = 128
MROW = 64
NT8 = 7
PIECE = 12
SP = 168


def split3(x):
    hi = x.astype(BF)
    rest = x - hi.astype(F32)
    mid = rest.astype(BF)
    return hi, mid, (rest - mid.astype(F32)).astype(BF)


def dot(x, y, dims):
    return lax.dot_general(x, y, dims, preferred_element_type=F32)


def lhs6(x, axis):
    h, m, l = x
    return jnp.concatenate([h, h, m, m, h, l], axis=axis)


def rhs6(x, axis):
    h, m, l = x
    return jnp.concatenate([h, m, h, m, l, h], axis=axis)


def kernel(nm, nl, nq, nd, ni, bt, mt, ct, out, bv, mv, cv, ctp, tr, sbuf, rbuf, own, mloc, mqr, mq, msp, gsend, grecv, jsend, jrecv, jfwd, zbuf, kacc, kin, kful, kmsg, krecv, gbuf,
           bsem, lsem, tsend, trecv, mzsend, mzrecv, mosend, morecv, gssem, grsem, jssem, jrsem, kxs, kxr, kss, krs):
    sy, a, o = lax.axis_index('sys'), lax.axis_index('aux'), lax.axis_index('orb')
    me = a * 4 + o
    dens, half = me // 2, me % 2
    nh = ni // 2
    npair = nh // 2

    def dev(aa, oo):
        return (sy, aa, oo)

    pltpu.make_async_copy(ct, cv, lsem.at[0]).start()
    pltpu.make_async_copy(bt.at[pl.ds(8 * NT8, 2)], bv.at[pl.ds(8 * NT8, 2)], lsem.at[2]).start()
    for t in range(NT8):
        pltpu.make_async_copy(bt.at[pl.ds(8 * t, 8)], bv.at[pl.ds(8 * t, 8)], bsem.at[t]).start()
        if t == 0:
            pltpu.make_async_copy(mt, mv, lsem.at[1]).start()
    barrier = pltpu.get_barrier_semaphore()

    def tell(k, c):
        g = lax.rem(me + k, 16)
        pl.semaphore_signal(barrier, inc=1, device_id=dev(g // 4, g % 4), device_id_type=MESH)
        return c
    lax.fori_loop(1, 16, tell, 0)

    pltpu.make_async_copy(ct, cv, lsem.at[0]).wait()
    ctp[...] = jnp.concatenate([cv[...], jnp.zeros((nd * ni, 256 - nl), F32)], axis=1)
    lhs = lhs6(split3(ctp[...]), 1)
    pltpu.make_async_copy(mt, mv, lsem.at[1]).wait()
    for b in range(4):
        blk = jnp.concatenate([mv[nq * b:nq * (b + 1), :], jnp.zeros((nq, LANES - nq), F32)], axis=1)
        mloc[b] = jnp.concatenate([blk, jnp.zeros((LANES - nq, LANES), F32)], axis=0)
    pl.semaphore_wait(barrier, 15)

    quarter = pl.ds(pl.multiple_of(o * 32, 32), 32)

    def nearer(x, y, z):
        dx, dy = jnp.abs(x - z), jnp.abs(y - z)
        return jnp.logical_or(dx < dy, jnp.logical_and(dx == dy, x < y))

    def metric_copies(act):
        for k in (2, 1, 3):
            to = lax.rem(a + 4 - k, 4)

            def block(row, slot):
                return pltpu.make_async_remote_copy(src_ref=mloc.at[row, quarter], dst_ref=mqr.at[slot, quarter], send_sem=mzsend,
                                                    recv_sem=mzrecv, device_id=dev(to, o), device_id_type=MESH)
            act(block(a, k - 1))
            for k2 in (1, 2, 3):
                if k2 == k:
                    continue
                b = lax.rem(to + k2, 4)

                @pl.when(nearer(a, b, to))
                def _():
                    act(block(b, k + k2))
    metric_copies(lambda c: c.start())

    gam = jnp.zeros((nd, LANES), F32)
    tr2 = tr

    lane = lax.broadcasted_iota(jnp.int32, (1, LANES), 1)
    data = lane < nq

    def tile(t, gam, tail, first):
        pltpu.make_async_copy(bt.at[pl.ds(0, 8)], bv.at[pl.ds(0, 8)], bsem.at[t]).wait()
        cols = pltpu.roll(ctp[...], lax.rem(512 - (nm * o + 8 * t), 256), 1)
        count = 0
        if tail is not None:
            count = min(8, 10 - first)
            spare = jnp.concatenate([bv[8 * NT8 + tail], jnp.zeros((nl, LANES - nq), F32)], axis=1)
            tcol = pltpu.roll(ctp[...], lax.rem(512 - (nm * o + 8 * NT8 + tail), 256), 1)[:, 0:1]
        for r in range(0, 8, 2):
            xs = []
            for e in range(2):
                x = jnp.concatenate([bv[8 * t + r + e], jnp.zeros((nl, LANES - nq), F32)], axis=1)
                if r + e < count:
                    x = jnp.where(data, x, pltpu.roll(spare, (nq - PIECE * (first + r + e)) % LANES, 1))
                xs.append(x)
            x = jnp.concatenate(xs, axis=1)
            x = jnp.concatenate([x, jnp.zeros((256 - nl, 2 * LANES), F32)], axis=0)
            y = dot(lhs, rhs6(split3(x), 0), NN)
            for e in range(2):
                ye = y[:, e * LANES:(e + 1) * LANES]
                tr2[pl.ds((r + e) * SP, nd * ni), :] = ye
                col = cols[:, r + e:r + e + 1]
                if r + e < count:
                    w = (ye * jnp.where(data, col, tcol)).reshape(ni, nd, LANES).sum(0)
                    moved = pltpu.roll(jnp.where(data, 0.0, w), (PIECE * (first + r + e) - nq) % LANES, 1)
                    gam = gam + jnp.where(data, w, 0.0) + moved
                else:
                    gam = gam + (ye * col).reshape(ni, nd, LANES).sum(0)
        for g in range(16):
            d, h = g // 2, g % 2
            for p in range(npair):
                two = [tr2[pl.ds((h * nh + 2 * p + e) * nd + d, 8, stride=SP), :] for e in range(2)]
                sbuf[g, p, t] = jnp.concatenate(two, axis=0).astype(BF)
        for p in range(npair):
            two = [tr2[pl.ds((half * nh + 2 * p + e) * nd + dens, 8, stride=SP), :] for e in range(2)]
            _, mid, low = split3(jnp.concatenate(two, axis=0))
            own[0, p, t] = mid
            own[1, p, t] = low
        return gam

    def send_t1(p, t0, nt):
        def one(k, c):
            j, u = k % 4, k // 4
            aa = lax.rem(a + 2 + j, 4)
            oo = lax.rem(o + 1 + u, 4)
            g = aa * 4 + oo
            src = sbuf.at[g, p, pl.ds(t0, nt)]
            dst = rbuf.at[a, p, o, pl.ds(t0, nt)]

            @pl.when(k != 14)
            def _():
                pltpu.make_async_remote_copy(src_ref=src, dst_ref=dst, send_sem=tsend, recv_sem=trecv.at[p],
                                             device_id=dev(aa, oo), device_id_type=MESH).start()

            @pl.when(k == 14)
            def _():
                pltpu.make_async_copy(src, dst, trecv.at[p]).start()
            return c
        lax.fori_loop(0, 16, one, 0)

    pltpu.make_async_copy(bt.at[pl.ds(0, 2)], bv.at[pl.ds(0, 2)], lsem.at[2]).wait()

    def two_tiles(u, gam):
        gam = tile(2 * u, gam, u, 0)
        gam = tile(2 * u + 1, gam, u, 8)
        send_t1(0, 2 * u, 2)
        return gam
    gam = lax.fori_loop(0, 2, two_tiles, gam)

    def one_tile(t, gam):
        gam = tile(t, gam, None, 0)
        send_t1(0, t, 1)
        return gam
    gam = lax.fori_loop(4, NT8, one_tile, gam)

    gsend[...] = gam

    def gs(k, c):
        g = lax.rem(me + k, 16)
        pltpu.make_async_remote_copy(src_ref=gsend, dst_ref=grecv.at[a, o], send_sem=gssem, recv_sem=grsem,
                                     device_id=dev(g // 4, g % 4), device_id_type=MESH).start()
        return c
    lax.fori_loop(1, 16, gs, 0)
    pltpu.make_async_copy(gsend, grecv.at[a, o], grsem).start()

    pltpu.make_async_copy(mqr.at[:, pl.ds(0, 32)], mqr.at[:, pl.ds(0, 32)], mzrecv).wait()

    def mo(k, c):
        oo = lax.rem(o + k, 4)
        pltpu.make_async_remote_copy(src_ref=mqr.at[:, quarter], dst_ref=mqr.at[:, quarter], send_sem=mosend, recv_sem=morecv,
                                     device_id=dev(a, oo), device_id_type=MESH).start()
        return c
    lax.fori_loop(1, 4, mo, 0)
    for p in range(1, 3):
        send_t1(p, 0, NT8)
    mq[a] = mloc[...]
    for k in range(1, 4):
        c1 = lax.rem(a + k, 4)
        mq[c1, a] = mloc[c1].T
    pltpu.make_async_copy(mqr.at[:, pl.ds(0, 96)], mqr.at[:, pl.ds(0, 96)], morecv).wait()
    for k in range(1, 4):
        c1 = lax.rem(a + k, 4)
        mq[c1, c1] = mqr[k - 1]
        for k2 in range(k + 1, 4):
            c2 = lax.rem(a + k2, 4)
            first = jnp.where(nearer(c1, c2, a), c1, c2)
            second = c1 + c2 - first
            blk = mqr[k + k2]
            mq[first, second] = blk
            mq[second, first] = blk.T
    for b in range(4):
        parts = split3(jnp.concatenate([mq[aa, b] for aa in range(4)], axis=1))
        for s in range(3):
            msp[s, pl.ds(b * LANES, LANES)] = parts[s]

    pltpu.make_async_copy(grecv, grecv, grsem).wait()
    graw = jnp.concatenate([grecv[aa, 0] + grecv[aa, 1] + grecv[aa, 2] + grecv[aa, 3] for aa in range(4)], axis=1)
    m3 = [msp[s] for s in range(3)]
    gfit = dot(lhs6(split3(graw), 1), rhs6(m3, 0), NN)
    mown = split3(jnp.concatenate([mloc[b] for b in range(4)], axis=0))
    wts = dot(lhs6(split3(gfit), 1), rhs6(mown, 0), NN)
    wl = lhs6(split3(wts), 1)
    low64 = lax.broadcasted_iota(jnp.int32, (nd, LANES), 1) < 64

    def jpair(u, c):
        ys = []
        for e in range(2):
            x = jnp.concatenate([bv[2 * u + e], jnp.zeros((nl, LANES - nq), F32)], axis=1)
            x = jnp.concatenate([x, jnp.zeros((256 - nl, LANES), F32)], axis=0)
            ys.append(dot(wl, rhs6(split3(x), 1), NT))
        for aa in range(4):
            lo = pltpu.roll(ys[0], (256 - nm * aa) % 256, 1)[:, :LANES]
            hi = pltpu.roll(ys[1], (256 + 64 - nm * aa) % 256, 1)[:, :LANES]
            jsend[aa, u] = jnp.where(low64, lo, hi)
        return c

    row8 = lax.broadcasted_iota(jnp.int32, (8, LANES), 0)
    lane8 = lax.broadcasted_iota(jnp.int32, (8, LANES), 1)
    at0 = lane8 - PIECE * row8
    at1 = lane8 - PIECE * (row8 + 8)
    here0 = jnp.logical_and(at0 >= 0, at0 < PIECE)
    here1 = jnp.logical_and(jnp.logical_and(at1 >= 0, at1 < PIECE), lane8 < nq)
    zbuf[:, NT8] = jnp.zeros((4, 2, 8, 512), F32)

    def tails(x):
        f = [x[t].astype(F32) for t in range(4)]
        out = []
        for e in range(2):
            for u in range(2):
                v0 = pltpu.roll(f[2 * u][8 * e:8 * e + 8], LANES - nq, 1, stride=PIECE, stride_axis=0)
                f1 = f[2 * u + 1][8 * e:8 * e + 8]
                v1 = jnp.where(row8 == 0, pltpu.roll(f1, (8 * PIECE - nq) % LANES, 1), pltpu.roll(f1, (9 * PIECE - nq) % LANES, 1))
                v = jnp.where(here0, v0, jnp.where(here1, v1, 0.0))
                out.append(v.sum(0, keepdims=True))
        return out

    def fit(p):
        pltpu.make_async_copy(rbuf.at[:, p], rbuf.at[:, p], trecv.at[p]).wait()
        xs = []
        for s in range(4):
            rest = [w for q in range(4) for w in tails(rbuf[s, p, q, pl.ds(0, 4)])]
            xs.append(jnp.concatenate([rbuf[s, p].reshape(4 * NT8 * 16, LANES), jnp.concatenate(rest, axis=0).astype(BF)], axis=0))
        x = jnp.concatenate(xs, axis=1)
        z = dot(jnp.concatenate([x, x, x], axis=1), msp[...].reshape(3 * 512, 512), NN)
        main = 4 * NT8 * 16
        zbuf[:, pl.ds(0, NT8)] = z[:main].reshape(4, NT8, 2, 8, 512)
        for q in range(4):
            for e in range(2):
                zbuf[q, NT8, e, pl.ds(0, 2)] = z[main + 4 * q + 2 * e:main + 4 * q + 2 * e + 2]
        ml = []
        for s in range(2):
            rest = tails(own[s, p, pl.ds(0, 4)]) + [jnp.zeros((12, LANES), F32)]
            ml.append(jnp.concatenate([own[s, p].reshape(NT8 * 16, LANES), jnp.concatenate(rest, axis=0).astype(BF)], axis=0))
        mid, low = ml
        rows = pl.ds(pl.multiple_of(a * LANES, LANES), LANES)
        mh, mm = msp[0, rows], msp[1, rows]
        z = dot(jnp.concatenate([mid, mid, low], axis=1), jnp.concatenate([mh, mm, mh], axis=0), NN)
        zbuf[o, pl.ds(0, NT8)] = zbuf[o, pl.ds(0, NT8)] + z[:NT8 * 16].reshape(NT8, 2, 8, 512)
        for e in range(2):
            zbuf[o, NT8, e, pl.ds(0, 2)] = zbuf[o, NT8, e, pl.ds(0, 2)] + z[NT8 * 16 + 2 * e:NT8 * 16 + 2 * e + 2]
        for e in range(2):
            s3 = split3(zbuf[:, :, e].reshape(4 * MROW, 512))
            k = dot(lhs6(s3, 1), rhs6(s3, 1), NT)
            if p == 0 and e == 0:
                kacc[0] = k[:, :LANES]
                kacc[1] = k[:, LANES:]
            else:
                kacc[0] = kacc[0] + k[:, :LANES]
                kacc[1] = kacc[1] + k[:, LANES:]

    lax.fori_loop(0, nm // 2, jpair, 0)
    near, far = a + 1 - 2 * (a % 2), lax.rem(a + 2, 4)
    hops = []
    for e, aa in enumerate((lax.rem(near + 2, 4), near)):
        hops.append(pltpu.make_async_remote_copy(src_ref=jsend.at[aa], dst_ref=jrecv.at[e], send_sem=jssem.at[e], recv_sem=jrsem.at[e],
                                                 device_id=dev(near, o), device_id_type=MESH))
        hops[-1].start()
    for p in range(3, npair):
        send_t1(p, 0, NT8)
    fit(0)
    fit(1)
    hops[0].wait_recv()
    jfwd[...] = jsend[far] + jrecv[0]
    cross = pltpu.make_async_remote_copy(src_ref=jfwd, dst_ref=jrecv.at[2], send_sem=jssem.at[2], recv_sem=jrsem.at[2],
                                         device_id=dev(far, o), device_id_type=MESH)
    cross.start()
    for p in range(2, npair):
        fit(p)

    mate = o + 1 - 2 * half
    swap = pltpu.make_async_remote_copy(src_ref=kacc.at[1 - half], dst_ref=kin, send_sem=kxs, recv_sem=kxr,
                                        device_id=dev(a, mate), device_id_type=MESH)
    swap.start()
    swap.wait_recv()
    kful[...] = kacc[half] + kin[...]
    low32 = lax.broadcasted_iota(jnp.int32, (32, LANES), 1) < 64
    for oo in range(4):
        ev = kful[pl.ds(MROW * oo, 32, stride=2), :]
        od = kful[pl.ds(MROW * oo + 1, 32, stride=2), :]
        kmsg[0, oo] = jnp.where(low32, ev, pltpu.roll(od, 64, 1))
        kmsg[1, oo] = jnp.where(low32, pltpu.roll(ev, 64, 1), od)

    def ks(k, c):
        al, oo = k // 4, k % 4
        aa = 2 * half + al
        same = jnp.logical_and(aa == a, oo == o)

        @pl.when(jnp.logical_not(same))
        def _():
            pltpu.make_async_remote_copy(src_ref=kmsg.at[al, oo], dst_ref=krecv.at[pl.ds(dens * 32, 32)], send_sem=kss, recv_sem=krs,
                                         device_id=dev(aa, oo), device_id_type=MESH).start()

        @pl.when(same)
        def _():
            cp = pltpu.make_async_copy(kmsg.at[al, oo], krecv.at[pl.ds(dens * 32, 32)], krs)
            cp.start()
        return c
    lax.fori_loop(0, 8, ks, 0)

    hops[1].wait_recv()
    cross.wait_recv()
    pltpu.make_async_copy(krecv, krecv, krs).wait()
    for u in range(nm // 2):
        j = jsend[a, u] + jrecv[1, u] + jrecv[2, u]
        g = 2.0 * j - krecv[pl.ds(u, nd, stride=32), :]
        out[2 * u] = g[:, :nm]
        out[2 * u + 1] = pltpu.roll(g, 64, 1)[:, :nm]

    pltpu.make_async_copy(sbuf.at[pl.ds(0, 15)], sbuf.at[pl.ds(0, 15)], tsend).wait()
    metric_copies(lambda c: c.wait_send())
    pltpu.make_async_copy(mqr.at[:, pl.ds(0, 96)], mqr.at[:, pl.ds(0, 96)], mosend).wait()
    pltpu.make_async_copy(gbuf, gbuf, gssem).wait()
    for c in hops + [cross]:
        c.wait_send()
    swap.wait_send()
    inset = (a // 2) == half

    @pl.when(inset)
    def _():
        pltpu.make_async_copy(krecv.at[pl.ds(0, 224)], krecv.at[pl.ds(0, 224)], kss).wait()

    @pl.when(jnp.logical_not(inset))
    def _():
        pltpu.make_async_copy(krecv, krecv, kss).wait()


def solution(mesh):
    def local_fock(ints_blk, metric_blk, orbitals):
        nq, nm, nl = ints_blk.shape
        nd, _, ni = orbitals.shape
        bt = jnp.transpose(ints_blk, (1, 2, 0))
        mt = metric_blk.T
        ct = jnp.transpose(orbitals, (2, 0, 1)).reshape(ni * nd, nl)
        npair = ni // 4
        V = pltpu.VMEM
        dma = pltpu.SemaphoreType.DMA
        g = pl.pallas_call(
            lambda *refs: kernel(nm, nl, nq, nd, ni, *refs),
            out_shape=jax.ShapeDtypeStruct((nm, nd, nm), F32),
            in_specs=[pl.BlockSpec(memory_space=pl.ANY)] * 3,
            out_specs=pl.BlockSpec(memory_space=pltpu.VMEM),
            scratch_shapes=[
                V((nm, nl, nq), F32), V((4 * nq, nq), F32), V((ni * nd, nl), F32), V((ni * nd, 256), F32),
                V((8 * SP, LANES), F32), V((16, npair, NT8, 16, LANES), BF), V((4, npair, 4, NT8, 16, LANES), BF),
                V((2, npair, NT8, 16, LANES), BF), V((4, LANES, LANES), F32), V((6, LANES, LANES), F32), V((4, 4, LANES, LANES), F32), V((3, 512, 512), BF),
                V((nd, LANES), F32), V((4, 4, nd, LANES), F32), V((4, nm // 2, nd, LANES), F32), V((3, nm // 2, nd, LANES), F32), V((nm // 2, nd, LANES), F32),
                V((4, 8, 2, 8, 512), F32), V((2, 256, LANES), F32), V((256, LANES), F32), V((256, LANES), F32), V((2, 4, 32, LANES), F32),
                V((8 * 32, LANES), F32), V((15, nd, LANES), F32),
                dma((NT8,)), dma((3,)), dma, dma((npair,)), dma, dma, dma, dma, dma, dma, dma((3,)), dma((3,)), dma, dma, dma, dma],
            compiler_params=pltpu.CompilerParams(collective_id=0, has_side_effects=True, vmem_limit_bytes=60 * 2**20),
        )(bt, mt, ct)
        return jnp.transpose(g, (1, 0, 2))

    return jax.shard_map(local_fock, mesh=mesh, in_specs=(P(('sys', 'aux'), 'orb', None), P(('sys', 'aux'), None), P('sys', None, None)), out_specs=P('sys', 'orb', 'aux'), check_vma=False)
```

```python
import jax
import jax.numpy as jnp
from jax import lax
from jax.experimental import pallas as pl
from jax.experimental.pallas import tpu as pltpu
from jax.sharding import PartitionSpec as P

F32 = jnp.float32
BF = jnp.bfloat16
MESH = pl.DeviceIdType.MESH
NN = (((1,), (0,)), ((), ()))
NT = (((1,), (1,)), ((), ()))
LANES = 128
MROW = 64
NT8 = 7
PIECE = 12
SP = 168


def split3(x):
    hi = x.astype(BF)
    rest = x - hi.astype(F32)
    mid = rest.astype(BF)
    return hi, mid, (rest - mid.astype(F32)).astype(BF)


def dot(x, y, dims):
    return lax.dot_general(x, y, dims, preferred_element_type=F32)


def lhs6(x, axis):
    h, m, l = x
    return jnp.concatenate([h, h, m, m, h, l], axis=axis)


def rhs6(x, axis):
    h, m, l = x
    return jnp.concatenate([h, m, h, m, l, h], axis=axis)


def kernel(nm, nl, nq, nd, ni, bt, mt, ct, out, bv, mv, cv, ctp, tr, sbuf, rbuf, own, mloc, mqr, mq, msp, gsend, grecv, jsend, jrecv, jfwd, zbuf, kacc, kin, kful, kmsg, krecv, gbuf,
           bsem, lsem, tsend, trecv, mzsend, mzrecv, mosend, morecv, gssem, grsem, jssem, jrsem, kxs, kxr, kss, krs):
    sy, a, o = lax.axis_index('sys'), lax.axis_index('aux'), lax.axis_index('orb')
    me = a * 4 + o
    dens, half = me // 2, me % 2
    nh = ni // 2
    npair = nh // 2

    def dev(aa, oo):
        return (sy, aa, oo)

    pltpu.make_async_copy(ct, cv, lsem.at[0]).start()
    pltpu.make_async_copy(bt.at[pl.ds(8 * NT8, 2)], bv.at[pl.ds(8 * NT8, 2)], lsem.at[2]).start()
    for t in range(NT8):
        pltpu.make_async_copy(bt.at[pl.ds(8 * t, 8)], bv.at[pl.ds(8 * t, 8)], bsem.at[t]).start()
        if t == 0:
            pltpu.make_async_copy(mt, mv, lsem.at[1]).start()
    barrier = pltpu.get_barrier_semaphore()

    def tell(k, c):
        g = lax.rem(me + k, 16)
        pl.semaphore_signal(barrier, inc=1, device_id=dev(g // 4, g % 4), device_id_type=MESH)
        return c
    lax.fori_loop(1, 16, tell, 0)

    pltpu.make_async_copy(ct, cv, lsem.at[0]).wait()
    ctp[...] = jnp.concatenate([cv[...], jnp.zeros((nd * ni, 256 - nl), F32)], axis=1)
    lhs = lhs6(split3(ctp[...]), 1)
    pltpu.make_async_copy(mt, mv, lsem.at[1]).wait()
    for b in range(4):
        blk = jnp.concatenate([mv[nq * b:nq * (b + 1), :], jnp.zeros((nq, LANES - nq), F32)], axis=1)
        mloc[b] = jnp.concatenate([blk, jnp.zeros((LANES - nq, LANES), F32)], axis=0)
    pl.semaphore_wait(barrier, 15)

    quarter = pl.ds(pl.multiple_of(o * 32, 32), 32)

    def nearer(x, y, z):
        dx, dy = jnp.abs(x - z), jnp.abs(y - z)
        return jnp.logical_or(dx < dy, jnp.logical_and(dx == dy, x < y))

    def metric_copies(act):
        for k in (2, 1, 3):
            to = lax.rem(a + 4 - k, 4)

            def block(row, slot):
                return pltpu.make_async_remote_copy(src_ref=mloc.at[row, quarter], dst_ref=mqr.at[slot, quarter], send_sem=mzsend,
                                                    recv_sem=mzrecv, device_id=dev(to, o), device_id_type=MESH)
            act(block(a, k - 1))
            for k2 in (1, 2, 3):
                if k2 == k:
                    continue
                b = lax.rem(to + k2, 4)

                @pl.when(nearer(a, b, to))
                def _():
                    act(block(b, k + k2))
    metric_copies(lambda c: c.start())

    gam = jnp.zeros((nd, LANES), F32)
    tr2 = tr

    lane = lax.broadcasted_iota(jnp.int32, (1, LANES), 1)
    data = lane < nq

    def tile(t, gam, tail, first):
        pltpu.make_async_copy(bt.at[pl.ds(0, 8)], bv.at[pl.ds(0, 8)], bsem.at[t]).wait()
        cols = pltpu.roll(ctp[...], lax.rem(512 - (nm * o + 8 * t), 256), 1)
        count = 0
        if tail is not None:
            count = min(8, 10 - first)
            spare = jnp.concatenate([bv[8 * NT8 + tail], jnp.zeros((nl, LANES - nq), F32)], axis=1)
            tcol = pltpu.roll(ctp[...], lax.rem(512 - (nm * o + 8 * NT8 + tail), 256), 1)[:, 0:1]
        for r in range(0, 8, 2):
            xs = []
            for e in range(2):
                x = jnp.concatenate([bv[8 * t + r + e], jnp.zeros((nl, LANES - nq), F32)], axis=1)
                if r + e < count:
                    x = jnp.where(data, x, pltpu.roll(spare, (nq - PIECE * (first + r + e)) % LANES, 1))
                xs.append(x)
            x = jnp.concatenate(xs, axis=1)
            x = jnp.concatenate([x, jnp.zeros((256 - nl, 2 * LANES), F32)], axis=0)
            y = dot(lhs, rhs6(split3(x), 0), NN)
            for e in range(2):
                ye = y[:, e * LANES:(e + 1) * LANES]
                tr2[pl.ds((r + e) * SP, nd * ni), :] = ye
                col = cols[:, r + e:r + e + 1]
                if r + e < count:
                    w = (ye * jnp.where(data, col, tcol)).reshape(ni, nd, LANES).sum(0)
                    moved = pltpu.roll(jnp.where(data, 0.0, w), (PIECE * (first + r + e) - nq) % LANES, 1)
                    gam = gam + jnp.where(data, w, 0.0) + moved
                else:
                    gam = gam + (ye * col).reshape(ni, nd, LANES).sum(0)
        for g in range(16):
            d, h = g // 2, g % 2
            for p in range(npair):
                two = [tr2[pl.ds((h * nh + 2 * p + e) * nd + d, 8, stride=SP), :] for e in range(2)]
                sbuf[g, p, t] = jnp.concatenate(two, axis=0).astype(BF)
        for p in range(npair):
            two = [tr2[pl.ds((half * nh + 2 * p + e) * nd + dens, 8, stride=SP), :] for e in range(2)]
            _, mid, low = split3(jnp.concatenate(two, axis=0))
            own[0, p, t] = mid
            own[1, p, t] = low
        return gam

    outer = jnp.logical_or(a == 0, a == 3)
    pair = a + 1 - 2 * (a % 2)

    def send_t1(p, t0, nt, cross):
        def one(k, c):
            if cross:
                aa = jnp.where(k % 2 == 0, 3 - a, 3 - pair)
                oo = lax.rem(o + 1 + k // 2, 4)
            else:
                aa = jnp.where(k % 2 == 0, pair, a)
                oo = lax.rem(o + 1 + k // 2, 4)
            g = aa * 4 + oo
            src = sbuf.at[g, p, pl.ds(t0, nt)]
            dst = rbuf.at[a, p, o, pl.ds(t0, nt)]

            def far():
                pltpu.make_async_remote_copy(src_ref=src, dst_ref=dst, send_sem=tsend, recv_sem=trecv.at[p],
                                             device_id=dev(aa, oo), device_id_type=MESH).start()
            if cross:
                far()
            else:
                pl.when(k != 7)(far)

                @pl.when(k == 7)
                def _():
                    pltpu.make_async_copy(src, dst, trecv.at[p]).start()
            return c
        lax.fori_loop(0, 8, one, 0)

    def send_early(p, t0, nt):
        @pl.when(jnp.logical_not(outer))
        def _():
            send_t1(p, t0, nt, True)
        send_t1(p, t0, nt, False)

    pltpu.make_async_copy(bt.at[pl.ds(0, 2)], bv.at[pl.ds(0, 2)], lsem.at[2]).wait()

    def two_tiles(u, gam):
        gam = tile(2 * u, gam, u, 0)
        gam = tile(2 * u + 1, gam, u, 8)
        send_early(0, 2 * u, 2)
        return gam
    gam = lax.fori_loop(0, 2, two_tiles, gam)

    def one_tile(t, gam):
        gam = tile(t, gam, None, 0)
        send_early(0, t, 1)
        return gam
    gam = lax.fori_loop(4, NT8, one_tile, gam)

    gsend[...] = gam

    def gs(k, c):
        g = lax.rem(me + k, 16)
        pltpu.make_async_remote_copy(src_ref=gsend, dst_ref=grecv.at[a, o], send_sem=gssem, recv_sem=grsem,
                                     device_id=dev(g // 4, g % 4), device_id_type=MESH).start()
        return c
    lax.fori_loop(1, 16, gs, 0)
    pltpu.make_async_copy(gsend, grecv.at[a, o], grsem).start()

    pltpu.make_async_copy(mqr.at[:, pl.ds(0, 32)], mqr.at[:, pl.ds(0, 32)], mzrecv).wait()

    def mo(k, c):
        oo = lax.rem(o + k, 4)
        pltpu.make_async_remote_copy(src_ref=mqr.at[:, quarter], dst_ref=mqr.at[:, quarter], send_sem=mosend, recv_sem=morecv,
                                     device_id=dev(a, oo), device_id_type=MESH).start()
        return c
    lax.fori_loop(1, 4, mo, 0)
    for p in range(1, npair):
        send_early(p, 0, NT8)
    mq[a] = mloc[...]
    for k in range(1, 4):
        c1 = lax.rem(a + k, 4)
        mq[c1, a] = mloc[c1].T
    pltpu.make_async_copy(mqr.at[:, pl.ds(0, 96)], mqr.at[:, pl.ds(0, 96)], morecv).wait()
    for k in range(1, 4):
        c1 = lax.rem(a + k, 4)
        mq[c1, c1] = mqr[k - 1]
        for k2 in range(k + 1, 4):
            c2 = lax.rem(a + k2, 4)
            first = jnp.where(nearer(c1, c2, a), c1, c2)
            second = c1 + c2 - first
            blk = mqr[k + k2]
            mq[first, second] = blk
            mq[second, first] = blk.T
    for b in range(4):
        parts = split3(jnp.concatenate([mq[aa, b] for aa in range(4)], axis=1))
        for s in range(3):
            msp[s, pl.ds(b * LANES, LANES)] = parts[s]

    pltpu.make_async_copy(grecv, grecv, grsem).wait()
    graw = jnp.concatenate([grecv[aa, 0] + grecv[aa, 1] + grecv[aa, 2] + grecv[aa, 3] for aa in range(4)], axis=1)
    m3 = [msp[s] for s in range(3)]
    gfit = dot(lhs6(split3(graw), 1), rhs6(m3, 0), NN)
    mown = split3(jnp.concatenate([mloc[b] for b in range(4)], axis=0))
    wts = dot(lhs6(split3(gfit), 1), rhs6(mown, 0), NN)
    wl = lhs6(split3(wts), 1)
    low64 = lax.broadcasted_iota(jnp.int32, (nd, LANES), 1) < 64

    def jpair(u, c):
        ys = []
        for e in range(2):
            x = jnp.concatenate([bv[2 * u + e], jnp.zeros((nl, LANES - nq), F32)], axis=1)
            x = jnp.concatenate([x, jnp.zeros((256 - nl, LANES), F32)], axis=0)
            ys.append(dot(wl, rhs6(split3(x), 1), NT))
        for aa in range(4):
            lo = pltpu.roll(ys[0], (256 - nm * aa) % 256, 1)[:, :LANES]
            hi = pltpu.roll(ys[1], (256 + 64 - nm * aa) % 256, 1)[:, :LANES]
            jsend[aa, u] = jnp.where(low64, lo, hi)
        return c

    row8 = lax.broadcasted_iota(jnp.int32, (8, LANES), 0)
    lane8 = lax.broadcasted_iota(jnp.int32, (8, LANES), 1)
    at0 = lane8 - PIECE * row8
    at1 = lane8 - PIECE * (row8 + 8)
    here0 = jnp.logical_and(at0 >= 0, at0 < PIECE)
    here1 = jnp.logical_and(jnp.logical_and(at1 >= 0, at1 < PIECE), lane8 < nq)
    zbuf[:, NT8] = jnp.zeros((4, 2, 8, 512), F32)

    def tails(x):
        f = [x[t].astype(F32) for t in range(4)]
        out = []
        for e in range(2):
            for u in range(2):
                v0 = pltpu.roll(f[2 * u][8 * e:8 * e + 8], LANES - nq, 1, stride=PIECE, stride_axis=0)
                f1 = f[2 * u + 1][8 * e:8 * e + 8]
                v1 = jnp.where(row8 == 0, pltpu.roll(f1, (8 * PIECE - nq) % LANES, 1), pltpu.roll(f1, (9 * PIECE - nq) % LANES, 1))
                v = jnp.where(here0, v0, jnp.where(here1, v1, 0.0))
                out.append(v.sum(0, keepdims=True))
        return out

    def fit(p):
        pltpu.make_async_copy(rbuf.at[:, p], rbuf.at[:, p], trecv.at[p]).wait()
        xs = []
        for s in range(4):
            rest = [w for q in range(4) for w in tails(rbuf[s, p, q, pl.ds(0, 4)])]
            xs.append(jnp.concatenate([rbuf[s, p].reshape(4 * NT8 * 16, LANES), jnp.concatenate(rest, axis=0).astype(BF)], axis=0))
        x = jnp.concatenate(xs, axis=1)
        z = dot(jnp.concatenate([x, x, x], axis=1), msp[...].reshape(3 * 512, 512), NN)
        main = 4 * NT8 * 16
        zbuf[:, pl.ds(0, NT8)] = z[:main].reshape(4, NT8, 2, 8, 512)
        for q in range(4):
            for e in range(2):
                zbuf[q, NT8, e, pl.ds(0, 2)] = z[main + 4 * q + 2 * e:main + 4 * q + 2 * e + 2]
        ml = []
        for s in range(2):
            rest = tails(own[s, p, pl.ds(0, 4)]) + [jnp.zeros((12, LANES), F32)]
            ml.append(jnp.concatenate([own[s, p].reshape(NT8 * 16, LANES), jnp.concatenate(rest, axis=0).astype(BF)], axis=0))
        mid, low = ml
        rows = pl.ds(pl.multiple_of(a * LANES, LANES), LANES)
        mh, mm = msp[0, rows], msp[1, rows]
        z = dot(jnp.concatenate([mid, mid, low], axis=1), jnp.concatenate([mh, mm, mh], axis=0), NN)
        zbuf[o, pl.ds(0, NT8)] = zbuf[o, pl.ds(0, NT8)] + z[:NT8 * 16].reshape(NT8, 2, 8, 512)
        for e in range(2):
            zbuf[o, NT8, e, pl.ds(0, 2)] = zbuf[o, NT8, e, pl.ds(0, 2)] + z[NT8 * 16 + 2 * e:NT8 * 16 + 2 * e + 2]
        for e in range(2):
            s3 = split3(zbuf[:, :, e].reshape(4 * MROW, 512))
            k = dot(lhs6(s3, 1), rhs6(s3, 1), NT)
            if p == 0 and e == 0:
                kacc[0] = k[:, :LANES]
                kacc[1] = k[:, LANES:]
            else:
                kacc[0] = kacc[0] + k[:, :LANES]
                kacc[1] = kacc[1] + k[:, LANES:]

    lax.fori_loop(0, nm // 2, jpair, 0)
    near, far = a + 1 - 2 * (a % 2), lax.rem(a + 2, 4)
    hops = []
    for e, aa in enumerate((lax.rem(near + 2, 4), near)):
        hops.append(pltpu.make_async_remote_copy(src_ref=jsend.at[aa], dst_ref=jrecv.at[e], send_sem=jssem.at[e], recv_sem=jrsem.at[e],
                                                 device_id=dev(near, o), device_id_type=MESH))
        hops[-1].start()
    @pl.when(outer)
    def _():
        for p in range(npair):
            send_t1(p, 0, NT8, True)
    for p in range(npair - 1):
        fit(p)
    hops[0].wait_recv()
    jfwd[...] = jsend[far] + jrecv[0]
    cross = pltpu.make_async_remote_copy(src_ref=jfwd, dst_ref=jrecv.at[2], send_sem=jssem.at[2], recv_sem=jrsem.at[2],
                                         device_id=dev(far, o), device_id_type=MESH)
    cross.start()
    fit(npair - 1)

    mate = o + 1 - 2 * half
    swap = pltpu.make_async_remote_copy(src_ref=kacc.at[1 - half], dst_ref=kin, send_sem=kxs, recv_sem=kxr,
                                        device_id=dev(a, mate), device_id_type=MESH)
    swap.start()
    swap.wait_recv()
    kful[...] = kacc[half] + kin[...]
    low32 = lax.broadcasted_iota(jnp.int32, (32, LANES), 1) < 64
    for oo in range(4):
        ev = kful[pl.ds(MROW * oo, 32, stride=2), :]
        od = kful[pl.ds(MROW * oo + 1, 32, stride=2), :]
        kmsg[0, oo] = jnp.where(low32, ev, pltpu.roll(od, 64, 1))
        kmsg[1, oo] = jnp.where(low32, pltpu.roll(ev, 64, 1), od)

    def ks(k, c):
        al, oo = k // 4, k % 4
        aa = 2 * half + al
        same = jnp.logical_and(aa == a, oo == o)

        @pl.when(jnp.logical_not(same))
        def _():
            pltpu.make_async_remote_copy(src_ref=kmsg.at[al, oo], dst_ref=krecv.at[pl.ds(dens * 32, 32)], send_sem=kss, recv_sem=krs,
                                         device_id=dev(aa, oo), device_id_type=MESH).start()

        @pl.when(same)
        def _():
            cp = pltpu.make_async_copy(kmsg.at[al, oo], krecv.at[pl.ds(dens * 32, 32)], krs)
            cp.start()
        return c
    lax.fori_loop(0, 8, ks, 0)

    hops[1].wait_recv()
    cross.wait_recv()
    pltpu.make_async_copy(krecv, krecv, krs).wait()
    for u in range(nm // 2):
        j = jsend[a, u] + jrecv[1, u] + jrecv[2, u]
        g = 2.0 * j - krecv[pl.ds(u, nd, stride=32), :]
        out[2 * u] = g[:, :nm]
        out[2 * u + 1] = pltpu.roll(g, 64, 1)[:, :nm]

    pltpu.make_async_copy(sbuf.at[pl.ds(0, 15)], sbuf.at[pl.ds(0, 15)], tsend).wait()
    metric_copies(lambda c: c.wait_send())
    pltpu.make_async_copy(mqr.at[:, pl.ds(0, 96)], mqr.at[:, pl.ds(0, 96)], mosend).wait()
    pltpu.make_async_copy(gbuf, gbuf, gssem).wait()
    for c in hops + [cross]:
        c.wait_send()
    swap.wait_send()
    inset = (a // 2) == half

    @pl.when(inset)
    def _():
        pltpu.make_async_copy(krecv.at[pl.ds(0, 224)], krecv.at[pl.ds(0, 224)], kss).wait()

    @pl.when(jnp.logical_not(inset))
    def _():
        pltpu.make_async_copy(krecv, krecv, kss).wait()


def solution(mesh):
    def local_fock(ints_blk, metric_blk, orbitals):
        nq, nm, nl = ints_blk.shape
        nd, _, ni = orbitals.shape
        bt = jnp.transpose(ints_blk, (1, 2, 0))
        mt = metric_blk.T
        ct = jnp.transpose(orbitals, (2, 0, 1)).reshape(ni * nd, nl)
        npair = ni // 4
        V = pltpu.VMEM
        dma = pltpu.SemaphoreType.DMA
        g = pl.pallas_call(
            lambda *refs: kernel(nm, nl, nq, nd, ni, *refs),
            out_shape=jax.ShapeDtypeStruct((nm, nd, nm), F32),
            in_specs=[pl.BlockSpec(memory_space=pl.ANY)] * 3,
            out_specs=pl.BlockSpec(memory_space=pltpu.VMEM),
            scratch_shapes=[
                V((nm, nl, nq), F32), V((4 * nq, nq), F32), V((ni * nd, nl), F32), V((ni * nd, 256), F32),
                V((8 * SP, LANES), F32), V((16, npair, NT8, 16, LANES), BF), V((4, npair, 4, NT8, 16, LANES), BF),
                V((2, npair, NT8, 16, LANES), BF), V((4, LANES, LANES), F32), V((6, LANES, LANES), F32), V((4, 4, LANES, LANES), F32), V((3, 512, 512), BF),
                V((nd, LANES), F32), V((4, 4, nd, LANES), F32), V((4, nm // 2, nd, LANES), F32), V((3, nm // 2, nd, LANES), F32), V((nm // 2, nd, LANES), F32),
                V((4, 8, 2, 8, 512), F32), V((2, 256, LANES), F32), V((256, LANES), F32), V((256, LANES), F32), V((2, 4, 32, LANES), F32),
                V((8 * 32, LANES), F32), V((15, nd, LANES), F32),
                dma((NT8,)), dma((3,)), dma, dma((npair,)), dma, dma, dma, dma, dma, dma, dma((3,)), dma((3,)), dma, dma, dma, dma],
            compiler_params=pltpu.CompilerParams(collective_id=0, has_side_effects=True, vmem_limit_bytes=60 * 2**20),
        )(bt, mt, ct)
        return jnp.transpose(g, (1, 0, 2))

    return jax.shard_map(local_fock, mesh=mesh, in_specs=(P(('sys', 'aux'), 'orb', None), P(('sys', 'aux'), None), P('sys', None, None)), out_specs=P('sys', 'orb', 'aux'), check_vma=False)
```

```python
import jax
import jax.numpy as jnp
from jax import lax
from jax.experimental import pallas as pl
from jax.experimental.pallas import tpu as pltpu
from jax.sharding import PartitionSpec as P

F32 = jnp.float32
BF = jnp.bfloat16
MESH = pl.DeviceIdType.MESH
NN = (((1,), (0,)), ((), ()))
NT = (((1,), (1,)), ((), ()))
LANES = 128
MROW = 64
NT8 = 7
PIECE = 12
SP = 168


def split3(x):
    hi = x.astype(BF)
    rest = x - hi.astype(F32)
    mid = rest.astype(BF)
    return hi, mid, (rest - mid.astype(F32)).astype(BF)


def dot(x, y, dims):
    return lax.dot_general(x, y, dims, preferred_element_type=F32)


def lhs6(x, axis):
    h, m, l = x
    return jnp.concatenate([h, h, m, m, h, l], axis=axis)


def rhs6(x, axis):
    h, m, l = x
    return jnp.concatenate([h, m, h, m, l, h], axis=axis)


def kernel(nm, nl, nq, nd, ni, bt, mt, ct, out, bv, mv, cv, ctp, tr, sbuf, rbuf, own, mloc, mqr, mq, msp, gsend, grecv, jsend, jrecv, jfwd, zbuf, kacc, kin, kful, kmsg, krecv, gbuf,
           bsem, lsem, tsend, trecv, mzsend, mzrecv, mosend, morecv, gssem, grsem, jssem, jrsem, kxs, kxr, kss, krs):
    sy, a, o = lax.axis_index('sys'), lax.axis_index('aux'), lax.axis_index('orb')
    me = a * 4 + o
    dens, half = me // 2, me % 2
    nh = ni // 2
    npair = nh // 2

    def dev(aa, oo):
        return (sy, aa, oo)

    pltpu.make_async_copy(ct, cv, lsem.at[0]).start()
    pltpu.make_async_copy(bt.at[pl.ds(8 * NT8, 2)], bv.at[pl.ds(8 * NT8, 2)], lsem.at[2]).start()
    for t in range(NT8):
        pltpu.make_async_copy(bt.at[pl.ds(8 * t, 8)], bv.at[pl.ds(8 * t, 8)], bsem.at[t]).start()
        if t == 0:
            pltpu.make_async_copy(mt, mv, lsem.at[1]).start()
    barrier = pltpu.get_barrier_semaphore()

    def tell(k, c):
        g = lax.rem(me + k, 16)
        pl.semaphore_signal(barrier, inc=1, device_id=dev(g // 4, g % 4), device_id_type=MESH)
        return c
    lax.fori_loop(1, 16, tell, 0)

    pltpu.make_async_copy(ct, cv, lsem.at[0]).wait()
    ctp[...] = jnp.concatenate([cv[...], jnp.zeros((nd * ni, 256 - nl), F32)], axis=1)
    lhs = lhs6(split3(ctp[...]), 1)
    pltpu.make_async_copy(mt, mv, lsem.at[1]).wait()
    for b in range(4):
        blk = jnp.concatenate([mv[nq * b:nq * (b + 1), :], jnp.zeros((nq, LANES - nq), F32)], axis=1)
        mloc[b] = jnp.concatenate([blk, jnp.zeros((LANES - nq, LANES), F32)], axis=0)
    pl.semaphore_wait(barrier, 15)

    quarter = pl.ds(pl.multiple_of(o * 32, 32), 32)

    def nearer(x, y, z):
        dx, dy = jnp.abs(x - z), jnp.abs(y - z)
        return jnp.logical_or(dx < dy, jnp.logical_and(dx == dy, x < y))

    def metric_copies(act):
        for k in (2, 1, 3):
            to = lax.rem(a + 4 - k, 4)

            def block(row, slot):
                return pltpu.make_async_remote_copy(src_ref=mloc.at[row, quarter], dst_ref=mqr.at[slot, quarter], send_sem=mzsend,
                                                    recv_sem=mzrecv, device_id=dev(to, o), device_id_type=MESH)
            act(block(a, k - 1))
            for k2 in (1, 2, 3):
                if k2 == k:
                    continue
                b = lax.rem(to + k2, 4)

                @pl.when(nearer(a, b, to))
                def _():
                    act(block(b, k + k2))
    metric_copies(lambda c: c.start())

    gam = jnp.zeros((nd, LANES), F32)
    tr2 = tr

    lane = lax.broadcasted_iota(jnp.int32, (1, LANES), 1)
    data = lane < nq

    def tile(t, gam, tail, first):
        pltpu.make_async_copy(bt.at[pl.ds(0, 8)], bv.at[pl.ds(0, 8)], bsem.at[t]).wait()
        cols = pltpu.roll(ctp[...], lax.rem(512 - (nm * o + 8 * t), 256), 1)
        count = 0
        if tail is not None:
            count = min(8, 10 - first)
            spare = jnp.concatenate([bv[8 * NT8 + tail], jnp.zeros((nl, LANES - nq), F32)], axis=1)
            tcol = pltpu.roll(ctp[...], lax.rem(512 - (nm * o + 8 * NT8 + tail), 256), 1)[:, 0:1]
        for r in range(0, 8, 2):
            xs = []
            for e in range(2):
                x = jnp.concatenate([bv[8 * t + r + e], jnp.zeros((nl, LANES - nq), F32)], axis=1)
                if r + e < count:
                    x = jnp.where(data, x, pltpu.roll(spare, (nq - PIECE * (first + r + e)) % LANES, 1))
                xs.append(x)
            x = jnp.concatenate(xs, axis=1)
            x = jnp.concatenate([x, jnp.zeros((256 - nl, 2 * LANES), F32)], axis=0)
            y = dot(lhs, rhs6(split3(x), 0), NN)
            for e in range(2):
                ye = y[:, e * LANES:(e + 1) * LANES]
                tr2[pl.ds((r + e) * SP, nd * ni), :] = ye
                col = cols[:, r + e:r + e + 1]
                if r + e < count:
                    w = (ye * jnp.where(data, col, tcol)).reshape(ni, nd, LANES).sum(0)
                    moved = pltpu.roll(jnp.where(data, 0.0, w), (PIECE * (first + r + e) - nq) % LANES, 1)
                    gam = gam + jnp.where(data, w, 0.0) + moved
                else:
                    gam = gam + (ye * col).reshape(ni, nd, LANES).sum(0)
        for g in range(16):
            d, h = g // 2, g % 2
            for p in range(npair):
                two = [tr2[pl.ds((h * nh + 2 * p + e) * nd + d, 8, stride=SP), :] for e in range(2)]
                sbuf[g, p, t] = jnp.concatenate(two, axis=0).astype(BF)
        for p in range(npair):
            two = [tr2[pl.ds((half * nh + 2 * p + e) * nd + dens, 8, stride=SP), :] for e in range(2)]
            _, mid, low = split3(jnp.concatenate(two, axis=0))
            own[0, p, t] = mid
            own[1, p, t] = low
        return gam

    def send_t1(p, t0, nt, np=1):
        def one(k, c):
            j, u = k % 4, k // 4
            aa = lax.rem(a + 2 + j, 4)
            oo = lax.rem(o + 1 + u, 4)
            g = aa * 4 + oo
            src = sbuf.at[g, pl.ds(p, np), pl.ds(t0, nt)]
            dst = rbuf.at[a, o, pl.ds(p, np), pl.ds(t0, nt)]

            @pl.when(k != 14)
            def _():
                pltpu.make_async_remote_copy(src_ref=src, dst_ref=dst, send_sem=tsend, recv_sem=trecv.at[p],
                                             device_id=dev(aa, oo), device_id_type=MESH).start()

            @pl.when(k == 14)
            def _():
                pltpu.make_async_copy(src, dst, trecv.at[p]).start()
            return c
        lax.fori_loop(0, 16, one, 0)

    pltpu.make_async_copy(bt.at[pl.ds(0, 2)], bv.at[pl.ds(0, 2)], lsem.at[2]).wait()

    def two_tiles(u, gam):
        gam = tile(2 * u, gam, u, 0)
        return tile(2 * u + 1, gam, u, 8)
    gam = lax.fori_loop(0, 2, two_tiles, gam)
    send_t1(0, 0, 4)

    def one_tile(t, gam):
        return tile(t, gam, None, 0)
    gam = lax.fori_loop(4, NT8, one_tile, gam)
    send_t1(0, 4, 3)

    gsend[...] = gam

    def gs(k, c):
        g = lax.rem(me + k, 16)
        pltpu.make_async_remote_copy(src_ref=gsend, dst_ref=grecv.at[a, o], send_sem=gssem, recv_sem=grsem,
                                     device_id=dev(g // 4, g % 4), device_id_type=MESH).start()
        return c
    lax.fori_loop(1, 16, gs, 0)
    pltpu.make_async_copy(gsend, grecv.at[a, o], grsem).start()

    pltpu.make_async_copy(mqr.at[:, pl.ds(0, 32)], mqr.at[:, pl.ds(0, 32)], mzrecv).wait()

    def mo(k, c):
        oo = lax.rem(o + k, 4)
        pltpu.make_async_remote_copy(src_ref=mqr.at[:, quarter], dst_ref=mqr.at[:, quarter], send_sem=mosend, recv_sem=morecv,
                                     device_id=dev(a, oo), device_id_type=MESH).start()
        return c
    lax.fori_loop(1, 4, mo, 0)
    send_t1(1, 0, NT8, 2)
    mq[a] = mloc[...]
    for k in range(1, 4):
        c1 = lax.rem(a + k, 4)
        mq[c1, a] = mloc[c1].T
    pltpu.make_async_copy(mqr.at[:, pl.ds(0, 96)], mqr.at[:, pl.ds(0, 96)], morecv).wait()
    for k in range(1, 4):
        c1 = lax.rem(a + k, 4)
        mq[c1, c1] = mqr[k - 1]
        for k2 in range(k + 1, 4):
            c2 = lax.rem(a + k2, 4)
            first = jnp.where(nearer(c1, c2, a), c1, c2)
            second = c1 + c2 - first
            blk = mqr[k + k2]
            mq[first, second] = blk
            mq[second, first] = blk.T
    for b in range(4):
        parts = split3(jnp.concatenate([mq[aa, b] for aa in range(4)], axis=1))
        for s in range(3):
            msp[s, pl.ds(b * LANES, LANES)] = parts[s]

    pltpu.make_async_copy(grecv, grecv, grsem).wait()
    graw = jnp.concatenate([grecv[aa, 0] + grecv[aa, 1] + grecv[aa, 2] + grecv[aa, 3] for aa in range(4)], axis=1)
    m3 = [msp[s] for s in range(3)]
    gfit = dot(lhs6(split3(graw), 1), rhs6(m3, 0), NN)
    mown = split3(jnp.concatenate([mloc[b] for b in range(4)], axis=0))
    wts = dot(lhs6(split3(gfit), 1), rhs6(mown, 0), NN)
    wl = lhs6(split3(wts), 1)
    low64 = lax.broadcasted_iota(jnp.int32, (nd, LANES), 1) < 64

    def jpair(u, c):
        ys = []
        for e in range(2):
            x = jnp.concatenate([bv[2 * u + e], jnp.zeros((nl, LANES - nq), F32)], axis=1)
            x = jnp.concatenate([x, jnp.zeros((256 - nl, LANES), F32)], axis=0)
            ys.append(dot(wl, rhs6(split3(x), 1), NT))
        for aa in range(4):
            lo = pltpu.roll(ys[0], (256 - nm * aa) % 256, 1)[:, :LANES]
            hi = pltpu.roll(ys[1], (256 + 64 - nm * aa) % 256, 1)[:, :LANES]
            jsend[aa, u] = jnp.where(low64, lo, hi)
        return c

    row8 = lax.broadcasted_iota(jnp.int32, (8, LANES), 0)
    lane8 = lax.broadcasted_iota(jnp.int32, (8, LANES), 1)
    at0 = lane8 - PIECE * row8
    at1 = lane8 - PIECE * (row8 + 8)
    here0 = jnp.logical_and(at0 >= 0, at0 < PIECE)
    here1 = jnp.logical_and(jnp.logical_and(at1 >= 0, at1 < PIECE), lane8 < nq)
    zbuf[:, NT8] = jnp.zeros((4, 2, 8, 512), F32)

    def tails(x):
        f = [x[t].astype(F32) for t in range(4)]
        out = []
        for e in range(2):
            for u in range(2):
                v0 = pltpu.roll(f[2 * u][8 * e:8 * e + 8], LANES - nq, 1, stride=PIECE, stride_axis=0)
                f1 = f[2 * u + 1][8 * e:8 * e + 8]
                v1 = jnp.where(row8 == 0, pltpu.roll(f1, (8 * PIECE - nq) % LANES, 1), pltpu.roll(f1, (9 * PIECE - nq) % LANES, 1))
                v = jnp.where(here0, v0, jnp.where(here1, v1, 0.0))
                out.append(v.sum(0, keepdims=True))
        return out

    def fit(p):
        if p == 0:
            pltpu.make_async_copy(rbuf.at[:, :, p], rbuf.at[:, :, p], trecv.at[p]).wait()
        elif p % 2 == 1:
            pltpu.make_async_copy(rbuf.at[:, :, pl.ds(p, 2)], rbuf.at[:, :, pl.ds(p, 2)], trecv.at[p]).wait()
        xs = []
        for s in range(4):
            rest = [w for q in range(4) for w in tails(rbuf[s, q, p, pl.ds(0, 4)])]
            xs.append(jnp.concatenate([rbuf[s, :, p].reshape(4 * NT8 * 16, LANES), jnp.concatenate(rest, axis=0).astype(BF)], axis=0))
        x = jnp.concatenate(xs, axis=1)
        z = dot(jnp.concatenate([x, x, x], axis=1), msp[...].reshape(3 * 512, 512), NN)
        main = 4 * NT8 * 16
        zbuf[:, pl.ds(0, NT8)] = z[:main].reshape(4, NT8, 2, 8, 512)
        for q in range(4):
            for e in range(2):
                zbuf[q, NT8, e, pl.ds(0, 2)] = z[main + 4 * q + 2 * e:main + 4 * q + 2 * e + 2]
        ml = []
        for s in range(2):
            rest = tails(own[s, p, pl.ds(0, 4)]) + [jnp.zeros((12, LANES), F32)]
            ml.append(jnp.concatenate([own[s, p].reshape(NT8 * 16, LANES), jnp.concatenate(rest, axis=0).astype(BF)], axis=0))
        mid, low = ml
        rows = pl.ds(pl.multiple_of(a * LANES, LANES), LANES)
        mh, mm = msp[0, rows], msp[1, rows]
        z = dot(jnp.concatenate([mid, mid, low], axis=1), jnp.concatenate([mh, mm, mh], axis=0), NN)
        zbuf[o, pl.ds(0, NT8)] = zbuf[o, pl.ds(0, NT8)] + z[:NT8 * 16].reshape(NT8, 2, 8, 512)
        for e in range(2):
            zbuf[o, NT8, e, pl.ds(0, 2)] = zbuf[o, NT8, e, pl.ds(0, 2)] + z[NT8 * 16 + 2 * e:NT8 * 16 + 2 * e + 2]
        for e in range(2):
            s3 = split3(zbuf[:, :, e].reshape(4 * MROW, 512))
            k = dot(lhs6(s3, 1), rhs6(s3, 1), NT)
            if p == 0 and e == 0:
                kacc[0] = k[:, :LANES]
                kacc[1] = k[:, LANES:]
            else:
                kacc[0] = kacc[0] + k[:, :LANES]
                kacc[1] = kacc[1] + k[:, LANES:]

    lax.fori_loop(0, nm // 2, jpair, 0)
    near, far = a + 1 - 2 * (a % 2), lax.rem(a + 2, 4)
    hops = []
    for e, aa in enumerate((lax.rem(near + 2, 4), near)):
        hops.append(pltpu.make_async_remote_copy(src_ref=jsend.at[aa], dst_ref=jrecv.at[e], send_sem=jssem.at[e], recv_sem=jrsem.at[e],
                                                 device_id=dev(near, o), device_id_type=MESH))
        hops[-1].start()
    send_t1(3, 0, NT8, 2)
    fit(0)
    fit(1)
    hops[0].wait_recv()
    jfwd[...] = jsend[far] + jrecv[0]
    cross = pltpu.make_async_remote_copy(src_ref=jfwd, dst_ref=jrecv.at[2], send_sem=jssem.at[2], recv_sem=jrsem.at[2],
                                         device_id=dev(far, o), device_id_type=MESH)
    cross.start()
    for p in range(2, npair):
        fit(p)

    mate = o + 1 - 2 * half
    swap = pltpu.make_async_remote_copy(src_ref=kacc.at[1 - half], dst_ref=kin, send_sem=kxs, recv_sem=kxr,
                                        device_id=dev(a, mate), device_id_type=MESH)
    swap.start()
    swap.wait_recv()
    kful[...] = kacc[half] + kin[...]
    low32 = lax.broadcasted_iota(jnp.int32, (32, LANES), 1) < 64
    for oo in range(4):
        ev = kful[pl.ds(MROW * oo, 32, stride=2), :]
        od = kful[pl.ds(MROW * oo + 1, 32, stride=2), :]
        kmsg[0, oo] = jnp.where(low32, ev, pltpu.roll(od, 64, 1))
        kmsg[1, oo] = jnp.where(low32, pltpu.roll(ev, 64, 1), od)

    def ks(k, c):
        al, oo = k // 4, k % 4
        aa = 2 * half + al
        same = jnp.logical_and(aa == a, oo == o)

        @pl.when(jnp.logical_not(same))
        def _():
            pltpu.make_async_remote_copy(src_ref=kmsg.at[al, oo], dst_ref=krecv.at[pl.ds(dens * 32, 32)], send_sem=kss, recv_sem=krs,
                                         device_id=dev(aa, oo), device_id_type=MESH).start()

        @pl.when(same)
        def _():
            cp = pltpu.make_async_copy(kmsg.at[al, oo], krecv.at[pl.ds(dens * 32, 32)], krs)
            cp.start()
        return c
    lax.fori_loop(0, 8, ks, 0)

    hops[1].wait_recv()
    cross.wait_recv()
    pltpu.make_async_copy(krecv, krecv, krs).wait()
    for u in range(nm // 2):
        j = jsend[a, u] + jrecv[1, u] + jrecv[2, u]
        g = 2.0 * j - krecv[pl.ds(u, nd, stride=32), :]
        out[2 * u] = g[:, :nm]
        out[2 * u + 1] = pltpu.roll(g, 64, 1)[:, :nm]

    pltpu.make_async_copy(sbuf.at[pl.ds(0, 15)], sbuf.at[pl.ds(0, 15)], tsend).wait()
    metric_copies(lambda c: c.wait_send())
    pltpu.make_async_copy(mqr.at[:, pl.ds(0, 96)], mqr.at[:, pl.ds(0, 96)], mosend).wait()
    pltpu.make_async_copy(gbuf, gbuf, gssem).wait()
    for c in hops + [cross]:
        c.wait_send()
    swap.wait_send()
    inset = (a // 2) == half

    @pl.when(inset)
    def _():
        pltpu.make_async_copy(krecv.at[pl.ds(0, 224)], krecv.at[pl.ds(0, 224)], kss).wait()

    @pl.when(jnp.logical_not(inset))
    def _():
        pltpu.make_async_copy(krecv, krecv, kss).wait()


def solution(mesh):
    def local_fock(ints_blk, metric_blk, orbitals):
        nq, nm, nl = ints_blk.shape
        nd, _, ni = orbitals.shape
        bt = jnp.transpose(ints_blk, (1, 2, 0))
        mt = metric_blk.T
        ct = jnp.transpose(orbitals, (2, 0, 1)).reshape(ni * nd, nl)
        npair = ni // 4
        V = pltpu.VMEM
        dma = pltpu.SemaphoreType.DMA
        g = pl.pallas_call(
            lambda *refs: kernel(nm, nl, nq, nd, ni, *refs),
            out_shape=jax.ShapeDtypeStruct((nm, nd, nm), F32),
            in_specs=[pl.BlockSpec(memory_space=pl.ANY)] * 3,
            out_specs=pl.BlockSpec(memory_space=pltpu.VMEM),
            scratch_shapes=[
                V((nm, nl, nq), F32), V((4 * nq, nq), F32), V((ni * nd, nl), F32), V((ni * nd, 256), F32),
                V((8 * SP, LANES), F32), V((16, npair, NT8, 16, LANES), BF), V((4, 4, npair, NT8, 16, LANES), BF),
                V((2, npair, NT8, 16, LANES), BF), V((4, LANES, LANES), F32), V((6, LANES, LANES), F32), V((4, 4, LANES, LANES), F32), V((3, 512, 512), BF),
                V((nd, LANES), F32), V((4, 4, nd, LANES), F32), V((4, nm // 2, nd, LANES), F32), V((3, nm // 2, nd, LANES), F32), V((nm // 2, nd, LANES), F32),
                V((4, 8, 2, 8, 512), F32), V((2, 256, LANES), F32), V((256, LANES), F32), V((256, LANES), F32), V((2, 4, 32, LANES), F32),
                V((8 * 32, LANES), F32), V((15, nd, LANES), F32),
                dma((NT8,)), dma((3,)), dma, dma((npair,)), dma, dma, dma, dma, dma, dma, dma((3,)), dma((3,)), dma, dma, dma, dma],
            compiler_params=pltpu.CompilerParams(collective_id=0, has_side_effects=True, vmem_limit_bytes=60 * 2**20),
        )(bt, mt, ct)
        return jnp.transpose(g, (1, 0, 2))

    return jax.shard_map(local_fock, mesh=mesh, in_specs=(P(('sys', 'aux'), 'orb', None), P(('sys', 'aux'), None), P('sys', None, None)), out_specs=P('sys', 'orb', 'aux'), check_vma=False)
```

```python
import jax
import jax.numpy as jnp
from jax import lax
from jax.experimental import pallas as pl
from jax.experimental.pallas import tpu as pltpu
from jax.sharding import PartitionSpec as P

F32 = jnp.float32
BF = jnp.bfloat16
MESH = pl.DeviceIdType.MESH
NN = (((1,), (0,)), ((), ()))
NT = (((1,), (1,)), ((), ()))
LANES = 128
MROW = 64
NT8 = 7
PIECE = 12
SP = 168


def split3(x):
    hi = x.astype(BF)
    rest = x - hi.astype(F32)
    mid = rest.astype(BF)
    return hi, mid, (rest - mid.astype(F32)).astype(BF)


def dot(x, y, dims):
    return lax.dot_general(x, y, dims, preferred_element_type=F32)


def lhs6(x, axis):
    h, m, l = x
    return jnp.concatenate([h, h, m, m, h, l], axis=axis)


def rhs6(x, axis):
    h, m, l = x
    return jnp.concatenate([h, m, h, m, l, h], axis=axis)


def kernel(nm, nl, nq, nd, ni, bt, mt, ct, out, bv, mv, cv, ctp, tr, sbuf, rbuf, own, mloc, mqr, mq, msp, gsend, grecv, jsend, jrecv, jfwd, zbuf, kacc, kin, kful, kmsg, krecv, gbuf,
           bsem, lsem, tsend, trecv, mzsend, mzrecv, mosend, morecv, gssem, grsem, jssem, jrsem, kxs, kxr, kss, krs):
    sy, a, o = lax.axis_index('sys'), lax.axis_index('aux'), lax.axis_index('orb')
    me = a * 4 + o
    dens, half = me // 2, me % 2
    nh = ni // 2
    npair = nh // 2

    def dev(aa, oo):
        return (sy, aa, oo)

    pltpu.make_async_copy(ct, cv, lsem.at[0]).start()
    pltpu.make_async_copy(bt.at[pl.ds(8 * NT8, 2)], bv.at[pl.ds(8 * NT8, 2)], lsem.at[2]).start()
    for t in range(NT8):
        pltpu.make_async_copy(bt.at[pl.ds(8 * t, 8)], bv.at[pl.ds(8 * t, 8)], bsem.at[t]).start()
        if t == 0:
            pltpu.make_async_copy(mt, mv, lsem.at[1]).start()
    barrier = pltpu.get_barrier_semaphore()

    def tell(k, c):
        g = lax.rem(me + k, 16)
        pl.semaphore_signal(barrier, inc=1, device_id=dev(g // 4, g % 4), device_id_type=MESH)
        return c
    lax.fori_loop(1, 16, tell, 0)

    pltpu.make_async_copy(ct, cv, lsem.at[0]).wait()
    ctp[...] = jnp.concatenate([cv[...], jnp.zeros((nd * ni, 256 - nl), F32)], axis=1)
    lhs = lhs6(split3(ctp[...]), 1)
    pltpu.make_async_copy(mt, mv, lsem.at[1]).wait()
    for b in range(4):
        blk = jnp.concatenate([mv[nq * b:nq * (b + 1), :], jnp.zeros((nq, LANES - nq), F32)], axis=1)
        mloc[b] = jnp.concatenate([blk, jnp.zeros((LANES - nq, LANES), F32)], axis=0)
    pl.semaphore_wait(barrier, 15)

    quarter = pl.ds(pl.multiple_of(o * 32, 32), 32)

    def nearer(x, y, z):
        dx, dy = jnp.abs(x - z), jnp.abs(y - z)
        return jnp.logical_or(dx < dy, jnp.logical_and(dx == dy, x < y))

    def metric_copies(act):
        for k in (2, 1, 3):
            to = lax.rem(a + 4 - k, 4)

            def block(row, slot):
                return pltpu.make_async_remote_copy(src_ref=mloc.at[row, quarter], dst_ref=mqr.at[slot, quarter], send_sem=mzsend,
                                                    recv_sem=mzrecv, device_id=dev(to, o), device_id_type=MESH)
            act(block(a, k - 1))
            for k2 in (1, 2, 3):
                if k2 == k:
                    continue
                b = lax.rem(to + k2, 4)

                @pl.when(nearer(a, b, to))
                def _():
                    act(block(b, k + k2))
    metric_copies(lambda c: c.start())

    gam = jnp.zeros((nd, LANES), F32)
    tr2 = tr

    lane = lax.broadcasted_iota(jnp.int32, (1, LANES), 1)
    data = lane < nq

    def tile(t, gam, tail, first):
        pltpu.make_async_copy(bt.at[pl.ds(0, 8)], bv.at[pl.ds(0, 8)], bsem.at[t]).wait()
        cols = pltpu.roll(ctp[...], lax.rem(512 - (nm * o + 8 * t), 256), 1)
        count = 0
        if tail is not None:
            count = min(8, 10 - first)
            spare = jnp.concatenate([bv[8 * NT8 + tail], jnp.zeros((nl, LANES - nq), F32)], axis=1)
            tcol = pltpu.roll(ctp[...], lax.rem(512 - (nm * o + 8 * NT8 + tail), 256), 1)[:, 0:1]
        for r in range(0, 8, 2):
            xs = []
            for e in range(2):
                x = jnp.concatenate([bv[8 * t + r + e], jnp.zeros((nl, LANES - nq), F32)], axis=1)
                if r + e < count:
                    x = jnp.where(data, x, pltpu.roll(spare, (nq - PIECE * (first + r + e)) % LANES, 1))
                xs.append(x)
            x = jnp.concatenate(xs, axis=1)
            x = jnp.concatenate([x, jnp.zeros((256 - nl, 2 * LANES), F32)], axis=0)
            y = dot(lhs, rhs6(split3(x), 0), NN)
            for e in range(2):
                ye = y[:, e * LANES:(e + 1) * LANES]
                tr2[pl.ds((r + e) * SP, nd * ni), :] = ye
                col = cols[:, r + e:r + e + 1]
                if r + e < count:
                    w = (ye * jnp.where(data, col, tcol)).reshape(ni, nd, LANES).sum(0)
                    moved = pltpu.roll(jnp.where(data, 0.0, w), (PIECE * (first + r + e) - nq) % LANES, 1)
                    gam = gam + jnp.where(data, w, 0.0) + moved
                else:
                    gam = gam + (ye * col).reshape(ni, nd, LANES).sum(0)
        for g in range(16):
            d, h = g // 2, g % 2
            for p in range(npair):
                two = [tr2[pl.ds((h * nh + 2 * p + e) * nd + d, 8, stride=SP), :] for e in range(2)]
                sbuf[g, p, t] = jnp.concatenate(two, axis=0).astype(BF)
        for p in range(npair):
            two = [tr2[pl.ds((half * nh + 2 * p + e) * nd + dens, 8, stride=SP), :] for e in range(2)]
            _, mid, low = split3(jnp.concatenate(two, axis=0))
            own[0, p, t] = mid
            own[1, p, t] = low
        return gam

    def send_t1(p, t0, nt):
        def one(k, c):
            j, u = k % 4, k // 4
            aa = lax.rem(a + 2 + j, 4)
            oo = lax.rem(o + 1 + u, 4)
            g = aa * 4 + oo
            src = sbuf.at[g, p, pl.ds(t0, nt)]
            dst = rbuf.at[a, p, o, pl.ds(t0, nt)]

            @pl.when(k != 14)
            def _():
                pltpu.make_async_remote_copy(src_ref=src, dst_ref=dst, send_sem=tsend, recv_sem=trecv.at[p],
                                             device_id=dev(aa, oo), device_id_type=MESH).start()

            @pl.when(k == 14)
            def _():
                pltpu.make_async_copy(src, dst, trecv.at[p]).start()
            return c
        lax.fori_loop(0, 16, one, 0)

    pltpu.make_async_copy(bt.at[pl.ds(0, 2)], bv.at[pl.ds(0, 2)], lsem.at[2]).wait()

    def two_tiles(u, gam):
        gam = tile(2 * u, gam, u, 0)
        send_t1(0, 2 * u, 1)
        gam = tile(2 * u + 1, gam, u, 8)
        send_t1(0, 2 * u + 1, 1)
        return gam
    gam = lax.fori_loop(0, 2, two_tiles, gam)

    def one_tile(t, gam):
        gam = tile(t, gam, None, 0)
        send_t1(0, t, 1)
        return gam
    gam = lax.fori_loop(4, NT8, one_tile, gam)

    gsend[...] = gam

    def gs(k, c):
        g = lax.rem(me + k, 16)
        pltpu.make_async_remote_copy(src_ref=gsend, dst_ref=grecv.at[a, o], send_sem=gssem, recv_sem=grsem,
                                     device_id=dev(g // 4, g % 4), device_id_type=MESH).start()
        return c
    lax.fori_loop(1, 16, gs, 0)
    pltpu.make_async_copy(gsend, grecv.at[a, o], grsem).start()

    pltpu.make_async_copy(mqr.at[:, pl.ds(0, 32)], mqr.at[:, pl.ds(0, 32)], mzrecv).wait()

    def mo(k, c):
        oo = lax.rem(o + k, 4)
        pltpu.make_async_remote_copy(src_ref=mqr.at[:, quarter], dst_ref=mqr.at[:, quarter], send_sem=mosend, recv_sem=morecv,
                                     device_id=dev(a, oo), device_id_type=MESH).start()
        return c
    lax.fori_loop(1, 4, mo, 0)
    for p in range(1, 3):
        send_t1(p, 0, NT8)
    mq[a] = mloc[...]
    for k in range(1, 4):
        c1 = lax.rem(a + k, 4)
        mq[c1, a] = mloc[c1].T
    pltpu.make_async_copy(mqr.at[:, pl.ds(0, 96)], mqr.at[:, pl.ds(0, 96)], morecv).wait()
    for k in range(1, 4):
        c1 = lax.rem(a + k, 4)
        mq[c1, c1] = mqr[k - 1]
        for k2 in range(k + 1, 4):
            c2 = lax.rem(a + k2, 4)
            first = jnp.where(nearer(c1, c2, a), c1, c2)
            second = c1 + c2 - first
            blk = mqr[k + k2]
            mq[first, second] = blk
            mq[second, first] = blk.T
    for b in range(4):
        parts = split3(jnp.concatenate([mq[aa, b] for aa in range(4)], axis=1))
        for s in range(3):
            msp[s, pl.ds(b * LANES, LANES)] = parts[s]

    pltpu.make_async_copy(grecv, grecv, grsem).wait()
    graw = jnp.concatenate([grecv[aa, 0] + grecv[aa, 1] + grecv[aa, 2] + grecv[aa, 3] for aa in range(4)], axis=1)
    m3 = [msp[s] for s in range(3)]
    gfit = dot(lhs6(split3(graw), 1), rhs6(m3, 0), NN)
    mown = split3(jnp.concatenate([mloc[b] for b in range(4)], axis=0))
    wts = dot(lhs6(split3(gfit), 1), rhs6(mown, 0), NN)
    wl = lhs6(split3(wts), 1)
    low64 = lax.broadcasted_iota(jnp.int32, (nd, LANES), 1) < 64

    def jpair(u, c):
        ys = []
        for e in range(2):
            x = jnp.concatenate([bv[2 * u + e], jnp.zeros((nl, LANES - nq), F32)], axis=1)
            x = jnp.concatenate([x, jnp.zeros((256 - nl, LANES), F32)], axis=0)
            ys.append(dot(wl, rhs6(split3(x), 1), NT))
        for aa in range(4):
            lo = pltpu.roll(ys[0], (256 - nm * aa) % 256, 1)[:, :LANES]
            hi = pltpu.roll(ys[1], (256 + 64 - nm * aa) % 256, 1)[:, :LANES]
            jsend[aa, u] = jnp.where(low64, lo, hi)
        return c

    row8 = lax.broadcasted_iota(jnp.int32, (8, LANES), 0)
    lane8 = lax.broadcasted_iota(jnp.int32, (8, LANES), 1)
    at0 = lane8 - PIECE * row8
    at1 = lane8 - PIECE * (row8 + 8)
    here0 = jnp.logical_and(at0 >= 0, at0 < PIECE)
    here1 = jnp.logical_and(jnp.logical_and(at1 >= 0, at1 < PIECE), lane8 < nq)
    zbuf[:, NT8] = jnp.zeros((4, 2, 8, 512), F32)

    def tails(x):
        f = [x[t].astype(F32) for t in range(4)]
        out = []
        for e in range(2):
            for u in range(2):
                v0 = pltpu.roll(f[2 * u][8 * e:8 * e + 8], LANES - nq, 1, stride=PIECE, stride_axis=0)
                f1 = f[2 * u + 1][8 * e:8 * e + 8]
                v1 = jnp.where(row8 == 0, pltpu.roll(f1, (8 * PIECE - nq) % LANES, 1), pltpu.roll(f1, (9 * PIECE - nq) % LANES, 1))
                v = jnp.where(here0, v0, jnp.where(here1, v1, 0.0))
                out.append(v.sum(0, keepdims=True))
        return out

    def fit(p):
        pltpu.make_async_copy(rbuf.at[:, p], rbuf.at[:, p], trecv.at[p]).wait()
        xs = []
        for s in range(4):
            rest = [w for q in range(4) for w in tails(rbuf[s, p, q, pl.ds(0, 4)])]
            xs.append(jnp.concatenate([rbuf[s, p].reshape(4 * NT8 * 16, LANES), jnp.concatenate(rest, axis=0).astype(BF)], axis=0))
        x = jnp.concatenate(xs, axis=1)
        z = dot(jnp.concatenate([x, x, x], axis=1), msp[...].reshape(3 * 512, 512), NN)
        main = 4 * NT8 * 16
        zbuf[:, pl.ds(0, NT8)] = z[:main].reshape(4, NT8, 2, 8, 512)
        for q in range(4):
            for e in range(2):
                zbuf[q, NT8, e, pl.ds(0, 2)] = z[main + 4 * q + 2 * e:main + 4 * q + 2 * e + 2]
        ml = []
        for s in range(2):
            rest = tails(own[s, p, pl.ds(0, 4)]) + [jnp.zeros((12, LANES), F32)]
            ml.append(jnp.concatenate([own[s, p].reshape(NT8 * 16, LANES), jnp.concatenate(rest, axis=0).astype(BF)], axis=0))
        mid, low = ml
        rows = pl.ds(pl.multiple_of(a * LANES, LANES), LANES)
        mh, mm = msp[0, rows], msp[1, rows]
        z = dot(jnp.concatenate([mid, mid, low], axis=1), jnp.concatenate([mh, mm, mh], axis=0), NN)
        zbuf[o, pl.ds(0, NT8)] = zbuf[o, pl.ds(0, NT8)] + z[:NT8 * 16].reshape(NT8, 2, 8, 512)
        for e in range(2):
            zbuf[o, NT8, e, pl.ds(0, 2)] = zbuf[o, NT8, e, pl.ds(0, 2)] + z[NT8 * 16 + 2 * e:NT8 * 16 + 2 * e + 2]
        for e in range(2):
            s3 = split3(zbuf[:, :, e].reshape(4 * MROW, 512))
            k = dot(lhs6(s3, 1), rhs6(s3, 1), NT)
            if p == 0 and e == 0:
                kacc[0] = k[:, :LANES]
                kacc[1] = k[:, LANES:]
            else:
                kacc[0] = kacc[0] + k[:, :LANES]
                kacc[1] = kacc[1] + k[:, LANES:]

    lax.fori_loop(0, nm // 2, jpair, 0)
    near, far = a + 1 - 2 * (a % 2), lax.rem(a + 2, 4)
    hops = []
    for e, aa in enumerate((lax.rem(near + 2, 4), near)):
        hops.append(pltpu.make_async_remote_copy(src_ref=jsend.at[aa], dst_ref=jrecv.at[e], send_sem=jssem.at[e], recv_sem=jrsem.at[e],
                                                 device_id=dev(near, o), device_id_type=MESH))
        hops[-1].start()
    for p in range(3, npair):
        send_t1(p, 0, NT8)
    for p in range(npair - 1):
        fit(p)
    hops[0].wait_recv()
    jfwd[...] = jsend[far] + jrecv[0]
    cross = pltpu.make_async_remote_copy(src_ref=jfwd, dst_ref=jrecv.at[2], send_sem=jssem.at[2], recv_sem=jrsem.at[2],
                                         device_id=dev(far, o), device_id_type=MESH)
    cross.start()
    fit(npair - 1)

    mate = o + 1 - 2 * half
    swap = pltpu.make_async_remote_copy(src_ref=kacc.at[1 - half], dst_ref=kin, send_sem=kxs, recv_sem=kxr,
                                        device_id=dev(a, mate), device_id_type=MESH)
    swap.start()
    swap.wait_recv()
    kful[...] = kacc[half] + kin[...]
    low32 = lax.broadcasted_iota(jnp.int32, (32, LANES), 1) < 64
    for oo in range(4):
        ev = kful[pl.ds(MROW * oo, 32, stride=2), :]
        od = kful[pl.ds(MROW * oo + 1, 32, stride=2), :]
        kmsg[0, oo] = jnp.where(low32, ev, pltpu.roll(od, 64, 1))
        kmsg[1, oo] = jnp.where(low32, pltpu.roll(ev, 64, 1), od)

    def ks(k, c):
        al, oo = k // 4, k % 4
        aa = 2 * half + al
        same = jnp.logical_and(aa == a, oo == o)

        @pl.when(jnp.logical_not(same))
        def _():
            pltpu.make_async_remote_copy(src_ref=kmsg.at[al, oo], dst_ref=krecv.at[pl.ds(dens * 32, 32)], send_sem=kss, recv_sem=krs,
                                         device_id=dev(aa, oo), device_id_type=MESH).start()

        @pl.when(same)
        def _():
            cp = pltpu.make_async_copy(kmsg.at[al, oo], krecv.at[pl.ds(dens * 32, 32)], krs)
            cp.start()
        return c
    lax.fori_loop(0, 8, ks, 0)

    hops[1].wait_recv()
    cross.wait_recv()
    pltpu.make_async_copy(krecv, krecv, krs).wait()
    for u in range(nm // 2):
        j = jsend[a, u] + jrecv[1, u] + jrecv[2, u]
        g = 2.0 * j - krecv[pl.ds(u, nd, stride=32), :]
        out[2 * u] = g[:, :nm]
        out[2 * u + 1] = pltpu.roll(g, 64, 1)[:, :nm]

    pltpu.make_async_copy(sbuf.at[pl.ds(0, 15)], sbuf.at[pl.ds(0, 15)], tsend).wait()
    metric_copies(lambda c: c.wait_send())
    pltpu.make_async_copy(mqr.at[:, pl.ds(0, 96)], mqr.at[:, pl.ds(0, 96)], mosend).wait()
    pltpu.make_async_copy(gbuf, gbuf, gssem).wait()
    for c in hops + [cross]:
        c.wait_send()
    swap.wait_send()
    inset = (a // 2) == half

    @pl.when(inset)
    def _():
        pltpu.make_async_copy(krecv.at[pl.ds(0, 224)], krecv.at[pl.ds(0, 224)], kss).wait()

    @pl.when(jnp.logical_not(inset))
    def _():
        pltpu.make_async_copy(krecv, krecv, kss).wait()


def solution(mesh):
    def local_fock(ints_blk, metric_blk, orbitals):
        nq, nm, nl = ints_blk.shape
        nd, _, ni = orbitals.shape
        bt = jnp.transpose(ints_blk, (1, 2, 0))
        mt = metric_blk.T
        ct = jnp.transpose(orbitals, (2, 0, 1)).reshape(ni * nd, nl)
        npair = ni // 4
        V = pltpu.VMEM
        dma = pltpu.SemaphoreType.DMA
        g = pl.pallas_call(
            lambda *refs: kernel(nm, nl, nq, nd, ni, *refs),
            out_shape=jax.ShapeDtypeStruct((nm, nd, nm), F32),
            in_specs=[pl.BlockSpec(memory_space=pl.ANY)] * 3,
            out_specs=pl.BlockSpec(memory_space=pltpu.VMEM),
            scratch_shapes=[
                V((nm, nl, nq), F32), V((4 * nq, nq), F32), V((ni * nd, nl), F32), V((ni * nd, 256), F32),
                V((8 * SP, LANES), F32), V((16, npair, NT8, 16, LANES), BF), V((4, npair, 4, NT8, 16, LANES), BF),
                V((2, npair, NT8, 16, LANES), BF), V((4, LANES, LANES), F32), V((6, LANES, LANES), F32), V((4, 4, LANES, LANES), F32), V((3, 512, 512), BF),
                V((nd, LANES), F32), V((4, 4, nd, LANES), F32), V((4, nm // 2, nd, LANES), F32), V((3, nm // 2, nd, LANES), F32), V((nm // 2, nd, LANES), F32),
                V((4, 8, 2, 8, 512), F32), V((2, 256, LANES), F32), V((256, LANES), F32), V((256, LANES), F32), V((2, 4, 32, LANES), F32),
                V((8 * 32, LANES), F32), V((15, nd, LANES), F32),
                dma((NT8,)), dma((3,)), dma, dma((npair,)), dma, dma, dma, dma, dma, dma, dma((3,)), dma((3,)), dma, dma, dma, dma],
            compiler_params=pltpu.CompilerParams(collective_id=0, has_side_effects=True, vmem_limit_bytes=60 * 2**20),
        )(bt, mt, ct)
        return jnp.transpose(g, (1, 0, 2))

    return jax.shard_map(local_fock, mesh=mesh, in_specs=(P(('sys', 'aux'), 'orb', None), P(('sys', 'aux'), None), P('sys', None, None)), out_specs=P('sys', 'orb', 'aux'), check_vma=False)
```

```python
import jax
import jax.numpy as jnp
from jax import lax
from jax.experimental import pallas as pl
from jax.experimental.pallas import tpu as pltpu
from jax.sharding import PartitionSpec as P

F32 = jnp.float32
BF = jnp.bfloat16
MESH = pl.DeviceIdType.MESH
NN = (((1,), (0,)), ((), ()))
NT = (((1,), (1,)), ((), ()))
LANES = 128
MROW = 64
NT8 = 7
PIECE = 12
SP = 168


def split3(x):
    hi = x.astype(BF)
    rest = x - hi.astype(F32)
    mid = rest.astype(BF)
    return hi, mid, (rest - mid.astype(F32)).astype(BF)


def dot(x, y, dims):
    return lax.dot_general(x, y, dims, preferred_element_type=F32)


def lhs6(x, axis):
    h, m, l = x
    return jnp.concatenate([h, h, m, m, h, l], axis=axis)


def rhs6(x, axis):
    h, m, l = x
    return jnp.concatenate([h, m, h, m, l, h], axis=axis)


def kernel(nm, nl, nq, nd, ni, bt, mt, ct, out, bv, mv, cv, ctp, tr, sbuf, rbuf, own, mloc, mqr, mq, msp, gsend, grecv, jsend, jrecv, jfwd, zbuf, kacc, kin, kful, kmsg, krecv, gbuf,
           bsem, lsem, tsend, trecv, mzsend, mzrecv, mosend, morecv, gssem, grsem, jssem, jrsem, kxs, kxr, kss, krs):
    sy, a, o = lax.axis_index('sys'), lax.axis_index('aux'), lax.axis_index('orb')
    me = a * 4 + o
    dens, half = me // 2, me % 2
    nh = ni // 2
    npair = nh // 2

    def dev(aa, oo):
        return (sy, aa, oo)

    pltpu.make_async_copy(ct, cv, lsem.at[0]).start()
    pltpu.make_async_copy(bt.at[pl.ds(8 * NT8, 2)], bv.at[pl.ds(8 * NT8, 2)], lsem.at[2]).start()
    for t in range(NT8):
        pltpu.make_async_copy(bt.at[pl.ds(8 * t, 8)], bv.at[pl.ds(8 * t, 8)], bsem.at[t]).start()
        if t == 0:
            pltpu.make_async_copy(mt, mv, lsem.at[1]).start()
    barrier = pltpu.get_barrier_semaphore()

    def tell(k, c):
        g = lax.rem(me + k, 16)
        pl.semaphore_signal(barrier, inc=1, device_id=dev(g // 4, g % 4), device_id_type=MESH)
        return c
    lax.fori_loop(1, 16, tell, 0)

    pltpu.make_async_copy(ct, cv, lsem.at[0]).wait()
    ctp[...] = jnp.concatenate([cv[...], jnp.zeros((nd * ni, 256 - nl), F32)], axis=1)
    lhs = lhs6(split3(ctp[...]), 1)
    pltpu.make_async_copy(mt, mv, lsem.at[1]).wait()
    for b in range(4):
        blk = jnp.concatenate([mv[nq * b:nq * (b + 1), :], jnp.zeros((nq, LANES - nq), F32)], axis=1)
        mloc[b] = jnp.concatenate([blk, jnp.zeros((LANES - nq, LANES), F32)], axis=0)
    pl.semaphore_wait(barrier, 15)

    quarter = pl.ds(pl.multiple_of(o * 32, 32), 32)

    def nearer(x, y, z):
        dx, dy = jnp.abs(x - z), jnp.abs(y - z)
        return jnp.logical_or(dx < dy, jnp.logical_and(dx == dy, x < y))

    def metric_copies(act):
        for k in (2, 1, 3):
            to = lax.rem(a + 4 - k, 4)

            def block(row, slot):
                return pltpu.make_async_remote_copy(src_ref=mloc.at[row, quarter], dst_ref=mqr.at[slot, quarter], send_sem=mzsend,
                                                    recv_sem=mzrecv, device_id=dev(to, o), device_id_type=MESH)
            act(block(a, k - 1))
            for k2 in (1, 2, 3):
                if k2 == k:
                    continue
                b = lax.rem(to + k2, 4)

                @pl.when(nearer(a, b, to))
                def _():
                    act(block(b, k + k2))
    metric_copies(lambda c: c.start())

    gam = jnp.zeros((nd, LANES), F32)
    tr2 = tr

    lane = lax.broadcasted_iota(jnp.int32, (1, LANES), 1)
    data = lane < nq

    def tile(t, gam, tail, first):
        pltpu.make_async_copy(bt.at[pl.ds(0, 8)], bv.at[pl.ds(0, 8)], bsem.at[t]).wait()
        cols = pltpu.roll(ctp[...], lax.rem(512 - (nm * o + 8 * t), 256), 1)
        count = 0
        if tail is not None:
            count = min(8, 10 - first)
            spare = jnp.concatenate([bv[8 * NT8 + tail], jnp.zeros((nl, LANES - nq), F32)], axis=1)
            tcol = pltpu.roll(ctp[...], lax.rem(512 - (nm * o + 8 * NT8 + tail), 256), 1)[:, 0:1]
        for r in range(0, 8, 2):
            xs = []
            for e in range(2):
                x = jnp.concatenate([bv[8 * t + r + e], jnp.zeros((nl, LANES - nq), F32)], axis=1)
                if r + e < count:
                    x = jnp.where(data, x, pltpu.roll(spare, (nq - PIECE * (first + r + e)) % LANES, 1))
                xs.append(x)
            x = jnp.concatenate(xs, axis=1)
            x = jnp.concatenate([x, jnp.zeros((256 - nl, 2 * LANES), F32)], axis=0)
            y = dot(lhs, rhs6(split3(x), 0), NN)
            for e in range(2):
                ye = y[:, e * LANES:(e + 1) * LANES]
                tr2[pl.ds((r + e) * SP, nd * ni), :] = ye
                col = cols[:, r + e:r + e + 1]
                if r + e < count:
                    w = (ye * jnp.where(data, col, tcol)).reshape(ni, nd, LANES).sum(0)
                    moved = pltpu.roll(jnp.where(data, 0.0, w), (PIECE * (first + r + e) - nq) % LANES, 1)
                    gam = gam + jnp.where(data, w, 0.0) + moved
                else:
                    gam = gam + (ye * col).reshape(ni, nd, LANES).sum(0)
        for g in range(16):
            d, h = g // 2, g % 2
            for p in range(npair):
                two = [tr2[pl.ds((h * nh + 2 * p + e) * nd + d, 8, stride=SP), :] for e in range(2)]
                sbuf[g, p, t] = jnp.concatenate(two, axis=0).astype(BF)
        for p in range(npair):
            two = [tr2[pl.ds((half * nh + 2 * p + e) * nd + dens, 8, stride=SP), :] for e in range(2)]
            _, mid, low = split3(jnp.concatenate(two, axis=0))
            own[0, p, t] = mid
            own[1, p, t] = low
        return gam

    def send_t1(p, t0, nt):
        def one(k, c):
            j, u = k % 4, k // 4
            aa = lax.rem(a + 2 + j, 4)
            oo = lax.rem(o + 1 + u, 4)
            g = aa * 4 + oo
            src = sbuf.at[g, p, pl.ds(t0, nt)]
            dst = rbuf.at[a, p, o, pl.ds(t0, nt)]

            @pl.when(k != 14)
            def _():
                pltpu.make_async_remote_copy(src_ref=src, dst_ref=dst, send_sem=tsend, recv_sem=trecv.at[p],
                                             device_id=dev(aa, oo), device_id_type=MESH).start()

            @pl.when(k == 14)
            def _():
                pltpu.make_async_copy(src, dst, trecv.at[p]).start()
            return c
        lax.fori_loop(0, 16, one, 0)

    outer = jnp.logical_or(a == 0, a == 3)
    pair = a + 1 - 2 * (a % 2)

    def send_half(p, t0, nt, cross):
        def one(k, c):
            if cross:
                aa = jnp.where(k % 2 == 0, 3 - a, 3 - pair)
                oo = lax.rem(o + 1 + k // 2, 4)
            else:
                aa = jnp.where(k % 2 == 0, pair, a)
                oo = lax.rem(o + 1 + k // 2, 4)
            g = aa * 4 + oo
            src = sbuf.at[g, p, pl.ds(t0, nt)]
            dst = rbuf.at[a, p, o, pl.ds(t0, nt)]

            def far():
                pltpu.make_async_remote_copy(src_ref=src, dst_ref=dst, send_sem=tsend, recv_sem=trecv.at[p],
                                             device_id=dev(aa, oo), device_id_type=MESH).start()
            if cross:
                far()
            else:
                pl.when(k != 7)(far)

                @pl.when(k == 7)
                def _():
                    pltpu.make_async_copy(src, dst, trecv.at[p]).start()
            return c
        lax.fori_loop(0, 8, one, 0)

    pltpu.make_async_copy(bt.at[pl.ds(0, 2)], bv.at[pl.ds(0, 2)], lsem.at[2]).wait()

    def two_tiles(u, gam):
        gam = tile(2 * u, gam, u, 0)
        send_t1(0, 2 * u, 1)
        gam = tile(2 * u + 1, gam, u, 8)
        send_t1(0, 2 * u + 1, 1)
        return gam
    gam = lax.fori_loop(0, 2, two_tiles, gam)

    def one_tile(t, gam):
        gam = tile(t, gam, None, 0)
        send_t1(0, t, 1)
        return gam
    gam = lax.fori_loop(4, NT8, one_tile, gam)

    gsend[...] = gam

    def gs(k, c):
        g = lax.rem(me + k, 16)
        pltpu.make_async_remote_copy(src_ref=gsend, dst_ref=grecv.at[a, o], send_sem=gssem, recv_sem=grsem,
                                     device_id=dev(g // 4, g % 4), device_id_type=MESH).start()
        return c
    lax.fori_loop(1, 16, gs, 0)
    pltpu.make_async_copy(gsend, grecv.at[a, o], grsem).start()

    pltpu.make_async_copy(mqr.at[:, pl.ds(0, 32)], mqr.at[:, pl.ds(0, 32)], mzrecv).wait()

    def mo(k, c):
        oo = lax.rem(o + k, 4)
        pltpu.make_async_remote_copy(src_ref=mqr.at[:, quarter], dst_ref=mqr.at[:, quarter], send_sem=mosend, recv_sem=morecv,
                                     device_id=dev(a, oo), device_id_type=MESH).start()
        return c
    lax.fori_loop(1, 4, mo, 0)
    @pl.when(outer)
    def _():
        for p in range(1, npair):
            send_half(p, 0, NT8, True)
        for p in range(1, npair):
            send_half(p, 0, NT8, False)

    @pl.when(jnp.logical_not(outer))
    def _():
        for p in range(1, 3):
            send_t1(p, 0, NT8)
    mq[a] = mloc[...]
    for k in range(1, 4):
        c1 = lax.rem(a + k, 4)
        mq[c1, a] = mloc[c1].T
    pltpu.make_async_copy(mqr.at[:, pl.ds(0, 96)], mqr.at[:, pl.ds(0, 96)], morecv).wait()
    for k in range(1, 4):
        c1 = lax.rem(a + k, 4)
        mq[c1, c1] = mqr[k - 1]
        for k2 in range(k + 1, 4):
            c2 = lax.rem(a + k2, 4)
            first = jnp.where(nearer(c1, c2, a), c1, c2)
            second = c1 + c2 - first
            blk = mqr[k + k2]
            mq[first, second] = blk
            mq[second, first] = blk.T
    for b in range(4):
        parts = split3(jnp.concatenate([mq[aa, b] for aa in range(4)], axis=1))
        for s in range(3):
            msp[s, pl.ds(b * LANES, LANES)] = parts[s]

    pltpu.make_async_copy(grecv, grecv, grsem).wait()
    graw = jnp.concatenate([grecv[aa, 0] + grecv[aa, 1] + grecv[aa, 2] + grecv[aa, 3] for aa in range(4)], axis=1)
    m3 = [msp[s] for s in range(3)]
    gfit = dot(lhs6(split3(graw), 1), rhs6(m3, 0), NN)
    mown = split3(jnp.concatenate([mloc[b] for b in range(4)], axis=0))
    wts = dot(lhs6(split3(gfit), 1), rhs6(mown, 0), NN)
    wl = lhs6(split3(wts), 1)
    low64 = lax.broadcasted_iota(jnp.int32, (nd, LANES), 1) < 64

    def jpair(u, c):
        ys = []
        for e in range(2):
            x = jnp.concatenate([bv[2 * u + e], jnp.zeros((nl, LANES - nq), F32)], axis=1)
            x = jnp.concatenate([x, jnp.zeros((256 - nl, LANES), F32)], axis=0)
            ys.append(dot(wl, rhs6(split3(x), 1), NT))
        for aa in range(4):
            lo = pltpu.roll(ys[0], (256 - nm * aa) % 256, 1)[:, :LANES]
            hi = pltpu.roll(ys[1], (256 + 64 - nm * aa) % 256, 1)[:, :LANES]
            jsend[aa, u] = jnp.where(low64, lo, hi)
        return c

    row8 = lax.broadcasted_iota(jnp.int32, (8, LANES), 0)
    lane8 = lax.broadcasted_iota(jnp.int32, (8, LANES), 1)
    at0 = lane8 - PIECE * row8
    at1 = lane8 - PIECE * (row8 + 8)
    here0 = jnp.logical_and(at0 >= 0, at0 < PIECE)
    here1 = jnp.logical_and(jnp.logical_and(at1 >= 0, at1 < PIECE), lane8 < nq)
    zbuf[:, NT8] = jnp.zeros((4, 2, 8, 512), F32)

    def tails(x):
        f = [x[t].astype(F32) for t in range(4)]
        out = []
        for e in range(2):
            for u in range(2):
                v0 = pltpu.roll(f[2 * u][8 * e:8 * e + 8], LANES - nq, 1, stride=PIECE, stride_axis=0)
                f1 = f[2 * u + 1][8 * e:8 * e + 8]
                v1 = jnp.where(row8 == 0, pltpu.roll(f1, (8 * PIECE - nq) % LANES, 1), pltpu.roll(f1, (9 * PIECE - nq) % LANES, 1))
                v = jnp.where(here0, v0, jnp.where(here1, v1, 0.0))
                out.append(v.sum(0, keepdims=True))
        return out

    def fit(p):
        pltpu.make_async_copy(rbuf.at[:, p], rbuf.at[:, p], trecv.at[p]).wait()
        xs = []
        for s in range(4):
            rest = [w for q in range(4) for w in tails(rbuf[s, p, q, pl.ds(0, 4)])]
            xs.append(jnp.concatenate([rbuf[s, p].reshape(4 * NT8 * 16, LANES), jnp.concatenate(rest, axis=0).astype(BF)], axis=0))
        x = jnp.concatenate(xs, axis=1)
        z = dot(jnp.concatenate([x, x, x], axis=1), msp[...].reshape(3 * 512, 512), NN)
        main = 4 * NT8 * 16
        zbuf[:, pl.ds(0, NT8)] = z[:main].reshape(4, NT8, 2, 8, 512)
        for q in range(4):
            for e in range(2):
                zbuf[q, NT8, e, pl.ds(0, 2)] = z[main + 4 * q + 2 * e:main + 4 * q + 2 * e + 2]
        ml = []
        for s in range(2):
            rest = tails(own[s, p, pl.ds(0, 4)]) + [jnp.zeros((12, LANES), F32)]
            ml.append(jnp.concatenate([own[s, p].reshape(NT8 * 16, LANES), jnp.concatenate(rest, axis=0).astype(BF)], axis=0))
        mid, low = ml
        rows = pl.ds(pl.multiple_of(a * LANES, LANES), LANES)
        mh, mm = msp[0, rows], msp[1, rows]
        z = dot(jnp.concatenate([mid, mid, low], axis=1), jnp.concatenate([mh, mm, mh], axis=0), NN)
        zbuf[o, pl.ds(0, NT8)] = zbuf[o, pl.ds(0, NT8)] + z[:NT8 * 16].reshape(NT8, 2, 8, 512)
        for e in range(2):
            zbuf[o, NT8, e, pl.ds(0, 2)] = zbuf[o, NT8, e, pl.ds(0, 2)] + z[NT8 * 16 + 2 * e:NT8 * 16 + 2 * e + 2]
        for e in range(2):
            s3 = split3(zbuf[:, :, e].reshape(4 * MROW, 512))
            k = dot(lhs6(s3, 1), rhs6(s3, 1), NT)
            if p == 0 and e == 0:
                kacc[0] = k[:, :LANES]
                kacc[1] = k[:, LANES:]
            else:
                kacc[0] = kacc[0] + k[:, :LANES]
                kacc[1] = kacc[1] + k[:, LANES:]

    lax.fori_loop(0, nm // 2, jpair, 0)
    near, far = a + 1 - 2 * (a % 2), lax.rem(a + 2, 4)
    hops = []
    for e, aa in enumerate((lax.rem(near + 2, 4), near)):
        hops.append(pltpu.make_async_remote_copy(src_ref=jsend.at[aa], dst_ref=jrecv.at[e], send_sem=jssem.at[e], recv_sem=jrsem.at[e],
                                                 device_id=dev(near, o), device_id_type=MESH))
        hops[-1].start()
    @pl.when(jnp.logical_not(outer))
    def _():
        for p in range(3, npair):
            send_t1(p, 0, NT8)
    for p in range(npair - 1):
        fit(p)
    hops[0].wait_recv()
    jfwd[...] = jsend[far] + jrecv[0]
    cross = pltpu.make_async_remote_copy(src_ref=jfwd, dst_ref=jrecv.at[2], send_sem=jssem.at[2], recv_sem=jrsem.at[2],
                                         device_id=dev(far, o), device_id_type=MESH)
    cross.start()
    fit(npair - 1)

    mate = o + 1 - 2 * half
    swap = pltpu.make_async_remote_copy(src_ref=kacc.at[1 - half], dst_ref=kin, send_sem=kxs, recv_sem=kxr,
                                        device_id=dev(a, mate), device_id_type=MESH)
    swap.start()
    swap.wait_recv()
    kful[...] = kacc[half] + kin[...]
    low32 = lax.broadcasted_iota(jnp.int32, (32, LANES), 1) < 64
    for oo in range(4):
        ev = kful[pl.ds(MROW * oo, 32, stride=2), :]
        od = kful[pl.ds(MROW * oo + 1, 32, stride=2), :]
        kmsg[0, oo] = jnp.where(low32, ev, pltpu.roll(od, 64, 1))
        kmsg[1, oo] = jnp.where(low32, pltpu.roll(ev, 64, 1), od)

    def ks(k, c):
        al, oo = k // 4, k % 4
        aa = 2 * half + al
        same = jnp.logical_and(aa == a, oo == o)

        @pl.when(jnp.logical_not(same))
        def _():
            pltpu.make_async_remote_copy(src_ref=kmsg.at[al, oo], dst_ref=krecv.at[pl.ds(dens * 32, 32)], send_sem=kss, recv_sem=krs,
                                         device_id=dev(aa, oo), device_id_type=MESH).start()

        @pl.when(same)
        def _():
            cp = pltpu.make_async_copy(kmsg.at[al, oo], krecv.at[pl.ds(dens * 32, 32)], krs)
            cp.start()
        return c
    lax.fori_loop(0, 8, ks, 0)

    hops[1].wait_recv()
    cross.wait_recv()
    pltpu.make_async_copy(krecv, krecv, krs).wait()
    for u in range(nm // 2):
        j = jsend[a, u] + jrecv[1, u] + jrecv[2, u]
        g = 2.0 * j - krecv[pl.ds(u, nd, stride=32), :]
        out[2 * u] = g[:, :nm]
        out[2 * u + 1] = pltpu.roll(g, 64, 1)[:, :nm]

    pltpu.make_async_copy(sbuf.at[pl.ds(0, 15)], sbuf.at[pl.ds(0, 15)], tsend).wait()
    metric_copies(lambda c: c.wait_send())
    pltpu.make_async_copy(mqr.at[:, pl.ds(0, 96)], mqr.at[:, pl.ds(0, 96)], mosend).wait()
    pltpu.make_async_copy(gbuf, gbuf, gssem).wait()
    for c in hops + [cross]:
        c.wait_send()
    swap.wait_send()
    inset = (a // 2) == half

    @pl.when(inset)
    def _():
        pltpu.make_async_copy(krecv.at[pl.ds(0, 224)], krecv.at[pl.ds(0, 224)], kss).wait()

    @pl.when(jnp.logical_not(inset))
    def _():
        pltpu.make_async_copy(krecv, krecv, kss).wait()


def solution(mesh):
    def local_fock(ints_blk, metric_blk, orbitals):
        nq, nm, nl = ints_blk.shape
        nd, _, ni = orbitals.shape
        bt = jnp.transpose(ints_blk, (1, 2, 0))
        mt = metric_blk.T
        ct = jnp.transpose(orbitals, (2, 0, 1)).reshape(ni * nd, nl)
        npair = ni // 4
        V = pltpu.VMEM
        dma = pltpu.SemaphoreType.DMA
        g = pl.pallas_call(
            lambda *refs: kernel(nm, nl, nq, nd, ni, *refs),
            out_shape=jax.ShapeDtypeStruct((nm, nd, nm), F32),
            in_specs=[pl.BlockSpec(memory_space=pl.ANY)] * 3,
            out_specs=pl.BlockSpec(memory_space=pltpu.VMEM),
            scratch_shapes=[
                V((nm, nl, nq), F32), V((4 * nq, nq), F32), V((ni * nd, nl), F32), V((ni * nd, 256), F32),
                V((8 * SP, LANES), F32), V((16, npair, NT8, 16, LANES), BF), V((4, npair, 4, NT8, 16, LANES), BF),
                V((2, npair, NT8, 16, LANES), BF), V((4, LANES, LANES), F32), V((6, LANES, LANES), F32), V((4, 4, LANES, LANES), F32), V((3, 512, 512), BF),
                V((nd, LANES), F32), V((4, 4, nd, LANES), F32), V((4, nm // 2, nd, LANES), F32), V((3, nm // 2, nd, LANES), F32), V((nm // 2, nd, LANES), F32),
                V((4, 8, 2, 8, 512), F32), V((2, 256, LANES), F32), V((256, LANES), F32), V((256, LANES), F32), V((2, 4, 32, LANES), F32),
                V((8 * 32, LANES), F32), V((15, nd, LANES), F32),
                dma((NT8,)), dma((3,)), dma, dma((npair,)), dma, dma, dma, dma, dma, dma, dma((3,)), dma((3,)), dma, dma, dma, dma],
            compiler_params=pltpu.CompilerParams(collective_id=0, has_side_effects=True, vmem_limit_bytes=60 * 2**20),
        )(bt, mt, ct)
        return jnp.transpose(g, (1, 0, 2))

    return jax.shard_map(local_fock, mesh=mesh, in_specs=(P(('sys', 'aux'), 'orb', None), P(('sys', 'aux'), None), P('sys', None, None)), out_specs=P('sys', 'orb', 'aux'), check_vma=False)
```

```python
import jax
import jax.numpy as jnp
from jax import lax
from jax.experimental import pallas as pl
from jax.experimental.pallas import tpu as pltpu
from jax.sharding import PartitionSpec as P

F32 = jnp.float32
BF = jnp.bfloat16
MESH = pl.DeviceIdType.MESH
NN = (((1,), (0,)), ((), ()))
NT = (((1,), (1,)), ((), ()))
LANES = 128
MROW = 64
NT8 = 7
PIECE = 12
SP = 168


def split3(x):
    hi = x.astype(BF)
    rest = x - hi.astype(F32)
    mid = rest.astype(BF)
    return hi, mid, (rest - mid.astype(F32)).astype(BF)


def dot(x, y, dims):
    return lax.dot_general(x, y, dims, preferred_element_type=F32)


def lhs6(x, axis):
    h, m, l = x
    return jnp.concatenate([h, h, m, m, h, l], axis=axis)


def rhs6(x, axis):
    h, m, l = x
    return jnp.concatenate([h, m, h, m, l, h], axis=axis)


def kernel(nm, nl, nq, nd, ni, bt, mt, ct, out, bv, mv, cv, ctp, tr, sbuf, rbuf, own, mloc, mqr, mq, msp, gsend, grecv, jsend, jrecv, jfwd, zbuf, kacc, kin, kful, kmsg, krecv, gbuf,
           bsem, lsem, tsend, trecv, mzsend, mzrecv, mosend, morecv, gssem, grsem, jssem, jrsem, kxs, kxr, kss, krs):
    sy, a, o = lax.axis_index('sys'), lax.axis_index('aux'), lax.axis_index('orb')
    me = a * 4 + o
    dens, half = me // 2, me % 2
    nh = ni // 2
    npair = nh // 2

    def dev(aa, oo):
        return (sy, aa, oo)

    pltpu.make_async_copy(ct, cv, lsem.at[0]).start()
    pltpu.make_async_copy(bt.at[pl.ds(8 * NT8, 2)], bv.at[pl.ds(8 * NT8, 2)], lsem.at[2]).start()
    for t in range(NT8):
        pltpu.make_async_copy(bt.at[pl.ds(8 * t, 8)], bv.at[pl.ds(8 * t, 8)], bsem.at[t]).start()
        if t == 0:
            pltpu.make_async_copy(mt, mv, lsem.at[1]).start()
    barrier = pltpu.get_barrier_semaphore()

    def tell(k, c):
        g = lax.rem(me + k, 16)
        pl.semaphore_signal(barrier, inc=1, device_id=dev(g // 4, g % 4), device_id_type=MESH)
        return c
    lax.fori_loop(1, 16, tell, 0)

    pltpu.make_async_copy(ct, cv, lsem.at[0]).wait()
    ctp[...] = jnp.concatenate([cv[...], jnp.zeros((nd * ni, 256 - nl), F32)], axis=1)
    lhs = lhs6(split3(ctp[...]), 1)
    pltpu.make_async_copy(mt, mv, lsem.at[1]).wait()
    for b in range(4):
        blk = jnp.concatenate([mv[nq * b:nq * (b + 1), :], jnp.zeros((nq, LANES - nq), F32)], axis=1)
        mloc[b] = jnp.concatenate([blk, jnp.zeros((LANES - nq, LANES), F32)], axis=0)
    pl.semaphore_wait(barrier, 15)

    quarter = pl.ds(pl.multiple_of(o * 32, 32), 32)

    def nearer(x, y, z):
        dx, dy = jnp.abs(x - z), jnp.abs(y - z)
        return jnp.logical_or(dx < dy, jnp.logical_and(dx == dy, x < y))

    def metric_copies(act):
        for k in (2, 1, 3):
            to = lax.rem(a + 4 - k, 4)

            def block(row, slot):
                return pltpu.make_async_remote_copy(src_ref=mloc.at[row, quarter], dst_ref=mqr.at[slot, quarter], send_sem=mzsend,
                                                    recv_sem=mzrecv, device_id=dev(to, o), device_id_type=MESH)
            act(block(a, k - 1))
            for k2 in (1, 2, 3):
                if k2 == k:
                    continue
                b = lax.rem(to + k2, 4)

                @pl.when(nearer(a, b, to))
                def _():
                    act(block(b, k + k2))
    metric_copies(lambda c: c.start())

    gam = jnp.zeros((nd, LANES), F32)
    tr2 = tr

    lane = lax.broadcasted_iota(jnp.int32, (1, LANES), 1)
    data = lane < nq

    def tile(t, gam, tail, first):
        pltpu.make_async_copy(bt.at[pl.ds(0, 8)], bv.at[pl.ds(0, 8)], bsem.at[t]).wait()
        cols = pltpu.roll(ctp[...], lax.rem(512 - (nm * o + 8 * t), 256), 1)
        count = 0
        if tail is not None:
            count = min(8, 10 - first)
            spare = jnp.concatenate([bv[8 * NT8 + tail], jnp.zeros((nl, LANES - nq), F32)], axis=1)
            tcol = pltpu.roll(ctp[...], lax.rem(512 - (nm * o + 8 * NT8 + tail), 256), 1)[:, 0:1]
        for r in range(0, 8, 2):
            xs = []
            for e in range(2):
                x = jnp.concatenate([bv[8 * t + r + e], jnp.zeros((nl, LANES - nq), F32)], axis=1)
                if r + e < count:
                    x = jnp.where(data, x, pltpu.roll(spare, (nq - PIECE * (first + r + e)) % LANES, 1))
                xs.append(x)
            x = jnp.concatenate(xs, axis=1)
            x = jnp.concatenate([x, jnp.zeros((256 - nl, 2 * LANES), F32)], axis=0)
            y = dot(lhs, rhs6(split3(x), 0), NN)
            for e in range(2):
                ye = y[:, e * LANES:(e + 1) * LANES]
                tr2[pl.ds((r + e) * SP, nd * ni), :] = ye
                col = cols[:, r + e:r + e + 1]
                if r + e < count:
                    w = (ye * jnp.where(data, col, tcol)).reshape(ni, nd, LANES).sum(0)
                    moved = pltpu.roll(jnp.where(data, 0.0, w), (PIECE * (first + r + e) - nq) % LANES, 1)
                    gam = gam + jnp.where(data, w, 0.0) + moved
                else:
                    gam = gam + (ye * col).reshape(ni, nd, LANES).sum(0)
        for g in range(16):
            d, h = g // 2, g % 2
            for p in range(npair):
                two = [tr2[pl.ds((h * nh + 2 * p + e) * nd + d, 8, stride=SP), :] for e in range(2)]
                sbuf[g, p, t] = jnp.concatenate(two, axis=0).astype(BF)
        for p in range(npair):
            two = [tr2[pl.ds((half * nh + 2 * p + e) * nd + dens, 8, stride=SP), :] for e in range(2)]
            _, mid, low = split3(jnp.concatenate(two, axis=0))
            own[0, p, t] = mid
            own[1, p, t] = low
        return gam

    def send_t1(p, t0, nt):
        def one(k, c):
            j, u = k % 4, k // 4
            aa = lax.rem(a + 2 + j, 4)
            oo = lax.rem(o + 1 + u, 4)
            g = aa * 4 + oo
            src = sbuf.at[g, p, pl.ds(t0, nt)]
            dst = rbuf.at[a, p, o, pl.ds(t0, nt)]

            @pl.when(k != 14)
            def _():
                pltpu.make_async_remote_copy(src_ref=src, dst_ref=dst, send_sem=tsend, recv_sem=trecv.at[p],
                                             device_id=dev(aa, oo), device_id_type=MESH).start()

            @pl.when(k == 14)
            def _():
                pltpu.make_async_copy(src, dst, trecv.at[p]).start()
            return c
        lax.fori_loop(0, 16, one, 0)

    outer = jnp.logical_or(a == 0, a == 3)
    pair = a + 1 - 2 * (a % 2)

    def send_half(p, t0, nt, cross):
        def one(k, c):
            if cross:
                aa = jnp.where(k % 2 == 0, 3 - a, 3 - pair)
                oo = lax.rem(o + 1 + k // 2, 4)
            else:
                aa = jnp.where(k % 2 == 0, pair, a)
                oo = lax.rem(o + 1 + k // 2, 4)
            g = aa * 4 + oo
            src = sbuf.at[g, p, pl.ds(t0, nt)]
            dst = rbuf.at[a, p, o, pl.ds(t0, nt)]

            def far():
                pltpu.make_async_remote_copy(src_ref=src, dst_ref=dst, send_sem=tsend, recv_sem=trecv.at[p],
                                             device_id=dev(aa, oo), device_id_type=MESH).start()
            if cross:
                far()
            else:
                pl.when(k != 7)(far)

                @pl.when(k == 7)
                def _():
                    pltpu.make_async_copy(src, dst, trecv.at[p]).start()
            return c
        lax.fori_loop(0, 8, one, 0)

    pltpu.make_async_copy(bt.at[pl.ds(0, 2)], bv.at[pl.ds(0, 2)], lsem.at[2]).wait()

    def two_tiles(u, gam):
        gam = tile(2 * u, gam, u, 0)
        send_t1(0, 2 * u, 1)
        gam = tile(2 * u + 1, gam, u, 8)
        send_t1(0, 2 * u + 1, 1)
        return gam
    gam = lax.fori_loop(0, 2, two_tiles, gam)

    def one_tile(t, gam):
        gam = tile(t, gam, None, 0)
        send_t1(0, t, 1)
        return gam
    gam = lax.fori_loop(4, NT8, one_tile, gam)

    gsend[...] = gam

    def gs(k, c):
        g = lax.rem(me + k, 16)
        pltpu.make_async_remote_copy(src_ref=gsend, dst_ref=grecv.at[a, o], send_sem=gssem, recv_sem=grsem,
                                     device_id=dev(g // 4, g % 4), device_id_type=MESH).start()
        return c
    lax.fori_loop(1, 16, gs, 0)
    pltpu.make_async_copy(gsend, grecv.at[a, o], grsem).start()

    pltpu.make_async_copy(mqr.at[:, pl.ds(0, 32)], mqr.at[:, pl.ds(0, 32)], mzrecv).wait()

    def mo(k, c):
        oo = lax.rem(o + k, 4)
        pltpu.make_async_remote_copy(src_ref=mqr.at[:, quarter], dst_ref=mqr.at[:, quarter], send_sem=mosend, recv_sem=morecv,
                                     device_id=dev(a, oo), device_id_type=MESH).start()
        return c
    lax.fori_loop(1, 4, mo, 0)
    @pl.when(outer)
    def _():
        send_half(1, 0, NT8, False)
        send_half(2, 0, NT8, False)
        send_half(1, 0, NT8, True)
        send_half(3, 0, NT8, False)
        send_half(4, 0, NT8, False)
        send_half(2, 0, NT8, True)

    @pl.when(jnp.logical_not(outer))
    def _():
        for p in range(1, 3):
            send_t1(p, 0, NT8)
    mq[a] = mloc[...]
    for k in range(1, 4):
        c1 = lax.rem(a + k, 4)
        mq[c1, a] = mloc[c1].T
    pltpu.make_async_copy(mqr.at[:, pl.ds(0, 96)], mqr.at[:, pl.ds(0, 96)], morecv).wait()
    for k in range(1, 4):
        c1 = lax.rem(a + k, 4)
        mq[c1, c1] = mqr[k - 1]
        for k2 in range(k + 1, 4):
            c2 = lax.rem(a + k2, 4)
            first = jnp.where(nearer(c1, c2, a), c1, c2)
            second = c1 + c2 - first
            blk = mqr[k + k2]
            mq[first, second] = blk
            mq[second, first] = blk.T
    for b in range(4):
        parts = split3(jnp.concatenate([mq[aa, b] for aa in range(4)], axis=1))
        for s in range(3):
            msp[s, pl.ds(b * LANES, LANES)] = parts[s]

    pltpu.make_async_copy(grecv, grecv, grsem).wait()
    graw = jnp.concatenate([grecv[aa, 0] + grecv[aa, 1] + grecv[aa, 2] + grecv[aa, 3] for aa in range(4)], axis=1)
    m3 = [msp[s] for s in range(3)]
    gfit = dot(lhs6(split3(graw), 1), rhs6(m3, 0), NN)
    mown = split3(jnp.concatenate([mloc[b] for b in range(4)], axis=0))
    wts = dot(lhs6(split3(gfit), 1), rhs6(mown, 0), NN)
    wl = lhs6(split3(wts), 1)
    low64 = lax.broadcasted_iota(jnp.int32, (nd, LANES), 1) < 64

    def jpair(u, c):
        ys = []
        for e in range(2):
            x = jnp.concatenate([bv[2 * u + e], jnp.zeros((nl, LANES - nq), F32)], axis=1)
            x = jnp.concatenate([x, jnp.zeros((256 - nl, LANES), F32)], axis=0)
            ys.append(dot(wl, rhs6(split3(x), 1), NT))
        for aa in range(4):
            lo = pltpu.roll(ys[0], (256 - nm * aa) % 256, 1)[:, :LANES]
            hi = pltpu.roll(ys[1], (256 + 64 - nm * aa) % 256, 1)[:, :LANES]
            jsend[aa, u] = jnp.where(low64, lo, hi)
        return c

    row8 = lax.broadcasted_iota(jnp.int32, (8, LANES), 0)
    lane8 = lax.broadcasted_iota(jnp.int32, (8, LANES), 1)
    at0 = lane8 - PIECE * row8
    at1 = lane8 - PIECE * (row8 + 8)
    here0 = jnp.logical_and(at0 >= 0, at0 < PIECE)
    here1 = jnp.logical_and(jnp.logical_and(at1 >= 0, at1 < PIECE), lane8 < nq)
    zbuf[:, NT8] = jnp.zeros((4, 2, 8, 512), F32)

    def tails(x):
        f = [x[t].astype(F32) for t in range(4)]
        out = []
        for e in range(2):
            for u in range(2):
                v0 = pltpu.roll(f[2 * u][8 * e:8 * e + 8], LANES - nq, 1, stride=PIECE, stride_axis=0)
                f1 = f[2 * u + 1][8 * e:8 * e + 8]
                v1 = jnp.where(row8 == 0, pltpu.roll(f1, (8 * PIECE - nq) % LANES, 1), pltpu.roll(f1, (9 * PIECE - nq) % LANES, 1))
                v = jnp.where(here0, v0, jnp.where(here1, v1, 0.0))
                out.append(v.sum(0, keepdims=True))
        return out

    def fit(p):
        pltpu.make_async_copy(rbuf.at[:, p], rbuf.at[:, p], trecv.at[p]).wait()
        xs = []
        for s in range(4):
            rest = [w for q in range(4) for w in tails(rbuf[s, p, q, pl.ds(0, 4)])]
            xs.append(jnp.concatenate([rbuf[s, p].reshape(4 * NT8 * 16, LANES), jnp.concatenate(rest, axis=0).astype(BF)], axis=0))
        x = jnp.concatenate(xs, axis=1)
        z = dot(jnp.concatenate([x, x, x], axis=1), msp[...].reshape(3 * 512, 512), NN)
        main = 4 * NT8 * 16
        zbuf[:, pl.ds(0, NT8)] = z[:main].reshape(4, NT8, 2, 8, 512)
        for q in range(4):
            for e in range(2):
                zbuf[q, NT8, e, pl.ds(0, 2)] = z[main + 4 * q + 2 * e:main + 4 * q + 2 * e + 2]
        ml = []
        for s in range(2):
            rest = tails(own[s, p, pl.ds(0, 4)]) + [jnp.zeros((12, LANES), F32)]
            ml.append(jnp.concatenate([own[s, p].reshape(NT8 * 16, LANES), jnp.concatenate(rest, axis=0).astype(BF)], axis=0))
        mid, low = ml
        rows = pl.ds(pl.multiple_of(a * LANES, LANES), LANES)
        mh, mm = msp[0, rows], msp[1, rows]
        z = dot(jnp.concatenate([mid, mid, low], axis=1), jnp.concatenate([mh, mm, mh], axis=0), NN)
        zbuf[o, pl.ds(0, NT8)] = zbuf[o, pl.ds(0, NT8)] + z[:NT8 * 16].reshape(NT8, 2, 8, 512)
        for e in range(2):
            zbuf[o, NT8, e, pl.ds(0, 2)] = zbuf[o, NT8, e, pl.ds(0, 2)] + z[NT8 * 16 + 2 * e:NT8 * 16 + 2 * e + 2]
        for e in range(2):
            s3 = split3(zbuf[:, :, e].reshape(4 * MROW, 512))
            k = dot(lhs6(s3, 1), rhs6(s3, 1), NT)
            if p == 0 and e == 0:
                kacc[0] = k[:, :LANES]
                kacc[1] = k[:, LANES:]
            else:
                kacc[0] = kacc[0] + k[:, :LANES]
                kacc[1] = kacc[1] + k[:, LANES:]

    lax.fori_loop(0, nm // 2, jpair, 0)
    near, far = a + 1 - 2 * (a % 2), lax.rem(a + 2, 4)
    hops = []
    for e, aa in enumerate((lax.rem(near + 2, 4), near)):
        hops.append(pltpu.make_async_remote_copy(src_ref=jsend.at[aa], dst_ref=jrecv.at[e], send_sem=jssem.at[e], recv_sem=jrsem.at[e],
                                                 device_id=dev(near, o), device_id_type=MESH))
        hops[-1].start()
    @pl.when(outer)
    def _():
        for p in range(3, npair):
            send_half(p, 0, NT8, True)

    @pl.when(jnp.logical_not(outer))
    def _():
        for p in range(3, npair):
            send_t1(p, 0, NT8)
    for p in range(npair - 1):
        fit(p)
    hops[0].wait_recv()
    jfwd[...] = jsend[far] + jrecv[0]
    cross = pltpu.make_async_remote_copy(src_ref=jfwd, dst_ref=jrecv.at[2], send_sem=jssem.at[2], recv_sem=jrsem.at[2],
                                         device_id=dev(far, o), device_id_type=MESH)
    cross.start()
    fit(npair - 1)

    mate = o + 1 - 2 * half
    swap = pltpu.make_async_remote_copy(src_ref=kacc.at[1 - half], dst_ref=kin, send_sem=kxs, recv_sem=kxr,
                                        device_id=dev(a, mate), device_id_type=MESH)
    swap.start()
    swap.wait_recv()
    kful[...] = kacc[half] + kin[...]
    low32 = lax.broadcasted_iota(jnp.int32, (32, LANES), 1) < 64
    for oo in range(4):
        ev = kful[pl.ds(MROW * oo, 32, stride=2), :]
        od = kful[pl.ds(MROW * oo + 1, 32, stride=2), :]
        kmsg[0, oo] = jnp.where(low32, ev, pltpu.roll(od, 64, 1))
        kmsg[1, oo] = jnp.where(low32, pltpu.roll(ev, 64, 1), od)

    def ks(k, c):
        al, oo = k // 4, k % 4
        aa = 2 * half + al
        same = jnp.logical_and(aa == a, oo == o)

        @pl.when(jnp.logical_not(same))
        def _():
            pltpu.make_async_remote_copy(src_ref=kmsg.at[al, oo], dst_ref=krecv.at[pl.ds(dens * 32, 32)], send_sem=kss, recv_sem=krs,
                                         device_id=dev(aa, oo), device_id_type=MESH).start()

        @pl.when(same)
        def _():
            cp = pltpu.make_async_copy(kmsg.at[al, oo], krecv.at[pl.ds(dens * 32, 32)], krs)
            cp.start()
        return c
    lax.fori_loop(0, 8, ks, 0)

    hops[1].wait_recv()
    cross.wait_recv()
    pltpu.make_async_copy(krecv, krecv, krs).wait()
    for u in range(nm // 2):
        j = jsend[a, u] + jrecv[1, u] + jrecv[2, u]
        g = 2.0 * j - krecv[pl.ds(u, nd, stride=32), :]
        out[2 * u] = g[:, :nm]
        out[2 * u + 1] = pltpu.roll(g, 64, 1)[:, :nm]

    pltpu.make_async_copy(sbuf.at[pl.ds(0, 15)], sbuf.at[pl.ds(0, 15)], tsend).wait()
    metric_copies(lambda c: c.wait_send())
    pltpu.make_async_copy(mqr.at[:, pl.ds(0, 96)], mqr.at[:, pl.ds(0, 96)], mosend).wait()
    pltpu.make_async_copy(gbuf, gbuf, gssem).wait()
    for c in hops + [cross]:
        c.wait_send()
    swap.wait_send()
    inset = (a // 2) == half

    @pl.when(inset)
    def _():
        pltpu.make_async_copy(krecv.at[pl.ds(0, 224)], krecv.at[pl.ds(0, 224)], kss).wait()

    @pl.when(jnp.logical_not(inset))
    def _():
        pltpu.make_async_copy(krecv, krecv, kss).wait()


def solution(mesh):
    def local_fock(ints_blk, metric_blk, orbitals):
        nq, nm, nl = ints_blk.shape
        nd, _, ni = orbitals.shape
        bt = jnp.transpose(ints_blk, (1, 2, 0))
        mt = metric_blk.T
        ct = jnp.transpose(orbitals, (2, 0, 1)).reshape(ni * nd, nl)
        npair = ni // 4
        V = pltpu.VMEM
        dma = pltpu.SemaphoreType.DMA
        g = pl.pallas_call(
            lambda *refs: kernel(nm, nl, nq, nd, ni, *refs),
            out_shape=jax.ShapeDtypeStruct((nm, nd, nm), F32),
            in_specs=[pl.BlockSpec(memory_space=pl.ANY)] * 3,
            out_specs=pl.BlockSpec(memory_space=pltpu.VMEM),
            scratch_shapes=[
                V((nm, nl, nq), F32), V((4 * nq, nq), F32), V((ni * nd, nl), F32), V((ni * nd, 256), F32),
                V((8 * SP, LANES), F32), V((16, npair, NT8, 16, LANES), BF), V((4, npair, 4, NT8, 16, LANES), BF),
                V((2, npair, NT8, 16, LANES), BF), V((4, LANES, LANES), F32), V((6, LANES, LANES), F32), V((4, 4, LANES, LANES), F32), V((3, 512, 512), BF),
                V((nd, LANES), F32), V((4, 4, nd, LANES), F32), V((4, nm // 2, nd, LANES), F32), V((3, nm // 2, nd, LANES), F32), V((nm // 2, nd, LANES), F32),
                V((4, 8, 2, 8, 512), F32), V((2, 256, LANES), F32), V((256, LANES), F32), V((256, LANES), F32), V((2, 4, 32, LANES), F32),
                V((8 * 32, LANES), F32), V((15, nd, LANES), F32),
                dma((NT8,)), dma((3,)), dma, dma((npair,)), dma, dma, dma, dma, dma, dma, dma((3,)), dma((3,)), dma, dma, dma, dma],
            compiler_params=pltpu.CompilerParams(collective_id=0, has_side_effects=True, vmem_limit_bytes=60 * 2**20),
        )(bt, mt, ct)
        return jnp.transpose(g, (1, 0, 2))

    return jax.shard_map(local_fock, mesh=mesh, in_specs=(P(('sys', 'aux'), 'orb', None), P(('sys', 'aux'), None), P('sys', None, None)), out_specs=P('sys', 'orb', 'aux'), check_vma=False)
```

```python
import jax
import jax.numpy as jnp
from jax import lax
from jax.experimental import pallas as pl
from jax.experimental.pallas import tpu as pltpu
from jax.sharding import PartitionSpec as P

F32 = jnp.float32
BF = jnp.bfloat16
MESH = pl.DeviceIdType.MESH
NN = (((1,), (0,)), ((), ()))
NT = (((1,), (1,)), ((), ()))
LANES = 128
MROW = 64
NT8 = 7
PIECE = 12
SP = 168


def split3(x):
    hi = x.astype(BF)
    rest = x - hi.astype(F32)
    mid = rest.astype(BF)
    return hi, mid, (rest - mid.astype(F32)).astype(BF)


def dot(x, y, dims):
    return lax.dot_general(x, y, dims, preferred_element_type=F32)


def lhs6(x, axis):
    h, m, l = x
    return jnp.concatenate([h, h, m, m, h, l], axis=axis)


def rhs6(x, axis):
    h, m, l = x
    return jnp.concatenate([h, m, h, m, l, h], axis=axis)


def kernel(nm, nl, nq, nd, ni, bt, mt, ct, out, bv, mv, cv, ctp, tr, sbuf, rbuf, own, mloc, mqr, mq, msp, gsend, grecv, jsend, jrecv, jfwd, zbuf, kacc, kin, kful, kmsg, krecv, gbuf,
           bsem, lsem, tsend, trecv, mzsend, mzrecv, mosend, morecv, gssem, grsem, jssem, jrsem, kxs, kxr, kss, krs):
    sy, a, o = lax.axis_index('sys'), lax.axis_index('aux'), lax.axis_index('orb')
    me = a * 4 + o
    dens, half = me // 2, me % 2
    nh = ni // 2
    npair = nh // 2

    def dev(aa, oo):
        return (sy, aa, oo)

    pltpu.make_async_copy(ct, cv, lsem.at[0]).start()
    pltpu.make_async_copy(bt.at[pl.ds(8 * NT8, 2)], bv.at[pl.ds(8 * NT8, 2)], lsem.at[2]).start()
    for t in range(NT8):
        pltpu.make_async_copy(bt.at[pl.ds(8 * t, 8)], bv.at[pl.ds(8 * t, 8)], bsem.at[t]).start()
        if t == 0:
            pltpu.make_async_copy(mt, mv, lsem.at[1]).start()
    barrier = pltpu.get_barrier_semaphore()

    def tell(k, c):
        g = lax.rem(me + k, 16)
        pl.semaphore_signal(barrier, inc=1, device_id=dev(g // 4, g % 4), device_id_type=MESH)
        return c
    lax.fori_loop(1, 16, tell, 0)

    pltpu.make_async_copy(ct, cv, lsem.at[0]).wait()
    ctp[...] = jnp.concatenate([cv[...], jnp.zeros((nd * ni, 256 - nl), F32)], axis=1)
    lhs = lhs6(split3(ctp[...]), 1)
    pltpu.make_async_copy(mt, mv, lsem.at[1]).wait()
    for b in range(4):
        blk = jnp.concatenate([mv[nq * b:nq * (b + 1), :], jnp.zeros((nq, LANES - nq), F32)], axis=1)
        mloc[b] = jnp.concatenate([blk, jnp.zeros((LANES - nq, LANES), F32)], axis=0)
    pl.semaphore_wait(barrier, 15)

    quarter = pl.ds(pl.multiple_of(o * 32, 32), 32)

    def nearer(x, y, z):
        dx, dy = jnp.abs(x - z), jnp.abs(y - z)
        return jnp.logical_or(dx < dy, jnp.logical_and(dx == dy, x < y))

    def metric_copies(act):
        for k in (2, 1, 3):
            to = lax.rem(a + 4 - k, 4)

            def block(row, slot):
                return pltpu.make_async_remote_copy(src_ref=mloc.at[row, quarter], dst_ref=mqr.at[slot, quarter], send_sem=mzsend,
                                                    recv_sem=mzrecv, device_id=dev(to, o), device_id_type=MESH)
            act(block(a, k - 1))
            for k2 in (1, 2, 3):
                if k2 == k:
                    continue
                b = lax.rem(to + k2, 4)

                @pl.when(nearer(a, b, to))
                def _():
                    act(block(b, k + k2))
    metric_copies(lambda c: c.start())

    gam = jnp.zeros((nd, LANES), F32)
    tr2 = tr

    lane = lax.broadcasted_iota(jnp.int32, (1, LANES), 1)
    data = lane < nq

    def tile(t, gam, tail, first):
        pltpu.make_async_copy(bt.at[pl.ds(0, 8)], bv.at[pl.ds(0, 8)], bsem.at[t]).wait()
        cols = pltpu.roll(ctp[...], lax.rem(512 - (nm * o + 8 * t), 256), 1)
        count = 0
        if tail is not None:
            count = min(8, 10 - first)
            spare = jnp.concatenate([bv[8 * NT8 + tail], jnp.zeros((nl, LANES - nq), F32)], axis=1)
            tcol = pltpu.roll(ctp[...], lax.rem(512 - (nm * o + 8 * NT8 + tail), 256), 1)[:, 0:1]
        for r in range(0, 8, 2):
            xs = []
            for e in range(2):
                x = jnp.concatenate([bv[8 * t + r + e], jnp.zeros((nl, LANES - nq), F32)], axis=1)
                if r + e < count:
                    x = jnp.where(data, x, pltpu.roll(spare, (nq - PIECE * (first + r + e)) % LANES, 1))
                xs.append(x)
            x = jnp.concatenate(xs, axis=1)
            x = jnp.concatenate([x, jnp.zeros((256 - nl, 2 * LANES), F32)], axis=0)
            y = dot(lhs, rhs6(split3(x), 0), NN)
            for e in range(2):
                ye = y[:, e * LANES:(e + 1) * LANES]
                tr2[pl.ds((r + e) * SP, nd * ni), :] = ye
                col = cols[:, r + e:r + e + 1]
                if r + e < count:
                    w = (ye * jnp.where(data, col, tcol)).reshape(ni, nd, LANES).sum(0)
                    moved = pltpu.roll(jnp.where(data, 0.0, w), (PIECE * (first + r + e) - nq) % LANES, 1)
                    gam = gam + jnp.where(data, w, 0.0) + moved
                else:
                    gam = gam + (ye * col).reshape(ni, nd, LANES).sum(0)
        for g in range(16):
            d, h = g // 2, g % 2
            for p in range(npair):
                two = [tr2[pl.ds((h * nh + 2 * p + e) * nd + d, 8, stride=SP), :] for e in range(2)]
                sbuf[g, p, t] = jnp.concatenate(two, axis=0).astype(BF)
        for p in range(npair):
            two = [tr2[pl.ds((half * nh + 2 * p + e) * nd + dens, 8, stride=SP), :] for e in range(2)]
            _, mid, low = split3(jnp.concatenate(two, axis=0))
            own[0, p, t] = mid
            own[1, p, t] = low
        return gam

    def send_t1(p, t0, nt):
        def one(k, c):
            j, u = k % 4, k // 4
            aa = lax.rem(a + 2 + j, 4)
            oo = lax.rem(o + 1 + u, 4)
            g = aa * 4 + oo
            src = sbuf.at[g, p, pl.ds(t0, nt)]
            dst = rbuf.at[a, p, o, pl.ds(t0, nt)]

            @pl.when(k != 14)
            def _():
                pltpu.make_async_remote_copy(src_ref=src, dst_ref=dst, send_sem=tsend, recv_sem=trecv.at[p],
                                             device_id=dev(aa, oo), device_id_type=MESH).start()

            @pl.when(k == 14)
            def _():
                pltpu.make_async_copy(src, dst, trecv.at[p]).start()
            return c
        lax.fori_loop(0, 16, one, 0)

    outer = jnp.logical_or(a == 0, a == 3)
    pair = a + 1 - 2 * (a % 2)

    def send_half(p, t0, nt, cross):
        def one(k, c):
            if cross:
                aa = jnp.where(k % 2 == 0, 3 - a, 3 - pair)
                oo = lax.rem(o + 1 + k // 2, 4)
            else:
                aa = jnp.where(k % 2 == 0, pair, a)
                oo = lax.rem(o + 1 + k // 2, 4)
            g = aa * 4 + oo
            src = sbuf.at[g, p, pl.ds(t0, nt)]
            dst = rbuf.at[a, p, o, pl.ds(t0, nt)]

            def far():
                pltpu.make_async_remote_copy(src_ref=src, dst_ref=dst, send_sem=tsend, recv_sem=trecv.at[p],
                                             device_id=dev(aa, oo), device_id_type=MESH).start()
            if cross:
                far()
            else:
                pl.when(k != 7)(far)

                @pl.when(k == 7)
                def _():
                    pltpu.make_async_copy(src, dst, trecv.at[p]).start()
            return c
        lax.fori_loop(0, 8, one, 0)

    pltpu.make_async_copy(bt.at[pl.ds(0, 2)], bv.at[pl.ds(0, 2)], lsem.at[2]).wait()

    def two_tiles(u, gam):
        gam = tile(2 * u, gam, u, 0)
        send_t1(0, 2 * u, 1)
        gam = tile(2 * u + 1, gam, u, 8)
        send_t1(0, 2 * u + 1, 1)
        return gam
    gam = lax.fori_loop(0, 2, two_tiles, gam)

    def one_tile(t, gam):
        gam = tile(t, gam, None, 0)
        send_t1(0, t, 1)
        return gam
    gam = lax.fori_loop(4, NT8, one_tile, gam)

    gsend[...] = gam

    def gs(k, c):
        g = lax.rem(me + k, 16)
        pltpu.make_async_remote_copy(src_ref=gsend, dst_ref=grecv.at[a, o], send_sem=gssem, recv_sem=grsem,
                                     device_id=dev(g // 4, g % 4), device_id_type=MESH).start()
        return c
    lax.fori_loop(1, 16, gs, 0)
    pltpu.make_async_copy(gsend, grecv.at[a, o], grsem).start()

    pltpu.make_async_copy(mqr.at[:, pl.ds(0, 32)], mqr.at[:, pl.ds(0, 32)], mzrecv).wait()

    def mo(k, c):
        oo = lax.rem(o + k, 4)
        pltpu.make_async_remote_copy(src_ref=mqr.at[:, quarter], dst_ref=mqr.at[:, quarter], send_sem=mosend, recv_sem=morecv,
                                     device_id=dev(a, oo), device_id_type=MESH).start()
        return c
    lax.fori_loop(1, 4, mo, 0)
    @pl.when(outer)
    def _():
        for p in range(1, npair):
            send_half(p, 0, NT8, False)
        send_half(1, 0, NT8, True)

    @pl.when(jnp.logical_not(outer))
    def _():
        for p in range(1, 3):
            send_t1(p, 0, NT8)
    mq[a] = mloc[...]
    for k in range(1, 4):
        c1 = lax.rem(a + k, 4)
        mq[c1, a] = mloc[c1].T
    pltpu.make_async_copy(mqr.at[:, pl.ds(0, 96)], mqr.at[:, pl.ds(0, 96)], morecv).wait()
    for k in range(1, 4):
        c1 = lax.rem(a + k, 4)
        mq[c1, c1] = mqr[k - 1]
        for k2 in range(k + 1, 4):
            c2 = lax.rem(a + k2, 4)
            first = jnp.where(nearer(c1, c2, a), c1, c2)
            second = c1 + c2 - first
            blk = mqr[k + k2]
            mq[first, second] = blk
            mq[second, first] = blk.T
    for b in range(4):
        parts = split3(jnp.concatenate([mq[aa, b] for aa in range(4)], axis=1))
        for s in range(3):
            msp[s, pl.ds(b * LANES, LANES)] = parts[s]

    pltpu.make_async_copy(grecv, grecv, grsem).wait()
    graw = jnp.concatenate([grecv[aa, 0] + grecv[aa, 1] + grecv[aa, 2] + grecv[aa, 3] for aa in range(4)], axis=1)
    m3 = [msp[s] for s in range(3)]
    gfit = dot(lhs6(split3(graw), 1), rhs6(m3, 0), NN)
    mown = split3(jnp.concatenate([mloc[b] for b in range(4)], axis=0))
    wts = dot(lhs6(split3(gfit), 1), rhs6(mown, 0), NN)
    wl = lhs6(split3(wts), 1)
    low64 = lax.broadcasted_iota(jnp.int32, (nd, LANES), 1) < 64

    def jpair(u, c):
        ys = []
        for e in range(2):
            x = jnp.concatenate([bv[2 * u + e], jnp.zeros((nl, LANES - nq), F32)], axis=1)
            x = jnp.concatenate([x, jnp.zeros((256 - nl, LANES), F32)], axis=0)
            ys.append(dot(wl, rhs6(split3(x), 1), NT))
        for aa in range(4):
            lo = pltpu.roll(ys[0], (256 - nm * aa) % 256, 1)[:, :LANES]
            hi = pltpu.roll(ys[1], (256 + 64 - nm * aa) % 256, 1)[:, :LANES]
            jsend[aa, u] = jnp.where(low64, lo, hi)
        return c

    row8 = lax.broadcasted_iota(jnp.int32, (8, LANES), 0)
    lane8 = lax.broadcasted_iota(jnp.int32, (8, LANES), 1)
    at0 = lane8 - PIECE * row8
    at1 = lane8 - PIECE * (row8 + 8)
    here0 = jnp.logical_and(at0 >= 0, at0 < PIECE)
    here1 = jnp.logical_and(jnp.logical_and(at1 >= 0, at1 < PIECE), lane8 < nq)
    zbuf[:, NT8] = jnp.zeros((4, 2, 8, 512), F32)

    def tails(x):
        f = [x[t].astype(F32) for t in range(4)]
        out = []
        for e in range(2):
            for u in range(2):
                v0 = pltpu.roll(f[2 * u][8 * e:8 * e + 8], LANES - nq, 1, stride=PIECE, stride_axis=0)
                f1 = f[2 * u + 1][8 * e:8 * e + 8]
                v1 = jnp.where(row8 == 0, pltpu.roll(f1, (8 * PIECE - nq) % LANES, 1), pltpu.roll(f1, (9 * PIECE - nq) % LANES, 1))
                v = jnp.where(here0, v0, jnp.where(here1, v1, 0.0))
                out.append(v.sum(0, keepdims=True))
        return out

    def fit(p):
        pltpu.make_async_copy(rbuf.at[:, p], rbuf.at[:, p], trecv.at[p]).wait()
        xs = []
        for s in range(4):
            rest = [w for q in range(4) for w in tails(rbuf[s, p, q, pl.ds(0, 4)])]
            xs.append(jnp.concatenate([rbuf[s, p].reshape(4 * NT8 * 16, LANES), jnp.concatenate(rest, axis=0).astype(BF)], axis=0))
        x = jnp.concatenate(xs, axis=1)
        z = dot(jnp.concatenate([x, x, x], axis=1), msp[...].reshape(3 * 512, 512), NN)
        main = 4 * NT8 * 16
        zbuf[:, pl.ds(0, NT8)] = z[:main].reshape(4, NT8, 2, 8, 512)
        for q in range(4):
            for e in range(2):
                zbuf[q, NT8, e, pl.ds(0, 2)] = z[main + 4 * q + 2 * e:main + 4 * q + 2 * e + 2]
        ml = []
        for s in range(2):
            rest = tails(own[s, p, pl.ds(0, 4)]) + [jnp.zeros((12, LANES), F32)]
            ml.append(jnp.concatenate([own[s, p].reshape(NT8 * 16, LANES), jnp.concatenate(rest, axis=0).astype(BF)], axis=0))
        mid, low = ml
        rows = pl.ds(pl.multiple_of(a * LANES, LANES), LANES)
        mh, mm = msp[0, rows], msp[1, rows]
        z = dot(jnp.concatenate([mid, mid, low], axis=1), jnp.concatenate([mh, mm, mh], axis=0), NN)
        zbuf[o, pl.ds(0, NT8)] = zbuf[o, pl.ds(0, NT8)] + z[:NT8 * 16].reshape(NT8, 2, 8, 512)
        for e in range(2):
            zbuf[o, NT8, e, pl.ds(0, 2)] = zbuf[o, NT8, e, pl.ds(0, 2)] + z[NT8 * 16 + 2 * e:NT8 * 16 + 2 * e + 2]
        for e in range(2):
            s3 = split3(zbuf[:, :, e].reshape(4 * MROW, 512))
            k = dot(lhs6(s3, 1), rhs6(s3, 1), NT)
            if p == 0 and e == 0:
                kacc[0] = k[:, :LANES]
                kacc[1] = k[:, LANES:]
            else:
                kacc[0] = kacc[0] + k[:, :LANES]
                kacc[1] = kacc[1] + k[:, LANES:]

    lax.fori_loop(0, nm // 2, jpair, 0)
    near, far = a + 1 - 2 * (a % 2), lax.rem(a + 2, 4)
    hops = []
    for e, aa in enumerate((lax.rem(near + 2, 4), near)):
        hops.append(pltpu.make_async_remote_copy(src_ref=jsend.at[aa], dst_ref=jrecv.at[e], send_sem=jssem.at[e], recv_sem=jrsem.at[e],
                                                 device_id=dev(near, o), device_id_type=MESH))
        hops[-1].start()
    @pl.when(outer)
    def _():
        for p in range(2, npair):
            send_half(p, 0, NT8, True)

    @pl.when(jnp.logical_not(outer))
    def _():
        for p in range(3, npair):
            send_t1(p, 0, NT8)
    for p in range(npair - 1):
        fit(p)
    hops[0].wait_recv()
    jfwd[...] = jsend[far] + jrecv[0]
    cross = pltpu.make_async_remote_copy(src_ref=jfwd, dst_ref=jrecv.at[2], send_sem=jssem.at[2], recv_sem=jrsem.at[2],
                                         device_id=dev(far, o), device_id_type=MESH)
    cross.start()
    fit(npair - 1)

    mate = o + 1 - 2 * half
    swap = pltpu.make_async_remote_copy(src_ref=kacc.at[1 - half], dst_ref=kin, send_sem=kxs, recv_sem=kxr,
                                        device_id=dev(a, mate), device_id_type=MESH)
    swap.start()
    swap.wait_recv()
    kful[...] = kacc[half] + kin[...]
    low32 = lax.broadcasted_iota(jnp.int32, (32, LANES), 1) < 64
    for oo in range(4):
        ev = kful[pl.ds(MROW * oo, 32, stride=2), :]
        od = kful[pl.ds(MROW * oo + 1, 32, stride=2), :]
        kmsg[0, oo] = jnp.where(low32, ev, pltpu.roll(od, 64, 1))
        kmsg[1, oo] = jnp.where(low32, pltpu.roll(ev, 64, 1), od)

    def ks(k, c):
        al, oo = k // 4, k % 4
        aa = 2 * half + al
        same = jnp.logical_and(aa == a, oo == o)

        @pl.when(jnp.logical_not(same))
        def _():
            pltpu.make_async_remote_copy(src_ref=kmsg.at[al, oo], dst_ref=krecv.at[pl.ds(dens * 32, 32)], send_sem=kss, recv_sem=krs,
                                         device_id=dev(aa, oo), device_id_type=MESH).start()

        @pl.when(same)
        def _():
            cp = pltpu.make_async_copy(kmsg.at[al, oo], krecv.at[pl.ds(dens * 32, 32)], krs)
            cp.start()
        return c
    lax.fori_loop(0, 8, ks, 0)

    hops[1].wait_recv()
    cross.wait_recv()
    pltpu.make_async_copy(krecv, krecv, krs).wait()
    for u in range(nm // 2):
        j = jsend[a, u] + jrecv[1, u] + jrecv[2, u]
        g = 2.0 * j - krecv[pl.ds(u, nd, stride=32), :]
        out[2 * u] = g[:, :nm]
        out[2 * u + 1] = pltpu.roll(g, 64, 1)[:, :nm]

    pltpu.make_async_copy(sbuf.at[pl.ds(0, 15)], sbuf.at[pl.ds(0, 15)], tsend).wait()
    metric_copies(lambda c: c.wait_send())
    pltpu.make_async_copy(mqr.at[:, pl.ds(0, 96)], mqr.at[:, pl.ds(0, 96)], mosend).wait()
    pltpu.make_async_copy(gbuf, gbuf, gssem).wait()
    for c in hops + [cross]:
        c.wait_send()
    swap.wait_send()
    inset = (a // 2) == half

    @pl.when(inset)
    def _():
        pltpu.make_async_copy(krecv.at[pl.ds(0, 224)], krecv.at[pl.ds(0, 224)], kss).wait()

    @pl.when(jnp.logical_not(inset))
    def _():
        pltpu.make_async_copy(krecv, krecv, kss).wait()


def solution(mesh):
    def local_fock(ints_blk, metric_blk, orbitals):
        nq, nm, nl = ints_blk.shape
        nd, _, ni = orbitals.shape
        bt = jnp.transpose(ints_blk, (1, 2, 0))
        mt = metric_blk.T
        ct = jnp.transpose(orbitals, (2, 0, 1)).reshape(ni * nd, nl)
        npair = ni // 4
        V = pltpu.VMEM
        dma = pltpu.SemaphoreType.DMA
        g = pl.pallas_call(
            lambda *refs: kernel(nm, nl, nq, nd, ni, *refs),
            out_shape=pltpu.VMEM((nm, nd, nm), F32),
            in_specs=[pl.BlockSpec(memory_space=pl.ANY)] * 3,
            out_specs=pl.BlockSpec(memory_space=pltpu.VMEM),
            scratch_shapes=[
                V((nm, nl, nq), F32), V((4 * nq, nq), F32), V((ni * nd, nl), F32), V((ni * nd, 256), F32),
                V((8 * SP, LANES), F32), V((16, npair, NT8, 16, LANES), BF), V((4, npair, 4, NT8, 16, LANES), BF),
                V((2, npair, NT8, 16, LANES), BF), V((4, LANES, LANES), F32), V((6, LANES, LANES), F32), V((4, 4, LANES, LANES), F32), V((3, 512, 512), BF),
                V((nd, LANES), F32), V((4, 4, nd, LANES), F32), V((4, nm // 2, nd, LANES), F32), V((3, nm // 2, nd, LANES), F32), V((nm // 2, nd, LANES), F32),
                V((4, 8, 2, 8, 512), F32), V((2, 256, LANES), F32), V((256, LANES), F32), V((256, LANES), F32), V((2, 4, 32, LANES), F32),
                V((8 * 32, LANES), F32), V((15, nd, LANES), F32),
                dma((NT8,)), dma((3,)), dma, dma((npair,)), dma, dma, dma, dma, dma, dma, dma((3,)), dma((3,)), dma, dma, dma, dma],
            compiler_params=pltpu.CompilerParams(collective_id=0, has_side_effects=True, vmem_limit_bytes=60 * 2**20),
        )(bt, mt, ct)
        return jnp.transpose(g, (1, 0, 2))

    return jax.shard_map(local_fock, mesh=mesh, in_specs=(P(('sys', 'aux'), 'orb', None), P(('sys', 'aux'), None), P('sys', None, None)), out_specs=P('sys', 'orb', 'aux'), check_vma=False)
```

```python
import jax
import jax.numpy as jnp
from jax import lax
from jax.experimental import pallas as pl
from jax.experimental.pallas import tpu as pltpu
from jax.sharding import PartitionSpec as P

F32 = jnp.float32
BF = jnp.bfloat16
MESH = pl.DeviceIdType.MESH
NN = (((1,), (0,)), ((), ()))
NT = (((1,), (1,)), ((), ()))
LANES = 128
MROW = 64
NT8 = 7
PIECE = 12
SP = 168


def split3(x):
    hi = x.astype(BF)
    rest = x - hi.astype(F32)
    mid = rest.astype(BF)
    return hi, mid, (rest - mid.astype(F32)).astype(BF)


def dot(x, y, dims):
    return lax.dot_general(x, y, dims, preferred_element_type=F32)


def lhs6(x, axis):
    h, m, l = x
    return jnp.concatenate([h, h, m, m, h, l], axis=axis)


def rhs6(x, axis):
    h, m, l = x
    return jnp.concatenate([h, m, h, m, l, h], axis=axis)


def kernel(nm, nl, nq, nd, ni, bt, mt, ct, out, bv, mv, cv, ctp, tr, sbuf, rbuf, own, mloc, mqr, mq, msp, gsend, grecv, jsend, jrecv, jfwd, zbuf, kacc, kin, kful, kmsg, krecv, gbuf,
           bsem, lsem, tsend, trecv, mzsend, mzrecv, mosend, morecv, gssem, grsem, jssem, jrsem, kxs, kxr, kss, krs):
    sy, a, o = lax.axis_index('sys'), lax.axis_index('aux'), lax.axis_index('orb')
    me = a * 4 + o
    dens, half = me // 2, me % 2
    nh = ni // 2
    npair = nh // 2

    def dev(aa, oo):
        return (sy, aa, oo)

    pltpu.make_async_copy(ct, cv, lsem.at[0]).start()
    pltpu.make_async_copy(bt.at[pl.ds(8 * NT8, 2)], bv.at[pl.ds(8 * NT8, 2)], lsem.at[2]).start()
    for t in range(NT8):
        pltpu.make_async_copy(bt.at[pl.ds(8 * t, 8)], bv.at[pl.ds(8 * t, 8)], bsem.at[t]).start()
        if t == 0:
            pltpu.make_async_copy(mt, mv, lsem.at[1]).start()
    barrier = pltpu.get_barrier_semaphore()

    def tell(k, c):
        g = lax.rem(me + k, 16)
        pl.semaphore_signal(barrier, inc=1, device_id=dev(g // 4, g % 4), device_id_type=MESH)
        return c
    lax.fori_loop(1, 16, tell, 0)

    pltpu.make_async_copy(ct, cv, lsem.at[0]).wait()
    ctp[...] = jnp.concatenate([cv[...], jnp.zeros((nd * ni, 256 - nl), F32)], axis=1)
    lhs = lhs6(split3(ctp[...]), 1)
    pltpu.make_async_copy(mt, mv, lsem.at[1]).wait()
    for b in range(4):
        blk = jnp.concatenate([mv[nq * b:nq * (b + 1), :], jnp.zeros((nq, LANES - nq), F32)], axis=1)
        mloc[b] = jnp.concatenate([blk, jnp.zeros((LANES - nq, LANES), F32)], axis=0)
    pl.semaphore_wait(barrier, 15)

    quarter = pl.ds(pl.multiple_of(o * 32, 32), 32)

    def nearer(x, y, z):
        dx, dy = jnp.abs(x - z), jnp.abs(y - z)
        return jnp.logical_or(dx < dy, jnp.logical_and(dx == dy, x < y))

    def metric_copies(act):
        for k in (2, 1, 3):
            to = lax.rem(a + 4 - k, 4)

            def block(row, slot):
                return pltpu.make_async_remote_copy(src_ref=mloc.at[row, quarter], dst_ref=mqr.at[slot, quarter], send_sem=mzsend,
                                                    recv_sem=mzrecv, device_id=dev(to, o), device_id_type=MESH)
            act(block(a, k - 1))
            for k2 in (1, 2, 3):
                if k2 == k:
                    continue
                b = lax.rem(to + k2, 4)

                @pl.when(nearer(a, b, to))
                def _():
                    act(block(b, k + k2))
    metric_copies(lambda c: c.start())

    gam = jnp.zeros((nd, LANES), F32)
    tr2 = tr

    lane = lax.broadcasted_iota(jnp.int32, (1, LANES), 1)
    data = lane < nq

    def tile(t, gam, tail, first):
        pltpu.make_async_copy(bt.at[pl.ds(0, 8)], bv.at[pl.ds(0, 8)], bsem.at[t]).wait()
        cols = pltpu.roll(ctp[...], lax.rem(512 - (nm * o + 8 * t), 256), 1)
        count = 0
        if tail is not None:
            count = min(8, 10 - first)
            spare = jnp.concatenate([bv[8 * NT8 + tail], jnp.zeros((nl, LANES - nq), F32)], axis=1)
            tcol = pltpu.roll(ctp[...], lax.rem(512 - (nm * o + 8 * NT8 + tail), 256), 1)[:, 0:1]
        for r in range(0, 8, 2):
            xs = []
            for e in range(2):
                x = jnp.concatenate([bv[8 * t + r + e], jnp.zeros((nl, LANES - nq), F32)], axis=1)
                if r + e < count:
                    x = jnp.where(data, x, pltpu.roll(spare, (nq - PIECE * (first + r + e)) % LANES, 1))
                xs.append(x)
            x = jnp.concatenate(xs, axis=1)
            x = jnp.concatenate([x, jnp.zeros((256 - nl, 2 * LANES), F32)], axis=0)
            y = dot(lhs, rhs6(split3(x), 0), NN)
            for e in range(2):
                ye = y[:, e * LANES:(e + 1) * LANES]
                tr2[pl.ds((r + e) * SP, nd * ni), :] = ye
                col = cols[:, r + e:r + e + 1]
                if r + e < count:
                    w = (ye * jnp.where(data, col, tcol)).reshape(ni, nd, LANES).sum(0)
                    moved = pltpu.roll(jnp.where(data, 0.0, w), (PIECE * (first + r + e) - nq) % LANES, 1)
                    gam = gam + jnp.where(data, w, 0.0) + moved
                else:
                    gam = gam + (ye * col).reshape(ni, nd, LANES).sum(0)
        for g in range(16):
            d, h = g // 2, g % 2
            for p in range(npair):
                two = [tr2[pl.ds((h * nh + 2 * p + e) * nd + d, 8, stride=SP), :] for e in range(2)]
                sbuf[g, p, t] = jnp.concatenate(two, axis=0).astype(BF)
        for p in range(npair):
            two = [tr2[pl.ds((half * nh + 2 * p + e) * nd + dens, 8, stride=SP), :] for e in range(2)]
            _, mid, low = split3(jnp.concatenate(two, axis=0))
            own[0, p, t] = mid
            own[1, p, t] = low
        return gam

    def send_t1(p, t0, nt):
        def one(k, c):
            j, u = k % 4, k // 4
            aa = lax.rem(a + 2 + j, 4)
            oo = lax.rem(o + 1 + u, 4)
            g = aa * 4 + oo
            src = sbuf.at[g, p, pl.ds(t0, nt)]
            dst = rbuf.at[a, p, o, pl.ds(t0, nt)]

            @pl.when(k != 14)
            def _():
                pltpu.make_async_remote_copy(src_ref=src, dst_ref=dst, send_sem=tsend, recv_sem=trecv.at[p],
                                             device_id=dev(aa, oo), device_id_type=MESH).start()

            @pl.when(k == 14)
            def _():
                pltpu.make_async_copy(src, dst, trecv.at[p]).start()
            return c
        lax.fori_loop(0, 16, one, 0)

    outer = jnp.logical_or(a == 0, a == 3)
    pair = a + 1 - 2 * (a % 2)

    def send_half(p, t0, nt, cross):
        def one(k, c):
            if cross:
                aa = jnp.where(k % 2 == 0, 3 - a, 3 - pair)
                oo = lax.rem(o + 1 + k // 2, 4)
            else:
                aa = jnp.where(k % 2 == 0, pair, a)
                oo = lax.rem(o + 1 + k // 2, 4)
            g = aa * 4 + oo
            src = sbuf.at[g, p, pl.ds(t0, nt)]
            dst = rbuf.at[a, p, o, pl.ds(t0, nt)]

            def far():
                pltpu.make_async_remote_copy(src_ref=src, dst_ref=dst, send_sem=tsend, recv_sem=trecv.at[p],
                                             device_id=dev(aa, oo), device_id_type=MESH).start()
            if cross:
                far()
            else:
                pl.when(k != 7)(far)

                @pl.when(k == 7)
                def _():
                    pltpu.make_async_copy(src, dst, trecv.at[p]).start()
            return c
        lax.fori_loop(0, 8, one, 0)

    pltpu.make_async_copy(bt.at[pl.ds(0, 2)], bv.at[pl.ds(0, 2)], lsem.at[2]).wait()

    def two_tiles(u, gam):
        gam = tile(2 * u, gam, u, 0)
        send_t1(0, 2 * u, 1)
        gam = tile(2 * u + 1, gam, u, 8)
        send_t1(0, 2 * u + 1, 1)
        return gam
    gam = lax.fori_loop(0, 2, two_tiles, gam)

    def one_tile(t, gam):
        gam = tile(t, gam, None, 0)
        send_t1(0, t, 1)
        return gam
    gam = lax.fori_loop(4, NT8, one_tile, gam)

    gsend[...] = gam

    def gs(k, c):
        g = lax.rem(me + k, 16)
        pltpu.make_async_remote_copy(src_ref=gsend, dst_ref=grecv.at[a, o], send_sem=gssem, recv_sem=grsem,
                                     device_id=dev(g // 4, g % 4), device_id_type=MESH).start()
        return c
    lax.fori_loop(1, 16, gs, 0)
    pltpu.make_async_copy(gsend, grecv.at[a, o], grsem).start()

    pltpu.make_async_copy(mqr.at[:, pl.ds(0, 32)], mqr.at[:, pl.ds(0, 32)], mzrecv).wait()

    def mo(k, c):
        oo = lax.rem(o + k, 4)
        pltpu.make_async_remote_copy(src_ref=mqr.at[:, quarter], dst_ref=mqr.at[:, quarter], send_sem=mosend, recv_sem=morecv,
                                     device_id=dev(a, oo), device_id_type=MESH).start()
        return c
    lax.fori_loop(1, 4, mo, 0)
    @pl.when(outer)
    def _():
        send_half(1, 0, NT8, False)
        send_half(2, 0, NT8, False)
        send_half(1, 0, NT8, True)
        send_half(3, 0, NT8, False)
        send_half(4, 0, NT8, False)
        send_half(2, 0, NT8, True)

    @pl.when(jnp.logical_not(outer))
    def _():
        for p in range(1, 3):
            send_t1(p, 0, NT8)
    mq[a] = mloc[...]
    for k in range(1, 4):
        c1 = lax.rem(a + k, 4)
        mq[c1, a] = mloc[c1].T
    pltpu.make_async_copy(mqr.at[:, pl.ds(0, 96)], mqr.at[:, pl.ds(0, 96)], morecv).wait()
    for k in range(1, 4):
        c1 = lax.rem(a + k, 4)
        mq[c1, c1] = mqr[k - 1]
        for k2 in range(k + 1, 4):
            c2 = lax.rem(a + k2, 4)
            first = jnp.where(nearer(c1, c2, a), c1, c2)
            second = c1 + c2 - first
            blk = mqr[k + k2]
            mq[first, second] = blk
            mq[second, first] = blk.T
    for b in range(4):
        parts = split3(jnp.concatenate([mq[aa, b] for aa in range(4)], axis=1))
        for s in range(3):
            msp[s, pl.ds(b * LANES, LANES)] = parts[s]

    pltpu.make_async_copy(grecv, grecv, grsem).wait()
    graw = jnp.concatenate([grecv[aa, 0] + grecv[aa, 1] + grecv[aa, 2] + grecv[aa, 3] for aa in range(4)], axis=1)
    m3 = [msp[s] for s in range(3)]
    gfit = dot(lhs6(split3(graw), 1), rhs6(m3, 0), NN)
    mown = split3(jnp.concatenate([mloc[b] for b in range(4)], axis=0))
    wts = dot(lhs6(split3(gfit), 1), rhs6(mown, 0), NN)
    wl = lhs6(split3(wts), 1)
    low64 = lax.broadcasted_iota(jnp.int32, (nd, LANES), 1) < 64

    def jpair(u, c):
        ys = []
        for e in range(2):
            x = jnp.concatenate([bv[2 * u + e], jnp.zeros((nl, LANES - nq), F32)], axis=1)
            x = jnp.concatenate([x, jnp.zeros((256 - nl, LANES), F32)], axis=0)
            ys.append(dot(wl, rhs6(split3(x), 1), NT))
        for aa in range(4):
            lo = pltpu.roll(ys[0], (256 - nm * aa) % 256, 1)[:, :LANES]
            hi = pltpu.roll(ys[1], (256 + 64 - nm * aa) % 256, 1)[:, :LANES]
            jsend[aa, u] = jnp.where(low64, lo, hi)
        return c

    row8 = lax.broadcasted_iota(jnp.int32, (8, LANES), 0)
    lane8 = lax.broadcasted_iota(jnp.int32, (8, LANES), 1)
    at0 = lane8 - PIECE * row8
    at1 = lane8 - PIECE * (row8 + 8)
    here0 = jnp.logical_and(at0 >= 0, at0 < PIECE)
    here1 = jnp.logical_and(jnp.logical_and(at1 >= 0, at1 < PIECE), lane8 < nq)
    zbuf[:, NT8] = jnp.zeros((4, 2, 8, 512), F32)

    def tails(x):
        f = [x[t].astype(F32) for t in range(4)]
        out = []
        for e in range(2):
            for u in range(2):
                v0 = pltpu.roll(f[2 * u][8 * e:8 * e + 8], LANES - nq, 1, stride=PIECE, stride_axis=0)
                f1 = f[2 * u + 1][8 * e:8 * e + 8]
                v1 = jnp.where(row8 == 0, pltpu.roll(f1, (8 * PIECE - nq) % LANES, 1), pltpu.roll(f1, (9 * PIECE - nq) % LANES, 1))
                v = jnp.where(here0, v0, jnp.where(here1, v1, 0.0))
                out.append(v.sum(0, keepdims=True))
        return out

    def fit(p):
        pltpu.make_async_copy(rbuf.at[:, p], rbuf.at[:, p], trecv.at[p]).wait()
        if p + 3 < npair:
            @pl.when(jnp.logical_not(outer))
            def _():
                send_half(p + 3, 0, NT8, True)
        xs = []
        for s in range(4):
            rest = [w for q in range(4) for w in tails(rbuf[s, p, q, pl.ds(0, 4)])]
            xs.append(jnp.concatenate([rbuf[s, p].reshape(4 * NT8 * 16, LANES), jnp.concatenate(rest, axis=0).astype(BF)], axis=0))
        x = jnp.concatenate(xs, axis=1)
        z = dot(jnp.concatenate([x, x, x], axis=1), msp[...].reshape(3 * 512, 512), NN)
        main = 4 * NT8 * 16
        zbuf[:, pl.ds(0, NT8)] = z[:main].reshape(4, NT8, 2, 8, 512)
        for q in range(4):
            for e in range(2):
                zbuf[q, NT8, e, pl.ds(0, 2)] = z[main + 4 * q + 2 * e:main + 4 * q + 2 * e + 2]
        ml = []
        for s in range(2):
            rest = tails(own[s, p, pl.ds(0, 4)]) + [jnp.zeros((12, LANES), F32)]
            ml.append(jnp.concatenate([own[s, p].reshape(NT8 * 16, LANES), jnp.concatenate(rest, axis=0).astype(BF)], axis=0))
        mid, low = ml
        rows = pl.ds(pl.multiple_of(a * LANES, LANES), LANES)
        mh, mm = msp[0, rows], msp[1, rows]
        z = dot(jnp.concatenate([mid, mid, low], axis=1), jnp.concatenate([mh, mm, mh], axis=0), NN)
        zbuf[o, pl.ds(0, NT8)] = zbuf[o, pl.ds(0, NT8)] + z[:NT8 * 16].reshape(NT8, 2, 8, 512)
        for e in range(2):
            zbuf[o, NT8, e, pl.ds(0, 2)] = zbuf[o, NT8, e, pl.ds(0, 2)] + z[NT8 * 16 + 2 * e:NT8 * 16 + 2 * e + 2]
        for e in range(2):
            s3 = split3(zbuf[:, :, e].reshape(4 * MROW, 512))
            k = dot(lhs6(s3, 1), rhs6(s3, 1), NT)
            if p == 0 and e == 0:
                kacc[0] = k[:, :LANES]
                kacc[1] = k[:, LANES:]
            else:
                kacc[0] = kacc[0] + k[:, :LANES]
                kacc[1] = kacc[1] + k[:, LANES:]

    lax.fori_loop(0, nm // 2, jpair, 0)
    near, far = a + 1 - 2 * (a % 2), lax.rem(a + 2, 4)
    hops = []
    for e, aa in enumerate((lax.rem(near + 2, 4), near)):
        hops.append(pltpu.make_async_remote_copy(src_ref=jsend.at[aa], dst_ref=jrecv.at[e], send_sem=jssem.at[e], recv_sem=jrsem.at[e],
                                                 device_id=dev(near, o), device_id_type=MESH))
        hops[-1].start()
    @pl.when(outer)
    def _():
        for p in range(3, npair):
            send_half(p, 0, NT8, True)

    @pl.when(jnp.logical_not(outer))
    def _():
        for p in range(3, npair):
            send_half(p, 0, NT8, False)
    for p in range(npair - 1):
        fit(p)
    hops[0].wait_recv()
    jfwd[...] = jsend[far] + jrecv[0]
    cross = pltpu.make_async_remote_copy(src_ref=jfwd, dst_ref=jrecv.at[2], send_sem=jssem.at[2], recv_sem=jrsem.at[2],
                                         device_id=dev(far, o), device_id_type=MESH)
    cross.start()
    fit(npair - 1)

    mate = o + 1 - 2 * half
    swap = pltpu.make_async_remote_copy(src_ref=kacc.at[1 - half], dst_ref=kin, send_sem=kxs, recv_sem=kxr,
                                        device_id=dev(a, mate), device_id_type=MESH)
    swap.start()
    swap.wait_recv()
    kful[...] = kacc[half] + kin[...]
    low32 = lax.broadcasted_iota(jnp.int32, (32, LANES), 1) < 64
    for oo in range(4):
        ev = kful[pl.ds(MROW * oo, 32, stride=2), :]
        od = kful[pl.ds(MROW * oo + 1, 32, stride=2), :]
        kmsg[0, oo] = jnp.where(low32, ev, pltpu.roll(od, 64, 1))
        kmsg[1, oo] = jnp.where(low32, pltpu.roll(ev, 64, 1), od)

    def ks(k, c):
        al, oo = k // 4, k % 4
        aa = 2 * half + al
        same = jnp.logical_and(aa == a, oo == o)

        @pl.when(jnp.logical_not(same))
        def _():
            pltpu.make_async_remote_copy(src_ref=kmsg.at[al, oo], dst_ref=krecv.at[pl.ds(dens * 32, 32)], send_sem=kss, recv_sem=krs,
                                         device_id=dev(aa, oo), device_id_type=MESH).start()

        @pl.when(same)
        def _():
            cp = pltpu.make_async_copy(kmsg.at[al, oo], krecv.at[pl.ds(dens * 32, 32)], krs)
            cp.start()
        return c
    lax.fori_loop(0, 8, ks, 0)

    hops[1].wait_recv()
    cross.wait_recv()
    pltpu.make_async_copy(krecv, krecv, krs).wait()
    for u in range(nm // 2):
        j = jsend[a, u] + jrecv[1, u] + jrecv[2, u]
        g = 2.0 * j - krecv[pl.ds(u, nd, stride=32), :]
        out[2 * u] = g[:, :nm]
        out[2 * u + 1] = pltpu.roll(g, 64, 1)[:, :nm]

    pltpu.make_async_copy(sbuf.at[pl.ds(0, 15)], sbuf.at[pl.ds(0, 15)], tsend).wait()
    metric_copies(lambda c: c.wait_send())
    pltpu.make_async_copy(mqr.at[:, pl.ds(0, 96)], mqr.at[:, pl.ds(0, 96)], mosend).wait()
    pltpu.make_async_copy(gbuf, gbuf, gssem).wait()
    for c in hops + [cross]:
        c.wait_send()
    swap.wait_send()
    inset = (a // 2) == half

    @pl.when(inset)
    def _():
        pltpu.make_async_copy(krecv.at[pl.ds(0, 224)], krecv.at[pl.ds(0, 224)], kss).wait()

    @pl.when(jnp.logical_not(inset))
    def _():
        pltpu.make_async_copy(krecv, krecv, kss).wait()


def solution(mesh):
    def local_fock(ints_blk, metric_blk, orbitals):
        nq, nm, nl = ints_blk.shape
        nd, _, ni = orbitals.shape
        bt = jnp.transpose(ints_blk, (1, 2, 0))
        mt = metric_blk.T
        ct = jnp.transpose(orbitals, (2, 0, 1)).reshape(ni * nd, nl)
        npair = ni // 4
        V = pltpu.VMEM
        dma = pltpu.SemaphoreType.DMA
        g = pl.pallas_call(
            lambda *refs: kernel(nm, nl, nq, nd, ni, *refs),
            out_shape=pltpu.VMEM((nm, nd, nm), F32),
            in_specs=[pl.BlockSpec(memory_space=pl.ANY)] * 3,
            out_specs=pl.BlockSpec(memory_space=pltpu.VMEM),
            scratch_shapes=[
                V((nm, nl, nq), F32), V((4 * nq, nq), F32), V((ni * nd, nl), F32), V((ni * nd, 256), F32),
                V((8 * SP, LANES), F32), V((16, npair, NT8, 16, LANES), BF), V((4, npair, 4, NT8, 16, LANES), BF),
                V((2, npair, NT8, 16, LANES), BF), V((4, LANES, LANES), F32), V((6, LANES, LANES), F32), V((4, 4, LANES, LANES), F32), V((3, 512, 512), BF),
                V((nd, LANES), F32), V((4, 4, nd, LANES), F32), V((4, nm // 2, nd, LANES), F32), V((3, nm // 2, nd, LANES), F32), V((nm // 2, nd, LANES), F32),
                V((4, 8, 2, 8, 512), F32), V((2, 256, LANES), F32), V((256, LANES), F32), V((256, LANES), F32), V((2, 4, 32, LANES), F32),
                V((8 * 32, LANES), F32), V((15, nd, LANES), F32),
                dma((NT8,)), dma((3,)), dma, dma((npair,)), dma, dma, dma, dma, dma, dma, dma((3,)), dma((3,)), dma, dma, dma, dma],
            compiler_params=pltpu.CompilerParams(collective_id=0, has_side_effects=True, vmem_limit_bytes=60 * 2**20),
        )(bt, mt, ct)
        return jnp.transpose(g, (1, 0, 2))

    return jax.shard_map(local_fock, mesh=mesh, in_specs=(P(('sys', 'aux'), 'orb', None), P(('sys', 'aux'), None), P('sys', None, None)), out_specs=P('sys', 'orb', 'aux'), check_vma=False)
```

```python
import jax
import jax.numpy as jnp
from jax import lax
from jax.experimental import pallas as pl
from jax.experimental.pallas import tpu as pltpu
from jax.sharding import PartitionSpec as P

F32 = jnp.float32
BF = jnp.bfloat16
MESH = pl.DeviceIdType.MESH
NN = (((1,), (0,)), ((), ()))
NT = (((1,), (1,)), ((), ()))
LANES = 128
MROW = 64
NT8 = 7
PIECE = 12
SP = 168


def split3(x):
    hi = x.astype(BF)
    rest = x - hi.astype(F32)
    mid = rest.astype(BF)
    return hi, mid, (rest - mid.astype(F32)).astype(BF)


def dot(x, y, dims):
    return lax.dot_general(x, y, dims, preferred_element_type=F32)


def lhs6(x, axis):
    h, m, l = x
    return jnp.concatenate([h, h, m, m, h, l], axis=axis)


def rhs6(x, axis):
    h, m, l = x
    return jnp.concatenate([h, m, h, m, l, h], axis=axis)


def kernel(nm, nl, nq, nd, ni, bt, mt, ct, out, bv, mv, cv, ctp, tr, sbuf, rbuf, own, mloc, mqr, mq, msp, gsend, grecv, jsend, jrecv, jfwd, zbuf, kacc, kin, kful, kmsg, krecv, gbuf,
           bsem, lsem, tsend, trecv, mzsend, mzrecv, mosend, morecv, gssem, grsem, jssem, jrsem, kxs, kxr, kss, krs):
    sy, a, o = lax.axis_index('sys'), lax.axis_index('aux'), lax.axis_index('orb')
    me = a * 4 + o
    dens, half = me // 2, me % 2
    nh = ni // 2
    npair = nh // 2

    def dev(aa, oo):
        return (sy, aa, oo)

    pltpu.make_async_copy(mt, mv, lsem.at[1]).start()
    pltpu.make_async_copy(ct, cv, lsem.at[0]).start()
    pltpu.make_async_copy(bt.at[pl.ds(8 * NT8, 2)], bv.at[pl.ds(8 * NT8, 2)], lsem.at[2]).start()
    for t in range(NT8):
        pltpu.make_async_copy(bt.at[pl.ds(8 * t, 8)], bv.at[pl.ds(8 * t, 8)], bsem.at[t]).start()
    barrier = pltpu.get_barrier_semaphore()

    def tell(k, c):
        g = lax.rem(me + k, 16)
        pl.semaphore_signal(barrier, inc=1, device_id=dev(g // 4, g % 4), device_id_type=MESH)
        return c
    lax.fori_loop(1, 16, tell, 0)

    pltpu.make_async_copy(mt, mv, lsem.at[1]).wait()
    for b in range(4):
        blk = jnp.concatenate([mv[nq * b:nq * (b + 1), :], jnp.zeros((nq, LANES - nq), F32)], axis=1)
        mloc[b] = jnp.concatenate([blk, jnp.zeros((LANES - nq, LANES), F32)], axis=0)
    pl.semaphore_wait(barrier, 15)

    quarter = pl.ds(pl.multiple_of(o * 32, 32), 32)

    def nearer(x, y, z):
        dx, dy = jnp.abs(x - z), jnp.abs(y - z)
        return jnp.logical_or(dx < dy, jnp.logical_and(dx == dy, x < y))

    def metric_copies(act):
        for k in (2, 1, 3):
            to = lax.rem(a + 4 - k, 4)

            def block(row, slot):
                return pltpu.make_async_remote_copy(src_ref=mloc.at[row, quarter], dst_ref=mqr.at[slot, quarter], send_sem=mzsend,
                                                    recv_sem=mzrecv, device_id=dev(to, o), device_id_type=MESH)
            act(block(a, k - 1))
            for k2 in (1, 2, 3):
                if k2 == k:
                    continue
                b = lax.rem(to + k2, 4)

                @pl.when(nearer(a, b, to))
                def _():
                    act(block(b, k + k2))
    metric_copies(lambda c: c.start())

    pltpu.make_async_copy(ct, cv, lsem.at[0]).wait()
    ctp[...] = jnp.concatenate([cv[...], jnp.zeros((nd * ni, 256 - nl), F32)], axis=1)
    lhs = lhs6(split3(ctp[...]), 1)

    gam = jnp.zeros((nd, LANES), F32)
    tr2 = tr

    lane = lax.broadcasted_iota(jnp.int32, (1, LANES), 1)
    data = lane < nq

    def tile(t, gam, tail, first):
        pltpu.make_async_copy(bt.at[pl.ds(0, 8)], bv.at[pl.ds(0, 8)], bsem.at[t]).wait()
        cols = pltpu.roll(ctp[...], lax.rem(512 - (nm * o + 8 * t), 256), 1)
        count = 0
        if tail is not None:
            count = min(8, 10 - first)
            spare = jnp.concatenate([bv[8 * NT8 + tail], jnp.zeros((nl, LANES - nq), F32)], axis=1)
            tcol = pltpu.roll(ctp[...], lax.rem(512 - (nm * o + 8 * NT8 + tail), 256), 1)[:, 0:1]
        for r in range(0, 8, 2):
            xs = []
            for e in range(2):
                x = jnp.concatenate([bv[8 * t + r + e], jnp.zeros((nl, LANES - nq), F32)], axis=1)
                if r + e < count:
                    x = jnp.where(data, x, pltpu.roll(spare, (nq - PIECE * (first + r + e)) % LANES, 1))
                xs.append(x)
            x = jnp.concatenate(xs, axis=1)
            x = jnp.concatenate([x, jnp.zeros((256 - nl, 2 * LANES), F32)], axis=0)
            y = dot(lhs, rhs6(split3(x), 0), NN)
            for e in range(2):
                ye = y[:, e * LANES:(e + 1) * LANES]
                tr2[pl.ds((r + e) * SP, nd * ni), :] = ye
                col = cols[:, r + e:r + e + 1]
                if r + e < count:
                    w = (ye * jnp.where(data, col, tcol)).reshape(ni, nd, LANES).sum(0)
                    moved = pltpu.roll(jnp.where(data, 0.0, w), (PIECE * (first + r + e) - nq) % LANES, 1)
                    gam = gam + jnp.where(data, w, 0.0) + moved
                else:
                    gam = gam + (ye * col).reshape(ni, nd, LANES).sum(0)
        for g in range(16):
            d, h = g // 2, g % 2
            for p in range(npair):
                two = [tr2[pl.ds((h * nh + 2 * p + e) * nd + d, 8, stride=SP), :] for e in range(2)]
                sbuf[g, p, t] = jnp.concatenate(two, axis=0).astype(BF)
        for p in range(npair):
            two = [tr2[pl.ds((half * nh + 2 * p + e) * nd + dens, 8, stride=SP), :] for e in range(2)]
            _, mid, low = split3(jnp.concatenate(two, axis=0))
            own[0, p, t] = mid
            own[1, p, t] = low
        return gam

    def send_t1(p, t0, nt):
        def one(k, c):
            j, u = k % 4, k // 4
            aa = lax.rem(a + 2 + j, 4)
            oo = lax.rem(o + 1 + u, 4)
            g = aa * 4 + oo
            src = sbuf.at[g, p, pl.ds(t0, nt)]
            dst = rbuf.at[a, p, o, pl.ds(t0, nt)]

            @pl.when(k != 14)
            def _():
                pltpu.make_async_remote_copy(src_ref=src, dst_ref=dst, send_sem=tsend, recv_sem=trecv.at[p],
                                             device_id=dev(aa, oo), device_id_type=MESH).start()

            @pl.when(k == 14)
            def _():
                pltpu.make_async_copy(src, dst, trecv.at[p]).start()
            return c
        lax.fori_loop(0, 16, one, 0)

    outer = jnp.logical_or(a == 0, a == 3)
    pair = a + 1 - 2 * (a % 2)

    def send_half(p, t0, nt, cross):
        def one(k, c):
            if cross:
                aa = jnp.where(k % 2 == 0, 3 - a, 3 - pair)
                oo = lax.rem(o + 1 + k // 2, 4)
            else:
                aa = jnp.where(k % 2 == 0, pair, a)
                oo = lax.rem(o + 1 + k // 2, 4)
            g = aa * 4 + oo
            src = sbuf.at[g, p, pl.ds(t0, nt)]
            dst = rbuf.at[a, p, o, pl.ds(t0, nt)]

            def far():
                pltpu.make_async_remote_copy(src_ref=src, dst_ref=dst, send_sem=tsend, recv_sem=trecv.at[p],
                                             device_id=dev(aa, oo), device_id_type=MESH).start()
            if cross:
                far()
            else:
                pl.when(k != 7)(far)

                @pl.when(k == 7)
                def _():
                    pltpu.make_async_copy(src, dst, trecv.at[p]).start()
            return c
        lax.fori_loop(0, 8, one, 0)

    pltpu.make_async_copy(bt.at[pl.ds(0, 2)], bv.at[pl.ds(0, 2)], lsem.at[2]).wait()

    def two_tiles(u, gam):
        gam = tile(2 * u, gam, u, 0)
        send_t1(0, 2 * u, 1)
        gam = tile(2 * u + 1, gam, u, 8)
        send_t1(0, 2 * u + 1, 1)
        return gam
    gam = lax.fori_loop(0, 2, two_tiles, gam)

    def one_tile(t, gam):
        gam = tile(t, gam, None, 0)
        send_t1(0, t, 1)
        return gam
    gam = lax.fori_loop(4, NT8, one_tile, gam)

    gsend[...] = gam

    def gs(k, c):
        g = lax.rem(me + k, 16)
        pltpu.make_async_remote_copy(src_ref=gsend, dst_ref=grecv.at[a, o], send_sem=gssem, recv_sem=grsem,
                                     device_id=dev(g // 4, g % 4), device_id_type=MESH).start()
        return c
    lax.fori_loop(1, 16, gs, 0)
    pltpu.make_async_copy(gsend, grecv.at[a, o], grsem).start()

    pltpu.make_async_copy(mqr.at[:, pl.ds(0, 32)], mqr.at[:, pl.ds(0, 32)], mzrecv).wait()

    def mo(k, c):
        oo = lax.rem(o + k, 4)
        pltpu.make_async_remote_copy(src_ref=mqr.at[:, quarter], dst_ref=mqr.at[:, quarter], send_sem=mosend, recv_sem=morecv,
                                     device_id=dev(a, oo), device_id_type=MESH).start()
        return c
    lax.fori_loop(1, 4, mo, 0)
    @pl.when(outer)
    def _():
        send_half(1, 0, NT8, False)
        send_half(2, 0, NT8, False)
        send_half(1, 0, NT8, True)
        send_half(3, 0, NT8, False)
        send_half(4, 0, NT8, False)
        send_half(2, 0, NT8, True)

    @pl.when(jnp.logical_not(outer))
    def _():
        for p in range(1, 3):
            send_t1(p, 0, NT8)
    mq[a] = mloc[...]
    for k in range(1, 4):
        c1 = lax.rem(a + k, 4)
        mq[c1, a] = mloc[c1].T
    pltpu.make_async_copy(mqr.at[:, pl.ds(0, 96)], mqr.at[:, pl.ds(0, 96)], morecv).wait()
    for k in range(1, 4):
        c1 = lax.rem(a + k, 4)
        mq[c1, c1] = mqr[k - 1]
        for k2 in range(k + 1, 4):
            c2 = lax.rem(a + k2, 4)
            first = jnp.where(nearer(c1, c2, a), c1, c2)
            second = c1 + c2 - first
            blk = mqr[k + k2]
            mq[first, second] = blk
            mq[second, first] = blk.T
    for b in range(4):
        parts = split3(jnp.concatenate([mq[aa, b] for aa in range(4)], axis=1))
        for s in range(3):
            msp[s, pl.ds(b * LANES, LANES)] = parts[s]

    pltpu.make_async_copy(grecv, grecv, grsem).wait()
    graw = jnp.concatenate([grecv[aa, 0] + grecv[aa, 1] + grecv[aa, 2] + grecv[aa, 3] for aa in range(4)], axis=1)
    m3 = [msp[s] for s in range(3)]
    gfit = dot(lhs6(split3(graw), 1), rhs6(m3, 0), NN)
    mown = split3(jnp.concatenate([mloc[b] for b in range(4)], axis=0))
    wts = dot(lhs6(split3(gfit), 1), rhs6(mown, 0), NN)
    wl = lhs6(split3(wts), 1)
    low64 = lax.broadcasted_iota(jnp.int32, (nd, LANES), 1) < 64

    def jpair(u, c):
        ys = []
        for e in range(2):
            x = jnp.concatenate([bv[2 * u + e], jnp.zeros((nl, LANES - nq), F32)], axis=1)
            x = jnp.concatenate([x, jnp.zeros((256 - nl, LANES), F32)], axis=0)
            ys.append(dot(wl, rhs6(split3(x), 1), NT))
        for aa in range(4):
            lo = pltpu.roll(ys[0], (256 - nm * aa) % 256, 1)[:, :LANES]
            hi = pltpu.roll(ys[1], (256 + 64 - nm * aa) % 256, 1)[:, :LANES]
            jsend[aa, u] = jnp.where(low64, lo, hi)
        return c

    row8 = lax.broadcasted_iota(jnp.int32, (8, LANES), 0)
    lane8 = lax.broadcasted_iota(jnp.int32, (8, LANES), 1)
    at0 = lane8 - PIECE * row8
    at1 = lane8 - PIECE * (row8 + 8)
    here0 = jnp.logical_and(at0 >= 0, at0 < PIECE)
    here1 = jnp.logical_and(jnp.logical_and(at1 >= 0, at1 < PIECE), lane8 < nq)
    zbuf[:, NT8] = jnp.zeros((4, 2, 8, 512), F32)

    def tails(x):
        f = [x[t].astype(F32) for t in range(4)]
        out = []
        for e in range(2):
            for u in range(2):
                v0 = pltpu.roll(f[2 * u][8 * e:8 * e + 8], LANES - nq, 1, stride=PIECE, stride_axis=0)
                f1 = f[2 * u + 1][8 * e:8 * e + 8]
                v1 = jnp.where(row8 == 0, pltpu.roll(f1, (8 * PIECE - nq) % LANES, 1), pltpu.roll(f1, (9 * PIECE - nq) % LANES, 1))
                v = jnp.where(here0, v0, jnp.where(here1, v1, 0.0))
                out.append(v.sum(0, keepdims=True))
        return out

    def fit(p):
        pltpu.make_async_copy(rbuf.at[:, p], rbuf.at[:, p], trecv.at[p]).wait()
        if p + 3 < npair:
            @pl.when(jnp.logical_not(outer))
            def _():
                send_half(p + 3, 0, NT8, True)
        xs = []
        for s in range(4):
            rest = [w for q in range(4) for w in tails(rbuf[s, p, q, pl.ds(0, 4)])]
            xs.append(jnp.concatenate([rbuf[s, p].reshape(4 * NT8 * 16, LANES), jnp.concatenate(rest, axis=0).astype(BF)], axis=0))
        x = jnp.concatenate(xs, axis=1)
        z = dot(jnp.concatenate([x, x, x], axis=1), msp[...].reshape(3 * 512, 512), NN)
        main = 4 * NT8 * 16
        zbuf[:, pl.ds(0, NT8)] = z[:main].reshape(4, NT8, 2, 8, 512)
        for q in range(4):
            for e in range(2):
                zbuf[q, NT8, e, pl.ds(0, 2)] = z[main + 4 * q + 2 * e:main + 4 * q + 2 * e + 2]
        ml = []
        for s in range(2):
            rest = tails(own[s, p, pl.ds(0, 4)]) + [jnp.zeros((12, LANES), F32)]
            ml.append(jnp.concatenate([own[s, p].reshape(NT8 * 16, LANES), jnp.concatenate(rest, axis=0).astype(BF)], axis=0))
        mid, low = ml
        rows = pl.ds(pl.multiple_of(a * LANES, LANES), LANES)
        mh, mm = msp[0, rows], msp[1, rows]
        z = dot(jnp.concatenate([mid, mid, low], axis=1), jnp.concatenate([mh, mm, mh], axis=0), NN)
        zbuf[o, pl.ds(0, NT8)] = zbuf[o, pl.ds(0, NT8)] + z[:NT8 * 16].reshape(NT8, 2, 8, 512)
        for e in range(2):
            zbuf[o, NT8, e, pl.ds(0, 2)] = zbuf[o, NT8, e, pl.ds(0, 2)] + z[NT8 * 16 + 2 * e:NT8 * 16 + 2 * e + 2]
        for e in range(2):
            s3 = split3(zbuf[:, :, e].reshape(4 * MROW, 512))
            k = dot(lhs6(s3, 1), rhs6(s3, 1), NT)
            if p == 0 and e == 0:
                kacc[0] = k[:, :LANES]
                kacc[1] = k[:, LANES:]
            else:
                kacc[0] = kacc[0] + k[:, :LANES]
                kacc[1] = kacc[1] + k[:, LANES:]

    lax.fori_loop(0, nm // 2, jpair, 0)
    inner = jnp.logical_not(outer)
    fars = (3 - pair, 3 - a)

    def jhop(aa, e):
        return pltpu.make_async_remote_copy(src_ref=jsend.at[aa], dst_ref=jrecv.at[e], send_sem=jssem.at[e], recv_sem=jrsem.at[e],
                                            device_id=dev(pair, o), device_id_type=MESH)

    def jcross(e):
        return pltpu.make_async_remote_copy(src_ref=jfwd.at[e], dst_ref=jrecv.at[3], send_sem=jssem.at[3 + e], recv_sem=jrsem.at[3],
                                            device_id=dev(fars[e], o), device_id_type=MESH)

    @pl.when(outer)
    def _():
        jhop(3 - a, 0).start()
        jhop(3 - pair, 1).start()
    jhop(pair, 2).start()
    @pl.when(outer)
    def _():
        for p in range(3, npair):
            send_half(p, 0, NT8, True)

    @pl.when(jnp.logical_not(outer))
    def _():
        for p in range(3, npair):
            send_half(p, 0, NT8, False)
    for p in range(3):
        fit(p)

    @pl.when(inner)
    def _():
        for e in range(2):
            jhop(pair, e).wait_recv()
            jfwd[e] = jsend[fars[e]] + jrecv[e]
            jcross(e).start()
    for p in range(3, npair):
        fit(p)

    mate = o + 1 - 2 * half
    swap = pltpu.make_async_remote_copy(src_ref=kacc.at[1 - half], dst_ref=kin, send_sem=kxs, recv_sem=kxr,
                                        device_id=dev(a, mate), device_id_type=MESH)
    swap.start()
    swap.wait_recv()
    kful[...] = kacc[half] + kin[...]
    low32 = lax.broadcasted_iota(jnp.int32, (32, LANES), 1) < 64
    for oo in range(4):
        ev = kful[pl.ds(MROW * oo, 32, stride=2), :]
        od = kful[pl.ds(MROW * oo + 1, 32, stride=2), :]
        kmsg[0, oo] = jnp.where(low32, ev, pltpu.roll(od, 64, 1))
        kmsg[1, oo] = jnp.where(low32, pltpu.roll(ev, 64, 1), od)

    def ks(k, c):
        al, oo = k // 4, k % 4
        aa = 2 * half + al
        same = jnp.logical_and(aa == a, oo == o)

        @pl.when(jnp.logical_not(same))
        def _():
            pltpu.make_async_remote_copy(src_ref=kmsg.at[al, oo], dst_ref=krecv.at[pl.ds(dens * 32, 32)], send_sem=kss, recv_sem=krs,
                                         device_id=dev(aa, oo), device_id_type=MESH).start()

        @pl.when(same)
        def _():
            cp = pltpu.make_async_copy(kmsg.at[al, oo], krecv.at[pl.ds(dens * 32, 32)], krs)
            cp.start()
        return c
    lax.fori_loop(0, 8, ks, 0)

    jhop(pair, 2).wait_recv()
    jcross(0).wait_recv()
    pltpu.make_async_copy(krecv, krecv, krs).wait()
    for u in range(nm // 2):
        j = jsend[a, u] + jrecv[2, u] + jrecv[3, u]
        g = 2.0 * j - krecv[pl.ds(u, nd, stride=32), :]
        out[2 * u] = g[:, :nm]
        out[2 * u + 1] = pltpu.roll(g, 64, 1)[:, :nm]

    pltpu.make_async_copy(sbuf.at[pl.ds(0, 15)], sbuf.at[pl.ds(0, 15)], tsend).wait()
    metric_copies(lambda c: c.wait_send())
    pltpu.make_async_copy(mqr.at[:, pl.ds(0, 96)], mqr.at[:, pl.ds(0, 96)], mosend).wait()
    pltpu.make_async_copy(gbuf, gbuf, gssem).wait()
    jhop(pair, 2).wait_send()

    @pl.when(outer)
    def _():
        jhop(3 - a, 0).wait_send()
        jhop(3 - pair, 1).wait_send()

    @pl.when(inner)
    def _():
        jcross(0).wait_send()
        jcross(1).wait_send()
    swap.wait_send()
    inset = (a // 2) == half

    @pl.when(inset)
    def _():
        pltpu.make_async_copy(krecv.at[pl.ds(0, 224)], krecv.at[pl.ds(0, 224)], kss).wait()

    @pl.when(jnp.logical_not(inset))
    def _():
        pltpu.make_async_copy(krecv, krecv, kss).wait()


def solution(mesh):
    def local_fock(ints_blk, metric_blk, orbitals):
        nq, nm, nl = ints_blk.shape
        nd, _, ni = orbitals.shape
        bt = jnp.transpose(ints_blk, (1, 2, 0))
        mt = metric_blk.T
        ct = jnp.transpose(orbitals, (2, 0, 1)).reshape(ni * nd, nl)
        npair = ni // 4
        V = pltpu.VMEM
        dma = pltpu.SemaphoreType.DMA
        g = pl.pallas_call(
            lambda *refs: kernel(nm, nl, nq, nd, ni, *refs),
            out_shape=pltpu.VMEM((nm, nd, nm), F32),
            in_specs=[pl.BlockSpec(memory_space=pl.ANY)] * 3,
            out_specs=pl.BlockSpec(memory_space=pltpu.VMEM),
            scratch_shapes=[
                V((nm, nl, nq), F32), V((4 * nq, nq), F32), V((ni * nd, nl), F32), V((ni * nd, 256), F32),
                V((8 * SP, LANES), F32), V((16, npair, NT8, 16, LANES), BF), V((4, npair, 4, NT8, 16, LANES), BF),
                V((2, npair, NT8, 16, LANES), BF), V((4, LANES, LANES), F32), V((6, LANES, LANES), F32), V((4, 4, LANES, LANES), F32), V((3, 512, 512), BF),
                V((nd, LANES), F32), V((4, 4, nd, LANES), F32), V((4, nm // 2, nd, LANES), F32), V((4, nm // 2, nd, LANES), F32), V((2, nm // 2, nd, LANES), F32),
                V((4, 8, 2, 8, 512), F32), V((2, 256, LANES), F32), V((256, LANES), F32), V((256, LANES), F32), V((2, 4, 32, LANES), F32),
                V((8 * 32, LANES), F32), V((15, nd, LANES), F32),
                dma((NT8,)), dma((3,)), dma, dma((npair,)), dma, dma, dma, dma, dma, dma, dma((5,)), dma((4,)), dma, dma, dma, dma],
            compiler_params=pltpu.CompilerParams(collective_id=0, has_side_effects=True, vmem_limit_bytes=60 * 2**20),
        )(bt, mt, ct)
        return jnp.transpose(g, (1, 0, 2))

    return jax.shard_map(local_fock, mesh=mesh, in_specs=(P(('sys', 'aux'), 'orb', None), P(('sys', 'aux'), None), P('sys', None, None)), out_specs=P('sys', 'orb', 'aux'), check_vma=False)
```

```python
import jax
import jax.numpy as jnp
from jax import lax
from jax.experimental import pallas as pl
from jax.experimental.pallas import tpu as pltpu
from jax.sharding import PartitionSpec as P

F32 = jnp.float32
BF = jnp.bfloat16
MESH = pl.DeviceIdType.MESH
NN = (((1,), (0,)), ((), ()))
NT = (((1,), (1,)), ((), ()))
LANES = 128
MROW = 64
NT8 = 7
PIECE = 12
SP = 168


def split3(x):
    hi = x.astype(BF)
    rest = x - hi.astype(F32)
    mid = rest.astype(BF)
    return hi, mid, (rest - mid.astype(F32)).astype(BF)


def dot(x, y, dims):
    return lax.dot_general(x, y, dims, preferred_element_type=F32)


def lhs6(x, axis):
    h, m, l = x
    return jnp.concatenate([h, h, m, m, h, l], axis=axis)


def rhs6(x, axis):
    h, m, l = x
    return jnp.concatenate([h, m, h, m, l, h], axis=axis)


def kernel(nm, nl, nq, nd, ni, bt, mt, ct, out, bv, mv, cv, ctp, tr, sbuf, rbuf, own, mloc, mqr, mq, msp, gsend, grecv, jsend, jrecv, jfwd, zbuf, kacc, kin, kful, kmsg, krecv, gbuf,
           bsem, lsem, tsend, trecv, mzsend, mzrecv, mosend, morecv, gssem, grsem, jssem, jrsem, kxs, kxr, kss, krs):
    sy, a, o = lax.axis_index('sys'), lax.axis_index('aux'), lax.axis_index('orb')
    me = a * 4 + o
    dens, half = me // 2, me % 2
    nh = ni // 2
    npair = nh // 2

    def dev(aa, oo):
        return (sy, aa, oo)

    pltpu.make_async_copy(mt, mv, lsem.at[1]).start()
    pltpu.make_async_copy(ct, cv, lsem.at[0]).start()
    pltpu.make_async_copy(bt.at[pl.ds(8 * NT8, 2)], bv.at[pl.ds(8 * NT8, 2)], lsem.at[2]).start()
    for t in range(NT8):
        pltpu.make_async_copy(bt.at[pl.ds(8 * t, 8)], bv.at[pl.ds(8 * t, 8)], bsem.at[t]).start()
    barrier = pltpu.get_barrier_semaphore()

    def tell(k, c):
        g = lax.rem(me + k, 16)
        pl.semaphore_signal(barrier, inc=1, device_id=dev(g // 4, g % 4), device_id_type=MESH)
        return c
    lax.fori_loop(1, 16, tell, 0)

    pltpu.make_async_copy(mt, mv, lsem.at[1]).wait()
    for b in range(4):
        blk = jnp.concatenate([mv[nq * b:nq * (b + 1), :], jnp.zeros((nq, LANES - nq), F32)], axis=1)
        mloc[b] = jnp.concatenate([blk, jnp.zeros((LANES - nq, LANES), F32)], axis=0)
    pl.semaphore_wait(barrier, 15)

    quarter = pl.ds(pl.multiple_of(o * 32, 32), 32)

    def nearer(x, y, z):
        dx, dy = jnp.abs(x - z), jnp.abs(y - z)
        return jnp.logical_or(dx < dy, jnp.logical_and(dx == dy, x < y))

    def metric_copies(act):
        for k in (2, 1, 3):
            to = lax.rem(a + 4 - k, 4)

            def block(row, slot):
                return pltpu.make_async_remote_copy(src_ref=mloc.at[row, quarter], dst_ref=mqr.at[slot, quarter], send_sem=mzsend,
                                                    recv_sem=mzrecv, device_id=dev(to, o), device_id_type=MESH)
            act(block(a, k - 1))
            for k2 in (1, 2, 3):
                if k2 == k:
                    continue
                b = lax.rem(to + k2, 4)

                @pl.when(nearer(a, b, to))
                def _():
                    act(block(b, k + k2))
    metric_copies(lambda c: c.start())

    pltpu.make_async_copy(ct, cv, lsem.at[0]).wait()
    ctp[...] = jnp.concatenate([cv[...], jnp.zeros((nd * ni, 256 - nl), F32)], axis=1)
    lhs = lhs6(split3(ctp[...]), 1)

    gam = jnp.zeros((nd, LANES), F32)
    tr2 = tr

    lane = lax.broadcasted_iota(jnp.int32, (1, LANES), 1)
    data = lane < nq

    def tile(t, gam, tail, first):
        pltpu.make_async_copy(bt.at[pl.ds(0, 8)], bv.at[pl.ds(0, 8)], bsem.at[t]).wait()
        cols = pltpu.roll(ctp[...], lax.rem(512 - (nm * o + 8 * t), 256), 1)
        count = 0
        if tail is not None:
            count = min(8, 10 - first)
            spare = jnp.concatenate([bv[8 * NT8 + tail], jnp.zeros((nl, LANES - nq), F32)], axis=1)
            tcol = pltpu.roll(ctp[...], lax.rem(512 - (nm * o + 8 * NT8 + tail), 256), 1)[:, 0:1]
        for r in range(0, 8, 2):
            xs = []
            for e in range(2):
                x = jnp.concatenate([bv[8 * t + r + e], jnp.zeros((nl, LANES - nq), F32)], axis=1)
                if r + e < count:
                    x = jnp.where(data, x, pltpu.roll(spare, (nq - PIECE * (first + r + e)) % LANES, 1))
                xs.append(x)
            x = jnp.concatenate(xs, axis=1)
            x = jnp.concatenate([x, jnp.zeros((256 - nl, 2 * LANES), F32)], axis=0)
            y = dot(lhs, rhs6(split3(x), 0), NN)
            for e in range(2):
                ye = y[:, e * LANES:(e + 1) * LANES]
                tr2[pl.ds((r + e) * SP, nd * ni), :] = ye
                col = cols[:, r + e:r + e + 1]
                if r + e < count:
                    w = (ye * jnp.where(data, col, tcol)).reshape(ni, nd, LANES).sum(0)
                    moved = pltpu.roll(jnp.where(data, 0.0, w), (PIECE * (first + r + e) - nq) % LANES, 1)
                    gam = gam + jnp.where(data, w, 0.0) + moved
                else:
                    gam = gam + (ye * col).reshape(ni, nd, LANES).sum(0)
        for g in range(16):
            d, h = g // 2, g % 2
            for p in range(npair):
                two = [tr2[pl.ds((h * nh + 2 * p + e) * nd + d, 8, stride=SP), :] for e in range(2)]
                sbuf[g, p, t] = jnp.concatenate(two, axis=0).astype(BF)
        for p in range(npair):
            two = [tr2[pl.ds((half * nh + 2 * p + e) * nd + dens, 8, stride=SP), :] for e in range(2)]
            _, mid, low = split3(jnp.concatenate(two, axis=0))
            own[0, p, t] = mid
            own[1, p, t] = low
        return gam

    def send_t1(p, t0, nt):
        def one(k, c):
            j, u = k % 4, k // 4
            aa = lax.rem(a + 2 + j, 4)
            oo = lax.rem(o + 1 + u, 4)
            g = aa * 4 + oo
            src = sbuf.at[g, p, pl.ds(t0, nt)]
            dst = rbuf.at[a, p, o, pl.ds(t0, nt)]

            @pl.when(k != 14)
            def _():
                pltpu.make_async_remote_copy(src_ref=src, dst_ref=dst, send_sem=tsend, recv_sem=trecv.at[p],
                                             device_id=dev(aa, oo), device_id_type=MESH).start()

            @pl.when(k == 14)
            def _():
                pltpu.make_async_copy(src, dst, trecv.at[p]).start()
            return c
        lax.fori_loop(0, 16, one, 0)

    outer = jnp.logical_or(a == 0, a == 3)
    pair = a + 1 - 2 * (a % 2)

    def send_half(p, t0, nt, cross):
        def one(k, c):
            if cross:
                aa = jnp.where(k % 2 == 0, 3 - a, 3 - pair)
                oo = lax.rem(o + 1 + k // 2, 4)
            else:
                aa = jnp.where(k % 2 == 0, pair, a)
                oo = lax.rem(o + 1 + k // 2, 4)
            g = aa * 4 + oo
            src = sbuf.at[g, p, pl.ds(t0, nt)]
            dst = rbuf.at[a, p, o, pl.ds(t0, nt)]

            def far():
                pltpu.make_async_remote_copy(src_ref=src, dst_ref=dst, send_sem=tsend, recv_sem=trecv.at[p],
                                             device_id=dev(aa, oo), device_id_type=MESH).start()
            if cross:
                far()
            else:
                pl.when(k != 7)(far)

                @pl.when(k == 7)
                def _():
                    pltpu.make_async_copy(src, dst, trecv.at[p]).start()
            return c
        lax.fori_loop(0, 8, one, 0)

    pltpu.make_async_copy(bt.at[pl.ds(0, 2)], bv.at[pl.ds(0, 2)], lsem.at[2]).wait()

    def two_tiles(u, gam):
        gam = tile(2 * u, gam, u, 0)
        send_t1(0, 2 * u, 1)
        gam = tile(2 * u + 1, gam, u, 8)
        send_t1(0, 2 * u + 1, 1)
        return gam
    gam = lax.fori_loop(0, 2, two_tiles, gam)

    def one_tile(t, gam):
        gam = tile(t, gam, None, 0)
        send_t1(0, t, 1)
        return gam
    gam = lax.fori_loop(4, NT8, one_tile, gam)

    gsend[...] = gam

    def gs(k, c):
        g = lax.rem(me + k, 16)
        pltpu.make_async_remote_copy(src_ref=gsend, dst_ref=grecv.at[a, o], send_sem=gssem, recv_sem=grsem,
                                     device_id=dev(g // 4, g % 4), device_id_type=MESH).start()
        return c
    lax.fori_loop(1, 16, gs, 0)
    pltpu.make_async_copy(gsend, grecv.at[a, o], grsem).start()

    pltpu.make_async_copy(mqr.at[:, pl.ds(0, 32)], mqr.at[:, pl.ds(0, 32)], mzrecv).wait()

    def mo(k, c):
        oo = lax.rem(o + k, 4)
        pltpu.make_async_remote_copy(src_ref=mqr.at[:, quarter], dst_ref=mqr.at[:, quarter], send_sem=mosend, recv_sem=morecv,
                                     device_id=dev(a, oo), device_id_type=MESH).start()
        return c
    lax.fori_loop(1, 4, mo, 0)
    @pl.when(outer)
    def _():
        send_half(1, 0, NT8, False)
        send_half(2, 0, NT8, False)
        send_half(1, 0, NT8, True)
        send_half(3, 0, NT8, False)
        send_half(4, 0, NT8, False)
        send_half(2, 0, NT8, True)

    @pl.when(jnp.logical_not(outer))
    def _():
        send_t1(1, 0, NT8)
        send_half(2, 0, NT8, False)
    mq[a] = mloc[...]
    for k in range(1, 4):
        c1 = lax.rem(a + k, 4)
        mq[c1, a] = mloc[c1].T
    pltpu.make_async_copy(mqr.at[:, pl.ds(0, 96)], mqr.at[:, pl.ds(0, 96)], morecv).wait()
    for k in range(1, 4):
        c1 = lax.rem(a + k, 4)
        mq[c1, c1] = mqr[k - 1]
        for k2 in range(k + 1, 4):
            c2 = lax.rem(a + k2, 4)
            first = jnp.where(nearer(c1, c2, a), c1, c2)
            second = c1 + c2 - first
            blk = mqr[k + k2]
            mq[first, second] = blk
            mq[second, first] = blk.T
    for b in range(4):
        parts = split3(jnp.concatenate([mq[aa, b] for aa in range(4)], axis=1))
        for s in range(3):
            msp[s, pl.ds(b * LANES, LANES)] = parts[s]

    pltpu.make_async_copy(grecv, grecv, grsem).wait()
    graw = jnp.concatenate([grecv[aa, 0] + grecv[aa, 1] + grecv[aa, 2] + grecv[aa, 3] for aa in range(4)], axis=1)
    m3 = [msp[s] for s in range(3)]
    gfit = dot(lhs6(split3(graw), 1), rhs6(m3, 0), NN)
    mown = split3(jnp.concatenate([mloc[b] for b in range(4)], axis=0))
    wts = dot(lhs6(split3(gfit), 1), rhs6(mown, 0), NN)
    wl = lhs6(split3(wts), 1)
    low64 = lax.broadcasted_iota(jnp.int32, (nd, LANES), 1) < 64

    def jpair(u, c):
        ys = []
        for e in range(2):
            x = jnp.concatenate([bv[2 * u + e], jnp.zeros((nl, LANES - nq), F32)], axis=1)
            x = jnp.concatenate([x, jnp.zeros((256 - nl, LANES), F32)], axis=0)
            ys.append(dot(wl, rhs6(split3(x), 1), NT))
        for aa in range(4):
            lo = pltpu.roll(ys[0], (256 - nm * aa) % 256, 1)[:, :LANES]
            hi = pltpu.roll(ys[1], (256 + 64 - nm * aa) % 256, 1)[:, :LANES]
            jsend[aa, u] = jnp.where(low64, lo, hi)
        return c

    row8 = lax.broadcasted_iota(jnp.int32, (8, LANES), 0)
    lane8 = lax.broadcasted_iota(jnp.int32, (8, LANES), 1)
    at0 = lane8 - PIECE * row8
    at1 = lane8 - PIECE * (row8 + 8)
    here0 = jnp.logical_and(at0 >= 0, at0 < PIECE)
    here1 = jnp.logical_and(jnp.logical_and(at1 >= 0, at1 < PIECE), lane8 < nq)
    zbuf[:, NT8] = jnp.zeros((4, 2, 8, 512), F32)

    def tails(x):
        f = [x[t].astype(F32) for t in range(4)]
        out = []
        for e in range(2):
            for u in range(2):
                v0 = pltpu.roll(f[2 * u][8 * e:8 * e + 8], LANES - nq, 1, stride=PIECE, stride_axis=0)
                f1 = f[2 * u + 1][8 * e:8 * e + 8]
                v1 = jnp.where(row8 == 0, pltpu.roll(f1, (8 * PIECE - nq) % LANES, 1), pltpu.roll(f1, (9 * PIECE - nq) % LANES, 1))
                v = jnp.where(here0, v0, jnp.where(here1, v1, 0.0))
                out.append(v.sum(0, keepdims=True))
        return out

    def fit(p):
        pltpu.make_async_copy(rbuf.at[:, p], rbuf.at[:, p], trecv.at[p]).wait()
        if p + 2 < npair:
            @pl.when(jnp.logical_not(outer))
            def _():
                send_half(p + 2, 0, NT8, True)
        xs = []
        for s in range(4):
            rest = [w for q in range(4) for w in tails(rbuf[s, p, q, pl.ds(0, 4)])]
            xs.append(jnp.concatenate([rbuf[s, p].reshape(4 * NT8 * 16, LANES), jnp.concatenate(rest, axis=0).astype(BF)], axis=0))
        x = jnp.concatenate(xs, axis=1)
        z = dot(jnp.concatenate([x, x, x], axis=1), msp[...].reshape(3 * 512, 512), NN)
        main = 4 * NT8 * 16
        zbuf[:, pl.ds(0, NT8)] = z[:main].reshape(4, NT8, 2, 8, 512)
        for q in range(4):
            for e in range(2):
                zbuf[q, NT8, e, pl.ds(0, 2)] = z[main + 4 * q + 2 * e:main + 4 * q + 2 * e + 2]
        ml = []
        for s in range(2):
            rest = tails(own[s, p, pl.ds(0, 4)]) + [jnp.zeros((12, LANES), F32)]
            ml.append(jnp.concatenate([own[s, p].reshape(NT8 * 16, LANES), jnp.concatenate(rest, axis=0).astype(BF)], axis=0))
        mid, low = ml
        rows = pl.ds(pl.multiple_of(a * LANES, LANES), LANES)
        mh, mm = msp[0, rows], msp[1, rows]
        z = dot(jnp.concatenate([mid, mid, low], axis=1), jnp.concatenate([mh, mm, mh], axis=0), NN)
        zbuf[o, pl.ds(0, NT8)] = zbuf[o, pl.ds(0, NT8)] + z[:NT8 * 16].reshape(NT8, 2, 8, 512)
        for e in range(2):
            zbuf[o, NT8, e, pl.ds(0, 2)] = zbuf[o, NT8, e, pl.ds(0, 2)] + z[NT8 * 16 + 2 * e:NT8 * 16 + 2 * e + 2]
        for e in range(2):
            s3 = split3(zbuf[:, :, e].reshape(4 * MROW, 512))
            k = dot(lhs6(s3, 1), rhs6(s3, 1), NT)
            if p == 0 and e == 0:
                kacc[0] = k[:, :LANES]
                kacc[1] = k[:, LANES:]
            else:
                kacc[0] = kacc[0] + k[:, :LANES]
                kacc[1] = kacc[1] + k[:, LANES:]

    lax.fori_loop(0, nm // 2, jpair, 0)
    near, far = a + 1 - 2 * (a % 2), lax.rem(a + 2, 4)
    hops = []
    for e, aa in enumerate((lax.rem(near + 2, 4), near)):
        hops.append(pltpu.make_async_remote_copy(src_ref=jsend.at[aa], dst_ref=jrecv.at[e], send_sem=jssem.at[e], recv_sem=jrsem.at[e],
                                                 device_id=dev(near, o), device_id_type=MESH))
        hops[-1].start()
    @pl.when(outer)
    def _():
        for p in range(3, npair):
            send_half(p, 0, NT8, True)

    @pl.when(jnp.logical_not(outer))
    def _():
        for p in range(3, npair):
            send_half(p, 0, NT8, False)
    for p in range(npair - 1):
        fit(p)
    hops[0].wait_recv()
    jfwd[...] = jsend[far] + jrecv[0]
    cross = pltpu.make_async_remote_copy(src_ref=jfwd, dst_ref=jrecv.at[2], send_sem=jssem.at[2], recv_sem=jrsem.at[2],
                                         device_id=dev(far, o), device_id_type=MESH)
    cross.start()
    fit(npair - 1)

    mate = o + 1 - 2 * half
    swap = pltpu.make_async_remote_copy(src_ref=kacc.at[1 - half], dst_ref=kin, send_sem=kxs, recv_sem=kxr,
                                        device_id=dev(a, mate), device_id_type=MESH)
    swap.start()
    swap.wait_recv()
    kful[...] = kacc[half] + kin[...]
    low32 = lax.broadcasted_iota(jnp.int32, (32, LANES), 1) < 64
    for oo in range(4):
        ev = kful[pl.ds(MROW * oo, 32, stride=2), :]
        od = kful[pl.ds(MROW * oo + 1, 32, stride=2), :]
        kmsg[0, oo] = jnp.where(low32, ev, pltpu.roll(od, 64, 1))
        kmsg[1, oo] = jnp.where(low32, pltpu.roll(ev, 64, 1), od)

    def ks(k, c):
        al, oo = k // 4, k % 4
        aa = 2 * half + al
        same = jnp.logical_and(aa == a, oo == o)

        @pl.when(jnp.logical_not(same))
        def _():
            pltpu.make_async_remote_copy(src_ref=kmsg.at[al, oo], dst_ref=krecv.at[pl.ds(dens * 32, 32)], send_sem=kss, recv_sem=krs,
                                         device_id=dev(aa, oo), device_id_type=MESH).start()

        @pl.when(same)
        def _():
            cp = pltpu.make_async_copy(kmsg.at[al, oo], krecv.at[pl.ds(dens * 32, 32)], krs)
            cp.start()
        return c
    lax.fori_loop(0, 8, ks, 0)

    hops[1].wait_recv()
    cross.wait_recv()
    pltpu.make_async_copy(krecv, krecv, krs).wait()
    for u in range(nm // 2):
        j = jsend[a, u] + jrecv[1, u] + jrecv[2, u]
        g = 2.0 * j - krecv[pl.ds(u, nd, stride=32), :]
        out[2 * u] = g[:, :nm]
        out[2 * u + 1] = pltpu.roll(g, 64, 1)[:, :nm]

    pltpu.make_async_copy(sbuf.at[pl.ds(0, 15)], sbuf.at[pl.ds(0, 15)], tsend).wait()
    metric_copies(lambda c: c.wait_send())
    pltpu.make_async_copy(mqr.at[:, pl.ds(0, 96)], mqr.at[:, pl.ds(0, 96)], mosend).wait()
    pltpu.make_async_copy(gbuf, gbuf, gssem).wait()
    for c in hops + [cross]:
        c.wait_send()
    swap.wait_send()
    inset = (a // 2) == half

    @pl.when(inset)
    def _():
        pltpu.make_async_copy(krecv.at[pl.ds(0, 224)], krecv.at[pl.ds(0, 224)], kss).wait()

    @pl.when(jnp.logical_not(inset))
    def _():
        pltpu.make_async_copy(krecv, krecv, kss).wait()


def solution(mesh):
    def local_fock(ints_blk, metric_blk, orbitals):
        nq, nm, nl = ints_blk.shape
        nd, _, ni = orbitals.shape
        bt = jnp.transpose(ints_blk, (1, 2, 0))
        mt = metric_blk.T
        ct = jnp.transpose(orbitals, (2, 0, 1)).reshape(ni * nd, nl)
        npair = ni // 4
        V = pltpu.VMEM
        dma = pltpu.SemaphoreType.DMA
        g = pl.pallas_call(
            lambda *refs: kernel(nm, nl, nq, nd, ni, *refs),
            out_shape=pltpu.VMEM((nm, nd, nm), F32),
            in_specs=[pl.BlockSpec(memory_space=pl.ANY)] * 3,
            out_specs=pl.BlockSpec(memory_space=pltpu.VMEM),
            scratch_shapes=[
                V((nm, nl, nq), F32), V((4 * nq, nq), F32), V((ni * nd, nl), F32), V((ni * nd, 256), F32),
                V((8 * SP, LANES), F32), V((16, npair, NT8, 16, LANES), BF), V((4, npair, 4, NT8, 16, LANES), BF),
                V((2, npair, NT8, 16, LANES), BF), V((4, LANES, LANES), F32), V((6, LANES, LANES), F32), V((4, 4, LANES, LANES), F32), V((3, 512, 512), BF),
                V((nd, LANES), F32), V((4, 4, nd, LANES), F32), V((4, nm // 2, nd, LANES), F32), V((3, nm // 2, nd, LANES), F32), V((nm // 2, nd, LANES), F32),
                V((4, 8, 2, 8, 512), F32), V((2, 256, LANES), F32), V((256, LANES), F32), V((256, LANES), F32), V((2, 4, 32, LANES), F32),
                V((8 * 32, LANES), F32), V((15, nd, LANES), F32),
                dma((NT8,)), dma((3,)), dma, dma((npair,)), dma, dma, dma, dma, dma, dma, dma((3,)), dma((3,)), dma, dma, dma, dma],
            compiler_params=pltpu.CompilerParams(collective_id=0, has_side_effects=True, vmem_limit_bytes=60 * 2**20),
        )(bt, mt, ct)
        return jnp.transpose(g, (1, 0, 2))

    return jax.shard_map(local_fock, mesh=mesh, in_specs=(P(('sys', 'aux'), 'orb', None), P(('sys', 'aux'), None), P('sys', None, None)), out_specs=P('sys', 'orb', 'aux'), check_vma=False)
```

```python
import jax
import jax.numpy as jnp
from jax import lax
from jax.experimental import pallas as pl
from jax.experimental.pallas import tpu as pltpu
from jax.sharding import PartitionSpec as P

F32 = jnp.float32
BF = jnp.bfloat16
MESH = pl.DeviceIdType.MESH
NN = (((1,), (0,)), ((), ()))
NT = (((1,), (1,)), ((), ()))
LANES = 128
MROW = 64
NT8 = 7
PIECE = 12
SP = 168


def split3(x):
    hi = x.astype(BF)
    rest = x - hi.astype(F32)
    mid = rest.astype(BF)
    return hi, mid, (rest - mid.astype(F32)).astype(BF)


def dot(x, y, dims):
    return lax.dot_general(x, y, dims, preferred_element_type=F32)


def lhs6(x, axis):
    h, m, l = x
    return jnp.concatenate([h, h, m, m, h, l], axis=axis)


def rhs6(x, axis):
    h, m, l = x
    return jnp.concatenate([h, m, h, m, l, h], axis=axis)


def kernel(nm, nl, nq, nd, ni, bt, mt, ct, out, bv, mv, cv, ctp, tr, sbuf, rbuf, own, mloc, mqr, mq, msp, gsend, grecv, jsend, jrecv, jfwd, zbuf, kacc, kin, kful, kmsg, krecv, gbuf,
           bsem, lsem, tsend, trecv, mzsend, mzrecv, mosend, morecv, gssem, grsem, jssem, jrsem, kxs, kxr, kss, krs):
    sy, a, o = lax.axis_index('sys'), lax.axis_index('aux'), lax.axis_index('orb')
    me = a * 4 + o
    dens, half = me // 2, me % 2
    nh = ni // 2
    npair = nh // 2

    def dev(aa, oo):
        return (sy, aa, oo)

    pltpu.make_async_copy(ct, cv, lsem.at[0]).start()
    pltpu.make_async_copy(bt.at[pl.ds(8 * NT8, 2)], bv.at[pl.ds(8 * NT8, 2)], lsem.at[2]).start()
    for t in range(NT8):
        pltpu.make_async_copy(bt.at[pl.ds(8 * t, 8)], bv.at[pl.ds(8 * t, 8)], bsem.at[t]).start()
        if t == 0:
            pltpu.make_async_copy(mt, mv, lsem.at[1]).start()
    barrier = pltpu.get_barrier_semaphore()

    def tell(k, c):
        g = lax.rem(me + k, 16)
        pl.semaphore_signal(barrier, inc=1, device_id=dev(g // 4, g % 4), device_id_type=MESH)
        return c
    lax.fori_loop(1, 16, tell, 0)

    pltpu.make_async_copy(ct, cv, lsem.at[0]).wait()
    ctp[...] = jnp.concatenate([cv[...], jnp.zeros((nd * ni, 256 - nl), F32)], axis=1)
    lhs = lhs6(split3(ctp[...]), 1)
    pltpu.make_async_copy(mt, mv, lsem.at[1]).wait()
    for b in range(4):
        blk = jnp.concatenate([mv[nq * b:nq * (b + 1), :], jnp.zeros((nq, LANES - nq), F32)], axis=1)
        mloc[b] = jnp.concatenate([blk, jnp.zeros((LANES - nq, LANES), F32)], axis=0)
    pl.semaphore_wait(barrier, 15)

    quarter = pl.ds(pl.multiple_of(o * 32, 32), 32)

    def nearer(x, y, z):
        dx, dy = jnp.abs(x - z), jnp.abs(y - z)
        return jnp.logical_or(dx < dy, jnp.logical_and(dx == dy, x < y))

    def metric_copies(act):
        for k in (2, 1, 3):
            to = lax.rem(a + 4 - k, 4)

            def block(row, slot):
                return pltpu.make_async_remote_copy(src_ref=mloc.at[row, quarter], dst_ref=mqr.at[slot, quarter], send_sem=mzsend,
                                                    recv_sem=mzrecv, device_id=dev(to, o), device_id_type=MESH)
            act(block(a, k - 1))
            for k2 in (1, 2, 3):
                if k2 == k:
                    continue
                b = lax.rem(to + k2, 4)

                @pl.when(nearer(a, b, to))
                def _():
                    act(block(b, k + k2))
    metric_copies(lambda c: c.start())

    gam = jnp.zeros((nd, LANES), F32)
    tr2 = tr

    lane = lax.broadcasted_iota(jnp.int32, (1, LANES), 1)
    data = lane < nq

    def tile(t, gam, tail, first):
        pltpu.make_async_copy(bt.at[pl.ds(0, 8)], bv.at[pl.ds(0, 8)], bsem.at[t]).wait()
        cols = pltpu.roll(ctp[...], lax.rem(512 - (nm * o + 8 * t), 256), 1)
        count = 0
        if tail is not None:
            count = min(8, 10 - first)
            spare = jnp.concatenate([bv[8 * NT8 + tail], jnp.zeros((nl, LANES - nq), F32)], axis=1)
            tcol = pltpu.roll(ctp[...], lax.rem(512 - (nm * o + 8 * NT8 + tail), 256), 1)[:, 0:1]
        for r in range(0, 8, 2):
            xs = []
            for e in range(2):
                x = jnp.concatenate([bv[8 * t + r + e], jnp.zeros((nl, LANES - nq), F32)], axis=1)
                if r + e < count:
                    x = jnp.where(data, x, pltpu.roll(spare, (nq - PIECE * (first + r + e)) % LANES, 1))
                xs.append(x)
            x = jnp.concatenate(xs, axis=1)
            x = jnp.concatenate([x, jnp.zeros((256 - nl, 2 * LANES), F32)], axis=0)
            y = dot(lhs, rhs6(split3(x), 0), NN)
            for e in range(2):
                ye = y[:, e * LANES:(e + 1) * LANES]
                tr2[pl.ds((r + e) * SP, nd * ni), :] = ye
                col = cols[:, r + e:r + e + 1]
                if r + e < count:
                    w = (ye * jnp.where(data, col, tcol)).reshape(ni, nd, LANES).sum(0)
                    moved = pltpu.roll(jnp.where(data, 0.0, w), (PIECE * (first + r + e) - nq) % LANES, 1)
                    gam = gam + jnp.where(data, w, 0.0) + moved
                else:
                    gam = gam + (ye * col).reshape(ni, nd, LANES).sum(0)
        for g in range(16):
            d, h = g // 2, g % 2
            for p in range(npair):
                two = [tr2[pl.ds((h * nh + 2 * p + e) * nd + d, 8, stride=SP), :] for e in range(2)]
                sbuf[g, p, t] = jnp.concatenate(two, axis=0).astype(BF)
        for p in range(npair):
            two = [tr2[pl.ds((half * nh + 2 * p + e) * nd + dens, 8, stride=SP), :] for e in range(2)]
            _, mid, low = split3(jnp.concatenate(two, axis=0))
            own[0, p, t] = mid
            own[1, p, t] = low
        return gam

    def send_t1(p, t0, nt):
        def one(k, c):
            j, u = k % 4, k // 4
            aa = lax.rem(a + 2 + j, 4)
            oo = lax.rem(o + 1 + u, 4)
            g = aa * 4 + oo
            src = sbuf.at[g, p, pl.ds(t0, nt)]
            dst = rbuf.at[a, p, o, pl.ds(t0, nt)]

            @pl.when(k != 14)
            def _():
                pltpu.make_async_remote_copy(src_ref=src, dst_ref=dst, send_sem=tsend, recv_sem=trecv.at[p],
                                             device_id=dev(aa, oo), device_id_type=MESH).start()

            @pl.when(k == 14)
            def _():
                pltpu.make_async_copy(src, dst, trecv.at[p]).start()
            return c
        lax.fori_loop(0, 16, one, 0)

    outer = jnp.logical_or(a == 0, a == 3)
    pair = a + 1 - 2 * (a % 2)

    def send_half(p, t0, nt, cross):
        def one(k, c):
            if cross:
                aa = jnp.where(k % 2 == 0, 3 - a, 3 - pair)
                oo = lax.rem(o + 1 + k // 2, 4)
            else:
                aa = jnp.where(k % 2 == 0, pair, a)
                oo = lax.rem(o + 1 + k // 2, 4)
            g = aa * 4 + oo
            src = sbuf.at[g, p, pl.ds(t0, nt)]
            dst = rbuf.at[a, p, o, pl.ds(t0, nt)]

            def far():
                pltpu.make_async_remote_copy(src_ref=src, dst_ref=dst, send_sem=tsend, recv_sem=trecv.at[p],
                                             device_id=dev(aa, oo), device_id_type=MESH).start()
            if cross:
                far()
            else:
                pl.when(k != 7)(far)

                @pl.when(k == 7)
                def _():
                    pltpu.make_async_copy(src, dst, trecv.at[p]).start()
            return c
        lax.fori_loop(0, 8, one, 0)

    pltpu.make_async_copy(bt.at[pl.ds(0, 2)], bv.at[pl.ds(0, 2)], lsem.at[2]).wait()

    def two_tiles(u, gam):
        gam = tile(2 * u, gam, u, 0)
        send_t1(0, 2 * u, 1)
        gam = tile(2 * u + 1, gam, u, 8)
        send_t1(0, 2 * u + 1, 1)
        return gam
    gam = lax.fori_loop(0, 2, two_tiles, gam)

    def one_tile(t, gam):
        gam = tile(t, gam, None, 0)
        send_t1(0, t, 1)
        return gam
    gam = lax.fori_loop(4, NT8, one_tile, gam)

    gsend[...] = gam

    def gs(k, c):
        g = lax.rem(me + k, 16)
        pltpu.make_async_remote_copy(src_ref=gsend, dst_ref=grecv.at[a, o], send_sem=gssem, recv_sem=grsem,
                                     device_id=dev(g // 4, g % 4), device_id_type=MESH).start()
        return c
    lax.fori_loop(1, 16, gs, 0)
    pltpu.make_async_copy(gsend, grecv.at[a, o], grsem).start()

    pltpu.make_async_copy(mqr.at[:, pl.ds(0, 32)], mqr.at[:, pl.ds(0, 32)], mzrecv).wait()

    def mo(k, c):
        oo = lax.rem(o + k, 4)
        pltpu.make_async_remote_copy(src_ref=mqr.at[:, quarter], dst_ref=mqr.at[:, quarter], send_sem=mosend, recv_sem=morecv,
                                     device_id=dev(a, oo), device_id_type=MESH).start()
        return c
    lax.fori_loop(1, 4, mo, 0)
    @pl.when(outer)
    def _():
        send_half(1, 0, NT8, False)
        send_half(2, 0, NT8, False)
        send_half(1, 0, NT8, True)
        send_half(3, 0, NT8, False)
        send_half(4, 0, NT8, False)
        send_half(2, 0, NT8, True)
        send_half(3, 0, NT8, True)

    @pl.when(jnp.logical_not(outer))
    def _():
        for p in range(1, 3):
            send_t1(p, 0, NT8)
    mq[a] = mloc[...]
    for k in range(1, 4):
        c1 = lax.rem(a + k, 4)
        mq[c1, a] = mloc[c1].T
    pltpu.make_async_copy(mqr.at[:, pl.ds(0, 96)], mqr.at[:, pl.ds(0, 96)], morecv).wait()
    for k in range(1, 4):
        c1 = lax.rem(a + k, 4)
        mq[c1, c1] = mqr[k - 1]
        for k2 in range(k + 1, 4):
            c2 = lax.rem(a + k2, 4)
            first = jnp.where(nearer(c1, c2, a), c1, c2)
            second = c1 + c2 - first
            blk = mqr[k + k2]
            mq[first, second] = blk
            mq[second, first] = blk.T
    for b in range(4):
        parts = split3(jnp.concatenate([mq[aa, b] for aa in range(4)], axis=1))
        for s in range(3):
            msp[s, pl.ds(b * LANES, LANES)] = parts[s]

    pltpu.make_async_copy(grecv, grecv, grsem).wait()
    graw = jnp.concatenate([grecv[aa, 0] + grecv[aa, 1] + grecv[aa, 2] + grecv[aa, 3] for aa in range(4)], axis=1)
    m3 = [msp[s] for s in range(3)]
    gfit = dot(lhs6(split3(graw), 1), rhs6(m3, 0), NN)
    mown = split3(jnp.concatenate([mloc[b] for b in range(4)], axis=0))
    wts = dot(lhs6(split3(gfit), 1), rhs6(mown, 0), NN)
    wl = lhs6(split3(wts), 1)
    low64 = lax.broadcasted_iota(jnp.int32, (nd, LANES), 1) < 64

    def jpair(u, c):
        ys = []
        for e in range(2):
            x = jnp.concatenate([bv[2 * u + e], jnp.zeros((nl, LANES - nq), F32)], axis=1)
            x = jnp.concatenate([x, jnp.zeros((256 - nl, LANES), F32)], axis=0)
            ys.append(dot(wl, rhs6(split3(x), 1), NT))
        for aa in range(4):
            lo = pltpu.roll(ys[0], (256 - nm * aa) % 256, 1)[:, :LANES]
            hi = pltpu.roll(ys[1], (256 + 64 - nm * aa) % 256, 1)[:, :LANES]
            jsend[aa, u] = jnp.where(low64, lo, hi)
        return c

    row8 = lax.broadcasted_iota(jnp.int32, (8, LANES), 0)
    lane8 = lax.broadcasted_iota(jnp.int32, (8, LANES), 1)
    at0 = lane8 - PIECE * row8
    at1 = lane8 - PIECE * (row8 + 8)
    here0 = jnp.logical_and(at0 >= 0, at0 < PIECE)
    here1 = jnp.logical_and(jnp.logical_and(at1 >= 0, at1 < PIECE), lane8 < nq)
    zbuf[:, NT8] = jnp.zeros((4, 2, 8, 512), F32)

    def tails(x):
        f = [x[t].astype(F32) for t in range(4)]
        out = []
        for e in range(2):
            for u in range(2):
                v0 = pltpu.roll(f[2 * u][8 * e:8 * e + 8], LANES - nq, 1, stride=PIECE, stride_axis=0)
                f1 = f[2 * u + 1][8 * e:8 * e + 8]
                v1 = jnp.where(row8 == 0, pltpu.roll(f1, (8 * PIECE - nq) % LANES, 1), pltpu.roll(f1, (9 * PIECE - nq) % LANES, 1))
                v = jnp.where(here0, v0, jnp.where(here1, v1, 0.0))
                out.append(v.sum(0, keepdims=True))
        return out

    def fit(p):
        pltpu.make_async_copy(rbuf.at[:, p], rbuf.at[:, p], trecv.at[p]).wait()
        if p + 3 < npair:
            @pl.when(jnp.logical_not(outer))
            def _():
                send_half(p + 3, 0, NT8, True)
        xs = []
        for s in range(4):
            rest = [w for q in range(4) for w in tails(rbuf[s, p, q, pl.ds(0, 4)])]
            xs.append(jnp.concatenate([rbuf[s, p].reshape(4 * NT8 * 16, LANES), jnp.concatenate(rest, axis=0).astype(BF)], axis=0))
        x = jnp.concatenate(xs, axis=1)
        z = dot(jnp.concatenate([x, x, x], axis=1), msp[...].reshape(3 * 512, 512), NN)
        main = 4 * NT8 * 16
        zbuf[:, pl.ds(0, NT8)] = z[:main].reshape(4, NT8, 2, 8, 512)
        for q in range(4):
            for e in range(2):
                zbuf[q, NT8, e, pl.ds(0, 2)] = z[main + 4 * q + 2 * e:main + 4 * q + 2 * e + 2]
        ml = []
        for s in range(2):
            rest = tails(own[s, p, pl.ds(0, 4)]) + [jnp.zeros((12, LANES), F32)]
            ml.append(jnp.concatenate([own[s, p].reshape(NT8 * 16, LANES), jnp.concatenate(rest, axis=0).astype(BF)], axis=0))
        mid, low = ml
        rows = pl.ds(pl.multiple_of(a * LANES, LANES), LANES)
        mh, mm = msp[0, rows], msp[1, rows]
        z = dot(jnp.concatenate([mid, mid, low], axis=1), jnp.concatenate([mh, mm, mh], axis=0), NN)
        zbuf[o, pl.ds(0, NT8)] = zbuf[o, pl.ds(0, NT8)] + z[:NT8 * 16].reshape(NT8, 2, 8, 512)
        for e in range(2):
            zbuf[o, NT8, e, pl.ds(0, 2)] = zbuf[o, NT8, e, pl.ds(0, 2)] + z[NT8 * 16 + 2 * e:NT8 * 16 + 2 * e + 2]
        for e in range(2):
            s3 = split3(zbuf[:, :, e].reshape(4 * MROW, 512))
            k = dot(lhs6(s3, 1), rhs6(s3, 1), NT)
            if p == 0 and e == 0:
                kacc[0] = k[:, :LANES]
                kacc[1] = k[:, LANES:]
            else:
                kacc[0] = kacc[0] + k[:, :LANES]
                kacc[1] = kacc[1] + k[:, LANES:]

    lax.fori_loop(0, nm // 2, jpair, 0)
    near, far = a + 1 - 2 * (a % 2), lax.rem(a + 2, 4)
    hops = []
    for e, aa in enumerate((lax.rem(near + 2, 4), near)):
        hops.append(pltpu.make_async_remote_copy(src_ref=jsend.at[aa], dst_ref=jrecv.at[e], send_sem=jssem.at[e], recv_sem=jrsem.at[e],
                                                 device_id=dev(near, o), device_id_type=MESH))
        hops[-1].start()
    @pl.when(outer)
    def _():
        send_half(npair - 1, 0, NT8, True)

    @pl.when(jnp.logical_not(outer))
    def _():
        for p in range(3, npair):
            send_half(p, 0, NT8, False)
    for p in range(npair - 1):
        fit(p)
    hops[0].wait_recv()
    jfwd[...] = jsend[far] + jrecv[0]
    cross = pltpu.make_async_remote_copy(src_ref=jfwd, dst_ref=jrecv.at[2], send_sem=jssem.at[2], recv_sem=jrsem.at[2],
                                         device_id=dev(far, o), device_id_type=MESH)
    cross.start()
    fit(npair - 1)

    mate = o + 1 - 2 * half
    swap = pltpu.make_async_remote_copy(src_ref=kacc.at[1 - half], dst_ref=kin, send_sem=kxs, recv_sem=kxr,
                                        device_id=dev(a, mate), device_id_type=MESH)
    swap.start()
    swap.wait_recv()
    kful[...] = kacc[half] + kin[...]
    low32 = lax.broadcasted_iota(jnp.int32, (32, LANES), 1) < 64
    for oo in range(4):
        ev = kful[pl.ds(MROW * oo, 32, stride=2), :]
        od = kful[pl.ds(MROW * oo + 1, 32, stride=2), :]
        kmsg[0, oo] = jnp.where(low32, ev, pltpu.roll(od, 64, 1))
        kmsg[1, oo] = jnp.where(low32, pltpu.roll(ev, 64, 1), od)

    def ks(k, c):
        al, oo = k // 4, k % 4
        aa = 2 * half + al
        same = jnp.logical_and(aa == a, oo == o)

        @pl.when(jnp.logical_not(same))
        def _():
            pltpu.make_async_remote_copy(src_ref=kmsg.at[al, oo], dst_ref=krecv.at[pl.ds(dens * 32, 32)], send_sem=kss, recv_sem=krs,
                                         device_id=dev(aa, oo), device_id_type=MESH).start()

        @pl.when(same)
        def _():
            cp = pltpu.make_async_copy(kmsg.at[al, oo], krecv.at[pl.ds(dens * 32, 32)], krs)
            cp.start()
        return c
    lax.fori_loop(0, 8, ks, 0)

    hops[1].wait_recv()
    cross.wait_recv()
    pltpu.make_async_copy(krecv, krecv, krs).wait()
    for u in range(nm // 2):
        j = jsend[a, u] + jrecv[1, u] + jrecv[2, u]
        g = 2.0 * j - krecv[pl.ds(u, nd, stride=32), :]
        out[2 * u] = g[:, :nm]
        out[2 * u + 1] = pltpu.roll(g, 64, 1)[:, :nm]

    pltpu.make_async_copy(sbuf.at[pl.ds(0, 15)], sbuf.at[pl.ds(0, 15)], tsend).wait()
    metric_copies(lambda c: c.wait_send())
    pltpu.make_async_copy(mqr.at[:, pl.ds(0, 96)], mqr.at[:, pl.ds(0, 96)], mosend).wait()
    pltpu.make_async_copy(gbuf, gbuf, gssem).wait()
    for c in hops + [cross]:
        c.wait_send()
    swap.wait_send()
    inset = (a // 2) == half

    @pl.when(inset)
    def _():
        pltpu.make_async_copy(krecv.at[pl.ds(0, 224)], krecv.at[pl.ds(0, 224)], kss).wait()

    @pl.when(jnp.logical_not(inset))
    def _():
        pltpu.make_async_copy(krecv, krecv, kss).wait()


def solution(mesh):
    def local_fock(ints_blk, metric_blk, orbitals):
        nq, nm, nl = ints_blk.shape
        nd, _, ni = orbitals.shape
        bt = jnp.transpose(ints_blk, (1, 2, 0))
        mt = metric_blk.T
        ct = jnp.transpose(orbitals, (2, 0, 1)).reshape(ni * nd, nl)
        npair = ni // 4
        V = pltpu.VMEM
        dma = pltpu.SemaphoreType.DMA
        g = pl.pallas_call(
            lambda *refs: kernel(nm, nl, nq, nd, ni, *refs),
            out_shape=pltpu.VMEM((nm, nd, nm), F32),
            in_specs=[pl.BlockSpec(memory_space=pl.ANY)] * 3,
            out_specs=pl.BlockSpec(memory_space=pltpu.VMEM),
            scratch_shapes=[
                V((nm, nl, nq), F32), V((4 * nq, nq), F32), V((ni * nd, nl), F32), V((ni * nd, 256), F32),
                V((8 * SP, LANES), F32), V((16, npair, NT8, 16, LANES), BF), V((4, npair, 4, NT8, 16, LANES), BF),
                V((2, npair, NT8, 16, LANES), BF), V((4, LANES, LANES), F32), V((6, LANES, LANES), F32), V((4, 4, LANES, LANES), F32), V((3, 512, 512), BF),
                V((nd, LANES), F32), V((4, 4, nd, LANES), F32), V((4, nm // 2, nd, LANES), F32), V((3, nm // 2, nd, LANES), F32), V((nm // 2, nd, LANES), F32),
                V((4, 8, 2, 8, 512), F32), V((2, 256, LANES), F32), V((256, LANES), F32), V((256, LANES), F32), V((2, 4, 32, LANES), F32),
                V((8 * 32, LANES), F32), V((15, nd, LANES), F32),
                dma((NT8,)), dma((3,)), dma, dma((npair,)), dma, dma, dma, dma, dma, dma, dma((3,)), dma((3,)), dma, dma, dma, dma],
            compiler_params=pltpu.CompilerParams(collective_id=0, has_side_effects=True, vmem_limit_bytes=60 * 2**20),
        )(bt, mt, ct)
        return jnp.transpose(g, (1, 0, 2))

    return jax.shard_map(local_fock, mesh=mesh, in_specs=(P(('sys', 'aux'), 'orb', None), P(('sys', 'aux'), None), P('sys', None, None)), out_specs=P('sys', 'orb', 'aux'), check_vma=False)
```

```python
import jax
import jax.numpy as jnp
from jax import lax
from jax.experimental import pallas as pl
from jax.experimental.pallas import tpu as pltpu
from jax.sharding import PartitionSpec as P

F32 = jnp.float32
BF = jnp.bfloat16
MESH = pl.DeviceIdType.MESH
NN = (((1,), (0,)), ((), ()))
NT = (((1,), (1,)), ((), ()))
LANES = 128
MROW = 64
NT8 = 7
PIECE = 12
SP = 168


def split3(x):
    hi = x.astype(BF)
    rest = x - hi.astype(F32)
    mid = rest.astype(BF)
    return hi, mid, (rest - mid.astype(F32)).astype(BF)


def dot(x, y, dims):
    return lax.dot_general(x, y, dims, preferred_element_type=F32)


def lhs6(x, axis):
    h, m, l = x
    return jnp.concatenate([h, h, m, m, h, l], axis=axis)


def rhs6(x, axis):
    h, m, l = x
    return jnp.concatenate([h, m, h, m, l, h], axis=axis)


def kernel(nm, nl, nq, nd, ni, bt, mt, ct, out, bv, mv, cv, ctp, tr, sbuf, rbuf, own, mloc, mqr, mq, msp, gsend, grecv, jsend, jrecv, jfwd, zbuf, kacc, kin, kful, kmsg, krecv, gbuf,
           bsem, lsem, tsend, nrecv, trecv, mzsend, mzrecv, mosend, morecv, gssem, grsem, jssem, jrsem, kxs, kxr, kss, krs):
    sy, a, o = lax.axis_index('sys'), lax.axis_index('aux'), lax.axis_index('orb')
    me = a * 4 + o
    dens, half = me // 2, me % 2
    nh = ni // 2
    npair = nh // 2

    def dev(aa, oo):
        return (sy, aa, oo)

    pltpu.make_async_copy(ct, cv, lsem.at[0]).start()
    pltpu.make_async_copy(bt.at[pl.ds(8 * NT8, 2)], bv.at[pl.ds(8 * NT8, 2)], lsem.at[2]).start()
    for t in range(NT8):
        pltpu.make_async_copy(bt.at[pl.ds(8 * t, 8)], bv.at[pl.ds(8 * t, 8)], bsem.at[t]).start()
        if t == 0:
            pltpu.make_async_copy(mt, mv, lsem.at[1]).start()
    barrier = pltpu.get_barrier_semaphore()

    def tell(k, c):
        g = lax.rem(me + k, 16)
        pl.semaphore_signal(barrier, inc=1, device_id=dev(g // 4, g % 4), device_id_type=MESH)
        return c
    lax.fori_loop(1, 16, tell, 0)

    pltpu.make_async_copy(ct, cv, lsem.at[0]).wait()
    ctp[...] = jnp.concatenate([cv[...], jnp.zeros((nd * ni, 256 - nl), F32)], axis=1)
    lhs = lhs6(split3(ctp[...]), 1)
    pltpu.make_async_copy(mt, mv, lsem.at[1]).wait()
    for b in range(4):
        blk = jnp.concatenate([mv[nq * b:nq * (b + 1), :], jnp.zeros((nq, LANES - nq), F32)], axis=1)
        mloc[b] = jnp.concatenate([blk, jnp.zeros((LANES - nq, LANES), F32)], axis=0)
    pl.semaphore_wait(barrier, 15)

    quarter = pl.ds(pl.multiple_of(o * 32, 32), 32)

    def nearer(x, y, z):
        dx, dy = jnp.abs(x - z), jnp.abs(y - z)
        return jnp.logical_or(dx < dy, jnp.logical_and(dx == dy, x < y))

    def metric_copies(act):
        for k in (2, 1, 3):
            to = lax.rem(a + 4 - k, 4)

            def block(row, slot):
                return pltpu.make_async_remote_copy(src_ref=mloc.at[row, quarter], dst_ref=mqr.at[slot, quarter], send_sem=mzsend,
                                                    recv_sem=mzrecv, device_id=dev(to, o), device_id_type=MESH)
            act(block(a, k - 1))
            for k2 in (1, 2, 3):
                if k2 == k:
                    continue
                b = lax.rem(to + k2, 4)

                @pl.when(nearer(a, b, to))
                def _():
                    act(block(b, k + k2))
    metric_copies(lambda c: c.start())

    gam = jnp.zeros((nd, LANES), F32)
    tr2 = tr

    lane = lax.broadcasted_iota(jnp.int32, (1, LANES), 1)
    data = lane < nq

    def tile(t, gam, tail, first):
        pltpu.make_async_copy(bt.at[pl.ds(0, 8)], bv.at[pl.ds(0, 8)], bsem.at[t]).wait()
        cols = pltpu.roll(ctp[...], lax.rem(512 - (nm * o + 8 * t), 256), 1)
        count = 0
        if tail is not None:
            count = min(8, 10 - first)
            spare = jnp.concatenate([bv[8 * NT8 + tail], jnp.zeros((nl, LANES - nq), F32)], axis=1)
            tcol = pltpu.roll(ctp[...], lax.rem(512 - (nm * o + 8 * NT8 + tail), 256), 1)[:, 0:1]
        for r in range(0, 8, 2):
            xs = []
            for e in range(2):
                x = jnp.concatenate([bv[8 * t + r + e], jnp.zeros((nl, LANES - nq), F32)], axis=1)
                if r + e < count:
                    x = jnp.where(data, x, pltpu.roll(spare, (nq - PIECE * (first + r + e)) % LANES, 1))
                xs.append(x)
            x = jnp.concatenate(xs, axis=1)
            x = jnp.concatenate([x, jnp.zeros((256 - nl, 2 * LANES), F32)], axis=0)
            y = dot(lhs, rhs6(split3(x), 0), NN)
            for e in range(2):
                ye = y[:, e * LANES:(e + 1) * LANES]
                tr2[pl.ds((r + e) * SP, nd * ni), :] = ye
                col = cols[:, r + e:r + e + 1]
                if r + e < count:
                    w = (ye * jnp.where(data, col, tcol)).reshape(ni, nd, LANES).sum(0)
                    moved = pltpu.roll(jnp.where(data, 0.0, w), (PIECE * (first + r + e) - nq) % LANES, 1)
                    gam = gam + jnp.where(data, w, 0.0) + moved
                else:
                    gam = gam + (ye * col).reshape(ni, nd, LANES).sum(0)
        for g in range(16):
            d, h = g // 2, g % 2
            for p in range(npair):
                two = [tr2[pl.ds((h * nh + 2 * p + e) * nd + d, 8, stride=SP), :] for e in range(2)]
                sbuf[g, p, t] = jnp.concatenate(two, axis=0).astype(BF)
        for p in range(npair):
            two = [tr2[pl.ds((half * nh + 2 * p + e) * nd + dens, 8, stride=SP), :] for e in range(2)]
            _, mid, low = split3(jnp.concatenate(two, axis=0))
            own[0, p, t] = mid
            own[1, p, t] = low
        return gam

    outer = jnp.logical_or(a == 0, a == 3)
    pair = a + 1 - 2 * (a % 2)

    def send_cross(p, t0, nt):
        def one(k, c):
            aa = jnp.where(k % 2 == 0, 3 - a, 3 - pair)
            oo = lax.rem(o + 1 + k // 2, 4)
            pltpu.make_async_remote_copy(src_ref=sbuf.at[aa * 4 + oo, p, pl.ds(t0, nt)], dst_ref=rbuf.at[a, p, o, pl.ds(t0, nt)],
                                         send_sem=tsend, recv_sem=trecv.at[p], device_id=dev(aa, oo), device_id_type=MESH).start()
            return c
        lax.fori_loop(0, 8, one, 0)

    def send_near(t):
        def one(k, c):
            aa = jnp.where(k % 2 == 0, pair, a)
            oo = lax.rem(o + 1 + k // 2, 4)
            src = sbuf.at[aa * 4 + oo, :, t]
            dst = rbuf.at[a, :, o, t]

            @pl.when(k != 7)
            def _():
                pltpu.make_async_remote_copy(src_ref=src, dst_ref=dst, send_sem=tsend, recv_sem=nrecv,
                                             device_id=dev(aa, oo), device_id_type=MESH).start()

            @pl.when(k == 7)
            def _():
                pltpu.make_async_copy(src, dst, nrecv).start()
            return c
        lax.fori_loop(0, 8, one, 0)

    pltpu.make_async_copy(bt.at[pl.ds(0, 2)], bv.at[pl.ds(0, 2)], lsem.at[2]).wait()

    def two_tiles(u, gam):
        gam = tile(2 * u, gam, u, 0)
        send_cross(0, 2 * u, 1)
        send_near(2 * u)
        gam = tile(2 * u + 1, gam, u, 8)
        send_cross(0, 2 * u + 1, 1)
        send_near(2 * u + 1)
        return gam
    gam = lax.fori_loop(0, 2, two_tiles, gam)

    def one_tile(t, gam):
        gam = tile(t, gam, None, 0)
        send_cross(0, t, 1)
        send_near(t)
        return gam
    gam = lax.fori_loop(4, NT8, one_tile, gam)

    gsend[...] = gam

    def gs(k, c):
        g = lax.rem(me + k, 16)
        pltpu.make_async_remote_copy(src_ref=gsend, dst_ref=grecv.at[a, o], send_sem=gssem, recv_sem=grsem,
                                     device_id=dev(g // 4, g % 4), device_id_type=MESH).start()
        return c
    lax.fori_loop(1, 16, gs, 0)
    pltpu.make_async_copy(gsend, grecv.at[a, o], grsem).start()

    pltpu.make_async_copy(mqr.at[:, pl.ds(0, 32)], mqr.at[:, pl.ds(0, 32)], mzrecv).wait()

    def mo(k, c):
        oo = lax.rem(o + k, 4)
        pltpu.make_async_remote_copy(src_ref=mqr.at[:, quarter], dst_ref=mqr.at[:, quarter], send_sem=mosend, recv_sem=morecv,
                                     device_id=dev(a, oo), device_id_type=MESH).start()
        return c
    lax.fori_loop(1, 4, mo, 0)
    send_cross(1, 0, NT8)
    send_cross(2, 0, NT8)

    @pl.when(outer)
    def _():
        send_cross(3, 0, NT8)
    mq[a] = mloc[...]
    for k in range(1, 4):
        c1 = lax.rem(a + k, 4)
        mq[c1, a] = mloc[c1].T
    pltpu.make_async_copy(mqr.at[:, pl.ds(0, 96)], mqr.at[:, pl.ds(0, 96)], morecv).wait()
    for k in range(1, 4):
        c1 = lax.rem(a + k, 4)
        mq[c1, c1] = mqr[k - 1]
        for k2 in range(k + 1, 4):
            c2 = lax.rem(a + k2, 4)
            first = jnp.where(nearer(c1, c2, a), c1, c2)
            second = c1 + c2 - first
            blk = mqr[k + k2]
            mq[first, second] = blk
            mq[second, first] = blk.T
    for b in range(4):
        parts = split3(jnp.concatenate([mq[aa, b] for aa in range(4)], axis=1))
        for s in range(3):
            msp[s, pl.ds(b * LANES, LANES)] = parts[s]

    pltpu.make_async_copy(grecv, grecv, grsem).wait()
    graw = jnp.concatenate([grecv[aa, 0] + grecv[aa, 1] + grecv[aa, 2] + grecv[aa, 3] for aa in range(4)], axis=1)
    m3 = [msp[s] for s in range(3)]
    gfit = dot(lhs6(split3(graw), 1), rhs6(m3, 0), NN)
    mown = split3(jnp.concatenate([mloc[b] for b in range(4)], axis=0))
    wts = dot(lhs6(split3(gfit), 1), rhs6(mown, 0), NN)
    wl = lhs6(split3(wts), 1)
    low64 = lax.broadcasted_iota(jnp.int32, (nd, LANES), 1) < 64

    def jpair(u, c):
        ys = []
        for e in range(2):
            x = jnp.concatenate([bv[2 * u + e], jnp.zeros((nl, LANES - nq), F32)], axis=1)
            x = jnp.concatenate([x, jnp.zeros((256 - nl, LANES), F32)], axis=0)
            ys.append(dot(wl, rhs6(split3(x), 1), NT))
        for aa in range(4):
            lo = pltpu.roll(ys[0], (256 - nm * aa) % 256, 1)[:, :LANES]
            hi = pltpu.roll(ys[1], (256 + 64 - nm * aa) % 256, 1)[:, :LANES]
            jsend[aa, u] = jnp.where(low64, lo, hi)
        return c

    row8 = lax.broadcasted_iota(jnp.int32, (8, LANES), 0)
    lane8 = lax.broadcasted_iota(jnp.int32, (8, LANES), 1)
    at0 = lane8 - PIECE * row8
    at1 = lane8 - PIECE * (row8 + 8)
    here0 = jnp.logical_and(at0 >= 0, at0 < PIECE)
    here1 = jnp.logical_and(jnp.logical_and(at1 >= 0, at1 < PIECE), lane8 < nq)
    zbuf[:, NT8] = jnp.zeros((4, 2, 8, 512), F32)

    def tails(x):
        f = [x[t].astype(F32) for t in range(4)]
        out = []
        for e in range(2):
            for u in range(2):
                v0 = pltpu.roll(f[2 * u][8 * e:8 * e + 8], LANES - nq, 1, stride=PIECE, stride_axis=0)
                f1 = f[2 * u + 1][8 * e:8 * e + 8]
                v1 = jnp.where(row8 == 0, pltpu.roll(f1, (8 * PIECE - nq) % LANES, 1), pltpu.roll(f1, (9 * PIECE - nq) % LANES, 1))
                v = jnp.where(here0, v0, jnp.where(here1, v1, 0.0))
                out.append(v.sum(0, keepdims=True))
        return out

    def fit(p):
        pltpu.make_async_copy(rbuf.at[pl.ds(0, 2), p], rbuf.at[pl.ds(0, 2), p], trecv.at[p]).wait()
        if p + 3 < npair:
            @pl.when(jnp.logical_not(outer))
            def _():
                send_cross(p + 3, 0, NT8)
        xs = []
        for s in range(4):
            rest = [w for q in range(4) for w in tails(rbuf[s, p, q, pl.ds(0, 4)])]
            xs.append(jnp.concatenate([rbuf[s, p].reshape(4 * NT8 * 16, LANES), jnp.concatenate(rest, axis=0).astype(BF)], axis=0))
        x = jnp.concatenate(xs, axis=1)
        z = dot(jnp.concatenate([x, x, x], axis=1), msp[...].reshape(3 * 512, 512), NN)
        main = 4 * NT8 * 16
        zbuf[:, pl.ds(0, NT8)] = z[:main].reshape(4, NT8, 2, 8, 512)
        for q in range(4):
            for e in range(2):
                zbuf[q, NT8, e, pl.ds(0, 2)] = z[main + 4 * q + 2 * e:main + 4 * q + 2 * e + 2]
        ml = []
        for s in range(2):
            rest = tails(own[s, p, pl.ds(0, 4)]) + [jnp.zeros((12, LANES), F32)]
            ml.append(jnp.concatenate([own[s, p].reshape(NT8 * 16, LANES), jnp.concatenate(rest, axis=0).astype(BF)], axis=0))
        mid, low = ml
        rows = pl.ds(pl.multiple_of(a * LANES, LANES), LANES)
        mh, mm = msp[0, rows], msp[1, rows]
        z = dot(jnp.concatenate([mid, mid, low], axis=1), jnp.concatenate([mh, mm, mh], axis=0), NN)
        zbuf[o, pl.ds(0, NT8)] = zbuf[o, pl.ds(0, NT8)] + z[:NT8 * 16].reshape(NT8, 2, 8, 512)
        for e in range(2):
            zbuf[o, NT8, e, pl.ds(0, 2)] = zbuf[o, NT8, e, pl.ds(0, 2)] + z[NT8 * 16 + 2 * e:NT8 * 16 + 2 * e + 2]
        for e in range(2):
            s3 = split3(zbuf[:, :, e].reshape(4 * MROW, 512))
            k = dot(lhs6(s3, 1), rhs6(s3, 1), NT)
            if p == 0 and e == 0:
                kacc[0] = k[:, :LANES]
                kacc[1] = k[:, LANES:]
            else:
                kacc[0] = kacc[0] + k[:, :LANES]
                kacc[1] = kacc[1] + k[:, LANES:]

    lax.fori_loop(0, nm // 2, jpair, 0)
    near, far = a + 1 - 2 * (a % 2), lax.rem(a + 2, 4)
    hops = []
    for e, aa in enumerate((lax.rem(near + 2, 4), near)):
        hops.append(pltpu.make_async_remote_copy(src_ref=jsend.at[aa], dst_ref=jrecv.at[e], send_sem=jssem.at[e], recv_sem=jrsem.at[e],
                                                 device_id=dev(near, o), device_id_type=MESH))
        hops[-1].start()
    @pl.when(outer)
    def _():
        send_cross(npair - 1, 0, NT8)
    pltpu.make_async_copy(rbuf.at[pl.ds(0, 2)], rbuf.at[pl.ds(0, 2)], nrecv).wait()
    for p in range(npair - 1):
        fit(p)
    hops[0].wait_recv()
    jfwd[...] = jsend[far] + jrecv[0]
    cross = pltpu.make_async_remote_copy(src_ref=jfwd, dst_ref=jrecv.at[2], send_sem=jssem.at[2], recv_sem=jrsem.at[2],
                                         device_id=dev(far, o), device_id_type=MESH)
    cross.start()
    fit(npair - 1)

    mate = o + 1 - 2 * half
    swap = pltpu.make_async_remote_copy(src_ref=kacc.at[1 - half], dst_ref=kin, send_sem=kxs, recv_sem=kxr,
                                        device_id=dev(a, mate), device_id_type=MESH)
    swap.start()
    swap.wait_recv()
    kful[...] = kacc[half] + kin[...]
    low32 = lax.broadcasted_iota(jnp.int32, (32, LANES), 1) < 64
    for oo in range(4):
        ev = kful[pl.ds(MROW * oo, 32, stride=2), :]
        od = kful[pl.ds(MROW * oo + 1, 32, stride=2), :]
        kmsg[0, oo] = jnp.where(low32, ev, pltpu.roll(od, 64, 1))
        kmsg[1, oo] = jnp.where(low32, pltpu.roll(ev, 64, 1), od)

    def ks(k, c):
        al, oo = k // 4, k % 4
        aa = 2 * half + al
        same = jnp.logical_and(aa == a, oo == o)

        @pl.when(jnp.logical_not(same))
        def _():
            pltpu.make_async_remote_copy(src_ref=kmsg.at[al, oo], dst_ref=krecv.at[pl.ds(dens * 32, 32)], send_sem=kss, recv_sem=krs,
                                         device_id=dev(aa, oo), device_id_type=MESH).start()

        @pl.when(same)
        def _():
            cp = pltpu.make_async_copy(kmsg.at[al, oo], krecv.at[pl.ds(dens * 32, 32)], krs)
            cp.start()
        return c
    lax.fori_loop(0, 8, ks, 0)

    hops[1].wait_recv()
    cross.wait_recv()
    pltpu.make_async_copy(krecv, krecv, krs).wait()
    for u in range(nm // 2):
        j = jsend[a, u] + jrecv[1, u] + jrecv[2, u]
        g = 2.0 * j - krecv[pl.ds(u, nd, stride=32), :]
        out[2 * u] = g[:, :nm]
        out[2 * u + 1] = pltpu.roll(g, 64, 1)[:, :nm]

    pltpu.make_async_copy(sbuf.at[pl.ds(0, 15)], sbuf.at[pl.ds(0, 15)], tsend).wait()
    metric_copies(lambda c: c.wait_send())
    pltpu.make_async_copy(mqr.at[:, pl.ds(0, 96)], mqr.at[:, pl.ds(0, 96)], mosend).wait()
    pltpu.make_async_copy(gbuf, gbuf, gssem).wait()
    for c in hops + [cross]:
        c.wait_send()
    swap.wait_send()
    inset = (a // 2) == half

    @pl.when(inset)
    def _():
        pltpu.make_async_copy(krecv.at[pl.ds(0, 224)], krecv.at[pl.ds(0, 224)], kss).wait()

    @pl.when(jnp.logical_not(inset))
    def _():
        pltpu.make_async_copy(krecv, krecv, kss).wait()


def solution(mesh):
    def local_fock(ints_blk, metric_blk, orbitals):
        nq, nm, nl = ints_blk.shape
        nd, _, ni = orbitals.shape
        bt = jnp.transpose(ints_blk, (1, 2, 0))
        mt = metric_blk.T
        ct = jnp.transpose(orbitals, (2, 0, 1)).reshape(ni * nd, nl)
        npair = ni // 4
        V = pltpu.VMEM
        dma = pltpu.SemaphoreType.DMA
        g = pl.pallas_call(
            lambda *refs: kernel(nm, nl, nq, nd, ni, *refs),
            out_shape=pltpu.VMEM((nm, nd, nm), F32),
            in_specs=[pl.BlockSpec(memory_space=pl.ANY)] * 3,
            out_specs=pl.BlockSpec(memory_space=pltpu.VMEM),
            scratch_shapes=[
                V((nm, nl, nq), F32), V((4 * nq, nq), F32), V((ni * nd, nl), F32), V((ni * nd, 256), F32),
                V((8 * SP, LANES), F32), V((16, npair, NT8, 16, LANES), BF), V((4, npair, 4, NT8, 16, LANES), BF),
                V((2, npair, NT8, 16, LANES), BF), V((4, LANES, LANES), F32), V((6, LANES, LANES), F32), V((4, 4, LANES, LANES), F32), V((3, 512, 512), BF),
                V((nd, LANES), F32), V((4, 4, nd, LANES), F32), V((4, nm // 2, nd, LANES), F32), V((3, nm // 2, nd, LANES), F32), V((nm // 2, nd, LANES), F32),
                V((4, 8, 2, 8, 512), F32), V((2, 256, LANES), F32), V((256, LANES), F32), V((256, LANES), F32), V((2, 4, 32, LANES), F32),
                V((8 * 32, LANES), F32), V((15, nd, LANES), F32),
                dma((NT8,)), dma((3,)), dma, dma, dma((npair,)), dma, dma, dma, dma, dma, dma, dma((3,)), dma((3,)), dma, dma, dma, dma],
            compiler_params=pltpu.CompilerParams(collective_id=0, has_side_effects=True, vmem_limit_bytes=60 * 2**20),
        )(bt, mt, ct)
        return jnp.transpose(g, (1, 0, 2))

    return jax.shard_map(local_fock, mesh=mesh, in_specs=(P(('sys', 'aux'), 'orb', None), P(('sys', 'aux'), None), P('sys', None, None)), out_specs=P('sys', 'orb', 'aux'), check_vma=False)
```

```python
import jax
import jax.numpy as jnp
from jax import lax
from jax.experimental import pallas as pl
from jax.experimental.pallas import tpu as pltpu
from jax.sharding import PartitionSpec as P

F32 = jnp.float32
BF = jnp.bfloat16
MESH = pl.DeviceIdType.MESH
NN = (((1,), (0,)), ((), ()))
NT = (((1,), (1,)), ((), ()))
LANES = 128
MROW = 64
NT8 = 7
PIECE = 12
SP = 168


def split3(x):
    hi = x.astype(BF)
    rest = x - hi.astype(F32)
    mid = rest.astype(BF)
    return hi, mid, (rest - mid.astype(F32)).astype(BF)


def dot(x, y, dims):
    return lax.dot_general(x, y, dims, preferred_element_type=F32)


def lhs6(x, axis):
    h, m, l = x
    return jnp.concatenate([h, h, m, m, h, l], axis=axis)


def rhs6(x, axis):
    h, m, l = x
    return jnp.concatenate([h, m, h, m, l, h], axis=axis)


def kernel(nm, nl, nq, nd, ni, bt, mt, ct, out, bv, mv, cv, ctp, tr, sbuf, rbuf, own, mloc, mqr, mq, msp, gsend, grecv, jsend, jrecv, jfwd, zbuf, kacc, kin, kful, kmsg, krecv, gbuf,
           bsem, lsem, tsend, trecv, mzsend, mzrecv, mosend, morecv, gssem, grsem, jssem, jrsem, kxs, kxr, kss, krs):
    sy, a, o = lax.axis_index('sys'), lax.axis_index('aux'), lax.axis_index('orb')
    me = a * 4 + o
    dens, half = me // 2, me % 2
    nh = ni // 2
    npair = nh // 2

    def dev(aa, oo):
        return (sy, aa, oo)

    pltpu.make_async_copy(ct, cv, lsem.at[0]).start()
    pltpu.make_async_copy(bt.at[pl.ds(8 * NT8, 2)], bv.at[pl.ds(8 * NT8, 2)], lsem.at[2]).start()
    for t in range(NT8):
        pltpu.make_async_copy(bt.at[pl.ds(8 * t, 8)], bv.at[pl.ds(8 * t, 8)], bsem.at[t]).start()
        if t == 0:
            pltpu.make_async_copy(mt, mv, lsem.at[1]).start()
    barrier = pltpu.get_barrier_semaphore()

    def tell(k, c):
        g = lax.rem(me + k, 16)
        pl.semaphore_signal(barrier, inc=1, device_id=dev(g // 4, g % 4), device_id_type=MESH)
        return c
    lax.fori_loop(1, 16, tell, 0)

    pltpu.make_async_copy(ct, cv, lsem.at[0]).wait()
    ctp[...] = jnp.concatenate([cv[...], jnp.zeros((nd * ni, 256 - nl), F32)], axis=1)
    lhs = lhs6(split3(ctp[...]), 1)
    pltpu.make_async_copy(mt, mv, lsem.at[1]).wait()
    for b in range(4):
        blk = jnp.concatenate([mv[nq * b:nq * (b + 1), :], jnp.zeros((nq, LANES - nq), F32)], axis=1)
        mloc[b] = jnp.concatenate([blk, jnp.zeros((LANES - nq, LANES), F32)], axis=0)
    pl.semaphore_wait(barrier, 15)

    quarter = pl.ds(pl.multiple_of(o * 32, 32), 32)

    def nearer(x, y, z):
        dx, dy = jnp.abs(x - z), jnp.abs(y - z)
        return jnp.logical_or(dx < dy, jnp.logical_and(dx == dy, x < y))

    def metric_copies(act):
        for k in (2, 1, 3):
            to = lax.rem(a + 4 - k, 4)

            def block(row, slot):
                return pltpu.make_async_remote_copy(src_ref=mloc.at[row, quarter], dst_ref=mqr.at[slot, quarter], send_sem=mzsend,
                                                    recv_sem=mzrecv, device_id=dev(to, o), device_id_type=MESH)
            act(block(a, k - 1))
            for k2 in (1, 2, 3):
                if k2 == k:
                    continue
                b = lax.rem(to + k2, 4)

                @pl.when(nearer(a, b, to))
                def _():
                    act(block(b, k + k2))
    metric_copies(lambda c: c.start())

    gam = jnp.zeros((nd, LANES), F32)
    tr2 = tr

    lane = lax.broadcasted_iota(jnp.int32, (1, LANES), 1)
    data = lane < nq

    def tile(t, gam, tail, first):
        pltpu.make_async_copy(bt.at[pl.ds(0, 8)], bv.at[pl.ds(0, 8)], bsem.at[t]).wait()
        cols = pltpu.roll(ctp[...], lax.rem(512 - (nm * o + 8 * t), 256), 1)
        count = 0
        if tail is not None:
            count = min(8, 10 - first)
            spare = jnp.concatenate([bv[8 * NT8 + tail], jnp.zeros((nl, LANES - nq), F32)], axis=1)
            tcol = pltpu.roll(ctp[...], lax.rem(512 - (nm * o + 8 * NT8 + tail), 256), 1)[:, 0:1]
        for r in range(0, 8, 2):
            xs = []
            for e in range(2):
                x = jnp.concatenate([bv[8 * t + r + e], jnp.zeros((nl, LANES - nq), F32)], axis=1)
                if r + e < count:
                    x = jnp.where(data, x, pltpu.roll(spare, (nq - PIECE * (first + r + e)) % LANES, 1))
                xs.append(x)
            x = jnp.concatenate(xs, axis=1)
            x = jnp.concatenate([x, jnp.zeros((256 - nl, 2 * LANES), F32)], axis=0)
            y = dot(lhs, rhs6(split3(x), 0), NN)
            for e in range(2):
                ye = y[:, e * LANES:(e + 1) * LANES]
                tr2[pl.ds((r + e) * SP, nd * ni), :] = ye
                col = cols[:, r + e:r + e + 1]
                if r + e < count:
                    w = (ye * jnp.where(data, col, tcol)).reshape(ni, nd, LANES).sum(0)
                    moved = pltpu.roll(jnp.where(data, 0.0, w), (PIECE * (first + r + e) - nq) % LANES, 1)
                    gam = gam + jnp.where(data, w, 0.0) + moved
                else:
                    gam = gam + (ye * col).reshape(ni, nd, LANES).sum(0)
        for g in range(16):
            d, h = g // 2, g % 2
            for p in range(npair):
                two = [tr2[pl.ds((h * nh + 2 * p + e) * nd + d, 8, stride=SP), :] for e in range(2)]
                sbuf[g, p, t] = jnp.concatenate(two, axis=0).astype(BF)
        for p in range(npair):
            two = [tr2[pl.ds((half * nh + 2 * p + e) * nd + dens, 8, stride=SP), :] for e in range(2)]
            _, mid, low = split3(jnp.concatenate(two, axis=0))
            own[0, p, t] = mid
            own[1, p, t] = low
        return gam

    def send_t1(p, t0, nt):
        def one(k, c):
            j, u = k % 4, k // 4
            aa = lax.rem(a + 2 + j, 4)
            oo = lax.rem(o + 1 + u, 4)
            g = aa * 4 + oo
            src = sbuf.at[g, p, pl.ds(t0, nt)]
            dst = rbuf.at[a, p, o, pl.ds(t0, nt)]

            @pl.when(k != 14)
            def _():
                pltpu.make_async_remote_copy(src_ref=src, dst_ref=dst, send_sem=tsend, recv_sem=trecv.at[p],
                                             device_id=dev(aa, oo), device_id_type=MESH).start()

            @pl.when(k == 14)
            def _():
                pltpu.make_async_copy(src, dst, trecv.at[p]).start()
            return c
        lax.fori_loop(0, 16, one, 0)

    outer = jnp.logical_or(a == 0, a == 3)
    pair = a + 1 - 2 * (a % 2)

    def send_part(p, t0, nt, cross):
        def one(k, c):
            if cross:
                aa = jnp.where(k % 2 == 0, 3 - a, 3 - pair)
                oo = lax.rem(o + 1 + k // 2, 4)
            else:
                aa = jnp.where(k % 2 == 0, pair, a)
                oo = lax.rem(o + 1 + k // 2, 4)
            g = aa * 4 + oo
            src = sbuf.at[g, p, pl.ds(t0, nt)]
            dst = rbuf.at[a, p, o, pl.ds(t0, nt)]

            def far():
                pltpu.make_async_remote_copy(src_ref=src, dst_ref=dst, send_sem=tsend, recv_sem=trecv.at[p],
                                             device_id=dev(aa, oo), device_id_type=MESH).start()
            if cross:
                far()
            else:
                pl.when(k != 7)(far)

                @pl.when(k == 7)
                def _():
                    pltpu.make_async_copy(src, dst, trecv.at[p]).start()
            return c
        lax.fori_loop(0, 8, one, 0)

    def send_half(p, t0, nt, cross):
        send_part(p, t0, 4, cross)
        send_part(p, t0 + 4, nt - 4, cross)

    def send_both(p):
        send_t1(p, 0, 4)
        send_t1(p, 4, NT8 - 4)

    pltpu.make_async_copy(bt.at[pl.ds(0, 2)], bv.at[pl.ds(0, 2)], lsem.at[2]).wait()

    def two_tiles(u, gam):
        gam = tile(2 * u, gam, u, 0)
        send_t1(0, 2 * u, 1)
        gam = tile(2 * u + 1, gam, u, 8)
        send_t1(0, 2 * u + 1, 1)
        return gam
    gam = lax.fori_loop(0, 2, two_tiles, gam)

    def one_tile(t, gam):
        gam = tile(t, gam, None, 0)
        send_t1(0, t, 1)
        return gam
    gam = lax.fori_loop(4, NT8, one_tile, gam)

    gsend[...] = gam

    def gs(k, c):
        g = lax.rem(me + k, 16)
        pltpu.make_async_remote_copy(src_ref=gsend, dst_ref=grecv.at[a, o], send_sem=gssem, recv_sem=grsem,
                                     device_id=dev(g // 4, g % 4), device_id_type=MESH).start()
        return c
    lax.fori_loop(1, 16, gs, 0)
    pltpu.make_async_copy(gsend, grecv.at[a, o], grsem).start()

    pltpu.make_async_copy(mqr.at[:, pl.ds(0, 32)], mqr.at[:, pl.ds(0, 32)], mzrecv).wait()

    def mo(k, c):
        oo = lax.rem(o + k, 4)
        pltpu.make_async_remote_copy(src_ref=mqr.at[:, quarter], dst_ref=mqr.at[:, quarter], send_sem=mosend, recv_sem=morecv,
                                     device_id=dev(a, oo), device_id_type=MESH).start()
        return c
    lax.fori_loop(1, 4, mo, 0)
    @pl.when(outer)
    def _():
        send_half(1, 0, NT8, False)
        send_half(2, 0, NT8, False)
        send_half(1, 0, NT8, True)
        send_half(3, 0, NT8, False)
        send_half(4, 0, NT8, False)
        send_half(2, 0, NT8, True)
        send_half(3, 0, NT8, True)

    @pl.when(jnp.logical_not(outer))
    def _():
        for p in range(1, 3):
            send_both(p)
    mq[a] = mloc[...]
    for k in range(1, 4):
        c1 = lax.rem(a + k, 4)
        mq[c1, a] = mloc[c1].T
    pltpu.make_async_copy(mqr.at[:, pl.ds(0, 96)], mqr.at[:, pl.ds(0, 96)], morecv).wait()
    for k in range(1, 4):
        c1 = lax.rem(a + k, 4)
        mq[c1, c1] = mqr[k - 1]
        for k2 in range(k + 1, 4):
            c2 = lax.rem(a + k2, 4)
            first = jnp.where(nearer(c1, c2, a), c1, c2)
            second = c1 + c2 - first
            blk = mqr[k + k2]
            mq[first, second] = blk
            mq[second, first] = blk.T
    for b in range(4):
        parts = split3(jnp.concatenate([mq[aa, b] for aa in range(4)], axis=1))
        for s in range(3):
            msp[s, pl.ds(b * LANES, LANES)] = parts[s]

    pltpu.make_async_copy(grecv, grecv, grsem).wait()
    graw = jnp.concatenate([grecv[aa, 0] + grecv[aa, 1] + grecv[aa, 2] + grecv[aa, 3] for aa in range(4)], axis=1)
    m3 = [msp[s] for s in range(3)]
    gfit = dot(lhs6(split3(graw), 1), rhs6(m3, 0), NN)
    mown = split3(jnp.concatenate([mloc[b] for b in range(4)], axis=0))
    wts = dot(lhs6(split3(gfit), 1), rhs6(mown, 0), NN)
    wl = lhs6(split3(wts), 1)
    low64 = lax.broadcasted_iota(jnp.int32, (nd, LANES), 1) < 64

    def jpair(u, c):
        ys = []
        for e in range(2):
            x = jnp.concatenate([bv[2 * u + e], jnp.zeros((nl, LANES - nq), F32)], axis=1)
            x = jnp.concatenate([x, jnp.zeros((256 - nl, LANES), F32)], axis=0)
            ys.append(dot(wl, rhs6(split3(x), 1), NT))
        for aa in range(4):
            lo = pltpu.roll(ys[0], (256 - nm * aa) % 256, 1)[:, :LANES]
            hi = pltpu.roll(ys[1], (256 + 64 - nm * aa) % 256, 1)[:, :LANES]
            jsend[aa, u] = jnp.where(low64, lo, hi)
        return c

    row8 = lax.broadcasted_iota(jnp.int32, (8, LANES), 0)
    lane8 = lax.broadcasted_iota(jnp.int32, (8, LANES), 1)
    at0 = lane8 - PIECE * row8
    at1 = lane8 - PIECE * (row8 + 8)
    here0 = jnp.logical_and(at0 >= 0, at0 < PIECE)
    here1 = jnp.logical_and(jnp.logical_and(at1 >= 0, at1 < PIECE), lane8 < nq)
    zbuf[:, NT8] = jnp.zeros((4, 2, 8, 512), F32)

    def tails(x):
        f = [x[t].astype(F32) for t in range(4)]
        out = []
        for e in range(2):
            for u in range(2):
                v0 = pltpu.roll(f[2 * u][8 * e:8 * e + 8], LANES - nq, 1, stride=PIECE, stride_axis=0)
                f1 = f[2 * u + 1][8 * e:8 * e + 8]
                v1 = jnp.where(row8 == 0, pltpu.roll(f1, (8 * PIECE - nq) % LANES, 1), pltpu.roll(f1, (9 * PIECE - nq) % LANES, 1))
                v = jnp.where(here0, v0, jnp.where(here1, v1, 0.0))
                out.append(v.sum(0, keepdims=True))
        return out

    def fit(p):
        pltpu.make_async_copy(rbuf.at[:, p], rbuf.at[:, p], trecv.at[p]).wait()
        if p + 3 < npair:
            @pl.when(jnp.logical_not(outer))
            def _():
                send_half(p + 3, 0, NT8, True)
        xs = []
        for s in range(4):
            rest = [w for q in range(4) for w in tails(rbuf[s, p, q, pl.ds(0, 4)])]
            xs.append(jnp.concatenate([rbuf[s, p].reshape(4 * NT8 * 16, LANES), jnp.concatenate(rest, axis=0).astype(BF)], axis=0))
        x = jnp.concatenate(xs, axis=1)
        z = dot(jnp.concatenate([x, x, x], axis=1), msp[...].reshape(3 * 512, 512), NN)
        main = 4 * NT8 * 16
        zbuf[:, pl.ds(0, NT8)] = z[:main].reshape(4, NT8, 2, 8, 512)
        for q in range(4):
            for e in range(2):
                zbuf[q, NT8, e, pl.ds(0, 2)] = z[main + 4 * q + 2 * e:main + 4 * q + 2 * e + 2]
        ml = []
        for s in range(2):
            rest = tails(own[s, p, pl.ds(0, 4)]) + [jnp.zeros((12, LANES), F32)]
            ml.append(jnp.concatenate([own[s, p].reshape(NT8 * 16, LANES), jnp.concatenate(rest, axis=0).astype(BF)], axis=0))
        mid, low = ml
        rows = pl.ds(pl.multiple_of(a * LANES, LANES), LANES)
        mh, mm = msp[0, rows], msp[1, rows]
        z = dot(jnp.concatenate([mid, mid, low], axis=1), jnp.concatenate([mh, mm, mh], axis=0), NN)
        zbuf[o, pl.ds(0, NT8)] = zbuf[o, pl.ds(0, NT8)] + z[:NT8 * 16].reshape(NT8, 2, 8, 512)
        for e in range(2):
            zbuf[o, NT8, e, pl.ds(0, 2)] = zbuf[o, NT8, e, pl.ds(0, 2)] + z[NT8 * 16 + 2 * e:NT8 * 16 + 2 * e + 2]
        for e in range(2):
            s3 = split3(zbuf[:, :, e].reshape(4 * MROW, 512))
            k = dot(lhs6(s3, 1), rhs6(s3, 1), NT)
            if p == 0 and e == 0:
                kacc[0] = k[:, :LANES]
                kacc[1] = k[:, LANES:]
            else:
                kacc[0] = kacc[0] + k[:, :LANES]
                kacc[1] = kacc[1] + k[:, LANES:]

    lax.fori_loop(0, nm // 2, jpair, 0)
    near, far = a + 1 - 2 * (a % 2), lax.rem(a + 2, 4)
    hops = []
    for e, aa in enumerate((lax.rem(near + 2, 4), near)):
        hops.append(pltpu.make_async_remote_copy(src_ref=jsend.at[aa], dst_ref=jrecv.at[e], send_sem=jssem.at[e], recv_sem=jrsem.at[e],
                                                 device_id=dev(near, o), device_id_type=MESH))
        hops[-1].start()
    @pl.when(outer)
    def _():
        send_half(npair - 1, 0, NT8, True)

    @pl.when(jnp.logical_not(outer))
    def _():
        for p in range(3, npair):
            send_half(p, 0, NT8, False)
    for p in range(npair - 1):
        fit(p)
    hops[0].wait_recv()
    jfwd[...] = jsend[far] + jrecv[0]
    cross = pltpu.make_async_remote_copy(src_ref=jfwd, dst_ref=jrecv.at[2], send_sem=jssem.at[2], recv_sem=jrsem.at[2],
                                         device_id=dev(far, o), device_id_type=MESH)
    cross.start()
    fit(npair - 1)

    mate = o + 1 - 2 * half
    swap = pltpu.make_async_remote_copy(src_ref=kacc.at[1 - half], dst_ref=kin, send_sem=kxs, recv_sem=kxr,
                                        device_id=dev(a, mate), device_id_type=MESH)
    swap.start()
    swap.wait_recv()
    kful[...] = kacc[half] + kin[...]
    low32 = lax.broadcasted_iota(jnp.int32, (32, LANES), 1) < 64
    for oo in range(4):
        ev = kful[pl.ds(MROW * oo, 32, stride=2), :]
        od = kful[pl.ds(MROW * oo + 1, 32, stride=2), :]
        kmsg[0, oo] = jnp.where(low32, ev, pltpu.roll(od, 64, 1))
        kmsg[1, oo] = jnp.where(low32, pltpu.roll(ev, 64, 1), od)

    def ks(k, c):
        al, oo = k // 4, k % 4
        aa = 2 * half + al
        same = jnp.logical_and(aa == a, oo == o)

        @pl.when(jnp.logical_not(same))
        def _():
            pltpu.make_async_remote_copy(src_ref=kmsg.at[al, oo], dst_ref=krecv.at[pl.ds(dens * 32, 32)], send_sem=kss, recv_sem=krs,
                                         device_id=dev(aa, oo), device_id_type=MESH).start()

        @pl.when(same)
        def _():
            cp = pltpu.make_async_copy(kmsg.at[al, oo], krecv.at[pl.ds(dens * 32, 32)], krs)
            cp.start()
        return c
    lax.fori_loop(0, 8, ks, 0)

    hops[1].wait_recv()
    cross.wait_recv()
    pltpu.make_async_copy(krecv, krecv, krs).wait()
    for u in range(nm // 2):
        j = jsend[a, u] + jrecv[1, u] + jrecv[2, u]
        g = 2.0 * j - krecv[pl.ds(u, nd, stride=32), :]
        out[2 * u] = g[:, :nm]
        out[2 * u + 1] = pltpu.roll(g, 64, 1)[:, :nm]

    pltpu.make_async_copy(sbuf.at[pl.ds(0, 15)], sbuf.at[pl.ds(0, 15)], tsend).wait()
    metric_copies(lambda c: c.wait_send())
    pltpu.make_async_copy(mqr.at[:, pl.ds(0, 96)], mqr.at[:, pl.ds(0, 96)], mosend).wait()
    pltpu.make_async_copy(gbuf, gbuf, gssem).wait()
    for c in hops + [cross]:
        c.wait_send()
    swap.wait_send()
    inset = (a // 2) == half

    @pl.when(inset)
    def _():
        pltpu.make_async_copy(krecv.at[pl.ds(0, 224)], krecv.at[pl.ds(0, 224)], kss).wait()

    @pl.when(jnp.logical_not(inset))
    def _():
        pltpu.make_async_copy(krecv, krecv, kss).wait()


def solution(mesh):
    def local_fock(ints_blk, metric_blk, orbitals):
        nq, nm, nl = ints_blk.shape
        nd, _, ni = orbitals.shape
        bt = jnp.transpose(ints_blk, (1, 2, 0))
        mt = metric_blk.T
        ct = jnp.transpose(orbitals, (2, 0, 1)).reshape(ni * nd, nl)
        npair = ni // 4
        V = pltpu.VMEM
        dma = pltpu.SemaphoreType.DMA
        g = pl.pallas_call(
            lambda *refs: kernel(nm, nl, nq, nd, ni, *refs),
            out_shape=pltpu.VMEM((nm, nd, nm), F32),
            in_specs=[pl.BlockSpec(memory_space=pl.ANY)] * 3,
            out_specs=pl.BlockSpec(memory_space=pltpu.VMEM),
            scratch_shapes=[
                V((nm, nl, nq), F32), V((4 * nq, nq), F32), V((ni * nd, nl), F32), V((ni * nd, 256), F32),
                V((8 * SP, LANES), F32), V((16, npair, NT8, 16, LANES), BF), V((4, npair, 4, NT8, 16, LANES), BF),
                V((2, npair, NT8, 16, LANES), BF), V((4, LANES, LANES), F32), V((6, LANES, LANES), F32), V((4, 4, LANES, LANES), F32), V((3, 512, 512), BF),
                V((nd, LANES), F32), V((4, 4, nd, LANES), F32), V((4, nm // 2, nd, LANES), F32), V((3, nm // 2, nd, LANES), F32), V((nm // 2, nd, LANES), F32),
                V((4, 8, 2, 8, 512), F32), V((2, 256, LANES), F32), V((256, LANES), F32), V((256, LANES), F32), V((2, 4, 32, LANES), F32),
                V((8 * 32, LANES), F32), V((15, nd, LANES), F32),
                dma((NT8,)), dma((3,)), dma, dma((npair,)), dma, dma, dma, dma, dma, dma, dma((3,)), dma((3,)), dma, dma, dma, dma],
            compiler_params=pltpu.CompilerParams(collective_id=0, has_side_effects=True, vmem_limit_bytes=60 * 2**20),
        )(bt, mt, ct)
        return jnp.transpose(g, (1, 0, 2))

    return jax.shard_map(local_fock, mesh=mesh, in_specs=(P(('sys', 'aux'), 'orb', None), P(('sys', 'aux'), None), P('sys', None, None)), out_specs=P('sys', 'orb', 'aux'), check_vma=False)
```

```python
import jax
import jax.numpy as jnp
from jax import lax
from jax.experimental import pallas as pl
from jax.experimental.pallas import tpu as pltpu
from jax.sharding import PartitionSpec as P

F32 = jnp.float32
BF = jnp.bfloat16
MESH = pl.DeviceIdType.MESH
NN = (((1,), (0,)), ((), ()))
NT = (((1,), (1,)), ((), ()))
LANES = 128
MROW = 64
NT8 = 7
PIECE = 12
SP = 168


def split3(x):
    hi = x.astype(BF)
    rest = x - hi.astype(F32)
    mid = rest.astype(BF)
    return hi, mid, (rest - mid.astype(F32)).astype(BF)


def dot(x, y, dims):
    return lax.dot_general(x, y, dims, preferred_element_type=F32)


def lhs6(x, axis):
    h, m, l = x
    return jnp.concatenate([h, h, m, m, h, l], axis=axis)


def rhs6(x, axis):
    h, m, l = x
    return jnp.concatenate([h, m, h, m, l, h], axis=axis)


def kernel(nm, nl, nq, nd, ni, bt, mt, ct, out, bv, mv, cv, ctp, tr, sbuf, rbuf, own, mloc, mqr, mq, msp, gsend, grecv, jsend, jrecv, jfwd, zbuf, kacc, kin, kful, kmsg, krecv, gbuf,
           bsem, lsem, tsend, trecv, mzsend, mzrecv, mosend, morecv, gssem, grsem, jssem, jrsem, kxs, kxr, kss, krs):
    sy, a, o = lax.axis_index('sys'), lax.axis_index('aux'), lax.axis_index('orb')
    me = a * 4 + o
    dens, half = me // 2, me % 2
    nh = ni // 2
    npair = nh // 2

    def dev(aa, oo):
        return (sy, aa, oo)

    pltpu.make_async_copy(ct, cv, lsem.at[0]).start()
    pltpu.make_async_copy(bt.at[pl.ds(8 * NT8, 2)], bv.at[pl.ds(8 * NT8, 2)], lsem.at[2]).start()
    for t in range(NT8):
        pltpu.make_async_copy(bt.at[pl.ds(8 * t, 8)], bv.at[pl.ds(8 * t, 8)], bsem.at[t]).start()
        if t == 0:
            pltpu.make_async_copy(mt, mv, lsem.at[1]).start()
    barrier = pltpu.get_barrier_semaphore()

    def tell(k, c):
        g = lax.rem(me + k, 16)
        pl.semaphore_signal(barrier, inc=1, device_id=dev(g // 4, g % 4), device_id_type=MESH)
        return c
    lax.fori_loop(1, 16, tell, 0)

    pltpu.make_async_copy(ct, cv, lsem.at[0]).wait()
    ctp[...] = jnp.concatenate([cv[...], jnp.zeros((nd * ni, 256 - nl), F32)], axis=1)
    lhs = lhs6(split3(ctp[...]), 1)
    pltpu.make_async_copy(mt, mv, lsem.at[1]).wait()
    for b in range(4):
        blk = jnp.concatenate([mv[nq * b:nq * (b + 1), :], jnp.zeros((nq, LANES - nq), F32)], axis=1)
        mloc[b] = jnp.concatenate([blk, jnp.zeros((LANES - nq, LANES), F32)], axis=0)
    pl.semaphore_wait(barrier, 15)

    quarter = pl.ds(pl.multiple_of(o * 32, 32), 32)

    def nearer(x, y, z):
        dx, dy = jnp.abs(x - z), jnp.abs(y - z)
        return jnp.logical_or(dx < dy, jnp.logical_and(dx == dy, x < y))

    def metric_copies(act):
        for k in (2, 1, 3):
            to = lax.rem(a + 4 - k, 4)

            def block(row, slot):
                return pltpu.make_async_remote_copy(src_ref=mloc.at[row, quarter], dst_ref=mqr.at[slot, quarter], send_sem=mzsend,
                                                    recv_sem=mzrecv, device_id=dev(to, o), device_id_type=MESH)
            act(block(a, k - 1))
            for k2 in (1, 2, 3):
                if k2 == k:
                    continue
                b = lax.rem(to + k2, 4)

                @pl.when(nearer(a, b, to))
                def _():
                    act(block(b, k + k2))
    metric_copies(lambda c: c.start())

    gam = jnp.zeros((nd, LANES), F32)
    tr2 = tr

    lane = lax.broadcasted_iota(jnp.int32, (1, LANES), 1)
    data = lane < nq

    def tile(t, gam, tail, first):
        pltpu.make_async_copy(bt.at[pl.ds(0, 8)], bv.at[pl.ds(0, 8)], bsem.at[t]).wait()
        cols = pltpu.roll(ctp[...], lax.rem(512 - (nm * o + 8 * t), 256), 1)
        count = 0
        if tail is not None:
            count = min(8, 10 - first)
            spare = jnp.concatenate([bv[8 * NT8 + tail], jnp.zeros((nl, LANES - nq), F32)], axis=1)
            tcol = pltpu.roll(ctp[...], lax.rem(512 - (nm * o + 8 * NT8 + tail), 256), 1)[:, 0:1]
        for r in range(0, 8, 2):
            xs = []
            for e in range(2):
                x = jnp.concatenate([bv[8 * t + r + e], jnp.zeros((nl, LANES - nq), F32)], axis=1)
                if r + e < count:
                    x = jnp.where(data, x, pltpu.roll(spare, (nq - PIECE * (first + r + e)) % LANES, 1))
                xs.append(x)
            x = jnp.concatenate(xs, axis=1)
            x = jnp.concatenate([x, jnp.zeros((256 - nl, 2 * LANES), F32)], axis=0)
            y = dot(lhs, rhs6(split3(x), 0), NN)
            for e in range(2):
                ye = y[:, e * LANES:(e + 1) * LANES]
                tr2[pl.ds((r + e) * SP, nd * ni), :] = ye
                col = cols[:, r + e:r + e + 1]
                if r + e < count:
                    w = (ye * jnp.where(data, col, tcol)).reshape(ni, nd, LANES).sum(0)
                    moved = pltpu.roll(jnp.where(data, 0.0, w), (PIECE * (first + r + e) - nq) % LANES, 1)
                    gam = gam + jnp.where(data, w, 0.0) + moved
                else:
                    gam = gam + (ye * col).reshape(ni, nd, LANES).sum(0)
        for g in range(16):
            d, h = g // 2, g % 2
            for p in range(npair):
                two = [tr2[pl.ds((h * nh + 2 * p + e) * nd + d, 8, stride=SP), :] for e in range(2)]
                sbuf[g, p, t] = jnp.concatenate(two, axis=0).astype(BF)
        for p in range(npair):
            two = [tr2[pl.ds((half * nh + 2 * p + e) * nd + dens, 8, stride=SP), :] for e in range(2)]
            _, mid, low = split3(jnp.concatenate(two, axis=0))
            own[0, p, t] = mid
            own[1, p, t] = low
        return gam

    def send_t1(p, t0, nt):
        def one(k, c):
            j, u = k % 4, k // 4
            aa = lax.rem(a + 2 + j, 4)
            oo = lax.rem(o + 1 + u, 4)
            g = aa * 4 + oo
            src = sbuf.at[g, p, pl.ds(t0, nt)]
            dst = rbuf.at[a, p, o, pl.ds(t0, nt)]

            @pl.when(k != 14)
            def _():
                pltpu.make_async_remote_copy(src_ref=src, dst_ref=dst, send_sem=tsend, recv_sem=trecv.at[p],
                                             device_id=dev(aa, oo), device_id_type=MESH).start()

            @pl.when(k == 14)
            def _():
                pltpu.make_async_copy(src, dst, trecv.at[p]).start()
            return c
        lax.fori_loop(0, 16, one, 0)

    outer = jnp.logical_or(a == 0, a == 3)
    pair = a + 1 - 2 * (a % 2)

    def send_half(p, t0, nt, cross):
        def one(k, c):
            if cross:
                aa = jnp.where(k % 2 == 0, 3 - a, 3 - pair)
                oo = lax.rem(o + 1 + k // 2, 4)
            else:
                aa = jnp.where(k % 2 == 0, pair, a)
                oo = lax.rem(o + 1 + k // 2, 4)
            g = aa * 4 + oo
            src = sbuf.at[g, p, pl.ds(t0, nt)]
            dst = rbuf.at[a, p, o, pl.ds(t0, nt)]

            def far():
                pltpu.make_async_remote_copy(src_ref=src, dst_ref=dst, send_sem=tsend, recv_sem=trecv.at[p],
                                             device_id=dev(aa, oo), device_id_type=MESH).start()
            if cross:
                far()
            else:
                pl.when(k != 7)(far)

                @pl.when(k == 7)
                def _():
                    pltpu.make_async_copy(src, dst, trecv.at[p]).start()
            return c
        lax.fori_loop(0, 8, one, 0)

    pltpu.make_async_copy(bt.at[pl.ds(0, 2)], bv.at[pl.ds(0, 2)], lsem.at[2]).wait()

    def two_tiles(u, gam):
        gam = tile(2 * u, gam, u, 0)
        gam = tile(2 * u + 1, gam, u, 8)
        send_t1(0, 2 * u, 2)
        return gam
    gam = lax.fori_loop(0, 2, two_tiles, gam)

    def one_tile(t, gam):
        return tile(t, gam, None, 0)
    gam = lax.fori_loop(4, NT8, one_tile, gam)
    send_t1(0, 4, NT8 - 4)

    gsend[...] = gam

    def gs(k, c):
        g = lax.rem(me + k, 16)
        pltpu.make_async_remote_copy(src_ref=gsend, dst_ref=grecv.at[a, o], send_sem=gssem, recv_sem=grsem,
                                     device_id=dev(g // 4, g % 4), device_id_type=MESH).start()
        return c
    lax.fori_loop(1, 16, gs, 0)
    pltpu.make_async_copy(gsend, grecv.at[a, o], grsem).start()

    pltpu.make_async_copy(mqr.at[:, pl.ds(0, 32)], mqr.at[:, pl.ds(0, 32)], mzrecv).wait()

    def mo(k, c):
        oo = lax.rem(o + k, 4)
        pltpu.make_async_remote_copy(src_ref=mqr.at[:, quarter], dst_ref=mqr.at[:, quarter], send_sem=mosend, recv_sem=morecv,
                                     device_id=dev(a, oo), device_id_type=MESH).start()
        return c
    lax.fori_loop(1, 4, mo, 0)
    @pl.when(outer)
    def _():
        send_half(1, 0, NT8, False)
        send_half(2, 0, NT8, False)
        send_half(1, 0, NT8, True)
        send_half(3, 0, NT8, False)
        send_half(4, 0, NT8, False)
        send_half(2, 0, NT8, True)
        send_half(3, 0, NT8, True)

    @pl.when(jnp.logical_not(outer))
    def _():
        for p in range(1, 3):
            send_t1(p, 0, NT8)
    mq[a] = mloc[...]
    for k in range(1, 4):
        c1 = lax.rem(a + k, 4)
        mq[c1, a] = mloc[c1].T
    pltpu.make_async_copy(mqr.at[:, pl.ds(0, 96)], mqr.at[:, pl.ds(0, 96)], morecv).wait()
    for k in range(1, 4):
        c1 = lax.rem(a + k, 4)
        mq[c1, c1] = mqr[k - 1]
        for k2 in range(k + 1, 4):
            c2 = lax.rem(a + k2, 4)
            first = jnp.where(nearer(c1, c2, a), c1, c2)
            second = c1 + c2 - first
            blk = mqr[k + k2]
            mq[first, second] = blk
            mq[second, first] = blk.T
    for b in range(4):
        parts = split3(jnp.concatenate([mq[aa, b] for aa in range(4)], axis=1))
        for s in range(3):
            msp[s, pl.ds(b * LANES, LANES)] = parts[s]

    pltpu.make_async_copy(grecv, grecv, grsem).wait()
    graw = jnp.concatenate([grecv[aa, 0] + grecv[aa, 1] + grecv[aa, 2] + grecv[aa, 3] for aa in range(4)], axis=1)
    m3 = [msp[s] for s in range(3)]
    gfit = dot(lhs6(split3(graw), 1), rhs6(m3, 0), NN)
    mown = split3(jnp.concatenate([mloc[b] for b in range(4)], axis=0))
    wts = dot(lhs6(split3(gfit), 1), rhs6(mown, 0), NN)
    wl = lhs6(split3(wts), 1)
    low64 = lax.broadcasted_iota(jnp.int32, (nd, LANES), 1) < 64

    def jpair(u, c):
        ys = []
        for e in range(2):
            x = jnp.concatenate([bv[2 * u + e], jnp.zeros((nl, LANES - nq), F32)], axis=1)
            x = jnp.concatenate([x, jnp.zeros((256 - nl, LANES), F32)], axis=0)
            ys.append(dot(wl, rhs6(split3(x), 1), NT))
        for aa in range(4):
            lo = pltpu.roll(ys[0], (256 - nm * aa) % 256, 1)[:, :LANES]
            hi = pltpu.roll(ys[1], (256 + 64 - nm * aa) % 256, 1)[:, :LANES]
            jsend[aa, u] = jnp.where(low64, lo, hi)
        return c

    row8 = lax.broadcasted_iota(jnp.int32, (8, LANES), 0)
    lane8 = lax.broadcasted_iota(jnp.int32, (8, LANES), 1)
    at0 = lane8 - PIECE * row8
    at1 = lane8 - PIECE * (row8 + 8)
    here0 = jnp.logical_and(at0 >= 0, at0 < PIECE)
    here1 = jnp.logical_and(jnp.logical_and(at1 >= 0, at1 < PIECE), lane8 < nq)
    zbuf[:, NT8] = jnp.zeros((4, 2, 8, 512), F32)

    def tails(x):
        f = [x[t].astype(F32) for t in range(4)]
        out = []
        for e in range(2):
            for u in range(2):
                v0 = pltpu.roll(f[2 * u][8 * e:8 * e + 8], LANES - nq, 1, stride=PIECE, stride_axis=0)
                f1 = f[2 * u + 1][8 * e:8 * e + 8]
                v1 = jnp.where(row8 == 0, pltpu.roll(f1, (8 * PIECE - nq) % LANES, 1), pltpu.roll(f1, (9 * PIECE - nq) % LANES, 1))
                v = jnp.where(here0, v0, jnp.where(here1, v1, 0.0))
                out.append(v.sum(0, keepdims=True))
        return out

    def fit(p):
        pltpu.make_async_copy(rbuf.at[:, p], rbuf.at[:, p], trecv.at[p]).wait()
        if p + 3 < npair:
            @pl.when(jnp.logical_not(outer))
            def _():
                send_half(p + 3, 0, NT8, True)
        xs = []
        for s in range(4):
            rest = [w for q in range(4) for w in tails(rbuf[s, p, q, pl.ds(0, 4)])]
            xs.append(jnp.concatenate([rbuf[s, p].reshape(4 * NT8 * 16, LANES), jnp.concatenate(rest, axis=0).astype(BF)], axis=0))
        x = jnp.concatenate(xs, axis=1)
        z = dot(jnp.concatenate([x, x, x], axis=1), msp[...].reshape(3 * 512, 512), NN)
        main = 4 * NT8 * 16
        zbuf[:, pl.ds(0, NT8)] = z[:main].reshape(4, NT8, 2, 8, 512)
        for q in range(4):
            for e in range(2):
                zbuf[q, NT8, e, pl.ds(0, 2)] = z[main + 4 * q + 2 * e:main + 4 * q + 2 * e + 2]
        ml = []
        for s in range(2):
            rest = tails(own[s, p, pl.ds(0, 4)]) + [jnp.zeros((12, LANES), F32)]
            ml.append(jnp.concatenate([own[s, p].reshape(NT8 * 16, LANES), jnp.concatenate(rest, axis=0).astype(BF)], axis=0))
        mid, low = ml
        rows = pl.ds(pl.multiple_of(a * LANES, LANES), LANES)
        mh, mm = msp[0, rows], msp[1, rows]
        z = dot(jnp.concatenate([mid, mid, low], axis=1), jnp.concatenate([mh, mm, mh], axis=0), NN)
        zbuf[o, pl.ds(0, NT8)] = zbuf[o, pl.ds(0, NT8)] + z[:NT8 * 16].reshape(NT8, 2, 8, 512)
        for e in range(2):
            zbuf[o, NT8, e, pl.ds(0, 2)] = zbuf[o, NT8, e, pl.ds(0, 2)] + z[NT8 * 16 + 2 * e:NT8 * 16 + 2 * e + 2]
        for e in range(2):
            s3 = split3(zbuf[:, :, e].reshape(4 * MROW, 512))
            k = dot(lhs6(s3, 1), rhs6(s3, 1), NT)
            if p == 0 and e == 0:
                kacc[0] = k[:, :LANES]
                kacc[1] = k[:, LANES:]
            else:
                kacc[0] = kacc[0] + k[:, :LANES]
                kacc[1] = kacc[1] + k[:, LANES:]

    lax.fori_loop(0, nm // 2, jpair, 0)
    near, far = a + 1 - 2 * (a % 2), lax.rem(a + 2, 4)
    hops = []
    for e, aa in enumerate((lax.rem(near + 2, 4), near)):
        hops.append(pltpu.make_async_remote_copy(src_ref=jsend.at[aa], dst_ref=jrecv.at[e], send_sem=jssem.at[e], recv_sem=jrsem.at[e],
                                                 device_id=dev(near, o), device_id_type=MESH))
        hops[-1].start()
    @pl.when(outer)
    def _():
        send_half(npair - 1, 0, NT8, True)

    @pl.when(jnp.logical_not(outer))
    def _():
        for p in range(3, npair):
            send_half(p, 0, NT8, False)
    for p in range(npair - 1):
        fit(p)
    hops[0].wait_recv()
    jfwd[...] = jsend[far] + jrecv[0]
    cross = pltpu.make_async_remote_copy(src_ref=jfwd, dst_ref=jrecv.at[2], send_sem=jssem.at[2], recv_sem=jrsem.at[2],
                                         device_id=dev(far, o), device_id_type=MESH)
    cross.start()
    fit(npair - 1)

    mate = o + 1 - 2 * half
    swap = pltpu.make_async_remote_copy(src_ref=kacc.at[1 - half], dst_ref=kin, send_sem=kxs, recv_sem=kxr,
                                        device_id=dev(a, mate), device_id_type=MESH)
    swap.start()
    swap.wait_recv()
    kful[...] = kacc[half] + kin[...]
    low32 = lax.broadcasted_iota(jnp.int32, (32, LANES), 1) < 64
    for oo in range(4):
        ev = kful[pl.ds(MROW * oo, 32, stride=2), :]
        od = kful[pl.ds(MROW * oo + 1, 32, stride=2), :]
        kmsg[0, oo] = jnp.where(low32, ev, pltpu.roll(od, 64, 1))
        kmsg[1, oo] = jnp.where(low32, pltpu.roll(ev, 64, 1), od)

    def ks(k, c):
        al, oo = k // 4, k % 4
        aa = 2 * half + al
        same = jnp.logical_and(aa == a, oo == o)

        @pl.when(jnp.logical_not(same))
        def _():
            pltpu.make_async_remote_copy(src_ref=kmsg.at[al, oo], dst_ref=krecv.at[pl.ds(dens * 32, 32)], send_sem=kss, recv_sem=krs,
                                         device_id=dev(aa, oo), device_id_type=MESH).start()

        @pl.when(same)
        def _():
            cp = pltpu.make_async_copy(kmsg.at[al, oo], krecv.at[pl.ds(dens * 32, 32)], krs)
            cp.start()
        return c
    lax.fori_loop(0, 8, ks, 0)

    hops[1].wait_recv()
    cross.wait_recv()
    pltpu.make_async_copy(krecv, krecv, krs).wait()
    for u in range(nm // 2):
        j = jsend[a, u] + jrecv[1, u] + jrecv[2, u]
        g = 2.0 * j - krecv[pl.ds(u, nd, stride=32), :]
        out[2 * u] = g[:, :nm]
        out[2 * u + 1] = pltpu.roll(g, 64, 1)[:, :nm]

    pltpu.make_async_copy(sbuf.at[pl.ds(0, 15)], sbuf.at[pl.ds(0, 15)], tsend).wait()
    metric_copies(lambda c: c.wait_send())
    pltpu.make_async_copy(mqr.at[:, pl.ds(0, 96)], mqr.at[:, pl.ds(0, 96)], mosend).wait()
    pltpu.make_async_copy(gbuf, gbuf, gssem).wait()
    for c in hops + [cross]:
        c.wait_send()
    swap.wait_send()
    inset = (a // 2) == half

    @pl.when(inset)
    def _():
        pltpu.make_async_copy(krecv.at[pl.ds(0, 224)], krecv.at[pl.ds(0, 224)], kss).wait()

    @pl.when(jnp.logical_not(inset))
    def _():
        pltpu.make_async_copy(krecv, krecv, kss).wait()


def solution(mesh):
    def local_fock(ints_blk, metric_blk, orbitals):
        nq, nm, nl = ints_blk.shape
        nd, _, ni = orbitals.shape
        bt = jnp.transpose(ints_blk, (1, 2, 0))
        mt = metric_blk.T
        ct = jnp.transpose(orbitals, (2, 0, 1)).reshape(ni * nd, nl)
        npair = ni // 4
        V = pltpu.VMEM
        dma = pltpu.SemaphoreType.DMA
        g = pl.pallas_call(
            lambda *refs: kernel(nm, nl, nq, nd, ni, *refs),
            out_shape=pltpu.VMEM((nm, nd, nm), F32),
            in_specs=[pl.BlockSpec(memory_space=pl.ANY)] * 3,
            out_specs=pl.BlockSpec(memory_space=pltpu.VMEM),
            scratch_shapes=[
                V((nm, nl, nq), F32), V((4 * nq, nq), F32), V((ni * nd, nl), F32), V((ni * nd, 256), F32),
                V((8 * SP, LANES), F32), V((16, npair, NT8, 16, LANES), BF), V((4, npair, 4, NT8, 16, LANES), BF),
                V((2, npair, NT8, 16, LANES), BF), V((4, LANES, LANES), F32), V((6, LANES, LANES), F32), V((4, 4, LANES, LANES), F32), V((3, 512, 512), BF),
                V((nd, LANES), F32), V((4, 4, nd, LANES), F32), V((4, nm // 2, nd, LANES), F32), V((3, nm // 2, nd, LANES), F32), V((nm // 2, nd, LANES), F32),
                V((4, 8, 2, 8, 512), F32), V((2, 256, LANES), F32), V((256, LANES), F32), V((256, LANES), F32), V((2, 4, 32, LANES), F32),
                V((8 * 32, LANES), F32), V((15, nd, LANES), F32),
                dma((NT8,)), dma((3,)), dma, dma((npair,)), dma, dma, dma, dma, dma, dma, dma((3,)), dma((3,)), dma, dma, dma, dma],
            compiler_params=pltpu.CompilerParams(collective_id=0, has_side_effects=True, vmem_limit_bytes=60 * 2**20),
        )(bt, mt, ct)
        return jnp.transpose(g, (1, 0, 2))

    return jax.shard_map(local_fock, mesh=mesh, in_specs=(P(('sys', 'aux'), 'orb', None), P(('sys', 'aux'), None), P('sys', None, None)), out_specs=P('sys', 'orb', 'aux'), check_vma=False)
```

```python
import jax
import jax.numpy as jnp
from jax import lax
from jax.experimental import pallas as pl
from jax.experimental.pallas import tpu as pltpu
from jax.sharding import PartitionSpec as P

F32 = jnp.float32
BF = jnp.bfloat16
MESH = pl.DeviceIdType.MESH
NN = (((1,), (0,)), ((), ()))
NT = (((1,), (1,)), ((), ()))
LANES = 128
MROW = 64
NT8 = 7
PIECE = 12
SP = 168


def split3(x):
    hi = x.astype(BF)
    rest = x - hi.astype(F32)
    mid = rest.astype(BF)
    return hi, mid, (rest - mid.astype(F32)).astype(BF)


def dot(x, y, dims):
    return lax.dot_general(x, y, dims, preferred_element_type=F32)


def lhs6(x, axis):
    h, m, l = x
    return jnp.concatenate([h, h, m, m, h, l], axis=axis)


def rhs6(x, axis):
    h, m, l = x
    return jnp.concatenate([h, m, h, m, l, h], axis=axis)


def kernel(nm, nl, nq, nd, ni, bt, mt, ct, out, bv, mv, cv, ctp, tr, sbuf, rbuf, own, mloc, mqr, mq, msp, gsend, grecv, jsend, jrecv, jfwd, zbuf, kacc, kin, kful, kmsg, krecv, gbuf,
           bsem, lsem, tsend, trecv, mzsend, mzrecv, mosend, morecv, gssem, grsem, jssem, jrsem, kxs, kxr, kss, krs):
    sy, a, o = lax.axis_index('sys'), lax.axis_index('aux'), lax.axis_index('orb')
    me = a * 4 + o
    dens, half = me // 2, me % 2
    nh = ni // 2
    npair = nh // 2

    def dev(aa, oo):
        return (sy, aa, oo)

    pltpu.make_async_copy(ct, cv, lsem.at[0]).start()
    pltpu.make_async_copy(bt.at[pl.ds(8 * NT8, 2)], bv.at[pl.ds(8 * NT8, 2)], lsem.at[2]).start()
    for t in range(NT8):
        pltpu.make_async_copy(bt.at[pl.ds(8 * t, 8)], bv.at[pl.ds(8 * t, 8)], bsem.at[t]).start()
        if t == 0:
            pltpu.make_async_copy(mt, mv, lsem.at[1]).start()
    barrier = pltpu.get_barrier_semaphore()

    def tell(k, c):
        g = lax.rem(me + k, 16)
        pl.semaphore_signal(barrier, inc=1, device_id=dev(g // 4, g % 4), device_id_type=MESH)
        return c
    lax.fori_loop(1, 16, tell, 0)

    pltpu.make_async_copy(ct, cv, lsem.at[0]).wait()
    ctp[...] = jnp.concatenate([cv[...], jnp.zeros((nd * ni, 256 - nl), F32)], axis=1)
    lhs = lhs6(split3(ctp[...]), 1)
    pltpu.make_async_copy(mt, mv, lsem.at[1]).wait()
    for b in range(4):
        blk = jnp.concatenate([mv[nq * b:nq * (b + 1), :], jnp.zeros((nq, LANES - nq), F32)], axis=1)
        mloc[b] = jnp.concatenate([blk, jnp.zeros((LANES - nq, LANES), F32)], axis=0)
    pl.semaphore_wait(barrier, 15)

    quarter = pl.ds(pl.multiple_of(o * 32, 32), 32)

    def nearer(x, y, z):
        dx, dy = jnp.abs(x - z), jnp.abs(y - z)
        return jnp.logical_or(dx < dy, jnp.logical_and(dx == dy, x < y))

    def metric_copies(act):
        for k in (2, 1, 3):
            to = lax.rem(a + 4 - k, 4)

            def block(row, slot):
                return pltpu.make_async_remote_copy(src_ref=mloc.at[row, quarter], dst_ref=mqr.at[slot, quarter], send_sem=mzsend,
                                                    recv_sem=mzrecv, device_id=dev(to, o), device_id_type=MESH)
            act(block(a, k - 1))
            for k2 in (1, 2, 3):
                if k2 == k:
                    continue
                b = lax.rem(to + k2, 4)

                @pl.when(nearer(a, b, to))
                def _():
                    act(block(b, k + k2))
    metric_copies(lambda c: c.start())

    gam = jnp.zeros((nd, LANES), F32)
    tr2 = tr

    lane = lax.broadcasted_iota(jnp.int32, (1, LANES), 1)
    data = lane < nq

    def tile(t, gam, tail, first):
        pltpu.make_async_copy(bt.at[pl.ds(0, 8)], bv.at[pl.ds(0, 8)], bsem.at[t]).wait()
        cols = pltpu.roll(ctp[...], lax.rem(512 - (nm * o + 8 * t), 256), 1)
        count = 0
        if tail is not None:
            count = min(8, 10 - first)
            spare = jnp.concatenate([bv[8 * NT8 + tail], jnp.zeros((nl, LANES - nq), F32)], axis=1)
            tcol = pltpu.roll(ctp[...], lax.rem(512 - (nm * o + 8 * NT8 + tail), 256), 1)[:, 0:1]
        for r in range(0, 8, 2):
            xs = []
            for e in range(2):
                x = jnp.concatenate([bv[8 * t + r + e], jnp.zeros((nl, LANES - nq), F32)], axis=1)
                if r + e < count:
                    x = jnp.where(data, x, pltpu.roll(spare, (nq - PIECE * (first + r + e)) % LANES, 1))
                xs.append(x)
            x = jnp.concatenate(xs, axis=1)
            x = jnp.concatenate([x, jnp.zeros((256 - nl, 2 * LANES), F32)], axis=0)
            y = dot(lhs, rhs6(split3(x), 0), NN)
            for e in range(2):
                ye = y[:, e * LANES:(e + 1) * LANES]
                tr2[pl.ds((r + e) * SP, nd * ni), :] = ye
                col = cols[:, r + e:r + e + 1]
                if r + e < count:
                    w = (ye * jnp.where(data, col, tcol)).reshape(ni, nd, LANES).sum(0)
                    moved = pltpu.roll(jnp.where(data, 0.0, w), (PIECE * (first + r + e) - nq) % LANES, 1)
                    gam = gam + jnp.where(data, w, 0.0) + moved
                else:
                    gam = gam + (ye * col).reshape(ni, nd, LANES).sum(0)
        for g in range(16):
            d, h = g // 2, g % 2
            for p in range(npair):
                two = [tr2[pl.ds((h * nh + 2 * p + e) * nd + d, 8, stride=SP), :] for e in range(2)]
                sbuf[g, p, t] = jnp.concatenate(two, axis=0).astype(BF)
        for p in range(npair):
            two = [tr2[pl.ds((half * nh + 2 * p + e) * nd + dens, 8, stride=SP), :] for e in range(2)]
            _, mid, low = split3(jnp.concatenate(two, axis=0))
            own[0, p, t] = mid
            own[1, p, t] = low
        return gam

    def send_t1(p, t0, nt):
        def one(k, c):
            j, u = k % 4, k // 4
            aa = lax.rem(a + 2 + j, 4)
            oo = lax.rem(o + 1 + u, 4)
            g = aa * 4 + oo
            src = sbuf.at[g, p, pl.ds(t0, nt)]
            dst = rbuf.at[a, p, o, pl.ds(t0, nt)]

            @pl.when(k != 14)
            def _():
                pltpu.make_async_remote_copy(src_ref=src, dst_ref=dst, send_sem=tsend, recv_sem=trecv.at[p],
                                             device_id=dev(aa, oo), device_id_type=MESH).start()

            @pl.when(k == 14)
            def _():
                pltpu.make_async_copy(src, dst, trecv.at[p]).start()
            return c
        lax.fori_loop(0, 16, one, 0)

    outer = jnp.logical_or(a == 0, a == 3)
    pair = a + 1 - 2 * (a % 2)

    def send_half(p, t0, nt, cross):
        def one(k, c):
            if cross:
                aa = jnp.where(k % 2 == 0, 3 - a, 3 - pair)
                oo = lax.rem(o + 1 + k // 2, 4)
            else:
                aa = jnp.where(k % 2 == 0, pair, a)
                oo = lax.rem(o + 1 + k // 2, 4)
            g = aa * 4 + oo
            src = sbuf.at[g, p, pl.ds(t0, nt)]
            dst = rbuf.at[a, p, o, pl.ds(t0, nt)]

            def far():
                pltpu.make_async_remote_copy(src_ref=src, dst_ref=dst, send_sem=tsend, recv_sem=trecv.at[p],
                                             device_id=dev(aa, oo), device_id_type=MESH).start()
            if cross:
                far()
            else:
                pl.when(k != 7)(far)

                @pl.when(k == 7)
                def _():
                    pltpu.make_async_copy(src, dst, trecv.at[p]).start()
            return c
        lax.fori_loop(0, 8, one, 0)

    pltpu.make_async_copy(bt.at[pl.ds(0, 2)], bv.at[pl.ds(0, 2)], lsem.at[2]).wait()

    def two_tiles(u, gam):
        gam = tile(2 * u, gam, u, 0)
        send_t1(0, 2 * u, 1)
        gam = tile(2 * u + 1, gam, u, 8)
        send_t1(0, 2 * u + 1, 1)
        return gam
    gam = lax.fori_loop(0, 2, two_tiles, gam)

    def one_tile(t, gam):
        gam = tile(t, gam, None, 0)
        send_t1(0, t, 1)
        return gam
    gam = lax.fori_loop(4, NT8, one_tile, gam)

    gsend[...] = gam

    def gs(k, c):
        g = lax.rem(me + k, 16)
        pltpu.make_async_remote_copy(src_ref=gsend, dst_ref=grecv.at[a, o], send_sem=gssem, recv_sem=grsem,
                                     device_id=dev(g // 4, g % 4), device_id_type=MESH).start()
        return c
    lax.fori_loop(1, 16, gs, 0)
    pltpu.make_async_copy(gsend, grecv.at[a, o], grsem).start()

    pltpu.make_async_copy(mqr.at[:, pl.ds(0, 32)], mqr.at[:, pl.ds(0, 32)], mzrecv).wait()

    def mo(k, c):
        oo = lax.rem(o + k, 4)
        pltpu.make_async_remote_copy(src_ref=mqr.at[:, quarter], dst_ref=mqr.at[:, quarter], send_sem=mosend, recv_sem=morecv,
                                     device_id=dev(a, oo), device_id_type=MESH).start()
        return c
    lax.fori_loop(1, 4, mo, 0)
    @pl.when(outer)
    def _():
        send_half(1, 0, NT8, False)
        send_half(2, 0, NT8, False)
        send_half(1, 0, NT8, True)
        send_half(3, 0, NT8, False)
        send_half(4, 0, NT8, False)
        send_half(2, 0, NT8, True)
        send_half(3, 0, NT8, True)

    @pl.when(jnp.logical_not(outer))
    def _():
        for p in range(1, 3):
            send_t1(p, 0, NT8)
    mq[a] = mloc[...]
    for k in range(1, 4):
        c1 = lax.rem(a + k, 4)
        mq[c1, a] = mloc[c1].T
    pltpu.make_async_copy(mqr.at[:, pl.ds(0, 96)], mqr.at[:, pl.ds(0, 96)], morecv).wait()
    for k in range(1, 4):
        c1 = lax.rem(a + k, 4)
        mq[c1, c1] = mqr[k - 1]
        for k2 in range(k + 1, 4):
            c2 = lax.rem(a + k2, 4)
            first = jnp.where(nearer(c1, c2, a), c1, c2)
            second = c1 + c2 - first
            blk = mqr[k + k2]
            mq[first, second] = blk
            mq[second, first] = blk.T
    for b in range(4):
        parts = split3(jnp.concatenate([mq[aa, b] for aa in range(4)], axis=1))
        for s in range(3):
            msp[s, pl.ds(b * LANES, LANES)] = parts[s]

    pltpu.make_async_copy(grecv, grecv, grsem).wait()
    graw = jnp.concatenate([grecv[aa, 0] + grecv[aa, 1] + grecv[aa, 2] + grecv[aa, 3] for aa in range(4)], axis=1)
    m3 = [msp[s] for s in range(3)]
    gfit = dot(lhs6(split3(graw), 1), rhs6(m3, 0), NN)
    mown = split3(jnp.concatenate([mloc[b] for b in range(4)], axis=0))
    wts = dot(lhs6(split3(gfit), 1), rhs6(mown, 0), NN)
    wl = lhs6(split3(wts), 1)
    low64 = lax.broadcasted_iota(jnp.int32, (nd, LANES), 1) < 64

    def jpair(u, c):
        ys = []
        for e in range(2):
            x = jnp.concatenate([bv[2 * u + e], jnp.zeros((nl, LANES - nq), F32)], axis=1)
            x = jnp.concatenate([x, jnp.zeros((256 - nl, LANES), F32)], axis=0)
            ys.append(dot(wl, rhs6(split3(x), 1), NT))
        for aa in range(4):
            lo = pltpu.roll(ys[0], (256 - nm * aa) % 256, 1)[:, :LANES]
            hi = pltpu.roll(ys[1], (256 + 64 - nm * aa) % 256, 1)[:, :LANES]
            jsend[aa, u] = jnp.where(low64, lo, hi)
        return c

    row8 = lax.broadcasted_iota(jnp.int32, (8, LANES), 0)
    lane8 = lax.broadcasted_iota(jnp.int32, (8, LANES), 1)
    at0 = lane8 - PIECE * row8
    at1 = lane8 - PIECE * (row8 + 8)
    here0 = jnp.logical_and(at0 >= 0, at0 < PIECE)
    here1 = jnp.logical_and(jnp.logical_and(at1 >= 0, at1 < PIECE), lane8 < nq)
    zbuf[:, NT8] = jnp.zeros((4, 2, 8, 512), F32)

    def tails(x):
        f = [x[t].astype(F32) for t in range(4)]
        out = []
        for e in range(2):
            for u in range(2):
                v0 = pltpu.roll(f[2 * u][8 * e:8 * e + 8], LANES - nq, 1, stride=PIECE, stride_axis=0)
                f1 = f[2 * u + 1][8 * e:8 * e + 8]
                v1 = jnp.where(row8 == 0, pltpu.roll(f1, (8 * PIECE - nq) % LANES, 1), pltpu.roll(f1, (9 * PIECE - nq) % LANES, 1))
                v = jnp.where(here0, v0, jnp.where(here1, v1, 0.0))
                out.append(v.sum(0, keepdims=True))
        return out

    def fit(p):
        pltpu.make_async_copy(rbuf.at[:, p], rbuf.at[:, p], trecv.at[p]).wait()
        if p + 3 < npair:
            @pl.when(jnp.logical_not(outer))
            def _():
                send_half(p + 3, 0, NT8, True)
        xs = []
        for s in range(4):
            rest = [w for q in range(4) for w in tails(rbuf[s, p, q, pl.ds(0, 4)])]
            xs.append(jnp.concatenate([rbuf[s, p].reshape(4 * NT8 * 16, LANES), jnp.concatenate(rest, axis=0).astype(BF)], axis=0))
        x = jnp.concatenate(xs, axis=1)
        z = dot(jnp.concatenate([x, x, x], axis=1), msp[...].reshape(3 * 512, 512), NN)
        main = 4 * NT8 * 16
        zbuf[:, pl.ds(0, NT8)] = z[:main].reshape(4, NT8, 2, 8, 512)
        for q in range(4):
            for e in range(2):
                zbuf[q, NT8, e, pl.ds(0, 2)] = z[main + 4 * q + 2 * e:main + 4 * q + 2 * e + 2]
        ml = []
        for s in range(2):
            rest = tails(own[s, p, pl.ds(0, 4)]) + [jnp.zeros((12, LANES), F32)]
            ml.append(jnp.concatenate([own[s, p].reshape(NT8 * 16, LANES), jnp.concatenate(rest, axis=0).astype(BF)], axis=0))
        mid, low = ml
        rows = pl.ds(pl.multiple_of(a * LANES, LANES), LANES)
        mh, mm = msp[0, rows], msp[1, rows]
        z = dot(jnp.concatenate([mid, mid, low], axis=1), jnp.concatenate([mh, mm, mh], axis=0), NN)
        zbuf[o, pl.ds(0, NT8)] = zbuf[o, pl.ds(0, NT8)] + z[:NT8 * 16].reshape(NT8, 2, 8, 512)
        for e in range(2):
            zbuf[o, NT8, e, pl.ds(0, 2)] = zbuf[o, NT8, e, pl.ds(0, 2)] + z[NT8 * 16 + 2 * e:NT8 * 16 + 2 * e + 2]
        for e in range(2):
            s3 = split3(zbuf[:, :, e].reshape(4 * MROW, 512))
            k = dot(lhs6(s3, 1), rhs6(s3, 1), NT)
            if p == 0 and e == 0:
                kacc[0] = k[:, :LANES]
                kacc[1] = k[:, LANES:]
            else:
                kacc[0] = kacc[0] + k[:, :LANES]
                kacc[1] = kacc[1] + k[:, LANES:]

    lax.fori_loop(0, nm // 2, jpair, 0)
    near, far = a + 1 - 2 * (a % 2), lax.rem(a + 2, 4)
    hops = []
    for e, aa in enumerate((lax.rem(near + 2, 4), near)):
        hops.append(pltpu.make_async_remote_copy(src_ref=jsend.at[aa], dst_ref=jrecv.at[e], send_sem=jssem.at[e], recv_sem=jrsem.at[e],
                                                 device_id=dev(near, o), device_id_type=MESH))
        hops[-1].start()
    @pl.when(outer)
    def _():
        send_half(npair - 1, 0, NT8, True)

    @pl.when(jnp.logical_not(outer))
    def _():
        for p in range(3, npair):
            send_half(p, 0, NT8, False)
    cross = pltpu.make_async_remote_copy(src_ref=jfwd, dst_ref=jrecv.at[2], send_sem=jssem.at[2], recv_sem=jrsem.at[2],
                                         device_id=dev(far, o), device_id_type=MESH)
    for p in range(3):
        fit(p)
    hops[0].wait_recv()
    jfwd[...] = jsend[far] + jrecv[0]

    @pl.when(jnp.logical_not(outer))
    def _():
        cross.start()
    fit(3)

    @pl.when(outer)
    def _():
        cross.start()
    fit(npair - 1)

    mate = o + 1 - 2 * half
    swap = pltpu.make_async_remote_copy(src_ref=kacc.at[1 - half], dst_ref=kin, send_sem=kxs, recv_sem=kxr,
                                        device_id=dev(a, mate), device_id_type=MESH)
    swap.start()
    swap.wait_recv()
    kful[...] = kacc[half] + kin[...]
    low32 = lax.broadcasted_iota(jnp.int32, (32, LANES), 1) < 64
    for oo in range(4):
        ev = kful[pl.ds(MROW * oo, 32, stride=2), :]
        od = kful[pl.ds(MROW * oo + 1, 32, stride=2), :]
        kmsg[0, oo] = jnp.where(low32, ev, pltpu.roll(od, 64, 1))
        kmsg[1, oo] = jnp.where(low32, pltpu.roll(ev, 64, 1), od)

    def ks(k, c):
        al, oo = k // 4, k % 4
        aa = 2 * half + al
        same = jnp.logical_and(aa == a, oo == o)

        @pl.when(jnp.logical_not(same))
        def _():
            pltpu.make_async_remote_copy(src_ref=kmsg.at[al, oo], dst_ref=krecv.at[pl.ds(dens * 32, 32)], send_sem=kss, recv_sem=krs,
                                         device_id=dev(aa, oo), device_id_type=MESH).start()

        @pl.when(same)
        def _():
            cp = pltpu.make_async_copy(kmsg.at[al, oo], krecv.at[pl.ds(dens * 32, 32)], krs)
            cp.start()
        return c
    lax.fori_loop(0, 8, ks, 0)

    hops[1].wait_recv()
    cross.wait_recv()
    pltpu.make_async_copy(krecv, krecv, krs).wait()
    for u in range(nm // 2):
        j = jsend[a, u] + jrecv[1, u] + jrecv[2, u]
        g = 2.0 * j - krecv[pl.ds(u, nd, stride=32), :]
        out[2 * u] = g[:, :nm]
        out[2 * u + 1] = pltpu.roll(g, 64, 1)[:, :nm]

    pltpu.make_async_copy(sbuf.at[pl.ds(0, 15)], sbuf.at[pl.ds(0, 15)], tsend).wait()
    metric_copies(lambda c: c.wait_send())
    pltpu.make_async_copy(mqr.at[:, pl.ds(0, 96)], mqr.at[:, pl.ds(0, 96)], mosend).wait()
    pltpu.make_async_copy(gbuf, gbuf, gssem).wait()
    for c in hops + [cross]:
        c.wait_send()
    swap.wait_send()
    inset = (a // 2) == half

    @pl.when(inset)
    def _():
        pltpu.make_async_copy(krecv.at[pl.ds(0, 224)], krecv.at[pl.ds(0, 224)], kss).wait()

    @pl.when(jnp.logical_not(inset))
    def _():
        pltpu.make_async_copy(krecv, krecv, kss).wait()


def solution(mesh):
    def local_fock(ints_blk, metric_blk, orbitals):
        nq, nm, nl = ints_blk.shape
        nd, _, ni = orbitals.shape
        bt = jnp.transpose(ints_blk, (1, 2, 0))
        mt = metric_blk.T
        ct = jnp.transpose(orbitals, (2, 0, 1)).reshape(ni * nd, nl)
        npair = ni // 4
        V = pltpu.VMEM
        dma = pltpu.SemaphoreType.DMA
        g = pl.pallas_call(
            lambda *refs: kernel(nm, nl, nq, nd, ni, *refs),
            out_shape=pltpu.VMEM((nm, nd, nm), F32),
            in_specs=[pl.BlockSpec(memory_space=pl.ANY)] * 3,
            out_specs=pl.BlockSpec(memory_space=pltpu.VMEM),
            scratch_shapes=[
                V((nm, nl, nq), F32), V((4 * nq, nq), F32), V((ni * nd, nl), F32), V((ni * nd, 256), F32),
                V((8 * SP, LANES), F32), V((16, npair, NT8, 16, LANES), BF), V((4, npair, 4, NT8, 16, LANES), BF),
                V((2, npair, NT8, 16, LANES), BF), V((4, LANES, LANES), F32), V((6, LANES, LANES), F32), V((4, 4, LANES, LANES), F32), V((3, 512, 512), BF),
                V((nd, LANES), F32), V((4, 4, nd, LANES), F32), V((4, nm // 2, nd, LANES), F32), V((3, nm // 2, nd, LANES), F32), V((nm // 2, nd, LANES), F32),
                V((4, 8, 2, 8, 512), F32), V((2, 256, LANES), F32), V((256, LANES), F32), V((256, LANES), F32), V((2, 4, 32, LANES), F32),
                V((8 * 32, LANES), F32), V((15, nd, LANES), F32),
                dma((NT8,)), dma((3,)), dma, dma((npair,)), dma, dma, dma, dma, dma, dma, dma((3,)), dma((3,)), dma, dma, dma, dma],
            compiler_params=pltpu.CompilerParams(collective_id=0, has_side_effects=True, vmem_limit_bytes=60 * 2**20),
        )(bt, mt, ct)
        return jnp.transpose(g, (1, 0, 2))

    return jax.shard_map(local_fock, mesh=mesh, in_specs=(P(('sys', 'aux'), 'orb', None), P(('sys', 'aux'), None), P('sys', None, None)), out_specs=P('sys', 'orb', 'aux'), check_vma=False)
```

```python
import jax
import jax.numpy as jnp
from jax import lax
from jax.experimental import pallas as pl
from jax.experimental.pallas import tpu as pltpu
from jax.sharding import PartitionSpec as P

F32 = jnp.float32
BF = jnp.bfloat16
MESH = pl.DeviceIdType.MESH
NN = (((1,), (0,)), ((), ()))
NT = (((1,), (1,)), ((), ()))
LANES = 128
MROW = 64
NT8 = 7
PIECE = 12
SP = 168


def split3(x):
    hi = x.astype(BF)
    rest = x - hi.astype(F32)
    mid = rest.astype(BF)
    return hi, mid, (rest - mid.astype(F32)).astype(BF)


def dot(x, y, dims):
    return lax.dot_general(x, y, dims, preferred_element_type=F32)


def lhs6(x, axis):
    h, m, l = x
    return jnp.concatenate([h, h, m, m, h, l], axis=axis)


def rhs6(x, axis):
    h, m, l = x
    return jnp.concatenate([h, m, h, m, l, h], axis=axis)


def kernel(nm, nl, nq, nd, ni, bt, mt, ct, out, bv, mv, cv, ctp, tr, sbuf, rbuf, own, mloc, mqr, mq, msp, gsend, grecv, jsend, jrecv, jfwd, zbuf, kacc, kin, kful, kmsg, krecv, gbuf, zown, sacc,
           bsem, lsem, tsend, trecv, mzsend, mzrecv, mosend, morecv, gssem, grsem, jssem, jrsem, kxs, kxr, kss, krs):
    sy, a, o = lax.axis_index('sys'), lax.axis_index('aux'), lax.axis_index('orb')
    me = a * 4 + o
    dens, half = me // 2, me % 2
    nh = ni // 2
    npair = nh // 2

    def dev(aa, oo):
        return (sy, aa, oo)

    pltpu.make_async_copy(ct, cv, lsem.at[0]).start()
    pltpu.make_async_copy(bt.at[pl.ds(8 * NT8, 2)], bv.at[pl.ds(8 * NT8, 2)], lsem.at[2]).start()
    for t in range(NT8):
        pltpu.make_async_copy(bt.at[pl.ds(8 * t, 8)], bv.at[pl.ds(8 * t, 8)], bsem.at[t]).start()
        if t == 0:
            pltpu.make_async_copy(mt, mv, lsem.at[1]).start()
    barrier = pltpu.get_barrier_semaphore()

    def tell(k, c):
        g = lax.rem(me + k, 16)
        pl.semaphore_signal(barrier, inc=1, device_id=dev(g // 4, g % 4), device_id_type=MESH)
        return c
    lax.fori_loop(1, 16, tell, 0)

    pltpu.make_async_copy(ct, cv, lsem.at[0]).wait()
    ctp[...] = jnp.concatenate([cv[...], jnp.zeros((nd * ni, 256 - nl), F32)], axis=1)
    lhs = lhs6(split3(ctp[...]), 1)
    pltpu.make_async_copy(mt, mv, lsem.at[1]).wait()
    for b in range(4):
        blk = jnp.concatenate([mv[nq * b:nq * (b + 1), :], jnp.zeros((nq, LANES - nq), F32)], axis=1)
        mloc[b] = jnp.concatenate([blk, jnp.zeros((LANES - nq, LANES), F32)], axis=0)
    pl.semaphore_wait(barrier, 15)

    quarter = pl.ds(pl.multiple_of(o * 32, 32), 32)

    def nearer(x, y, z):
        dx, dy = jnp.abs(x - z), jnp.abs(y - z)
        return jnp.logical_or(dx < dy, jnp.logical_and(dx == dy, x < y))

    def metric_copies(act):
        for k in (2, 1, 3):
            to = lax.rem(a + 4 - k, 4)

            def block(row, slot):
                return pltpu.make_async_remote_copy(src_ref=mloc.at[row, quarter], dst_ref=mqr.at[slot, quarter], send_sem=mzsend,
                                                    recv_sem=mzrecv, device_id=dev(to, o), device_id_type=MESH)
            act(block(a, k - 1))
            for k2 in (1, 2, 3):
                if k2 == k:
                    continue
                b = lax.rem(to + k2, 4)

                @pl.when(nearer(a, b, to))
                def _():
                    act(block(b, k + k2))
    metric_copies(lambda c: c.start())

    gam = jnp.zeros((nd, LANES), F32)
    tr2 = tr

    lane = lax.broadcasted_iota(jnp.int32, (1, LANES), 1)
    data = lane < nq

    def tile(t, gam, tail, first):
        pltpu.make_async_copy(bt.at[pl.ds(0, 8)], bv.at[pl.ds(0, 8)], bsem.at[t]).wait()
        cols = pltpu.roll(ctp[...], lax.rem(512 - (nm * o + 8 * t), 256), 1)
        count = 0
        if tail is not None:
            count = min(8, 10 - first)
            spare = jnp.concatenate([bv[8 * NT8 + tail], jnp.zeros((nl, LANES - nq), F32)], axis=1)
            tcol = pltpu.roll(ctp[...], lax.rem(512 - (nm * o + 8 * NT8 + tail), 256), 1)[:, 0:1]
        for r in range(0, 8, 2):
            xs = []
            for e in range(2):
                x = jnp.concatenate([bv[8 * t + r + e], jnp.zeros((nl, LANES - nq), F32)], axis=1)
                if r + e < count:
                    x = jnp.where(data, x, pltpu.roll(spare, (nq - PIECE * (first + r + e)) % LANES, 1))
                xs.append(x)
            x = jnp.concatenate(xs, axis=1)
            x = jnp.concatenate([x, jnp.zeros((256 - nl, 2 * LANES), F32)], axis=0)
            y = dot(lhs, rhs6(split3(x), 0), NN)
            for e in range(2):
                ye = y[:, e * LANES:(e + 1) * LANES]
                tr2[pl.ds((r + e) * SP, nd * ni), :] = ye
                col = cols[:, r + e:r + e + 1]
                if r + e < count:
                    w = (ye * jnp.where(data, col, tcol)).reshape(ni, nd, LANES).sum(0)
                    moved = pltpu.roll(jnp.where(data, 0.0, w), (PIECE * (first + r + e) - nq) % LANES, 1)
                    gam = gam + jnp.where(data, w, 0.0) + moved
                else:
                    gam = gam + (ye * col).reshape(ni, nd, LANES).sum(0)
        for g in range(16):
            d, h = g // 2, g % 2
            for p in range(npair):
                two = [tr2[pl.ds((h * nh + 2 * p + e) * nd + d, 8, stride=SP), :] for e in range(2)]
                sbuf[g, p, t] = jnp.concatenate(two, axis=0).astype(BF)
        for p in range(npair):
            two = [tr2[pl.ds((half * nh + 2 * p + e) * nd + dens, 8, stride=SP), :] for e in range(2)]
            _, mid, low = split3(jnp.concatenate(two, axis=0))
            own[0, p, t] = mid
            own[1, p, t] = low
        return gam

    def send_t1(p, t0, nt):
        def one(k, c):
            j, u = k % 4, k // 4
            aa = lax.rem(a + 2 + j, 4)
            oo = lax.rem(o + 1 + u, 4)
            g = aa * 4 + oo
            src = sbuf.at[g, p, pl.ds(t0, nt)]
            dst = rbuf.at[a, p, o, pl.ds(t0, nt)]

            @pl.when(k != 14)
            def _():
                pltpu.make_async_remote_copy(src_ref=src, dst_ref=dst, send_sem=tsend, recv_sem=trecv.at[p],
                                             device_id=dev(aa, oo), device_id_type=MESH).start()

            @pl.when(k == 14)
            def _():
                pltpu.make_async_copy(src, dst, trecv.at[p]).start()
            return c
        lax.fori_loop(0, 16, one, 0)

    outer = jnp.logical_or(a == 0, a == 3)
    pair = a + 1 - 2 * (a % 2)

    def send_half(p, t0, nt, cross):
        def one(k, c):
            if cross:
                aa = jnp.where(k % 2 == 0, 3 - a, 3 - pair)
                oo = lax.rem(o + 1 + k // 2, 4)
            else:
                aa = jnp.where(k % 2 == 0, pair, a)
                oo = lax.rem(o + 1 + k // 2, 4)
            g = aa * 4 + oo
            src = sbuf.at[g, p, pl.ds(t0, nt)]
            dst = rbuf.at[a, p, o, pl.ds(t0, nt)]

            def far():
                pltpu.make_async_remote_copy(src_ref=src, dst_ref=dst, send_sem=tsend, recv_sem=trecv.at[p],
                                             device_id=dev(aa, oo), device_id_type=MESH).start()
            if cross:
                far()
            else:
                pl.when(k != 7)(far)

                @pl.when(k == 7)
                def _():
                    pltpu.make_async_copy(src, dst, trecv.at[p]).start()
            return c
        lax.fori_loop(0, 8, one, 0)

    pltpu.make_async_copy(bt.at[pl.ds(0, 2)], bv.at[pl.ds(0, 2)], lsem.at[2]).wait()

    def two_tiles(u, gam):
        gam = tile(2 * u, gam, u, 0)
        send_t1(0, 2 * u, 1)
        gam = tile(2 * u + 1, gam, u, 8)
        send_t1(0, 2 * u + 1, 1)
        return gam
    gam = lax.fori_loop(0, 2, two_tiles, gam)

    def one_tile(t, gam):
        gam = tile(t, gam, None, 0)
        send_t1(0, t, 1)
        return gam
    gam = lax.fori_loop(4, NT8, one_tile, gam)

    gsend[...] = gam

    def gs(k, c):
        g = lax.rem(me + k, 16)
        pltpu.make_async_remote_copy(src_ref=gsend, dst_ref=grecv.at[a, o], send_sem=gssem, recv_sem=grsem,
                                     device_id=dev(g // 4, g % 4), device_id_type=MESH).start()
        return c
    lax.fori_loop(1, 16, gs, 0)
    pltpu.make_async_copy(gsend, grecv.at[a, o], grsem).start()

    pltpu.make_async_copy(mqr.at[:, pl.ds(0, 32)], mqr.at[:, pl.ds(0, 32)], mzrecv).wait()

    def mo(k, c):
        oo = lax.rem(o + k, 4)
        pltpu.make_async_remote_copy(src_ref=mqr.at[:, quarter], dst_ref=mqr.at[:, quarter], send_sem=mosend, recv_sem=morecv,
                                     device_id=dev(a, oo), device_id_type=MESH).start()
        return c
    lax.fori_loop(1, 4, mo, 0)
    @pl.when(outer)
    def _():
        send_half(1, 0, NT8, False)
        send_half(2, 0, NT8, False)
        send_half(1, 0, NT8, True)
        send_half(3, 0, NT8, False)
        send_half(4, 0, NT8, False)
        send_half(2, 0, NT8, True)
        send_half(3, 0, NT8, True)

    @pl.when(jnp.logical_not(outer))
    def _():
        for p in range(1, 3):
            send_t1(p, 0, NT8)
    mq[a] = mloc[...]
    for k in range(1, 4):
        c1 = lax.rem(a + k, 4)
        mq[c1, a] = mloc[c1].T
    pltpu.make_async_copy(mqr.at[:, pl.ds(0, 96)], mqr.at[:, pl.ds(0, 96)], morecv).wait()
    for k in range(1, 4):
        c1 = lax.rem(a + k, 4)
        mq[c1, c1] = mqr[k - 1]
        for k2 in range(k + 1, 4):
            c2 = lax.rem(a + k2, 4)
            first = jnp.where(nearer(c1, c2, a), c1, c2)
            second = c1 + c2 - first
            blk = mqr[k + k2]
            mq[first, second] = blk
            mq[second, first] = blk.T
    for b in range(4):
        parts = split3(jnp.concatenate([mq[aa, b] for aa in range(4)], axis=1))
        for s in range(3):
            msp[s, pl.ds(b * LANES, LANES)] = parts[s]

    pltpu.make_async_copy(grecv, grecv, grsem).wait()
    graw = jnp.concatenate([grecv[aa, 0] + grecv[aa, 1] + grecv[aa, 2] + grecv[aa, 3] for aa in range(4)], axis=1)
    m3 = [msp[s] for s in range(3)]
    gfit = dot(lhs6(split3(graw), 1), rhs6(m3, 0), NN)
    mown = split3(jnp.concatenate([mloc[b] for b in range(4)], axis=0))
    wts = dot(lhs6(split3(gfit), 1), rhs6(mown, 0), NN)
    wl = lhs6(split3(wts), 1)
    low64 = lax.broadcasted_iota(jnp.int32, (nd, LANES), 1) < 64

    def jpair(u, c):
        ys = []
        for e in range(2):
            x = jnp.concatenate([bv[2 * u + e], jnp.zeros((nl, LANES - nq), F32)], axis=1)
            x = jnp.concatenate([x, jnp.zeros((256 - nl, LANES), F32)], axis=0)
            ys.append(dot(wl, rhs6(split3(x), 1), NT))
        for aa in range(4):
            lo = pltpu.roll(ys[0], (256 - nm * aa) % 256, 1)[:, :LANES]
            hi = pltpu.roll(ys[1], (256 + 64 - nm * aa) % 256, 1)[:, :LANES]
            jsend[aa, u] = jnp.where(low64, lo, hi)
        return c

    row8 = lax.broadcasted_iota(jnp.int32, (8, LANES), 0)
    lane8 = lax.broadcasted_iota(jnp.int32, (8, LANES), 1)
    at0 = lane8 - PIECE * row8
    at1 = lane8 - PIECE * (row8 + 8)
    here0 = jnp.logical_and(at0 >= 0, at0 < PIECE)
    here1 = jnp.logical_and(jnp.logical_and(at1 >= 0, at1 < PIECE), lane8 < nq)
    zbuf[:, NT8] = jnp.zeros((4, 2, 8, 512), F32)

    def tails(x):
        f = [x[t].astype(F32) for t in range(4)]
        out = []
        for e in range(2):
            for u in range(2):
                v0 = pltpu.roll(f[2 * u][8 * e:8 * e + 8], LANES - nq, 1, stride=PIECE, stride_axis=0)
                f1 = f[2 * u + 1][8 * e:8 * e + 8]
                v1 = jnp.where(row8 == 0, pltpu.roll(f1, (8 * PIECE - nq) % LANES, 1), pltpu.roll(f1, (9 * PIECE - nq) % LANES, 1))
                v = jnp.where(here0, v0, jnp.where(here1, v1, 0.0))
                out.append(v.sum(0, keepdims=True))
        return out

    def fit(p):
        ml = []
        for s in range(2):
            rest = tails(own[s, p, pl.ds(0, 4)]) + [jnp.zeros((12, LANES), F32)]
            ml.append(jnp.concatenate([own[s, p].reshape(NT8 * 16, LANES), jnp.concatenate(rest, axis=0).astype(BF)], axis=0))
        mid, low = ml
        rows = pl.ds(pl.multiple_of(a * LANES, LANES), LANES)
        mh, mm = msp[0, rows], msp[1, rows]
        zown[...] = dot(jnp.concatenate([mid, mid, low], axis=1), jnp.concatenate([mh, mm, mh], axis=0), NN)
        if p == npair - 1:
            s = sacc[...]
            s = s + s.T
            kacc[0] = kacc[0] + s[:, :LANES]
            kacc[1] = kacc[1] + s[:, LANES:]
        pltpu.make_async_copy(rbuf.at[:, p], rbuf.at[:, p], trecv.at[p]).wait()
        if p + 3 < npair:
            @pl.when(jnp.logical_not(outer))
            def _():
                send_half(p + 3, 0, NT8, True)
        xs = []
        for s in range(4):
            rest = [w for q in range(4) for w in tails(rbuf[s, p, q, pl.ds(0, 4)])]
            xs.append(jnp.concatenate([rbuf[s, p].reshape(4 * NT8 * 16, LANES), jnp.concatenate(rest, axis=0).astype(BF)], axis=0))
        x = jnp.concatenate(xs, axis=1)
        z = dot(jnp.concatenate([x, x, x], axis=1), msp[...].reshape(3 * 512, 512), NN)
        main = 4 * NT8 * 16
        zbuf[:, pl.ds(0, NT8)] = z[:main].reshape(4, NT8, 2, 8, 512)
        for q in range(4):
            for e in range(2):
                zbuf[q, NT8, e, pl.ds(0, 2)] = z[main + 4 * q + 2 * e:main + 4 * q + 2 * e + 2]
        z = zown[...]
        zbuf[o, pl.ds(0, NT8)] = zbuf[o, pl.ds(0, NT8)] + z[:NT8 * 16].reshape(NT8, 2, 8, 512)
        for e in range(2):
            zbuf[o, NT8, e, pl.ds(0, 2)] = zbuf[o, NT8, e, pl.ds(0, 2)] + z[NT8 * 16 + 2 * e:NT8 * 16 + 2 * e + 2]
        for e in range(2):
            s3 = split3(zbuf[:, :, e].reshape(4 * MROW, 512))
            if p == npair - 1:
                k = dot(lhs6(s3, 1), rhs6(s3, 1), NT)
            else:
                hi, mid, low = s3
                both = jnp.concatenate([hi, mid], axis=1)
                k = dot(both, both, NT)
                half_sum = dot(jnp.concatenate([hi, hi], axis=1), jnp.concatenate([mid, low], axis=1), NT)
                if p == 0 and e == 0:
                    sacc[...] = half_sum
                else:
                    sacc[...] = sacc[...] + half_sum
            if p == 0 and e == 0:
                kacc[0] = k[:, :LANES]
                kacc[1] = k[:, LANES:]
            else:
                kacc[0] = kacc[0] + k[:, :LANES]
                kacc[1] = kacc[1] + k[:, LANES:]

    lax.fori_loop(0, nm // 2, jpair, 0)
    near, far = a + 1 - 2 * (a % 2), lax.rem(a + 2, 4)
    hops = []
    for e, aa in enumerate((lax.rem(near + 2, 4), near)):
        hops.append(pltpu.make_async_remote_copy(src_ref=jsend.at[aa], dst_ref=jrecv.at[e], send_sem=jssem.at[e], recv_sem=jrsem.at[e],
                                                 device_id=dev(near, o), device_id_type=MESH))
        hops[-1].start()
    @pl.when(outer)
    def _():
        send_half(npair - 1, 0, NT8, True)

    @pl.when(jnp.logical_not(outer))
    def _():
        for p in range(3, npair):
            send_half(p, 0, NT8, False)
    for p in range(npair - 1):
        fit(p)
    hops[0].wait_recv()
    jfwd[...] = jsend[far] + jrecv[0]
    cross = pltpu.make_async_remote_copy(src_ref=jfwd, dst_ref=jrecv.at[2], send_sem=jssem.at[2], recv_sem=jrsem.at[2],
                                         device_id=dev(far, o), device_id_type=MESH)
    cross.start()
    fit(npair - 1)

    mate = o + 1 - 2 * half
    swap = pltpu.make_async_remote_copy(src_ref=kacc.at[1 - half], dst_ref=kin, send_sem=kxs, recv_sem=kxr,
                                        device_id=dev(a, mate), device_id_type=MESH)
    swap.start()
    swap.wait_recv()
    kful[...] = kacc[half] + kin[...]
    low32 = lax.broadcasted_iota(jnp.int32, (32, LANES), 1) < 64
    kland = krecv.at[pl.ds(pl.multiple_of(dens * 32, 32), 32)]
    for oo in range(4):
        ev = kful[pl.ds(MROW * oo, 32, stride=2), :]
        od = kful[pl.ds(MROW * oo + 1, 32, stride=2), :]
        kmsg[0, oo] = jnp.where(low32, ev, pltpu.roll(od, 64, 1))
        kmsg[1, oo] = jnp.where(low32, pltpu.roll(ev, 64, 1), od)
        for al in range(2):
            aa = 2 * half + al
            same = jnp.logical_and(aa == a, oo == o)

            @pl.when(jnp.logical_not(same))
            def _():
                pltpu.make_async_remote_copy(src_ref=kmsg.at[al, oo], dst_ref=kland, send_sem=kss, recv_sem=krs,
                                             device_id=dev(aa, oo), device_id_type=MESH).start()

            @pl.when(same)
            def _():
                pltpu.make_async_copy(kmsg.at[al, oo], kland, krs).start()

    hops[1].wait_recv()
    cross.wait_recv()
    pltpu.make_async_copy(krecv, krecv, krs).wait()
    for u in range(nm // 2):
        j = jsend[a, u] + jrecv[1, u] + jrecv[2, u]
        g = 2.0 * j - krecv[pl.ds(u, nd, stride=32), :]
        out[2 * u] = g[:, :nm]
        out[2 * u + 1] = pltpu.roll(g, 64, 1)[:, :nm]

    pltpu.make_async_copy(sbuf.at[pl.ds(0, 15)], sbuf.at[pl.ds(0, 15)], tsend).wait()
    metric_copies(lambda c: c.wait_send())
    pltpu.make_async_copy(mqr.at[:, pl.ds(0, 96)], mqr.at[:, pl.ds(0, 96)], mosend).wait()
    pltpu.make_async_copy(gbuf, gbuf, gssem).wait()
    for c in hops + [cross]:
        c.wait_send()
    swap.wait_send()
    inset = (a // 2) == half

    @pl.when(inset)
    def _():
        pltpu.make_async_copy(krecv.at[pl.ds(0, 224)], krecv.at[pl.ds(0, 224)], kss).wait()

    @pl.when(jnp.logical_not(inset))
    def _():
        pltpu.make_async_copy(krecv, krecv, kss).wait()


def solution(mesh):
    def local_fock(ints_blk, metric_blk, orbitals):
        nq, nm, nl = ints_blk.shape
        nd, _, ni = orbitals.shape
        bt = jnp.transpose(ints_blk, (1, 2, 0))
        mt = metric_blk.T
        ct = jnp.transpose(orbitals, (2, 0, 1)).reshape(ni * nd, nl)
        npair = ni // 4
        V = pltpu.VMEM
        dma = pltpu.SemaphoreType.DMA
        g = pl.pallas_call(
            lambda *refs: kernel(nm, nl, nq, nd, ni, *refs),
            out_shape=pltpu.VMEM((nm, nd, nm), F32),
            in_specs=[pl.BlockSpec(memory_space=pl.ANY)] * 3,
            out_specs=pl.BlockSpec(memory_space=pltpu.VMEM),
            scratch_shapes=[
                V((nm, nl, nq), F32), V((4 * nq, nq), F32), V((ni * nd, nl), F32), V((ni * nd, 256), F32),
                V((8 * SP, LANES), F32), V((16, npair, NT8, 16, LANES), BF), V((4, npair, 4, NT8, 16, LANES), BF),
                V((2, npair, NT8, 16, LANES), BF), V((4, LANES, LANES), F32), V((6, LANES, LANES), F32), V((4, 4, LANES, LANES), F32), V((3, 512, 512), BF),
                V((nd, LANES), F32), V((4, 4, nd, LANES), F32), V((4, nm // 2, nd, LANES), F32), V((3, nm // 2, nd, LANES), F32), V((nm // 2, nd, LANES), F32),
                V((4, 8, 2, 8, 512), F32), V((2, 256, LANES), F32), V((256, LANES), F32), V((256, LANES), F32), V((2, 4, 32, LANES), F32),
                V((8 * 32, LANES), F32), V((15, nd, LANES), F32), V((LANES, 512), F32), V((256, 256), F32),
                dma((NT8,)), dma((3,)), dma, dma((npair,)), dma, dma, dma, dma, dma, dma, dma((3,)), dma((3,)), dma, dma, dma, dma],
            compiler_params=pltpu.CompilerParams(collective_id=0, has_side_effects=True, vmem_limit_bytes=60 * 2**20),
        )(bt, mt, ct)
        return jnp.transpose(g, (1, 0, 2))

    return jax.shard_map(local_fock, mesh=mesh, in_specs=(P(('sys', 'aux'), 'orb', None), P(('sys', 'aux'), None), P('sys', None, None)), out_specs=P('sys', 'orb', 'aux'), check_vma=False)
```

```python
import jax
import jax.numpy as jnp
from jax import lax
from jax.experimental import pallas as pl
from jax.experimental.pallas import tpu as pltpu
from jax.sharding import PartitionSpec as P

F32 = jnp.float32
BF = jnp.bfloat16
MESH = pl.DeviceIdType.MESH
NN = (((1,), (0,)), ((), ()))
NT = (((1,), (1,)), ((), ()))
LANES = 128
MROW = 64
NT8 = 7
PIECE = 12
SP = 168


def split3(x):
    hi = x.astype(BF)
    rest = x - hi.astype(F32)
    mid = rest.astype(BF)
    return hi, mid, (rest - mid.astype(F32)).astype(BF)


def dot(x, y, dims):
    return lax.dot_general(x, y, dims, preferred_element_type=F32)


def lhs6(x, axis):
    h, m, l = x
    return jnp.concatenate([h, h, m, m, h, l], axis=axis)


def rhs6(x, axis):
    h, m, l = x
    return jnp.concatenate([h, m, h, m, l, h], axis=axis)


def kernel(nm, nl, nq, nd, ni, bt, mt, ct, out, bv, mv, cv, ctp, tr, sbuf, rbuf, own, mloc, mqr, mq, msp, gsend, grecv, jsend, jrecv, jfwd, zbuf, kacc, kin, kful, kmsg, krecv, gbuf, zown, sacc,
           bsem, lsem, tsend, trecv, mzsend, mzrecv, mosend, morecv, gssem, grsem, jssem, jrsem, kxs, kxr, kss, krs):
    sy, a, o = lax.axis_index('sys'), lax.axis_index('aux'), lax.axis_index('orb')
    me = a * 4 + o
    dens, half = me // 2, me % 2
    nh = ni // 2
    npair = nh // 2

    def dev(aa, oo):
        return (sy, aa, oo)

    pltpu.make_async_copy(ct, cv, lsem.at[0]).start()
    pltpu.make_async_copy(bt.at[pl.ds(8 * NT8, 2)], bv.at[pl.ds(8 * NT8, 2)], lsem.at[2]).start()
    for t in range(NT8):
        pltpu.make_async_copy(bt.at[pl.ds(8 * t, 8)], bv.at[pl.ds(8 * t, 8)], bsem.at[t]).start()
        if t == 0:
            pltpu.make_async_copy(mt, mv, lsem.at[1]).start()
    barrier = pltpu.get_barrier_semaphore()

    def tell(k, c):
        g = lax.rem(me + k, 16)
        pl.semaphore_signal(barrier, inc=1, device_id=dev(g // 4, g % 4), device_id_type=MESH)
        return c
    lax.fori_loop(1, 16, tell, 0)

    pltpu.make_async_copy(ct, cv, lsem.at[0]).wait()
    ctp[...] = jnp.concatenate([cv[...], jnp.zeros((nd * ni, 256 - nl), F32)], axis=1)
    lhs = lhs6(split3(ctp[...]), 1)
    pltpu.make_async_copy(mt, mv, lsem.at[1]).wait()
    for b in range(4):
        blk = jnp.concatenate([mv[nq * b:nq * (b + 1), :], jnp.zeros((nq, LANES - nq), F32)], axis=1)
        mloc[b] = jnp.concatenate([blk, jnp.zeros((LANES - nq, LANES), F32)], axis=0)
    pl.semaphore_wait(barrier, 15)

    quarter = pl.ds(pl.multiple_of(o * 32, 32), 32)

    def nearer(x, y, z):
        dx, dy = jnp.abs(x - z), jnp.abs(y - z)
        return jnp.logical_or(dx < dy, jnp.logical_and(dx == dy, x < y))

    def metric_copies(act):
        for k in (2, 1, 3):
            to = lax.rem(a + 4 - k, 4)

            def block(row, slot):
                return pltpu.make_async_remote_copy(src_ref=mloc.at[row, quarter], dst_ref=mqr.at[slot, quarter], send_sem=mzsend,
                                                    recv_sem=mzrecv, device_id=dev(to, o), device_id_type=MESH)
            act(block(a, k - 1))
            for k2 in (1, 2, 3):
                if k2 == k:
                    continue
                b = lax.rem(to + k2, 4)

                @pl.when(nearer(a, b, to))
                def _():
                    act(block(b, k + k2))
    metric_copies(lambda c: c.start())

    gam = jnp.zeros((nd, LANES), F32)
    tr2 = tr

    lane = lax.broadcasted_iota(jnp.int32, (1, LANES), 1)
    data = lane < nq

    def tile(t, gam, tail, first):
        pltpu.make_async_copy(bt.at[pl.ds(0, 8)], bv.at[pl.ds(0, 8)], bsem.at[t]).wait()
        cols = pltpu.roll(ctp[...], lax.rem(512 - (nm * o + 8 * t), 256), 1)
        count = 0
        if tail is not None:
            count = min(8, 10 - first)
            spare = jnp.concatenate([bv[8 * NT8 + tail], jnp.zeros((nl, LANES - nq), F32)], axis=1)
            tcol = pltpu.roll(ctp[...], lax.rem(512 - (nm * o + 8 * NT8 + tail), 256), 1)[:, 0:1]
        for r in range(0, 8, 2):
            xs = []
            for e in range(2):
                x = jnp.concatenate([bv[8 * t + r + e], jnp.zeros((nl, LANES - nq), F32)], axis=1)
                if r + e < count:
                    x = jnp.where(data, x, pltpu.roll(spare, (nq - PIECE * (first + r + e)) % LANES, 1))
                xs.append(x)
            x = jnp.concatenate(xs, axis=1)
            x = jnp.concatenate([x, jnp.zeros((256 - nl, 2 * LANES), F32)], axis=0)
            y = dot(lhs, rhs6(split3(x), 0), NN)
            for e in range(2):
                ye = y[:, e * LANES:(e + 1) * LANES]
                tr2[pl.ds((r + e) * SP, nd * ni), :] = ye
                col = cols[:, r + e:r + e + 1]
                if r + e < count:
                    w = (ye * jnp.where(data, col, tcol)).reshape(ni, nd, LANES).sum(0)
                    moved = pltpu.roll(jnp.where(data, 0.0, w), (PIECE * (first + r + e) - nq) % LANES, 1)
                    gam = gam + jnp.where(data, w, 0.0) + moved
                else:
                    gam = gam + (ye * col).reshape(ni, nd, LANES).sum(0)
        for g in range(16):
            d, h = g // 2, g % 2
            for p in range(npair):
                two = [tr2[pl.ds((h * nh + 2 * p + e) * nd + d, 8, stride=SP), :] for e in range(2)]
                sbuf[g, p, t] = jnp.concatenate(two, axis=0).astype(BF)
        for p in range(npair):
            two = [tr2[pl.ds((half * nh + 2 * p + e) * nd + dens, 8, stride=SP), :] for e in range(2)]
            _, mid, low = split3(jnp.concatenate(two, axis=0))
            own[0, p, t] = mid
            own[1, p, t] = low
        return gam

    def send_t1(p, t0, nt):
        def one(k, c):
            j, u = k % 4, k // 4
            aa = lax.rem(a + 2 + j, 4)
            oo = lax.rem(o + 1 + u, 4)
            g = aa * 4 + oo
            src = sbuf.at[g, p, pl.ds(t0, nt)]
            dst = rbuf.at[a, p, o, pl.ds(t0, nt)]

            @pl.when(k != 14)
            def _():
                pltpu.make_async_remote_copy(src_ref=src, dst_ref=dst, send_sem=tsend, recv_sem=trecv.at[p],
                                             device_id=dev(aa, oo), device_id_type=MESH).start()

            @pl.when(k == 14)
            def _():
                pltpu.make_async_copy(src, dst, trecv.at[p]).start()
            return c
        lax.fori_loop(0, 16, one, 0)

    outer = jnp.logical_or(a == 0, a == 3)
    pair = a + 1 - 2 * (a % 2)

    def send_half(p, t0, nt, cross):
        def one(k, c):
            if cross:
                aa = jnp.where(k % 2 == 0, 3 - a, 3 - pair)
                oo = lax.rem(o + 1 + k // 2, 4)
            else:
                aa = jnp.where(k % 2 == 0, pair, a)
                oo = lax.rem(o + 1 + k // 2, 4)
            g = aa * 4 + oo
            src = sbuf.at[g, p, pl.ds(t0, nt)]
            dst = rbuf.at[a, p, o, pl.ds(t0, nt)]

            def far():
                pltpu.make_async_remote_copy(src_ref=src, dst_ref=dst, send_sem=tsend, recv_sem=trecv.at[p],
                                             device_id=dev(aa, oo), device_id_type=MESH).start()
            if cross:
                far()
            else:
                pl.when(k != 7)(far)

                @pl.when(k == 7)
                def _():
                    pltpu.make_async_copy(src, dst, trecv.at[p]).start()
            return c
        lax.fori_loop(0, 8, one, 0)

    pltpu.make_async_copy(bt.at[pl.ds(0, 2)], bv.at[pl.ds(0, 2)], lsem.at[2]).wait()

    def two_tiles(u, gam):
        gam = tile(2 * u, gam, u, 0)
        send_t1(0, 2 * u, 1)
        gam = tile(2 * u + 1, gam, u, 8)
        send_t1(0, 2 * u + 1, 1)
        return gam
    gam = lax.fori_loop(0, 2, two_tiles, gam)

    def one_tile(t, gam):
        gam = tile(t, gam, None, 0)
        send_t1(0, t, 1)
        return gam
    gam = lax.fori_loop(4, NT8, one_tile, gam)

    gsend[...] = gam

    def gs(k, c):
        g = lax.rem(me + k, 16)
        pltpu.make_async_remote_copy(src_ref=gsend, dst_ref=grecv.at[a, o], send_sem=gssem, recv_sem=grsem,
                                     device_id=dev(g // 4, g % 4), device_id_type=MESH).start()
        return c
    lax.fori_loop(1, 16, gs, 0)
    pltpu.make_async_copy(gsend, grecv.at[a, o], grsem).start()

    pltpu.make_async_copy(mqr.at[:, pl.ds(0, 32)], mqr.at[:, pl.ds(0, 32)], mzrecv).wait()

    def mo(k, c):
        oo = lax.rem(o + k, 4)
        pltpu.make_async_remote_copy(src_ref=mqr.at[:, quarter], dst_ref=mqr.at[:, quarter], send_sem=mosend, recv_sem=morecv,
                                     device_id=dev(a, oo), device_id_type=MESH).start()
        return c
    lax.fori_loop(1, 4, mo, 0)
    @pl.when(outer)
    def _():
        send_half(1, 0, NT8, False)
        send_half(2, 0, NT8, False)
        send_half(1, 0, NT8, True)
        send_half(3, 0, NT8, False)
        send_half(4, 0, NT8, False)
        send_half(2, 0, NT8, True)
        send_half(3, 0, NT8, True)

    @pl.when(jnp.logical_not(outer))
    def _():
        for p in range(1, 3):
            send_t1(p, 0, NT8)
    mq[a] = mloc[...]
    for k in range(1, 4):
        c1 = lax.rem(a + k, 4)
        mq[c1, a] = mloc[c1].T
    pltpu.make_async_copy(mqr.at[:, pl.ds(0, 96)], mqr.at[:, pl.ds(0, 96)], morecv).wait()
    for k in range(1, 4):
        c1 = lax.rem(a + k, 4)
        mq[c1, c1] = mqr[k - 1]
        for k2 in range(k + 1, 4):
            c2 = lax.rem(a + k2, 4)
            first = jnp.where(nearer(c1, c2, a), c1, c2)
            second = c1 + c2 - first
            blk = mqr[k + k2]
            mq[first, second] = blk
            mq[second, first] = blk.T
    for b in range(4):
        parts = split3(jnp.concatenate([mq[aa, b] for aa in range(4)], axis=1))
        for s in range(3):
            msp[s, pl.ds(b * LANES, LANES)] = parts[s]

    pltpu.make_async_copy(grecv, grecv, grsem).wait()
    graw = jnp.concatenate([grecv[aa, 0] + grecv[aa, 1] + grecv[aa, 2] + grecv[aa, 3] for aa in range(4)], axis=1)
    m3 = [msp[s] for s in range(3)]
    gfit = dot(lhs6(split3(graw), 1), rhs6(m3, 0), NN)
    mown = split3(jnp.concatenate([mloc[b] for b in range(4)], axis=0))
    wts = dot(lhs6(split3(gfit), 1), rhs6(mown, 0), NN)
    wl = lhs6(split3(wts), 1)
    low64 = lax.broadcasted_iota(jnp.int32, (nd, LANES), 1) < 64

    def jpair(u, c):
        ys = []
        for e in range(2):
            x = jnp.concatenate([bv[2 * u + e], jnp.zeros((nl, LANES - nq), F32)], axis=1)
            x = jnp.concatenate([x, jnp.zeros((256 - nl, LANES), F32)], axis=0)
            ys.append(dot(wl, rhs6(split3(x), 1), NT))
        for aa in range(4):
            lo = pltpu.roll(ys[0], (256 - nm * aa) % 256, 1)[:, :LANES]
            hi = pltpu.roll(ys[1], (256 + 64 - nm * aa) % 256, 1)[:, :LANES]
            jsend[aa, u] = jnp.where(low64, lo, hi)
        return c

    row8 = lax.broadcasted_iota(jnp.int32, (8, LANES), 0)
    lane8 = lax.broadcasted_iota(jnp.int32, (8, LANES), 1)
    at0 = lane8 - PIECE * row8
    at1 = lane8 - PIECE * (row8 + 8)
    here0 = jnp.logical_and(at0 >= 0, at0 < PIECE)
    here1 = jnp.logical_and(jnp.logical_and(at1 >= 0, at1 < PIECE), lane8 < nq)
    zbuf[:, NT8] = jnp.zeros((4, 2, 8, 512), F32)

    def tails(x):
        f = [x[t].astype(F32) for t in range(4)]
        out = []
        for e in range(2):
            for u in range(2):
                v0 = pltpu.roll(f[2 * u][8 * e:8 * e + 8], LANES - nq, 1, stride=PIECE, stride_axis=0)
                f1 = f[2 * u + 1][8 * e:8 * e + 8]
                v1 = jnp.where(row8 == 0, pltpu.roll(f1, (8 * PIECE - nq) % LANES, 1), pltpu.roll(f1, (9 * PIECE - nq) % LANES, 1))
                v = jnp.where(here0, v0, jnp.where(here1, v1, 0.0))
                out.append(v.sum(0, keepdims=True))
        return out

    def fit(p):
        ml = []
        for s in range(2):
            rest = tails(own[s, p, pl.ds(0, 4)]) + [jnp.zeros((12, LANES), F32)]
            ml.append(jnp.concatenate([own[s, p].reshape(NT8 * 16, LANES), jnp.concatenate(rest, axis=0).astype(BF)], axis=0))
        mid, low = ml
        rows = pl.ds(pl.multiple_of(a * LANES, LANES), LANES)
        mh, mm = msp[0, rows], msp[1, rows]
        zown[...] = dot(jnp.concatenate([mid, mid, low], axis=1), jnp.concatenate([mh, mm, mh], axis=0), NN)
        if p == npair - 1:
            s = sacc[...]
            s = s + s.T
            kacc[0] = kacc[0] + s[:, :LANES]
            kacc[1] = kacc[1] + s[:, LANES:]
        pltpu.make_async_copy(rbuf.at[:, p], rbuf.at[:, p], trecv.at[p]).wait()
        if p in (0, 2):
            @pl.when(jnp.logical_not(outer))
            def _():
                send_half(3 if p == 0 else 4, 0, NT8, True)
        xs = []
        for s in range(4):
            rest = [w for q in range(4) for w in tails(rbuf[s, p, q, pl.ds(0, 4)])]
            xs.append(jnp.concatenate([rbuf[s, p].reshape(4 * NT8 * 16, LANES), jnp.concatenate(rest, axis=0).astype(BF)], axis=0))
        x = jnp.concatenate(xs, axis=1)
        z = dot(jnp.concatenate([x, x, x], axis=1), msp[...].reshape(3 * 512, 512), NN)
        main = 4 * NT8 * 16
        zbuf[:, pl.ds(0, NT8)] = z[:main].reshape(4, NT8, 2, 8, 512)
        for q in range(4):
            for e in range(2):
                zbuf[q, NT8, e, pl.ds(0, 2)] = z[main + 4 * q + 2 * e:main + 4 * q + 2 * e + 2]
        z = zown[...]
        zbuf[o, pl.ds(0, NT8)] = zbuf[o, pl.ds(0, NT8)] + z[:NT8 * 16].reshape(NT8, 2, 8, 512)
        for e in range(2):
            zbuf[o, NT8, e, pl.ds(0, 2)] = zbuf[o, NT8, e, pl.ds(0, 2)] + z[NT8 * 16 + 2 * e:NT8 * 16 + 2 * e + 2]
        for e in range(2):
            s3 = split3(zbuf[:, :, e].reshape(4 * MROW, 512))
            if p == npair - 1:
                k = dot(lhs6(s3, 1), rhs6(s3, 1), NT)
            else:
                hi, mid, low = s3
                both = jnp.concatenate([hi, mid], axis=1)
                k = dot(both, both, NT)
                half_sum = dot(jnp.concatenate([hi, hi], axis=1), jnp.concatenate([mid, low], axis=1), NT)
                if p == 0 and e == 0:
                    sacc[...] = half_sum
                else:
                    sacc[...] = sacc[...] + half_sum
            if p == 0 and e == 0:
                kacc[0] = k[:, :LANES]
                kacc[1] = k[:, LANES:]
            else:
                kacc[0] = kacc[0] + k[:, :LANES]
                kacc[1] = kacc[1] + k[:, LANES:]

    lax.fori_loop(0, nm // 2, jpair, 0)
    near, far = a + 1 - 2 * (a % 2), lax.rem(a + 2, 4)
    hops = []
    for e, aa in enumerate((lax.rem(near + 2, 4), near)):
        hops.append(pltpu.make_async_remote_copy(src_ref=jsend.at[aa], dst_ref=jrecv.at[e], send_sem=jssem.at[e], recv_sem=jrsem.at[e],
                                                 device_id=dev(near, o), device_id_type=MESH))
        hops[-1].start()
    @pl.when(outer)
    def _():
        send_half(npair - 1, 0, NT8, True)

    @pl.when(jnp.logical_not(outer))
    def _():
        for p in range(3, npair):
            send_half(p, 0, NT8, False)
    for p in range(npair - 1):
        fit(p)
    hops[0].wait_recv()
    jfwd[...] = jsend[far] + jrecv[0]
    cross = pltpu.make_async_remote_copy(src_ref=jfwd, dst_ref=jrecv.at[2], send_sem=jssem.at[2], recv_sem=jrsem.at[2],
                                         device_id=dev(far, o), device_id_type=MESH)
    cross.start()
    fit(npair - 1)

    mate = o + 1 - 2 * half
    swap = pltpu.make_async_remote_copy(src_ref=kacc.at[1 - half], dst_ref=kin, send_sem=kxs, recv_sem=kxr,
                                        device_id=dev(a, mate), device_id_type=MESH)
    swap.start()
    swap.wait_recv()
    kful[...] = kacc[half] + kin[...]
    low32 = lax.broadcasted_iota(jnp.int32, (32, LANES), 1) < 64
    for oo in range(4):
        ev = kful[pl.ds(MROW * oo, 32, stride=2), :]
        od = kful[pl.ds(MROW * oo + 1, 32, stride=2), :]
        kmsg[0, oo] = jnp.where(low32, ev, pltpu.roll(od, 64, 1))
        kmsg[1, oo] = jnp.where(low32, pltpu.roll(ev, 64, 1), od)

    def ks(k, c):
        al, oo = k // 4, k % 4
        aa = 2 * half + al
        same = jnp.logical_and(aa == a, oo == o)

        @pl.when(jnp.logical_not(same))
        def _():
            pltpu.make_async_remote_copy(src_ref=kmsg.at[al, oo], dst_ref=krecv.at[pl.ds(dens * 32, 32)], send_sem=kss, recv_sem=krs,
                                         device_id=dev(aa, oo), device_id_type=MESH).start()

        @pl.when(same)
        def _():
            cp = pltpu.make_async_copy(kmsg.at[al, oo], krecv.at[pl.ds(dens * 32, 32)], krs)
            cp.start()
        return c
    lax.fori_loop(0, 8, ks, 0)

    hops[1].wait_recv()
    cross.wait_recv()
    pltpu.make_async_copy(krecv, krecv, krs).wait()
    for u in range(nm // 2):
        j = jsend[a, u] + jrecv[1, u] + jrecv[2, u]
        g = 2.0 * j - krecv[pl.ds(u, nd, stride=32), :]
        out[2 * u] = g[:, :nm]
        out[2 * u + 1] = pltpu.roll(g, 64, 1)[:, :nm]

    pltpu.make_async_copy(sbuf.at[pl.ds(0, 15)], sbuf.at[pl.ds(0, 15)], tsend).wait()
    metric_copies(lambda c: c.wait_send())
    pltpu.make_async_copy(mqr.at[:, pl.ds(0, 96)], mqr.at[:, pl.ds(0, 96)], mosend).wait()
    pltpu.make_async_copy(gbuf, gbuf, gssem).wait()
    for c in hops + [cross]:
        c.wait_send()
    swap.wait_send()
    inset = (a // 2) == half

    @pl.when(inset)
    def _():
        pltpu.make_async_copy(krecv.at[pl.ds(0, 224)], krecv.at[pl.ds(0, 224)], kss).wait()

    @pl.when(jnp.logical_not(inset))
    def _():
        pltpu.make_async_copy(krecv, krecv, kss).wait()


def solution(mesh):
    def local_fock(ints_blk, metric_blk, orbitals):
        nq, nm, nl = ints_blk.shape
        nd, _, ni = orbitals.shape
        bt = jnp.transpose(ints_blk, (1, 2, 0))
        mt = metric_blk.T
        ct = jnp.transpose(orbitals, (2, 0, 1)).reshape(ni * nd, nl)
        npair = ni // 4
        V = pltpu.VMEM
        dma = pltpu.SemaphoreType.DMA
        g = pl.pallas_call(
            lambda *refs: kernel(nm, nl, nq, nd, ni, *refs),
            out_shape=pltpu.VMEM((nm, nd, nm), F32),
            in_specs=[pl.BlockSpec(memory_space=pl.ANY)] * 3,
            out_specs=pl.BlockSpec(memory_space=pltpu.VMEM),
            scratch_shapes=[
                V((nm, nl, nq), F32), V((4 * nq, nq), F32), V((ni * nd, nl), F32), V((ni * nd, 256), F32),
                V((8 * SP, LANES), F32), V((16, npair, NT8, 16, LANES), BF), V((4, npair, 4, NT8, 16, LANES), BF),
                V((2, npair, NT8, 16, LANES), BF), V((4, LANES, LANES), F32), V((6, LANES, LANES), F32), V((4, 4, LANES, LANES), F32), V((3, 512, 512), BF),
                V((nd, LANES), F32), V((4, 4, nd, LANES), F32), V((4, nm // 2, nd, LANES), F32), V((3, nm // 2, nd, LANES), F32), V((nm // 2, nd, LANES), F32),
                V((4, 8, 2, 8, 512), F32), V((2, 256, LANES), F32), V((256, LANES), F32), V((256, LANES), F32), V((2, 4, 32, LANES), F32),
                V((8 * 32, LANES), F32), V((15, nd, LANES), F32), V((LANES, 512), F32), V((256, 256), F32),
                dma((NT8,)), dma((3,)), dma, dma((npair,)), dma, dma, dma, dma, dma, dma, dma((3,)), dma((3,)), dma, dma, dma, dma],
            compiler_params=pltpu.CompilerParams(collective_id=0, has_side_effects=True, vmem_limit_bytes=60 * 2**20),
        )(bt, mt, ct)
        return jnp.transpose(g, (1, 0, 2))

    return jax.shard_map(local_fock, mesh=mesh, in_specs=(P(('sys', 'aux'), 'orb', None), P(('sys', 'aux'), None), P('sys', None, None)), out_specs=P('sys', 'orb', 'aux'), check_vma=False)
```

```python
import jax
import jax.numpy as jnp
from jax import lax
from jax.experimental import pallas as pl
from jax.experimental.pallas import tpu as pltpu
from jax.sharding import PartitionSpec as P

F32 = jnp.float32
BF = jnp.bfloat16
MESH = pl.DeviceIdType.MESH
NN = (((1,), (0,)), ((), ()))
NT = (((1,), (1,)), ((), ()))
LANES = 128
MROW = 64
NT8 = 7
PIECE = 12
SP = 168


def split3(x):
    hi = x.astype(BF)
    rest = x - hi.astype(F32)
    mid = rest.astype(BF)
    return hi, mid, (rest - mid.astype(F32)).astype(BF)


def dot(x, y, dims):
    return lax.dot_general(x, y, dims, preferred_element_type=F32)


def lhs6(x, axis):
    h, m, l = x
    return jnp.concatenate([h, h, m, m, h, l], axis=axis)


def rhs6(x, axis):
    h, m, l = x
    return jnp.concatenate([h, m, h, m, l, h], axis=axis)


def kernel(nm, nl, nq, nd, ni, bt, mt, ct, out, bv, mv, cv, ctp, tr, sbuf, rbuf, own, mloc, mqr, mq, msp, gsend, grecv, jsend, jrecv, jfwd, zbuf, kacc, kin, kful, kmsg, krecv, gbuf,
           bsem, lsem, tsend, trecv, mzsend, mzrecv, mosend, morecv, gssem, grsem, jssem, jrsem, kxs, kxr, kss, krs):
    sy, a, o = lax.axis_index('sys'), lax.axis_index('aux'), lax.axis_index('orb')
    me = a * 4 + o
    dens, half = me // 2, me % 2
    nh = ni // 2
    npair = nh // 2

    def dev(aa, oo):
        return (sy, aa, oo)

    pltpu.make_async_copy(ct, cv, lsem.at[0]).start()
    pltpu.make_async_copy(bt.at[pl.ds(8 * NT8, 2)], bv.at[pl.ds(8 * NT8, 2)], lsem.at[2]).start()
    for t in range(NT8):
        pltpu.make_async_copy(bt.at[pl.ds(8 * t, 8)], bv.at[pl.ds(8 * t, 8)], bsem.at[t]).start()
        if t == 0:
            pltpu.make_async_copy(mt, mv, lsem.at[1]).start()
    barrier = pltpu.get_barrier_semaphore()

    def tell(k, c):
        g = lax.rem(me + k, 16)
        pl.semaphore_signal(barrier, inc=1, device_id=dev(g // 4, g % 4), device_id_type=MESH)
        return c
    lax.fori_loop(1, 16, tell, 0)

    pltpu.make_async_copy(ct, cv, lsem.at[0]).wait()
    ctp[...] = jnp.concatenate([cv[...], jnp.zeros((nd * ni, 256 - nl), F32)], axis=1)
    lhs = lhs6(split3(ctp[...]), 1)
    gam = jnp.zeros((nd, LANES), F32)
    tr2 = tr

    lane = lax.broadcasted_iota(jnp.int32, (1, LANES), 1)
    data = lane < nq

    def tile(t, gam, tail, first):
        pltpu.make_async_copy(bt.at[pl.ds(0, 8)], bv.at[pl.ds(0, 8)], bsem.at[t]).wait()
        cols = pltpu.roll(ctp[...], lax.rem(512 - (nm * o + 8 * t), 256), 1)
        count = 0
        if tail is not None:
            count = min(8, 10 - first)
            spare = jnp.concatenate([bv[8 * NT8 + tail], jnp.zeros((nl, LANES - nq), F32)], axis=1)
            tcol = pltpu.roll(ctp[...], lax.rem(512 - (nm * o + 8 * NT8 + tail), 256), 1)[:, 0:1]
        for r in range(0, 8, 2):
            xs = []
            for e in range(2):
                x = jnp.concatenate([bv[8 * t + r + e], jnp.zeros((nl, LANES - nq), F32)], axis=1)
                if r + e < count:
                    x = jnp.where(data, x, pltpu.roll(spare, (nq - PIECE * (first + r + e)) % LANES, 1))
                xs.append(x)
            x = jnp.concatenate(xs, axis=1)
            x = jnp.concatenate([x, jnp.zeros((256 - nl, 2 * LANES), F32)], axis=0)
            y = dot(lhs, rhs6(split3(x), 0), NN)
            for e in range(2):
                ye = y[:, e * LANES:(e + 1) * LANES]
                tr2[pl.ds((r + e) * SP, nd * ni), :] = ye
                col = cols[:, r + e:r + e + 1]
                if r + e < count:
                    w = (ye * jnp.where(data, col, tcol)).reshape(ni, nd, LANES).sum(0)
                    moved = pltpu.roll(jnp.where(data, 0.0, w), (PIECE * (first + r + e) - nq) % LANES, 1)
                    gam = gam + jnp.where(data, w, 0.0) + moved
                else:
                    gam = gam + (ye * col).reshape(ni, nd, LANES).sum(0)
        for g in range(16):
            d, h = g // 2, g % 2
            for p in range(npair):
                two = [tr2[pl.ds((h * nh + 2 * p + e) * nd + d, 8, stride=SP), :] for e in range(2)]
                sbuf[g, p, t] = jnp.concatenate(two, axis=0).astype(BF)
        for p in range(npair):
            two = [tr2[pl.ds((half * nh + 2 * p + e) * nd + dens, 8, stride=SP), :] for e in range(2)]
            _, mid, low = split3(jnp.concatenate(two, axis=0))
            own[0, p, t] = mid
            own[1, p, t] = low
        return gam

    def send_t1(p, t0, nt):
        def one(k, c):
            j, u = k % 4, k // 4
            aa = lax.rem(a + 2 + j, 4)
            oo = lax.rem(o + 1 + u, 4)
            g = aa * 4 + oo
            src = sbuf.at[g, p, pl.ds(t0, nt)]
            dst = rbuf.at[a, p, o, pl.ds(t0, nt)]

            @pl.when(k != 14)
            def _():
                pltpu.make_async_remote_copy(src_ref=src, dst_ref=dst, send_sem=tsend, recv_sem=trecv.at[p],
                                             device_id=dev(aa, oo), device_id_type=MESH).start()

            @pl.when(k == 14)
            def _():
                pltpu.make_async_copy(src, dst, trecv.at[p]).start()
            return c
        lax.fori_loop(0, 16, one, 0)

    outer = jnp.logical_or(a == 0, a == 3)
    pair = a + 1 - 2 * (a % 2)

    def send_half(p, t0, nt, cross):
        def one(k, c):
            if cross:
                aa = jnp.where(k % 2 == 0, 3 - a, 3 - pair)
                oo = lax.rem(o + 1 + k // 2, 4)
            else:
                aa = jnp.where(k % 2 == 0, pair, a)
                oo = lax.rem(o + 1 + k // 2, 4)
            g = aa * 4 + oo
            src = sbuf.at[g, p, pl.ds(t0, nt)]
            dst = rbuf.at[a, p, o, pl.ds(t0, nt)]

            def far():
                pltpu.make_async_remote_copy(src_ref=src, dst_ref=dst, send_sem=tsend, recv_sem=trecv.at[p],
                                             device_id=dev(aa, oo), device_id_type=MESH).start()
            if cross:
                far()
            else:
                pl.when(k != 7)(far)

                @pl.when(k == 7)
                def _():
                    pltpu.make_async_copy(src, dst, trecv.at[p]).start()
            return c
        lax.fori_loop(0, 8, one, 0)

    pltpu.make_async_copy(bt.at[pl.ds(0, 2)], bv.at[pl.ds(0, 2)], lsem.at[2]).wait()

    gam = tile(0, gam, 0, 0)
    pltpu.make_async_copy(mt, mv, lsem.at[1]).wait()
    for b in range(4):
        blk = jnp.concatenate([mv[nq * b:nq * (b + 1), :], jnp.zeros((nq, LANES - nq), F32)], axis=1)
        mloc[b] = jnp.concatenate([blk, jnp.zeros((LANES - nq, LANES), F32)], axis=0)
    pl.semaphore_wait(barrier, 15)

    quarter = pl.ds(pl.multiple_of(o * 32, 32), 32)

    def nearer(x, y, z):
        dx, dy = jnp.abs(x - z), jnp.abs(y - z)
        return jnp.logical_or(dx < dy, jnp.logical_and(dx == dy, x < y))

    def metric_copies(act):
        for k in (2, 1, 3):
            to = lax.rem(a + 4 - k, 4)

            def block(row, slot):
                return pltpu.make_async_remote_copy(src_ref=mloc.at[row, quarter], dst_ref=mqr.at[slot, quarter], send_sem=mzsend,
                                                    recv_sem=mzrecv, device_id=dev(to, o), device_id_type=MESH)
            act(block(a, k - 1))
            for k2 in (1, 2, 3):
                if k2 == k:
                    continue
                b = lax.rem(to + k2, 4)

                @pl.when(nearer(a, b, to))
                def _():
                    act(block(b, k + k2))
    metric_copies(lambda c: c.start())

    send_t1(0, 0, 1)
    gam = tile(1, gam, 0, 8)
    send_t1(0, 1, 1)
    gam = tile(2, gam, 1, 0)
    send_t1(0, 2, 1)
    gam = tile(3, gam, 1, 8)
    send_t1(0, 3, 1)

    def one_tile(t, gam):
        gam = tile(t, gam, None, 0)
        send_t1(0, t, 1)
        return gam
    gam = lax.fori_loop(4, NT8, one_tile, gam)

    gsend[...] = gam

    def gs(k, c):
        g = lax.rem(me + k, 16)
        pltpu.make_async_remote_copy(src_ref=gsend, dst_ref=grecv.at[a, o], send_sem=gssem, recv_sem=grsem,
                                     device_id=dev(g // 4, g % 4), device_id_type=MESH).start()
        return c
    lax.fori_loop(1, 16, gs, 0)
    pltpu.make_async_copy(gsend, grecv.at[a, o], grsem).start()

    pltpu.make_async_copy(mqr.at[:, pl.ds(0, 32)], mqr.at[:, pl.ds(0, 32)], mzrecv).wait()

    def mo(k, c):
        oo = lax.rem(o + k, 4)
        pltpu.make_async_remote_copy(src_ref=mqr.at[:, quarter], dst_ref=mqr.at[:, quarter], send_sem=mosend, recv_sem=morecv,
                                     device_id=dev(a, oo), device_id_type=MESH).start()
        return c
    lax.fori_loop(1, 4, mo, 0)
    @pl.when(outer)
    def _():
        send_half(1, 0, NT8, False)
        send_half(2, 0, NT8, False)
        send_half(1, 0, NT8, True)
        send_half(3, 0, NT8, False)
        send_half(4, 0, NT8, False)
        send_half(2, 0, NT8, True)
        send_half(3, 0, NT8, True)

    @pl.when(jnp.logical_not(outer))
    def _():
        for p in range(1, 3):
            send_t1(p, 0, NT8)
    mq[a] = mloc[...]
    for k in range(1, 4):
        c1 = lax.rem(a + k, 4)
        mq[c1, a] = mloc[c1].T
    pltpu.make_async_copy(mqr.at[:, pl.ds(0, 96)], mqr.at[:, pl.ds(0, 96)], morecv).wait()
    for k in range(1, 4):
        c1 = lax.rem(a + k, 4)
        mq[c1, c1] = mqr[k - 1]
        for k2 in range(k + 1, 4):
            c2 = lax.rem(a + k2, 4)
            first = jnp.where(nearer(c1, c2, a), c1, c2)
            second = c1 + c2 - first
            blk = mqr[k + k2]
            mq[first, second] = blk
            mq[second, first] = blk.T
    for b in range(4):
        parts = split3(jnp.concatenate([mq[aa, b] for aa in range(4)], axis=1))
        for s in range(3):
            msp[s, pl.ds(b * LANES, LANES)] = parts[s]

    pltpu.make_async_copy(grecv, grecv, grsem).wait()
    graw = jnp.concatenate([grecv[aa, 0] + grecv[aa, 1] + grecv[aa, 2] + grecv[aa, 3] for aa in range(4)], axis=1)
    m3 = [msp[s] for s in range(3)]
    gfit = dot(lhs6(split3(graw), 1), rhs6(m3, 0), NN)
    mown = split3(jnp.concatenate([mloc[b] for b in range(4)], axis=0))
    wts = dot(lhs6(split3(gfit), 1), rhs6(mown, 0), NN)
    wl = lhs6(split3(wts), 1)
    low64 = lax.broadcasted_iota(jnp.int32, (nd, LANES), 1) < 64

    def jpair(u, c):
        ys = []
        for e in range(2):
            x = jnp.concatenate([bv[2 * u + e], jnp.zeros((nl, LANES - nq), F32)], axis=1)
            x = jnp.concatenate([x, jnp.zeros((256 - nl, LANES), F32)], axis=0)
            ys.append(dot(wl, rhs6(split3(x), 1), NT))
        for aa in range(4):
            lo = pltpu.roll(ys[0], (256 - nm * aa) % 256, 1)[:, :LANES]
            hi = pltpu.roll(ys[1], (256 + 64 - nm * aa) % 256, 1)[:, :LANES]
            jsend[aa, u] = jnp.where(low64, lo, hi)
        return c

    row8 = lax.broadcasted_iota(jnp.int32, (8, LANES), 0)
    lane8 = lax.broadcasted_iota(jnp.int32, (8, LANES), 1)
    at0 = lane8 - PIECE * row8
    at1 = lane8 - PIECE * (row8 + 8)
    here0 = jnp.logical_and(at0 >= 0, at0 < PIECE)
    here1 = jnp.logical_and(jnp.logical_and(at1 >= 0, at1 < PIECE), lane8 < nq)
    zbuf[:, NT8] = jnp.zeros((4, 2, 8, 512), F32)

    def tails(x):
        f = [x[t].astype(F32) for t in range(4)]
        out = []
        for e in range(2):
            for u in range(2):
                v0 = pltpu.roll(f[2 * u][8 * e:8 * e + 8], LANES - nq, 1, stride=PIECE, stride_axis=0)
                f1 = f[2 * u + 1][8 * e:8 * e + 8]
                v1 = jnp.where(row8 == 0, pltpu.roll(f1, (8 * PIECE - nq) % LANES, 1), pltpu.roll(f1, (9 * PIECE - nq) % LANES, 1))
                v = jnp.where(here0, v0, jnp.where(here1, v1, 0.0))
                out.append(v.sum(0, keepdims=True))
        return out

    def fit(p):
        pltpu.make_async_copy(rbuf.at[:, p], rbuf.at[:, p], trecv.at[p]).wait()
        if p + 3 < npair:
            @pl.when(jnp.logical_not(outer))
            def _():
                send_half(p + 3, 0, NT8, True)
        xs = []
        for s in range(4):
            rest = [w for q in range(4) for w in tails(rbuf[s, p, q, pl.ds(0, 4)])]
            xs.append(jnp.concatenate([rbuf[s, p].reshape(4 * NT8 * 16, LANES), jnp.concatenate(rest, axis=0).astype(BF)], axis=0))
        x = jnp.concatenate(xs, axis=1)
        z = dot(jnp.concatenate([x, x, x], axis=1), msp[...].reshape(3 * 512, 512), NN)
        main = 4 * NT8 * 16
        zbuf[:, pl.ds(0, NT8)] = z[:main].reshape(4, NT8, 2, 8, 512)
        for q in range(4):
            for e in range(2):
                zbuf[q, NT8, e, pl.ds(0, 2)] = z[main + 4 * q + 2 * e:main + 4 * q + 2 * e + 2]
        ml = []
        for s in range(2):
            rest = tails(own[s, p, pl.ds(0, 4)]) + [jnp.zeros((12, LANES), F32)]
            ml.append(jnp.concatenate([own[s, p].reshape(NT8 * 16, LANES), jnp.concatenate(rest, axis=0).astype(BF)], axis=0))
        mid, low = ml
        rows = pl.ds(pl.multiple_of(a * LANES, LANES), LANES)
        mh, mm = msp[0, rows], msp[1, rows]
        z = dot(jnp.concatenate([mid, mid, low], axis=1), jnp.concatenate([mh, mm, mh], axis=0), NN)
        zbuf[o, pl.ds(0, NT8)] = zbuf[o, pl.ds(0, NT8)] + z[:NT8 * 16].reshape(NT8, 2, 8, 512)
        for e in range(2):
            zbuf[o, NT8, e, pl.ds(0, 2)] = zbuf[o, NT8, e, pl.ds(0, 2)] + z[NT8 * 16 + 2 * e:NT8 * 16 + 2 * e + 2]
        for e in range(2):
            s3 = split3(zbuf[:, :, e].reshape(4 * MROW, 512))
            k = dot(lhs6(s3, 1), rhs6(s3, 1), NT)
            if p == 0 and e == 0:
                kacc[0] = k[:, :LANES]
                kacc[1] = k[:, LANES:]
            else:
                kacc[0] = kacc[0] + k[:, :LANES]
                kacc[1] = kacc[1] + k[:, LANES:]

    lax.fori_loop(0, nm // 2, jpair, 0)
    near, far = a + 1 - 2 * (a % 2), lax.rem(a + 2, 4)
    hops = []
    for e, aa in enumerate((lax.rem(near + 2, 4), near)):
        hops.append(pltpu.make_async_remote_copy(src_ref=jsend.at[aa], dst_ref=jrecv.at[e], send_sem=jssem.at[e], recv_sem=jrsem.at[e],
                                                 device_id=dev(near, o), device_id_type=MESH))
        hops[-1].start()
    @pl.when(outer)
    def _():
        send_half(npair - 1, 0, NT8, True)

    @pl.when(jnp.logical_not(outer))
    def _():
        for p in range(3, npair):
            send_half(p, 0, NT8, False)
    for p in range(npair - 1):
        fit(p)
    hops[0].wait_recv()
    jfwd[...] = jsend[far] + jrecv[0]
    cross = pltpu.make_async_remote_copy(src_ref=jfwd, dst_ref=jrecv.at[2], send_sem=jssem.at[2], recv_sem=jrsem.at[2],
                                         device_id=dev(far, o), device_id_type=MESH)
    cross.start()
    fit(npair - 1)

    mate = o + 1 - 2 * half
    swap = pltpu.make_async_remote_copy(src_ref=kacc.at[1 - half], dst_ref=kin, send_sem=kxs, recv_sem=kxr,
                                        device_id=dev(a, mate), device_id_type=MESH)
    swap.start()
    swap.wait_recv()
    kful[...] = kacc[half] + kin[...]
    low32 = lax.broadcasted_iota(jnp.int32, (32, LANES), 1) < 64
    for oo in range(4):
        ev = kful[pl.ds(MROW * oo, 32, stride=2), :]
        od = kful[pl.ds(MROW * oo + 1, 32, stride=2), :]
        kmsg[0, oo] = jnp.where(low32, ev, pltpu.roll(od, 64, 1))
        kmsg[1, oo] = jnp.where(low32, pltpu.roll(ev, 64, 1), od)

    def ks(k, c):
        al, oo = k // 4, k % 4
        aa = 2 * half + al
        same = jnp.logical_and(aa == a, oo == o)

        @pl.when(jnp.logical_not(same))
        def _():
            pltpu.make_async_remote_copy(src_ref=kmsg.at[al, oo], dst_ref=krecv.at[pl.ds(dens * 32, 32)], send_sem=kss, recv_sem=krs,
                                         device_id=dev(aa, oo), device_id_type=MESH).start()

        @pl.when(same)
        def _():
            cp = pltpu.make_async_copy(kmsg.at[al, oo], krecv.at[pl.ds(dens * 32, 32)], krs)
            cp.start()
        return c
    lax.fori_loop(0, 8, ks, 0)

    hops[1].wait_recv()
    cross.wait_recv()
    pltpu.make_async_copy(krecv, krecv, krs).wait()
    for u in range(nm // 2):
        j = jsend[a, u] + jrecv[1, u] + jrecv[2, u]
        g = 2.0 * j - krecv[pl.ds(u, nd, stride=32), :]
        out[2 * u] = g[:, :nm]
        out[2 * u + 1] = pltpu.roll(g, 64, 1)[:, :nm]

    pltpu.make_async_copy(sbuf.at[pl.ds(0, 15)], sbuf.at[pl.ds(0, 15)], tsend).wait()
    metric_copies(lambda c: c.wait_send())
    pltpu.make_async_copy(mqr.at[:, pl.ds(0, 96)], mqr.at[:, pl.ds(0, 96)], mosend).wait()
    pltpu.make_async_copy(gbuf, gbuf, gssem).wait()
    for c in hops + [cross]:
        c.wait_send()
    swap.wait_send()
    inset = (a // 2) == half

    @pl.when(inset)
    def _():
        pltpu.make_async_copy(krecv.at[pl.ds(0, 224)], krecv.at[pl.ds(0, 224)], kss).wait()

    @pl.when(jnp.logical_not(inset))
    def _():
        pltpu.make_async_copy(krecv, krecv, kss).wait()


def solution(mesh):
    def local_fock(ints_blk, metric_blk, orbitals):
        nq, nm, nl = ints_blk.shape
        nd, _, ni = orbitals.shape
        bt = jnp.transpose(ints_blk, (1, 2, 0))
        mt = metric_blk.T
        ct = jnp.transpose(orbitals, (2, 0, 1)).reshape(ni * nd, nl)
        npair = ni // 4
        V = pltpu.VMEM
        dma = pltpu.SemaphoreType.DMA
        g = pl.pallas_call(
            lambda *refs: kernel(nm, nl, nq, nd, ni, *refs),
            out_shape=pltpu.VMEM((nm, nd, nm), F32),
            in_specs=[pl.BlockSpec(memory_space=pl.ANY)] * 3,
            out_specs=pl.BlockSpec(memory_space=pltpu.VMEM),
            scratch_shapes=[
                V((nm, nl, nq), F32), V((4 * nq, nq), F32), V((ni * nd, nl), F32), V((ni * nd, 256), F32),
                V((8 * SP, LANES), F32), V((16, npair, NT8, 16, LANES), BF), V((4, npair, 4, NT8, 16, LANES), BF),
                V((2, npair, NT8, 16, LANES), BF), V((4, LANES, LANES), F32), V((6, LANES, LANES), F32), V((4, 4, LANES, LANES), F32), V((3, 512, 512), BF),
                V((nd, LANES), F32), V((4, 4, nd, LANES), F32), V((4, nm // 2, nd, LANES), F32), V((3, nm // 2, nd, LANES), F32), V((nm // 2, nd, LANES), F32),
                V((4, 8, 2, 8, 512), F32), V((2, 256, LANES), F32), V((256, LANES), F32), V((256, LANES), F32), V((2, 4, 32, LANES), F32),
                V((8 * 32, LANES), F32), V((15, nd, LANES), F32),
                dma((NT8,)), dma((3,)), dma, dma((npair,)), dma, dma, dma, dma, dma, dma, dma((3,)), dma((3,)), dma, dma, dma, dma],
            compiler_params=pltpu.CompilerParams(collective_id=0, has_side_effects=True, vmem_limit_bytes=60 * 2**20),
        )(bt, mt, ct)
        return jnp.transpose(g, (1, 0, 2))

    return jax.shard_map(local_fock, mesh=mesh, in_specs=(P(('sys', 'aux'), 'orb', None), P(('sys', 'aux'), None), P('sys', None, None)), out_specs=P('sys', 'orb', 'aux'), check_vma=False)
```

```python
import jax
import jax.numpy as jnp
from jax import lax
from jax.experimental import pallas as pl
from jax.experimental.pallas import tpu as pltpu
from jax.sharding import PartitionSpec as P

F32 = jnp.float32
BF = jnp.bfloat16
MESH = pl.DeviceIdType.MESH
NN = (((1,), (0,)), ((), ()))
NT = (((1,), (1,)), ((), ()))
LANES = 128
MROW = 64
NT8 = 7
PIECE = 12
SP = 168


def split3(x):
    hi = x.astype(BF)
    rest = x - hi.astype(F32)
    mid = rest.astype(BF)
    return hi, mid, (rest - mid.astype(F32)).astype(BF)


def dot(x, y, dims):
    return lax.dot_general(x, y, dims, preferred_element_type=F32)


def lhs6(x, axis):
    h, m, l = x
    return jnp.concatenate([h, h, m, m, h, l], axis=axis)


def rhs6(x, axis):
    h, m, l = x
    return jnp.concatenate([h, m, h, m, l, h], axis=axis)


def kernel(nm, nl, nq, nd, ni, bt, mt, ct, out, bv, mv, cv, ctp, tr, sbuf, rbuf, own, mloc, mqr, mq, msp, gsend, grecv, jsend, jrecv, jfwd, zbuf, kacc, kin, kful, kmsg, krecv, gbuf,
           bsem, lsem, tsend, trecv, mzsend, mzrecv, mosend, morecv, gssem, grsem, jssem, jrsem, kxs, kxr, kss, krs):
    sy, a, o = lax.axis_index('sys'), lax.axis_index('aux'), lax.axis_index('orb')
    me = a * 4 + o
    dens, half = me // 2, me % 2
    nh = ni // 2
    npair = nh // 2

    def dev(aa, oo):
        return (sy, aa, oo)

    pltpu.make_async_copy(mt, mv, lsem.at[1]).start()
    pltpu.make_async_copy(ct, cv, lsem.at[0]).start()
    pltpu.make_async_copy(bt.at[pl.ds(8 * NT8, 2)], bv.at[pl.ds(8 * NT8, 2)], lsem.at[2]).start()
    for t in range(NT8):
        pltpu.make_async_copy(bt.at[pl.ds(8 * t, 8)], bv.at[pl.ds(8 * t, 8)], bsem.at[t]).start()
    barrier = pltpu.get_barrier_semaphore()

    def tell(k, c):
        g = lax.rem(me + k, 16)
        pl.semaphore_signal(barrier, inc=1, device_id=dev(g // 4, g % 4), device_id_type=MESH)
        return c
    lax.fori_loop(1, 16, tell, 0)

    pltpu.make_async_copy(mt, mv, lsem.at[1]).wait()
    for b in range(4):
        blk = jnp.concatenate([mv[nq * b:nq * (b + 1), :], jnp.zeros((nq, LANES - nq), F32)], axis=1)
        mloc[b] = jnp.concatenate([blk, jnp.zeros((LANES - nq, LANES), F32)], axis=0)
    pl.semaphore_wait(barrier, 15)

    quarter = pl.ds(pl.multiple_of(o * 32, 32), 32)

    def nearer(x, y, z):
        dx, dy = jnp.abs(x - z), jnp.abs(y - z)
        return jnp.logical_or(dx < dy, jnp.logical_and(dx == dy, x < y))

    def metric_copies(act):
        for k in (2, 1, 3):
            to = lax.rem(a + 4 - k, 4)

            def block(row, slot):
                return pltpu.make_async_remote_copy(src_ref=mloc.at[row, quarter], dst_ref=mqr.at[slot, quarter], send_sem=mzsend,
                                                    recv_sem=mzrecv, device_id=dev(to, o), device_id_type=MESH)
            act(block(a, k - 1))
            for k2 in (1, 2, 3):
                if k2 == k:
                    continue
                b = lax.rem(to + k2, 4)

                @pl.when(nearer(a, b, to))
                def _():
                    act(block(b, k + k2))
    metric_copies(lambda c: c.start())

    pltpu.make_async_copy(ct, cv, lsem.at[0]).wait()
    ctp[...] = jnp.concatenate([cv[...], jnp.zeros((nd * ni, 256 - nl), F32)], axis=1)
    lhs = lhs6(split3(ctp[...]), 1)

    gam = jnp.zeros((nd, LANES), F32)
    tr2 = tr

    lane = lax.broadcasted_iota(jnp.int32, (1, LANES), 1)
    data = lane < nq

    def tile(t, gam, tail, first):
        pltpu.make_async_copy(bt.at[pl.ds(0, 8)], bv.at[pl.ds(0, 8)], bsem.at[t]).wait()
        cols = pltpu.roll(ctp[...], lax.rem(512 - (nm * o + 8 * t), 256), 1)
        count = 0
        if tail is not None:
            count = min(8, 10 - first)
            spare = jnp.concatenate([bv[8 * NT8 + tail], jnp.zeros((nl, LANES - nq), F32)], axis=1)
            tcol = pltpu.roll(ctp[...], lax.rem(512 - (nm * o + 8 * NT8 + tail), 256), 1)[:, 0:1]
        for r in range(0, 8, 2):
            xs = []
            for e in range(2):
                x = jnp.concatenate([bv[8 * t + r + e], jnp.zeros((nl, LANES - nq), F32)], axis=1)
                if r + e < count:
                    x = jnp.where(data, x, pltpu.roll(spare, (nq - PIECE * (first + r + e)) % LANES, 1))
                xs.append(x)
            x = jnp.concatenate(xs, axis=1)
            x = jnp.concatenate([x, jnp.zeros((256 - nl, 2 * LANES), F32)], axis=0)
            y = dot(lhs, rhs6(split3(x), 0), NN)
            for e in range(2):
                ye = y[:, e * LANES:(e + 1) * LANES]
                tr2[pl.ds((r + e) * SP, nd * ni), :] = ye
                col = cols[:, r + e:r + e + 1]
                if r + e < count:
                    w = (ye * jnp.where(data, col, tcol)).reshape(ni, nd, LANES).sum(0)
                    moved = pltpu.roll(jnp.where(data, 0.0, w), (PIECE * (first + r + e) - nq) % LANES, 1)
                    gam = gam + jnp.where(data, w, 0.0) + moved
                else:
                    gam = gam + (ye * col).reshape(ni, nd, LANES).sum(0)
        for g in range(16):
            d, h = g // 2, g % 2
            for p in range(npair):
                two = [tr2[pl.ds((h * nh + 2 * p + e) * nd + d, 8, stride=SP), :] for e in range(2)]
                sbuf[g, p, t] = jnp.concatenate(two, axis=0).astype(BF)
        for p in range(npair):
            two = [tr2[pl.ds((half * nh + 2 * p + e) * nd + dens, 8, stride=SP), :] for e in range(2)]
            _, mid, low = split3(jnp.concatenate(two, axis=0))
            own[0, p, t] = mid
            own[1, p, t] = low
        return gam

    def send_t1(p, t0, nt):
        def one(k, c):
            j, u = k % 4, k // 4
            aa = lax.rem(a + 2 + j, 4)
            oo = lax.rem(o + 1 + u, 4)
            g = aa * 4 + oo
            src = sbuf.at[g, p, pl.ds(t0, nt)]
            dst = rbuf.at[a, p, o, pl.ds(t0, nt)]

            @pl.when(k != 14)
            def _():
                pltpu.make_async_remote_copy(src_ref=src, dst_ref=dst, send_sem=tsend, recv_sem=trecv.at[p],
                                             device_id=dev(aa, oo), device_id_type=MESH).start()

            @pl.when(k == 14)
            def _():
                pltpu.make_async_copy(src, dst, trecv.at[p]).start()
            return c
        lax.fori_loop(0, 16, one, 0)

    outer = jnp.logical_or(a == 0, a == 3)
    pair = a + 1 - 2 * (a % 2)

    def send_half(p, t0, nt, cross):
        def one(k, c):
            if cross:
                aa = jnp.where(k % 2 == 0, 3 - a, 3 - pair)
                oo = lax.rem(o + 1 + k // 2, 4)
            else:
                aa = jnp.where(k % 2 == 0, pair, a)
                oo = lax.rem(o + 1 + k // 2, 4)
            g = aa * 4 + oo
            src = sbuf.at[g, p, pl.ds(t0, nt)]
            dst = rbuf.at[a, p, o, pl.ds(t0, nt)]

            def far():
                pltpu.make_async_remote_copy(src_ref=src, dst_ref=dst, send_sem=tsend, recv_sem=trecv.at[p],
                                             device_id=dev(aa, oo), device_id_type=MESH).start()
            if cross:
                far()
            else:
                pl.when(k != 7)(far)

                @pl.when(k == 7)
                def _():
                    pltpu.make_async_copy(src, dst, trecv.at[p]).start()
            return c
        lax.fori_loop(0, 8, one, 0)

    pltpu.make_async_copy(bt.at[pl.ds(0, 2)], bv.at[pl.ds(0, 2)], lsem.at[2]).wait()

    def two_tiles(u, gam):
        gam = tile(2 * u, gam, u, 0)
        send_t1(0, 2 * u, 1)
        gam = tile(2 * u + 1, gam, u, 8)
        send_t1(0, 2 * u + 1, 1)
        return gam
    gam = lax.fori_loop(0, 2, two_tiles, gam)

    def one_tile(t, gam):
        gam = tile(t, gam, None, 0)
        send_t1(0, t, 1)
        return gam
    gam = lax.fori_loop(4, NT8, one_tile, gam)

    gsend[...] = gam

    def gs(k, c):
        g = lax.rem(me + k, 16)
        pltpu.make_async_remote_copy(src_ref=gsend, dst_ref=grecv.at[a, o], send_sem=gssem, recv_sem=grsem,
                                     device_id=dev(g // 4, g % 4), device_id_type=MESH).start()
        return c
    lax.fori_loop(1, 16, gs, 0)
    pltpu.make_async_copy(gsend, grecv.at[a, o], grsem).start()

    pltpu.make_async_copy(mqr.at[:, pl.ds(0, 32)], mqr.at[:, pl.ds(0, 32)], mzrecv).wait()

    def mo(k, c):
        oo = lax.rem(o + k, 4)
        pltpu.make_async_remote_copy(src_ref=mqr.at[:, quarter], dst_ref=mqr.at[:, quarter], send_sem=mosend, recv_sem=morecv,
                                     device_id=dev(a, oo), device_id_type=MESH).start()
        return c
    lax.fori_loop(1, 4, mo, 0)
    @pl.when(outer)
    def _():
        send_half(1, 0, NT8, False)
        send_half(2, 0, NT8, False)
        send_half(1, 0, NT8, True)
        send_half(3, 0, NT8, False)
        send_half(4, 0, NT8, False)
        send_half(2, 0, NT8, True)
        send_half(3, 0, NT8, True)

    @pl.when(jnp.logical_not(outer))
    def _():
        for p in range(1, 3):
            send_t1(p, 0, NT8)
    mq[a] = mloc[...]
    for k in range(1, 4):
        c1 = lax.rem(a + k, 4)
        mq[c1, a] = mloc[c1].T
    pltpu.make_async_copy(mqr.at[:, pl.ds(0, 96)], mqr.at[:, pl.ds(0, 96)], morecv).wait()
    for k in range(1, 4):
        c1 = lax.rem(a + k, 4)
        mq[c1, c1] = mqr[k - 1]
        for k2 in range(k + 1, 4):
            c2 = lax.rem(a + k2, 4)
            first = jnp.where(nearer(c1, c2, a), c1, c2)
            second = c1 + c2 - first
            blk = mqr[k + k2]
            mq[first, second] = blk
            mq[second, first] = blk.T
    for b in range(4):
        parts = split3(jnp.concatenate([mq[aa, b] for aa in range(4)], axis=1))
        for s in range(3):
            msp[s, pl.ds(b * LANES, LANES)] = parts[s]

    pltpu.make_async_copy(grecv, grecv, grsem).wait()
    graw = jnp.concatenate([grecv[aa, 0] + grecv[aa, 1] + grecv[aa, 2] + grecv[aa, 3] for aa in range(4)], axis=1)
    m3 = [msp[s] for s in range(3)]
    gfit = dot(lhs6(split3(graw), 1), rhs6(m3, 0), NN)
    mown = split3(jnp.concatenate([mloc[b] for b in range(4)], axis=0))
    wts = dot(lhs6(split3(gfit), 1), rhs6(mown, 0), NN)
    wl = lhs6(split3(wts), 1)
    low64 = lax.broadcasted_iota(jnp.int32, (nd, LANES), 1) < 64

    def jpair(u, c):
        ys = []
        for e in range(2):
            x = jnp.concatenate([bv[2 * u + e], jnp.zeros((nl, LANES - nq), F32)], axis=1)
            x = jnp.concatenate([x, jnp.zeros((256 - nl, LANES), F32)], axis=0)
            ys.append(dot(wl, rhs6(split3(x), 1), NT))
        for aa in range(4):
            lo = pltpu.roll(ys[0], (256 - nm * aa) % 256, 1)[:, :LANES]
            hi = pltpu.roll(ys[1], (256 + 64 - nm * aa) % 256, 1)[:, :LANES]
            jsend[aa, u] = jnp.where(low64, lo, hi)
        return c

    row8 = lax.broadcasted_iota(jnp.int32, (8, LANES), 0)
    lane8 = lax.broadcasted_iota(jnp.int32, (8, LANES), 1)
    at0 = lane8 - PIECE * row8
    at1 = lane8 - PIECE * (row8 + 8)
    here0 = jnp.logical_and(at0 >= 0, at0 < PIECE)
    here1 = jnp.logical_and(jnp.logical_and(at1 >= 0, at1 < PIECE), lane8 < nq)
    zbuf[:, NT8] = jnp.zeros((4, 2, 8, 512), F32)

    def tails(x):
        f = [x[t].astype(F32) for t in range(4)]
        out = []
        for e in range(2):
            for u in range(2):
                v0 = pltpu.roll(f[2 * u][8 * e:8 * e + 8], LANES - nq, 1, stride=PIECE, stride_axis=0)
                f1 = f[2 * u + 1][8 * e:8 * e + 8]
                v1 = jnp.where(row8 == 0, pltpu.roll(f1, (8 * PIECE - nq) % LANES, 1), pltpu.roll(f1, (9 * PIECE - nq) % LANES, 1))
                v = jnp.where(here0, v0, jnp.where(here1, v1, 0.0))
                out.append(v.sum(0, keepdims=True))
        return out

    def fit(p):
        pltpu.make_async_copy(rbuf.at[:, p], rbuf.at[:, p], trecv.at[p]).wait()
        if p + 3 < npair:
            @pl.when(jnp.logical_not(outer))
            def _():
                send_half(p + 3, 0, NT8, True)
        xs = []
        for s in range(4):
            rest = [w for q in range(4) for w in tails(rbuf[s, p, q, pl.ds(0, 4)])]
            xs.append(jnp.concatenate([rbuf[s, p].reshape(4 * NT8 * 16, LANES), jnp.concatenate(rest, axis=0).astype(BF)], axis=0))
        x = jnp.concatenate(xs, axis=1)
        z = dot(jnp.concatenate([x, x, x], axis=1), msp[...].reshape(3 * 512, 512), NN)
        main = 4 * NT8 * 16
        zbuf[:, pl.ds(0, NT8)] = z[:main].reshape(4, NT8, 2, 8, 512)
        for q in range(4):
            for e in range(2):
                zbuf[q, NT8, e, pl.ds(0, 2)] = z[main + 4 * q + 2 * e:main + 4 * q + 2 * e + 2]
        ml = []
        for s in range(2):
            rest = tails(own[s, p, pl.ds(0, 4)]) + [jnp.zeros((12, LANES), F32)]
            ml.append(jnp.concatenate([own[s, p].reshape(NT8 * 16, LANES), jnp.concatenate(rest, axis=0).astype(BF)], axis=0))
        mid, low = ml
        rows = pl.ds(pl.multiple_of(a * LANES, LANES), LANES)
        mh, mm = msp[0, rows], msp[1, rows]
        z = dot(jnp.concatenate([mid, mid, low], axis=1), jnp.concatenate([mh, mm, mh], axis=0), NN)
        zbuf[o, pl.ds(0, NT8)] = zbuf[o, pl.ds(0, NT8)] + z[:NT8 * 16].reshape(NT8, 2, 8, 512)
        for e in range(2):
            zbuf[o, NT8, e, pl.ds(0, 2)] = zbuf[o, NT8, e, pl.ds(0, 2)] + z[NT8 * 16 + 2 * e:NT8 * 16 + 2 * e + 2]
        for e in range(2):
            s3 = split3(zbuf[:, :, e].reshape(4 * MROW, 512))
            k = dot(lhs6(s3, 1), rhs6(s3, 1), NT)
            if p == 0 and e == 0:
                kacc[0] = k[:, :LANES]
                kacc[1] = k[:, LANES:]
            else:
                kacc[0] = kacc[0] + k[:, :LANES]
                kacc[1] = kacc[1] + k[:, LANES:]

    lax.fori_loop(0, nm // 2, jpair, 0)
    near, far = a + 1 - 2 * (a % 2), lax.rem(a + 2, 4)
    hops = []
    for e, aa in enumerate((lax.rem(near + 2, 4), near)):
        hops.append(pltpu.make_async_remote_copy(src_ref=jsend.at[aa], dst_ref=jrecv.at[e], send_sem=jssem.at[e], recv_sem=jrsem.at[e],
                                                 device_id=dev(near, o), device_id_type=MESH))
        hops[-1].start()
    @pl.when(outer)
    def _():
        send_half(npair - 1, 0, NT8, True)

    @pl.when(jnp.logical_not(outer))
    def _():
        for p in range(3, npair):
            send_half(p, 0, NT8, False)
    for p in range(npair - 1):
        fit(p)
    hops[0].wait_recv()
    jfwd[...] = jsend[far] + jrecv[0]
    cross = pltpu.make_async_remote_copy(src_ref=jfwd, dst_ref=jrecv.at[2], send_sem=jssem.at[2], recv_sem=jrsem.at[2],
                                         device_id=dev(far, o), device_id_type=MESH)
    cross.start()
    fit(npair - 1)

    mate = o + 1 - 2 * half
    swap = pltpu.make_async_remote_copy(src_ref=kacc.at[1 - half], dst_ref=kin, send_sem=kxs, recv_sem=kxr,
                                        device_id=dev(a, mate), device_id_type=MESH)
    swap.start()
    swap.wait_recv()
    kful[...] = kacc[half] + kin[...]
    low32 = lax.broadcasted_iota(jnp.int32, (32, LANES), 1) < 64
    for oo in range(4):
        ev = kful[pl.ds(MROW * oo, 32, stride=2), :]
        od = kful[pl.ds(MROW * oo + 1, 32, stride=2), :]
        kmsg[0, oo] = jnp.where(low32, ev, pltpu.roll(od, 64, 1))
        kmsg[1, oo] = jnp.where(low32, pltpu.roll(ev, 64, 1), od)

    def ks(k, c):
        al, oo = k // 4, k % 4
        aa = 2 * half + al
        same = jnp.logical_and(aa == a, oo == o)

        @pl.when(jnp.logical_not(same))
        def _():
            pltpu.make_async_remote_copy(src_ref=kmsg.at[al, oo], dst_ref=krecv.at[pl.ds(dens * 32, 32)], send_sem=kss, recv_sem=krs,
                                         device_id=dev(aa, oo), device_id_type=MESH).start()

        @pl.when(same)
        def _():
            cp = pltpu.make_async_copy(kmsg.at[al, oo], krecv.at[pl.ds(dens * 32, 32)], krs)
            cp.start()
        return c
    lax.fori_loop(0, 8, ks, 0)

    hops[1].wait_recv()
    cross.wait_recv()
    pltpu.make_async_copy(krecv, krecv, krs).wait()
    for u in range(nm // 2):
        j = jsend[a, u] + jrecv[1, u] + jrecv[2, u]
        g = 2.0 * j - krecv[pl.ds(u, nd, stride=32), :]
        out[2 * u] = g[:, :nm]
        out[2 * u + 1] = pltpu.roll(g, 64, 1)[:, :nm]

    pltpu.make_async_copy(sbuf.at[pl.ds(0, 15)], sbuf.at[pl.ds(0, 15)], tsend).wait()
    metric_copies(lambda c: c.wait_send())
    pltpu.make_async_copy(mqr.at[:, pl.ds(0, 96)], mqr.at[:, pl.ds(0, 96)], mosend).wait()
    pltpu.make_async_copy(gbuf, gbuf, gssem).wait()
    for c in hops + [cross]:
        c.wait_send()
    swap.wait_send()
    inset = (a // 2) == half

    @pl.when(inset)
    def _():
        pltpu.make_async_copy(krecv.at[pl.ds(0, 224)], krecv.at[pl.ds(0, 224)], kss).wait()

    @pl.when(jnp.logical_not(inset))
    def _():
        pltpu.make_async_copy(krecv, krecv, kss).wait()


def solution(mesh):
    def local_fock(ints_blk, metric_blk, orbitals):
        nq, nm, nl = ints_blk.shape
        nd, _, ni = orbitals.shape
        bt = jnp.transpose(ints_blk, (1, 2, 0))
        mt = metric_blk.T
        ct = jnp.transpose(orbitals, (2, 0, 1)).reshape(ni * nd, nl)
        npair = ni // 4
        V = pltpu.VMEM
        dma = pltpu.SemaphoreType.DMA
        g = pl.pallas_call(
            lambda *refs: kernel(nm, nl, nq, nd, ni, *refs),
            out_shape=pltpu.VMEM((nm, nd, nm), F32),
            in_specs=[pl.BlockSpec(memory_space=pl.ANY)] * 3,
            out_specs=pl.BlockSpec(memory_space=pltpu.VMEM),
            scratch_shapes=[
                V((nm, nl, nq), F32), V((4 * nq, nq), F32), V((ni * nd, nl), F32), V((ni * nd, 256), F32),
                V((8 * SP, LANES), F32), V((16, npair, NT8, 16, LANES), BF), V((4, npair, 4, NT8, 16, LANES), BF),
                V((2, npair, NT8, 16, LANES), BF), V((4, LANES, LANES), F32), V((6, LANES, LANES), F32), V((4, 4, LANES, LANES), F32), V((3, 512, 512), BF),
                V((nd, LANES), F32), V((4, 4, nd, LANES), F32), V((4, nm // 2, nd, LANES), F32), V((3, nm // 2, nd, LANES), F32), V((nm // 2, nd, LANES), F32),
                V((4, 8, 2, 8, 512), F32), V((2, 256, LANES), F32), V((256, LANES), F32), V((256, LANES), F32), V((2, 4, 32, LANES), F32),
                V((8 * 32, LANES), F32), V((15, nd, LANES), F32),
                dma((NT8,)), dma((3,)), dma, dma((npair,)), dma, dma, dma, dma, dma, dma, dma((3,)), dma((3,)), dma, dma, dma, dma],
            compiler_params=pltpu.CompilerParams(collective_id=0, has_side_effects=True, vmem_limit_bytes=60 * 2**20),
        )(bt, mt, ct)
        return jnp.transpose(g, (1, 0, 2))

    return jax.shard_map(local_fock, mesh=mesh, in_specs=(P(('sys', 'aux'), 'orb', None), P(('sys', 'aux'), None), P('sys', None, None)), out_specs=P('sys', 'orb', 'aux'), check_vma=False)
```
